32 devices in a mesh: dp: 2 (over y), seq: 4 (over z), chan: 4 (over x, core).
Axes of the slice: x: 2, y: 2, z: 4, core: 2. Of those that a mesh axis runs over, the one named last changes fastest.
Arguments:
- layer_input: bfloat16 [2, 512, 2560], P('dp', ('seq', 'chan')), may hold values from -6 to 6
- inner_weight: bfloat16 [2560, 2560], P(None, 'chan'), may hold values from -0.125 to 0.125
- mixer_weight: bfloat16 [2560, 256], replicated, may hold values from -0.01171875 to 0.01171875
- step_weight: bfloat16 [2560, 40], P(None, 'chan'), may hold values from -0.125 to 0.125
- conv_inner: float32 [4, 2560], P(None, 'chan'), may hold values from -3 to 3
- conv_mixer: float32 [4, 256], replicated, may hold values from -3 to 3
- step_bias: float32 [40], P('chan'), may hold values from -2 to 1
- decay_log: float32 [40], P('chan'), as said below
- skip_gain: float32 [40], P('chan'), may hold values from 0.5 to 1.5
- output_grad: bfloat16 [2, 512, 2560], P('dp', 'seq', 'chan'), may hold values from -6 to 6
Outputs:
- input_grad: bfloat16 [2, 512, 2560], P('dp', ('seq', 'chan'))
- inner_weight_grad: float32 [2560, 2560], P(('dp', 'seq'), 'chan')
- mixer_weight_grad: float32 [2560, 256], P(('dp', 'seq', 'chan'))
- step_weight_grad: float32 [2560, 40], P(('dp', 'seq'), 'chan')
The draws below stay inside these ranges and needn't reach their ends.
Inputs may be any that keep to these rules, and one draw needn't show every extreme that they name: exp(decay_log) is at least 0.2 / 512.
All inputs are finite; a program needn't handle non-finite values.
Results may differ from the reference program's by a relative error of at most 0.014.
Values may be sent and summed in bfloat16 or wider, within the bound.
A program may use at most 128 MiB of HBM per device.

```python
import math
import jax
import jax.numpy as jnp
from jax import lax

D = 2560
HEADS = 40
HDIM = 64
STATE = 128
KW = 4
BATCH = 2
LENGTH = 512
TOKENS = 1024
INNER = 2560


def draw_decay_log(key, part):
    base = jax.random.fold_in(key, 71)
    order_key, slow_key, fast_key = jax.random.split(base, 3)
    ranks = jax.random.permutation(order_key, HEADS)
    slow_count = HEADS // 2
    is_slow = ranks < slow_count
    slow_rate = jnp.exp(jax.random.uniform(slow_key, (HEADS,), jnp.float32, jnp.log(0.2), jnp.log(2.0))) / LENGTH
    fast_rate = jnp.exp(jax.random.uniform(fast_key, (HEADS,), jnp.float32, jnp.log(0.02), jnp.log(0.06)))
    return jnp.log(jnp.where(is_slow, slow_rate, fast_rate)).astype(jnp.float32)


def spiked(entries, own_key, source, target, parts, factor):
    def block_of(dim):
        return (jnp.arange(entries.shape[dim]) // (entries.shape[dim] // parts)).reshape((-1,) + (1,) * (entries.ndim - 1 - dim))

    first = jax.random.permutation(own_key, parts)[block_of(target)]
    other_side = (block_of(target) + parts // 2) % parts
    return jnp.where((block_of(source) == first) | (block_of(source) == other_side), factor * entries, entries)


def shard_levels(key, dims, cuts, least, top_value):
    gain = 1.0
    for position, shards_of in cuts:
        steps = jax.random.uniform(jax.random.fold_in(jax.random.fold_in(key, 6), position), (shards_of,), jnp.float32, least / len(cuts), top_value / len(cuts))
        gain = gain * jnp.repeat(jnp.exp(steps), dims[position] // shards_of).reshape((-1,) + (1,) * (len(dims) - 1 - position))
    return gain


def gaussian(stream_key, shape, width, most, cuts=(), held_as=jnp.bfloat16):
    values = jax.random.normal(stream_key, shape, jnp.float32) * width
    if len(cuts) > 0:
        values = shard_levels(stream_key, shape, cuts, -0.22, 0.18) * values
    return jnp.clip(values, min=-most, max=most).astype(held_as)


def noise_with(own_key, dims, width, most, cuts, heavy, kind=jnp.bfloat16):
    drawn = width * jax.random.normal(own_key, dims, jnp.float32)
    if cuts:
        drawn = drawn * shard_levels(own_key, dims, cuts, -0.22, 0.18)
    return jnp.clip(spiked(drawn, jax.random.fold_in(own_key, 3), *heavy), -most, most).astype(kind)


def setup_inputs(seed: int = 0) -> dict:
    splits = jax.random.split(jax.random.key(seed), 11)
    return {
        "layer_input": noise_with(splits[0], (BATCH, LENGTH, D), 1.0, 6.0, ((0, 2), (1, 16)), (1, 2, 16, 2.0)),
        "inner_weight": gaussian(splits[1], (D, INNER), D ** -0.5, 0.125, ((1, 4),)),
        "mixer_weight": gaussian(splits[2], (D, 2 * STATE), (0.1 / D ** 0.5), 0.01171875),
        "step_weight": gaussian(splits[3], (D, HEADS), D ** -0.5, 0.125, ((1, 4),)),
        "conv_inner": gaussian(splits[4], (KW, INNER), KW ** -0.5, 3.0, ((1, 4),), jnp.float32),
        "conv_mixer": gaussian(splits[5], (KW, 2 * STATE), KW ** -0.5, 3.0, (), jnp.float32),
        "step_bias": jnp.clip(-2.0 + 3.0 * jax.random.uniform(splits[6], (HEADS,), jnp.float32) ** shard_levels(splits[6], (HEADS,), ((0, 4),), -0.2, 0.2), -2.0, 1.0),
        "decay_log": draw_decay_log(jax.random.fold_in(splits[10], 71), 0),
        "skip_gain": jnp.clip(0.5 + 1.0 * jax.random.uniform(splits[8], (HEADS,), jnp.float32) ** shard_levels(splits[8], (HEADS,), ((0, 4),), -0.2, 0.2), 0.5, 1.5),
        "output_grad": gaussian(splits[9], (BATCH, LENGTH, INNER), 1.0, 6.0, ((0, 2), (1, 4), (2, 4))),
    }


block_tokens = 256

def conv_silu(inputs, history, kernel):
    length = inputs.shape[0]
    padded = jnp.concatenate([history, inputs], axis=0)
    summed = kernel[0][None, :] * padded[0:length]
    for offset in range(1, kernel.shape[0]):
        summed = summed + kernel[offset][None, :] * padded[offset:offset + length]
    return jax.nn.silu(summed)

def activations(inner_proj, mixer_proj, step_raw, inner_hist, mixer_hist, conv_inner, conv_mixer, step_bias, decay_log):
    length = inner_proj.shape[0]
    head_count = step_bias.shape[0]
    state_width = mixer_proj.shape[1] // 2
    inner_act = conv_silu(inner_proj, inner_hist, conv_inner).reshape(length, head_count, -1)
    mixer_act = conv_silu(mixer_proj, mixer_hist, conv_mixer)
    step_size = jax.nn.softplus(step_raw + step_bias[None, :])
    log_decay = -step_size * jnp.exp(decay_log)[None, :]
    return (inner_act, mixer_act[:, :state_width], mixer_act[:, state_width:], step_size, log_decay)

def spanned_scan(inner_act, input_mix, output_mix, step_size, log_decay, skip_gain, initial):
    length, head_count, head_dim = inner_act.shape
    block_len = min(block_tokens, length)
    blocks = length // block_len
    highest = lax.Precision.HIGHEST

    def to_blocks(values):
        return values.reshape((blocks, block_len) + values.shape[1:])

    def advance(carry_state, pieces):
        part_inner, part_input, part_output, part_step, part_decay = pieces
        cumulative = jnp.cumsum(part_decay, axis=0)
        scores = jnp.dot(part_output, part_input.T, precision=highest)
        causal = (jnp.arange(block_len)[:, None] >= jnp.arange(block_len)[None, :])[:, :, None]
        spread = cumulative[:, None, :] - cumulative[None, :, :]
        weights = jnp.where(causal, jnp.exp(jnp.where(causal, spread, 0.0)), 0.0)
        weights = weights * scores[:, :, None] * part_step[None, :, :]
        within = jnp.einsum('ijh,jhp->ihp', weights, part_inner, precision=highest)
        carried = jnp.exp(cumulative)[:, :, None] * jnp.einsum('in,hpn->ihp', part_output, carry_state, precision=highest)
        result = within + carried + skip_gain[None, :, None] * part_inner
        tail_weight = jnp.exp(cumulative[-1][None, :] - cumulative) * part_step
        update_term = jnp.einsum('jh,jhp,jn->hpn', tail_weight, part_inner, part_input, precision=highest)
        carry_state = jnp.exp(cumulative[-1])[:, None, None] * carry_state + update_term
        return (carry_state, result)
    final, results = lax.scan(jax.checkpoint(advance), initial, (to_blocks(inner_act), to_blocks(input_mix), to_blocks(output_mix), to_blocks(step_size), to_blocks(log_decay)))
    return (results.reshape(length, head_count, head_dim), final)

def contract_rows(left_rows, right_rows):
    return lax.dot_general(left_rows, right_rows, (((0,), (0,)), ((), ())), preferred_element_type=jnp.float32)

def project_back(gradient, weight):
    return lax.dot_general(gradient, weight, (((1,), (1,)), ((), ())), preferred_element_type=jnp.float32)

def reference(layer_input, inner_weight, mixer_weight, step_weight, conv_inner, conv_mixer, step_bias, decay_log, skip_gain, output_grad):
    history_len = KW - 1
    highest = lax.Precision.HIGHEST
    inner_acc = jnp.zeros((D, INNER), jnp.float32)
    mixer_acc = jnp.zeros((D, 2 * STATE), jnp.float32)
    step_acc = jnp.zeros((D, HEADS), jnp.float32)
    input_grads = []
    zero_inner = jnp.zeros((history_len, INNER), jnp.float32)
    zero_mixer = jnp.zeros((history_len, 2 * STATE), jnp.float32)
    initial = jnp.zeros((HEADS, HDIM, STATE), jnp.float32)
    for batch_row in range(BATCH):
        tokens = layer_input[batch_row]
        inner_proj = jnp.dot(tokens, inner_weight, preferred_element_type=jnp.float32).astype(jnp.bfloat16)
        mixer_proj = jnp.dot(tokens, mixer_weight, preferred_element_type=jnp.float32).astype(jnp.bfloat16)
        step_raw = jnp.dot(tokens, step_weight, preferred_element_type=jnp.float32)
        inner_wide = lax.optimization_barrier(inner_proj).astype(jnp.float32)
        mixer_wide = lax.optimization_barrier(mixer_proj).astype(jnp.float32)

        def layer(inner_in, mixer_in, step_in):
            acts = activations(inner_in, mixer_in, step_in, zero_inner, zero_mixer, conv_inner, conv_mixer, step_bias, decay_log)
            result, final = spanned_scan(acts[0], acts[1], acts[2], acts[3], acts[4], skip_gain, initial)
            return result.reshape(LENGTH, INNER)
        unused, pull = jax.vjp(layer, inner_wide, mixer_wide, step_raw)
        grad_inner, grad_mixer, grad_step = pull(output_grad[batch_row].astype(jnp.float32))
        grad_inner = grad_inner.astype(jnp.bfloat16)
        grad_step = grad_step.astype(jnp.bfloat16)
        summed = project_back(grad_inner, inner_weight) + project_back(grad_step, step_weight)
        summed = summed + lax.dot_general(grad_mixer, mixer_weight.astype(jnp.float32), (((1,), (1,)), ((), ())), precision=highest)
        input_grads.append(summed.astype(jnp.bfloat16))
        inner_acc = inner_acc + contract_rows(tokens, grad_inner)
        step_acc = step_acc + contract_rows(tokens, grad_step)
        mixer_acc = mixer_acc + lax.dot_general(tokens.astype(jnp.float32), grad_mixer, (((0,), (0,)), ((), ())), precision=highest)
    norm_factor = 1.0 / math.sqrt(TOKENS)
    return (jnp.stack(input_grads, axis=0), inner_acc * norm_factor, mixer_acc * norm_factor, step_acc * norm_factor)
```

```python
import functools
import math

import jax
import jax.numpy as jnp
from jax import lax
from jax.experimental import pallas as pl
from jax.experimental.pallas import tpu as pltpu
from jax.sharding import PartitionSpec as P

MESH = pl.DeviceIdType.MESH
HDIM = 64
PAD = 16
LANES = 128
LIMIT = 60 * 2**20
BF = jnp.bfloat16
F32 = jnp.float32
HIGH = lax.Precision.HIGHEST


def size_of(axes, sizes):
    return math.prod(sizes[a] for a in axes)


def index_of(axes, sizes):
    index = 0
    for a in axes:
        index = index * sizes[a] + lax.axis_index(a)
    return index


def coords(axes, sizes, index):
    place = {}
    for a in reversed(axes):
        place[a] = lax.rem(index, sizes[a])
        index = lax.div(index, sizes[a])
    return place


def each(n, step):
    if n <= 12:
        for d in range(1, n):
            step(d)
    else:

        def one(d, carry):
            step(d)
            return carry

        lax.fori_loop(1, n, one, 0)


def exchange_kernel(jobs, tail, plugged, sizes, *refs):
    count = len(jobs)
    extra = 1 if tail else 0
    fed = count + (1 if tail == "up" else 0)
    plug_ins, plug_outs, plug_scratch = plugged.counts if plugged else (0, 0, 0)
    cuts = (fed, plug_ins, count + extra, plug_outs, 2 * (count + extra), plug_scratch)
    groups, at = [], 0
    for cut in cuts:
        groups.append(refs[at : at + cut])
        at += cut
    ins, plug_in, outs, plug_out, sems, scratch = groups
    plug = plugged.bind(sizes, plug_in, plug_out, scratch) if plugged else None
    barrier = pltpu.get_barrier_semaphore()
    chans, seqs = sizes["chan"], sizes["seq"]
    greeted = 0
    for axes in dict.fromkeys(job[0] for job in jobs):
        n, me = size_of(axes, sizes), index_of(axes, sizes)

        def greet(d, axes=axes, n=n, me=me):
            where = coords(axes, sizes, lax.rem(me + d, n))
            pl.semaphore_signal(barrier, inc=1, device_id=where, device_id_type=MESH)

        each(n, greet)
        greeted += n - 1
    if tail:
        spot = lax.axis_index("seq")
        after, before = lax.rem(spot + 1, seqs), lax.rem(spot + seqs - 1, seqs)
        ending = lax.axis_index("chan") == chans - 1
        source = {"seq": before, "chan": jnp.int32(chans - 1)}
        signal_to(barrier, source if tail == "up" else {"seq": before})

        if tail == "up":

            @pl.when(ending)
            def _():
                for c in range(chans):
                    signal_to(barrier, {"seq": after, "chan": jnp.int32(c)})

            greeted += 1 + chans * lax.div(lax.axis_index("chan"), chans - 1)
        else:
            signal_to(barrier, {"seq": after})
            greeted += 2
    if plug:
        greeted += plug.greet(barrier)
    pl.semaphore_wait(barrier, greeted)
    if plug:
        plug.start()

    def describe(k, q, landing, signal):
        axes, mode = jobs[k]
        src = ins[k] if mode == "gather" else ins[k].at[:, q] if mode == "cross" else ins[k].at[q]
        return pltpu.make_async_remote_copy(
            src_ref=src,
            dst_ref=outs[k].at[landing],
            send_sem=sems[2 * k].at[q],
            recv_sem=sems[2 * k + 1].at[signal],
            device_id=coords(axes, sizes, q),
            device_id_type=MESH,
        )

    for k, (axes, mode) in enumerate(jobs):
        n, me = size_of(axes, sizes), index_of(axes, sizes)
        each(n, lambda d, k=k, n=n, me=me: describe(k, lax.rem(me + d, n), me, me).start())
    if tail:
        tail_out = outs[count]
        tail_in = ins[count] if tail == "up" else ins[0].at[pl.ds(ins[0].shape[0] - PAD, PAD)]
        tail_send, tail_recv = sems[2 * count], sems[2 * count + 1]

        def down(c):
            return pltpu.make_async_remote_copy(
                src_ref=tail_in if c == chans - 1 else tail_out,
                dst_ref=tail_out,
                send_sem=tail_send.at[c],
                recv_sem=tail_recv.at[0],
                device_id={"seq": after} if c == chans - 1 else {"chan": jnp.int32(c)},
                device_id_type=MESH,
            )

        def up(slot):
            return pltpu.make_async_remote_copy(
                src_ref=tail_in,
                dst_ref=tail_out.at[slot],
                send_sem=tail_send.at[0],
                recv_sem=tail_recv.at[slot],
                device_id=source,
                device_id_type=MESH,
            )

        if tail == "down":

            @pl.when(ending)
            def _():
                down(chans - 1).start()
        else:
            up(lax.axis_index("chan")).start()
    for k, (axes, mode) in enumerate(jobs):
        me = index_of(axes, sizes)
        kept = ins[k][...] if mode == "gather" else ins[k][:, me] if mode == "cross" else ins[k][me]
        outs[k][me] = kept
    if tail == "down":
        down(chans - 1).wait_recv()

        @pl.when(ending)
        def _():
            for c in range(chans - 1):
                down(c).start()

    if plug:
        plug.run()
    for k, (axes, mode) in enumerate(jobs):
        n, me = size_of(axes, sizes), index_of(axes, sizes)

        def finish(d, k=k, n=n, me=me):
            q = lax.rem(me + d, n)
            describe(k, q, q, q).wait()

        each(n, finish)
    if tail == "down":
        @pl.when(ending)
        def _():
            for c in range(chans):
                down(c).wait_send()
    if tail == "up":
        up(lax.axis_index("chan")).wait_send()

        @pl.when(ending)
        def _():
            for c in range(chans):
                up(c).wait_recv()


def signal_to(barrier, where):
    pl.semaphore_signal(barrier, inc=1, device_id=where, device_id_type=MESH)


def greet_line(barrier, n):
    me = lax.axis_index("seq")
    signal_to(barrier, {"seq": lax.rem(me + 1, n)})
    signal_to(barrier, {"seq": lax.rem(me + n - 1, n)})
    return 2


class Chain:
    counts = (3, 2, 6)
    pieces = 5

    def shapes(self, sizes, arrays):
        shape = jax.ShapeDtypeStruct(arrays[0].shape, BF)
        sems = [pltpu.SemaphoreType.DMA((self.pieces,)) for unused in range(4)]
        return [shape, shape], [pltpu.VMEM(shape.shape, BF)] * 2 + sems

    def bind(self, sizes, ins, outs, scratch):
        bound = Chain()
        bound.n, bound.ins, bound.outs, bound.scratch = sizes["seq"], ins, outs, scratch
        return bound

    def greet(self, barrier):
        return greet_line(barrier, self.n)

    def copy(self, way, piece):
        me = lax.axis_index("seq")
        rows = self.outs[0].shape[0] // self.pieces
        part = pl.ds(pl.multiple_of(piece * rows, rows), rows)
        target = lax.rem(me + 1, self.n) if way == 0 else lax.rem(me + self.n - 1, self.n)
        return pltpu.make_async_remote_copy(
            src_ref=self.scratch[way].at[part],
            dst_ref=self.outs[way].at[part],
            send_sem=self.scratch[2 + way].at[piece],
            recv_sem=self.scratch[4 + way].at[piece],
            device_id={"seq": target},
            device_id_type=MESH,
        )

    def start(self):
        me = lax.axis_index("seq")
        for way, edge in ((0, 0), (1, self.n - 1)):

            @pl.when(me == edge)
            def _(way=way):
                self.outs[way][...] = jnp.zeros(self.outs[way].shape, BF)

    def beat(self, t):
        me = lax.axis_index("seq")
        rows = self.outs[0].shape[0] // self.pieces
        for way in (0, 1):
            place = me if way == 0 else self.n - 1 - me
            piece = t - place
            active = (piece >= 0) & (piece < self.pieces)

            @pl.when(active & (place > 0))
            def _(way=way, piece=piece):
                self.copy(way, piece).wait_recv()

            @pl.when(active & (place < self.n - 1))
            def _(way=way, piece=piece):
                part = pl.ds(pl.multiple_of(piece * rows, rows), rows)
                before = self.outs[way][part, :].astype(F32)
                term = self.ins[way][part, :].astype(F32)
                self.scratch[way][part, :] = (self.ins[2][part, :] * before + term).astype(BF)
                self.copy(way, piece).start()

    def run(self, middle):
        me = lax.axis_index("seq")
        half = self.pieces
        for t in range(1, half):
            self.beat(t)
        middle()
        rest = self.n - 1
        if rest <= 12:
            for t in range(half, half + rest):
                self.beat(t)
        else:
            lax.fori_loop(half, half + rest, lambda t, c: (self.beat(t), c)[1], 0)

        for way in (0, 1):

            @pl.when(me != (self.n - 1 if way == 0 else 0))
            def _(way=way):
                for piece in range(self.pieces):
                    self.copy(way, piece).wait_send()


def exchange(sizes, call_id, jobs, arrays, tail=None, tail_array=None, plug=None, plug_arrays=()):
    plan, out_shapes, sems = [], [], []
    for (axes, mode), array in zip(jobs, arrays):
        n = size_of(axes, sizes)
        shape = (n,) + array.shape if mode == "gather" else array.shape
        if mode == "cross":
            shape = (n, array.shape[0]) + array.shape[2:]
        plan.append((axes, mode))
        out_shapes.append(jax.ShapeDtypeStruct(shape, array.dtype))
        sems += [pltpu.SemaphoreType.DMA((n,)), pltpu.SemaphoreType.DMA((n,))]
    arrays = list(arrays)
    if tail:
        if tail == "up":
            arrays.append(tail_array)
            shape = (sizes["chan"],) + tail_array.shape
        else:
            shape = (PAD,) + arrays[0].shape[1:]
        out_shapes.append(jax.ShapeDtypeStruct(shape, arrays[0].dtype))
        sems += [pltpu.SemaphoreType.DMA((sizes["chan"],)), pltpu.SemaphoreType.DMA((sizes["chan"],))]
    if plug:
        arrays += plug_arrays
        plug_shapes, plug_scratch = plug.shapes(sizes, plug_arrays)
        out_shapes += plug_shapes
        sems += plug_scratch
    vmem = pl.BlockSpec(memory_space=pltpu.VMEM)
    return pl.pallas_call(
        functools.partial(exchange_kernel, tuple(plan), tail, plug, sizes),
        out_shape=out_shapes,
        in_specs=[vmem] * len(arrays),
        out_specs=[vmem] * len(out_shapes),
        scratch_shapes=sems,
        compiler_params=pltpu.CompilerParams(
            collective_id=call_id, has_side_effects=True, vmem_limit_bytes=LIMIT
        ),
        name=f"exchange_{call_id}",
    )(*arrays)


def mm(a, b, da, db):
    return lax.dot_general(
        a.astype(BF), b.astype(BF), (((da,), (db,)), ((), ())), preferred_element_type=F32
    )


def exact(a, b, da=1, db=0):
    return lax.dot_general(
        a, b, (((da,), (db,)), ((), ())), precision=HIGH, preferred_element_type=F32
    )


def softplus(v):
    return jnp.maximum(v, 0.0) + jnp.log1p(jnp.exp(-jnp.abs(v)))


def head_mask(width, heads_first):
    shape = (LANES, width) if heads_first else (width, LANES)
    head = lax.broadcasted_iota(jnp.int32, shape, 0 if heads_first else 1)
    column = lax.broadcasted_iota(jnp.int32, shape, 1 if heads_first else 0)
    return (column // HDIM == head).astype(F32)


def decays(raw, bias, decay_log):
    length = raw.shape[0]
    step = softplus(raw + bias)
    rate = jnp.exp(decay_log)
    row = lax.broadcasted_iota(jnp.int32, (length, length), 0)
    col = lax.broadcasted_iota(jnp.int32, (length, length), 1)
    lower = (row >= col).astype(F32)
    cumulative = exact(lower, -step * rate)
    return step, rate, cumulative, row, col, lower


def forward_kernel(
    inner_ref, mixer_ref, raw_ref, conv_inner_ref, conv_mixer_ref, bias_ref, log_ref, grad_ref,
    summed_inner_ref, summed_mixer_ref, state_ref, back_ref, decay_ref, wide_inner, wide_mixer,
):
    length = raw_ref.shape[0]
    width = conv_inner_ref.shape[1]
    taps = conv_inner_ref.shape[0]
    wide_inner[...] = inner_ref[...].astype(F32)
    wide_mixer[...] = mixer_ref[...].astype(F32)
    first = PAD - (taps - 1)

    def convolved(wide, kernel):
        total = kernel[0:1, :] * wide[pl.ds(first, length), :]
        for k in range(1, taps):
            total = total + kernel[k : k + 1, :] * wide[pl.ds(first + k, length), :]
        return total

    inner = convolved(wide_inner, conv_inner_ref)
    mixer = convolved(wide_mixer, conv_mixer_ref)
    summed_inner_ref[...] = inner
    summed_mixer_ref[...] = mixer
    act = inner * jax.nn.sigmoid(inner)
    mix = mixer * jax.nn.sigmoid(mixer)
    half = mix.shape[1] // 2
    step, rate, cumulative, row, col, lower = decays(raw_ref[...], bias_ref[...], log_ref[...])
    last = cumulative[length - 1 : length, :]
    spread = head_mask(width, True)
    tail = exact(jnp.exp(last - cumulative) * step, spread)
    grown = exact(jnp.exp(cumulative), spread)
    upstream = grad_ref[...].astype(F32)
    state_ref[...] = mm(act * tail, mix[:, :half], 0, 0).astype(BF)
    back_ref[...] = mm(grown * upstream, mix[:, half:], 0, 0).astype(BF)
    row_decay = jnp.sum(head_mask(width, False) * jnp.exp(last), axis=1, keepdims=True)
    decay_ref[...] = jnp.broadcast_to(row_decay, decay_ref.shape)


def backward_kernel(
    heads, inner_ref, mixer_ref, raw_ref, bias_ref, log_ref, skip_ref, grad_ref, start_ref, end_ref,
    a_in_ref, a_mix_ref, step_ref, z_ref, y_ref,
):
    length = raw_ref.shape[0]
    width = inner_ref.shape[1]
    spread = head_mask(width, True)
    spread_down = head_mask(width, False)
    start, end = start_ref[...].astype(F32), end_ref[...].astype(F32)
    inner, mixer = inner_ref[...], mixer_ref[...]
    inner_gate, mixer_gate = jax.nn.sigmoid(inner), jax.nn.sigmoid(mixer)
    act, mix = inner * inner_gate, mixer * mixer_gate
    half = mix.shape[1] // 2
    into, out_of = mix[:, :half], mix[:, half:]
    raw = raw_ref[...]
    step, rate, cumulative, row, col, lower = decays(raw, bias_ref[...], log_ref[...])
    last = cumulative[length - 1 : length, :]
    step_wide = exact(step, spread)
    grown = exact(jnp.exp(cumulative), spread)
    fading = exact(jnp.exp(last - cumulative), spread)
    upstream_low = grad_ref[...]
    upstream = upstream_low.astype(F32)
    stepped_low = (act * step_wide).astype(BF)
    stepped = stepped_low.astype(F32)
    scores = mm(out_of, into, 1, 1)
    causal = row >= col
    across = cumulative.T
    score_grad = jnp.zeros((length, length), F32)
    for h in range(heads):
        cols = slice(h * HDIM, (h + 1) * HDIM)
        gap = cumulative[:, h : h + 1] - across[h : h + 1, :]
        decay = jnp.where(causal, jnp.exp(jnp.where(causal, gap, 0.0)), 0.0)
        weights = (decay * scores).astype(BF)
        grad_h, step_h = upstream_low[:, cols], stepped_low[:, cols]
        score_grad = score_grad + decay * mm(grad_h, step_h, 1, 1)
        z_ref[:, cols] = mm(weights, grad_h, 0, 0)
        y_ref[:, cols] = mm(weights, step_h, 1, 0)
    z = z_ref[...]
    carried = grown * mm(out_of, start, 1, 1)
    ending = fading * mm(into, end, 1, 1)
    act_grad = step_wide * (z + ending) + exact(skip_ref[...], spread)[0:1, :] * upstream
    to_heads = functools.partial(exact, b=spread, da=1, db=1)
    step_grad = to_heads(act * (z + ending))
    tail_term = to_heads(stepped * ending)
    sum_grad = to_heads(upstream * (y_ref[...] + carried) - stepped * z) - tail_term
    held = jnp.sum(start * end, axis=1, keepdims=True)
    overall = jnp.sum(tail_term, axis=0, keepdims=True) + jnp.exp(last) * jnp.sum(
        spread_down * held, axis=0, keepdims=True
    )
    decay_grad = exact(lower, sum_grad, 0, 0) + overall
    step_grad = (step_grad - rate * decay_grad) * jax.nn.sigmoid(raw + bias_ref[...])
    out_grad = mm(score_grad, into, 1, 0) + mm(grown * upstream, start, 1, 0)
    into_grad = mm(score_grad, out_of, 0, 0) + mm(fading * stepped, end, 1, 0)
    inner_slope = inner_gate * (1.0 + inner * (1.0 - inner_gate))
    mixer_slope = mixer_gate * (1.0 + mixer * (1.0 - mixer_gate))
    a_in_ref[...] = act_grad * inner_slope
    a_mix_ref[:, :half] = into_grad * mixer_slope[:, :half]
    a_mix_ref[:, half:] = out_grad * mixer_slope[:, half:]
    step_ref[...] = step_grad


def rcopy(src, dst, send, recv, **where):
    return pltpu.make_async_remote_copy(
        src_ref=src, dst_ref=dst, send_sem=send, recv_sem=recv, device_id=where, device_id_type=MESH
    )


def greet_all(barrier, axis, n):
    me = lax.axis_index(axis)
    each(n, lambda d: signal_to(barrier, {axis: lax.rem(me + d, n)}))
    return n - 1


def mid_kernel(
    sizes, cols, state, back, decay, xc, start, end, scr0, scr1, xs, cross_s, cross_r, gat_s, gat_r, *chain_sems
):
    n, chans = sizes["seq"], sizes["chan"]
    me, ch = lax.axis_index("seq"), lax.axis_index("chan")
    barrier = pltpu.get_barrier_semaphore()
    total = greet_all(barrier, "seq", n) + greet_all(barrier, "chan", chans)
    chain = Chain()
    chain.n, chain.ins, chain.outs = n, (state, back, decay), (start, end)
    chain.scratch = (scr0, scr1) + chain_sems
    pl.semaphore_wait(barrier, total)
    chain.start()

    def cross(q, landing, slot):
        return rcopy(cols.at[:, q], xs.at[landing], cross_s.at[q], cross_r.at[slot], seq=q)

    def gather(q, landing, slot):
        return rcopy(xs, xc.at[:, :, landing], gat_s.at[q], gat_r.at[slot], chan=q)

    def middle():
        each(n, lambda d: cross(lax.rem(me + d, n), me, lax.rem(me + d, n)).wait_recv())
        each(chans, lambda d: gather(lax.rem(ch + d, chans), ch, ch).start())
        xc[:, :, ch] = xs[...]

    chain.beat(0)
    each(n, lambda d: cross(lax.rem(me + d, n), me, me).start())
    xs[me] = cols[:, me]
    chain.run(middle)

    def settle(d):
        q = lax.rem(me + d, n)
        cross(q, me, q).wait_send()

    each(n, settle)

    def settle_gather(d):
        q = lax.rem(ch + d, chans)
        gather(q, q, q).wait()

    each(chans, settle_gather)


def back_kernel(
    sizes, heads,
    a_in, a_mix, st, conv_in, conv_mix, w_in_h, w_mix_h, w_step_h, xc,
    o_ig, o_dw, o_dwm, o_dws,
    w_in, w_mix, w_step, pad_in, pad_mix, gin, gsm, hal_o, hal_i, gmp, gm_in, p_o, p_i, m_o, m_i,
    w_sem, hal_sem, z_r, c_r, u_s, d_s, x_s, c2_r, z2_r, x2_s, u2_s, d2_s,
    gm_s, gm_r, p_s, p_r, m_s, m_r,
):
    D, S, C = sizes["dp"], sizes["seq"], sizes["chan"]
    mine, me, ch = lax.axis_index("dp"), lax.axis_index("seq"), lax.axis_index("chan")
    length, width = a_in.shape
    mixed = a_mix.shape[1]
    taps = conv_in.shape[0]
    model = w_in.shape[0]
    rows = length // C
    parts = C
    barrier = pltpu.get_barrier_semaphore()
    total = greet_all(barrier, "dp", D) + greet_all(barrier, "chan", C) + greet_line(barrier, S)
    weights = [
        pltpu.make_async_copy(h, v, w_sem.at[i])
        for i, (h, v) in enumerate(((w_in_h, w_in), (w_mix_h, w_mix), (w_step_h, w_step)))
    ]
    for copy in weights:
        copy.start()
    hal_o[:, :width] = a_in[0:8, :]
    hal_o[:, width:] = a_mix[0:8, :]
    pad_in[0:length, :] = a_in[...]
    pad_mix[0:length, :] = a_mix[...]
    pad_in[length:, :] = jnp.zeros((8, width), F32)
    pad_mix[length:, :] = jnp.zeros((8, mixed), F32)

    def spread_back(pad, kernel, first, count):
        total = None
        for k in range(taps):
            term = kernel[k : k + 1, :] * pad[pl.ds(first + taps - 1 - k, count), :]
            total = term if total is None else total + term
        return total.astype(BF)

    last = length - rows
    gin[me, mine, 0:last, :] = spread_back(pad_in, conv_in, 0, last)
    gmp[0:last, :] = spread_back(pad_mix, conv_mix, 0, last)
    gsm[me, mine, rows:, 0:LANES] = st[...].T[0:PAD, :].astype(BF)
    pl.semaphore_wait(barrier, total)

    def others():
        return [lax.rem(mine + e, D) for e in range(1, D)]

    def halo():
        return rcopy(hal_o, hal_i, hal_sem.at[0], hal_sem.at[1], seq=lax.rem(me + S - 1, S))

    @pl.when(me > 0)
    def _():
        halo().start()

    def part(p, e, k):
        return gin.at[k, e, pl.ds(p * rows, rows)]

    def zcopy(p, way, k):
        to = lax.rem(me + (1 if way == "up" else S - 1), S)
        send = (u_s if way == "up" else d_s).at[p, k]
        return rcopy(part(p, mine, k), part(p, mine, k), send, z_r.at[p, k], seq=to)

    def ccopy(p, k, e, to):
        return rcopy(part(p, e, k), part(p, e, k), x_s.at[p, to, k], c_r.at[p, e, k], dp=to)

    def zsmall(way, e, k):
        to = lax.rem(me + (1 if way == "up" else S - 1), S)
        send = (u2_s if way == "up" else d2_s).at[e, k]
        return rcopy(gsm.at[k, e], gsm.at[k, e], send, z2_r.at[e, k], seq=to)

    def csmall(e, to):
        return rcopy(gsm.at[me, e], gsm.at[me, e], x2_s.at[to], c2_r.at[e], dp=to)

    def onward(make, k):
        @pl.when(me < S - 1)
        def _():
            make("up", k).start()

        @pl.when(me > 0)
        def _():
            make("down", k).start()

    def own_part(p):
        onward(functools.partial(zcopy, p), me)
        for e in others():
            ccopy(p, me, mine, e).start()

    def forward(d, p):
        for way, k, there, more in (
            ("up", me - d, me >= d, me < S - 1),
            ("down", me + d, me + d < S, me > 0),
        ):

            @pl.when(there)
            def _(way=way, k=k):
                zcopy(p, way, k).wait_recv()

            @pl.when(there & more)
            def _(way=way, k=k):
                zcopy(p, way, k).start()

            @pl.when(there)
            def _(k=k):
                for e in others():
                    ccopy(p, k, mine, e).start()

    def own_small():
        for e in others():
            csmall(mine, e).start()
        onward(lambda way, k: zsmall(way, mine, k), me)

    def cross_small():
        for e in others():
            csmall(e, e).wait_recv()
            onward(lambda way, k, e=e: zsmall(way, e, k), me)

    def forward_small(d):
        for way, k, there, more in (
            ("up", me - d, me >= d, me < S - 1),
            ("down", me + d, me + d < S, me > 0),
        ):
            for e in [mine] + others():

                @pl.when(there)
                def _(way=way, k=k, e=e):
                    zsmall(way, e, k).wait_recv()

                @pl.when(there & more)
                def _(way=way, k=k, e=e):
                    zsmall(way, e, k).start()

    norm = 1.0 / math.sqrt(D * S * length)

    def columns_of(k):
        block = xc[k]
        return block.reshape(D * length, block.shape[-1])

    def weight_term(k, first=False):
        for e in others():
            for p in range(parts):
                ccopy(p, k, e, e).wait_recv()
        x = columns_of(k)
        term = norm * mm(x, gin[k].reshape(D * length, width), 0, 0)
        o_dw[...] = term if first else o_dw[...] + term

    def weight_terms(d):
        for k, there in ((me - d, me >= d), (me + d, me + d < S)):

            @pl.when(there)
            def _(k=k):
                weight_term(k)

    for p in range(parts - 1):
        own_part(p)

    @pl.when(me < S - 1)
    def _():
        halo().wait_recv()
        pad_in[length:, :] = hal_i[:, :width]
        pad_mix[length:, :] = hal_i[:, width:]

    gin[me, mine, last:, :] = spread_back(pad_in, conv_in, last, rows)
    gmp[last:, :] = spread_back(pad_mix, conv_mix, last, rows)
    own_part(parts - 1)

    def share_mix(q, landing, slot):
        return rcopy(gmp.at[pl.ds(q * rows, rows)], gm_in.at[landing], gm_s.at[q], gm_r.at[slot], chan=q)

    each(C, lambda d: share_mix(lax.rem(ch + d, C), ch, ch).start())
    for copy in weights:
        copy.wait()
    cut = model // parts

    def share_p(j, q, landing, slot):
        piece = pl.ds(j * cut, cut)
        return rcopy(
            p_o.at[q, :, piece], p_i.at[landing, :, piece], p_s.at[j, q], p_r.at[j, slot], chan=q
        )

    grads = gin[me, mine]
    mixes = gmp[...]
    steps = st[...].astype(BF)

    def back_project(j):
        piece = slice(j * cut, (j + 1) * cut)
        out = mm(grads, w_in[piece, :], 1, 1) + mm(mixes, w_mix[piece, :], 1, 1)
        out = out + mm(steps, w_step[piece, :], 1, 1)
        p_o[:, :, piece] = out.astype(BF).reshape(C, rows, cut)
        each(C, lambda d: share_p(j, lax.rem(ch + d, C), ch, ch).start())

    def finish_mix():
        gm_in[ch] = gmp[pl.ds(pl.multiple_of(ch * rows, rows), rows), :]
        each(C, lambda d: share_mix(lax.rem(ch + d, C), ch, lax.rem(ch + d, C)).wait_recv())
        mix = gm_in[0].astype(F32)
        for q in range(1, C):
            mix = mix + gm_in[q].astype(F32)
        gsm[me, mine, 0:rows, :] = mix.astype(BF)
        own_small()

    for j in range(parts):
        back_project(j)
        forward(1, j)
        if j == 0:
            finish_mix()
    weight_term(me, True)

    def hop(d):
        for p in range(parts):
            forward(d, p)
        if isinstance(d, int) and d == 2:
            cross_small()
        forward_small(d - 1)
        weight_terms(d - 1)

    hop(2)
    if S > 3:
        if S <= 12:
            for d in range(3, S):
                hop(d)
        else:
            lax.fori_loop(3, S, lambda d, c: (hop(d), c)[1], 0)
    forward_small(S - 1)

    mixer_columns = xc[:, :, ch].reshape(S * D * rows, xc.shape[-1])
    mixer_grads = gsm[:, :, 0:rows, :].reshape(S * D * rows, mixed)
    mixer_term = norm * mm(mixer_columns, mixer_grads, 0, 0)
    band = mixer_term.shape[0] // C
    for q in range(C):
        m_o[q] = mixer_term[q * band : (q + 1) * band, :].astype(BF)

    def share_m(q, landing, slot):
        return rcopy(m_o.at[q], m_i.at[landing], m_s.at[q], m_r.at[slot], chan=q)

    each(C, lambda d: share_m(lax.rem(ch + d, C), ch, ch).start())
    step_total = None
    for k in range(S) if S <= 12 else ():
        for e in range(D):
            x = xc[k, e].reshape(length, xc.shape[-1])
            term = mm(x, gsm[k, e, rows:, 0:LANES], 0, 1)
            step_total = term if step_total is None else step_total + term
    if step_total is None:

        def one(k, carry):
            for e in range(D):
                x = xc[k, e].reshape(length, xc.shape[-1])
                carry = carry + mm(x, gsm[k, e, rows:, 0:LANES], 0, 1)
            return carry

        step_total = lax.fori_loop(0, S, one, jnp.zeros((xc.shape[-1], PAD), F32))
    o_dws[...] = (norm * step_total)[:, :heads]

    p_i[ch] = p_o[ch]
    for j in range(parts):
        each(C, lambda d, j=j: share_p(j, lax.rem(ch + d, C), ch, lax.rem(ch + d, C)).wait_recv())
    total_ig = p_i[0].astype(F32)
    for q in range(1, C):
        total_ig = total_ig + p_i[q].astype(F32)
    o_ig[...] = total_ig.astype(BF)
    weight_terms(S - 1)
    m_i[ch] = m_o[ch]
    each(C, lambda d: share_m(lax.rem(ch + d, C), ch, lax.rem(ch + d, C)).wait_recv())
    total_m = m_i[0].astype(F32)
    for q in range(1, C):
        total_m = total_m + m_i[q].astype(F32)
    o_dwm[...] = total_m

    @pl.when(me > 0)
    def _():
        halo().wait_send()

    def settle_chan(d):
        q = lax.rem(ch + d, C)
        share_mix(q, ch, ch).wait_send()
        share_m(q, ch, ch).wait_send()
        for j in range(parts):
            share_p(j, q, ch, ch).wait_send()

    each(C, settle_chan)

    def settle_line(k):
        for e in others():
            for p in range(parts):
                ccopy(p, k, mine, e).wait_send()
        for way, sent in (("up", (k <= me) & (me < S - 1)), ("down", (k >= me) & (me > 0))):

            @pl.when(sent)
            def _(way=way):
                for p in range(parts):
                    zcopy(p, way, k).wait_send()
                for e in [mine] + others():
                    zsmall(way, e, k).wait_send()

    settle_line(0)
    each(S, settle_line)
    for e in others():
        csmall(mine, e).wait_send()


def local_call(kernel, out_shapes, scratch, name, *arrays):
    vmem = pl.BlockSpec(memory_space=pltpu.VMEM)
    return pl.pallas_call(
        kernel,
        out_shape=out_shapes,
        in_specs=[vmem] * len(arrays),
        out_specs=jax.tree.map(lambda unused: vmem, out_shapes),
        scratch_shapes=scratch,
        compiler_params=pltpu.CompilerParams(vmem_limit_bytes=LIMIT),
        name=name,
    )(*arrays)


def body(
    sizes,
    layer_input,
    inner_weight,
    mixer_weight,
    step_weight,
    conv_inner,
    conv_mixer,
    step_bias,
    decay_log,
    skip_gain,
    output_grad,
):
    own = layer_input[0]
    rows, model = own.shape
    chans, seqs, dps = sizes["chan"], sizes["seq"], sizes["dp"]
    groups = dps * seqs
    length = rows * chans
    width = inner_weight.shape[1]
    mixed = mixer_weight.shape[1]
    heads = step_bias.shape[0]
    blocks = own.reshape(rows, dps, seqs, model // groups).transpose(1, 2, 0, 3)
    gathered, own_columns, history = exchange(
        sizes, 0, ((("chan",), "gather"), (("dp",), "swap")), (own, blocks), "down"
    )
    history = jnp.where(lax.axis_index("seq") > 0, history, jnp.zeros_like(history))
    tokens = jnp.concatenate([history, gathered.reshape(length, model)], axis=0)
    lane_pad = ((0, 0), (0, LANES - heads))
    step_wide = jnp.pad(step_weight, lane_pad)
    inner_proj = jnp.dot(tokens, inner_weight, preferred_element_type=F32).astype(BF)
    mixer_proj = jnp.dot(tokens, mixer_weight, preferred_element_type=F32).astype(BF)
    step_raw = jnp.dot(tokens[PAD:], step_wide, preferred_element_type=F32)
    vectors = jnp.pad(jnp.stack((step_bias, decay_log, skip_gain)), ((0, 5), lane_pad[1]))
    bias, rates, skips = vectors[0:1], vectors[1:2], vectors[2:3]
    upstream = output_grad[0]
    inner_sum, mixer_sum, state, back_state, decay = local_call(
        forward_kernel,
        (
            jax.ShapeDtypeStruct((length, width), F32),
            jax.ShapeDtypeStruct((length, mixed), F32),
            jax.ShapeDtypeStruct((width, mixed // 2), BF),
            jax.ShapeDtypeStruct((width, mixed // 2), BF),
            jax.ShapeDtypeStruct((width, mixed // 2), F32),
        ),
        [pltpu.VMEM((PAD + length, width), F32), pltpu.VMEM((PAD + length, mixed), F32)],
        "forward",
        inner_proj, mixer_proj, step_raw, conv_inner, conv_mixer, bias, rates, upstream,
    )
    assert length == LANES and heads + conv_inner.shape[0] - 1 <= PAD
    cols = model // groups
    dma = pltpu.SemaphoreType.DMA
    vmem = pl.BlockSpec(memory_space=pltpu.VMEM)
    hbm = pl.BlockSpec(memory_space=pl.ANY)
    xc, start, end = pl.pallas_call(
        functools.partial(mid_kernel, sizes),
        out_shape=(
            jax.ShapeDtypeStruct((seqs, dps, chans, rows, cols), BF),
            jax.ShapeDtypeStruct(state.shape, BF),
            jax.ShapeDtypeStruct(state.shape, BF),
        ),
        in_specs=[vmem] * 4,
        out_specs=(vmem,) * 3,
        scratch_shapes=[
            pltpu.VMEM(state.shape, BF),
            pltpu.VMEM(state.shape, BF),
            pltpu.VMEM((seqs, dps, rows, cols), BF),
            dma((seqs,)), dma((seqs,)), dma((chans,)), dma((chans,)),
        ]
        + [dma((Chain.pieces,)) for unused in range(4)],
        compiler_params=pltpu.CompilerParams(
            collective_id=1, has_side_effects=True, vmem_limit_bytes=LIMIT
        ),
        name="middle",
    )(own_columns, state, back_state, decay)
    a_in, a_mix, steps = local_call(
        functools.partial(backward_kernel, heads),
        (
            jax.ShapeDtypeStruct((length, width), F32),
            jax.ShapeDtypeStruct((length, mixed), F32),
            jax.ShapeDtypeStruct((length, LANES), F32),
        ),
        [pltpu.VMEM((length, width), F32), pltpu.VMEM((length, width), F32)],
        "backward",
        inner_sum, mixer_sum, step_raw, bias, rates,
        jnp.broadcast_to(skips, (8, LANES)), upstream, start, end,
    )
    small = rows + PAD
    band = cols // chans
    input_grad, inner_grad, mixer_grad, step_grad = pl.pallas_call(
        functools.partial(back_kernel, sizes, heads),
        out_shape=(
            jax.ShapeDtypeStruct((rows, model), BF),
            jax.ShapeDtypeStruct((cols, width), F32),
            jax.ShapeDtypeStruct((band, mixed), F32),
            jax.ShapeDtypeStruct((cols, heads), F32),
        ),
        in_specs=[vmem] * 5 + [hbm] * 3 + [vmem],
        out_specs=(vmem,) * 4,
        scratch_shapes=[
            pltpu.VMEM((model, width), BF),
            pltpu.VMEM((model, mixed), BF),
            pltpu.VMEM((model, LANES), BF),
            pltpu.VMEM((length + 8, width), F32),
            pltpu.VMEM((length + 8, mixed), F32),
            pltpu.VMEM((seqs, dps, length, width), BF),
            pltpu.VMEM((seqs, dps, small, mixed), BF),
            pltpu.VMEM((8, width + mixed), F32),
            pltpu.VMEM((8, width + mixed), F32),
            pltpu.VMEM((length, mixed), BF),
            pltpu.VMEM((chans, rows, mixed), BF),
            pltpu.VMEM((chans, rows, model), BF),
            pltpu.VMEM((chans, rows, model), BF),
            pltpu.VMEM((chans, band, mixed), BF),
            pltpu.VMEM((chans, band, mixed), BF),
            dma((3,)), dma((2,)),
            dma((chans, seqs)), dma((chans, dps, seqs)),
            dma((chans, seqs)), dma((chans, seqs)), dma((chans, dps, seqs)),
            dma((dps,)), dma((dps, seqs)), dma((dps,)), dma((dps, seqs)), dma((dps, seqs)),
            dma((chans,)), dma((chans,)),
            dma((chans, chans)), dma((chans, chans)),
            dma((chans,)), dma((chans,)),
        ],
        compiler_params=pltpu.CompilerParams(
            collective_id=2, has_side_effects=True, vmem_limit_bytes=LIMIT
        ),
        name="back",
    )(a_in, a_mix, steps, conv_inner, conv_mixer, inner_weight, mixer_weight, step_wide, xc)
    return input_grad[None], inner_grad, mixer_grad, step_grad


def solution(mesh):
    sizes = dict(mesh.shape)
    in_specs = (
        P("dp", ("seq", "chan"), None),
        P(None, "chan"),
        P(),
        P(None, "chan"),
        P(None, "chan"),
        P(),
        P("chan"),
        P("chan"),
        P("chan"),
        P("dp", "seq", "chan"),
    )
    out_specs = (
        P("dp", ("seq", "chan"), None),
        P(("dp", "seq"), "chan"),
        P(("dp", "seq", "chan"), None),
        P(("dp", "seq"), "chan"),
    )
    return jax.shard_map(
        functools.partial(body, sizes),
        mesh=mesh,
        in_specs=in_specs,
        out_specs=out_specs,
        check_vma=False,
    )
```

```python
import functools
import math

import jax
import jax.numpy as jnp
from jax import lax
from jax.experimental import pallas as pl
from jax.experimental.pallas import tpu as pltpu
from jax.sharding import PartitionSpec as P

MESH = pl.DeviceIdType.MESH
HDIM = 64
PAD = 16
LANES = 128
LIMIT = 40 * 2**20
BF = jnp.bfloat16
F32 = jnp.float32
HIGH = lax.Precision.HIGHEST


def each(n, step):
    if n <= 12:
        for d in range(1, n):
            step(d)
    else:

        def one(d, carry):
            step(d)
            return carry

        lax.fori_loop(1, n, one, 0)


def signal_to(barrier, where):
    pl.semaphore_signal(barrier, inc=1, device_id=where, device_id_type=MESH)


def greet_line(barrier, n):
    me = lax.axis_index("seq")
    signal_to(barrier, {"seq": lax.rem(me + 1, n)})
    signal_to(barrier, {"seq": lax.rem(me + n - 1, n)})
    return 2


class Chain:
    pieces = 5

    def copy(self, way, piece):
        me = lax.axis_index("seq")
        rows = self.outs[0].shape[0] // self.pieces
        part = pl.ds(pl.multiple_of(piece * rows, rows), rows)
        target = lax.rem(me + 1, self.n) if way == 0 else lax.rem(me + self.n - 1, self.n)
        return pltpu.make_async_remote_copy(
            src_ref=self.scratch[way].at[part],
            dst_ref=self.outs[way].at[part],
            send_sem=self.scratch[2 + way].at[piece],
            recv_sem=self.scratch[4 + way].at[piece],
            device_id={"seq": target},
            device_id_type=MESH,
        )

    def start(self):
        me = lax.axis_index("seq")
        for way, edge in ((0, 0), (1, self.n - 1)):

            @pl.when(me == edge)
            def _(way=way):
                self.outs[way][...] = jnp.zeros(self.outs[way].shape, BF)

    def beat(self, t):
        me = lax.axis_index("seq")
        rows = self.outs[0].shape[0] // self.pieces
        for way in (0, 1):
            place = me if way == 0 else self.n - 1 - me
            piece = t - place
            active = (piece >= 0) & (piece < self.pieces)

            @pl.when(active & (place > 0))
            def _(way=way, piece=piece):
                self.copy(way, piece).wait_recv()

            @pl.when(active & (place < self.n - 1))
            def _(way=way, piece=piece):
                part = pl.ds(pl.multiple_of(piece * rows, rows), rows)
                before = self.outs[way][part, :].astype(F32)
                term = self.ins[way][part, :].astype(F32)
                self.scratch[way][part, :] = (self.ins[2][part, :] * before + term).astype(BF)
                self.copy(way, piece).start()

    def run(self):
        me = lax.axis_index("seq")
        half = self.pieces
        for t in range(1, half):
            self.beat(t)
        rest = self.n - 1
        if rest <= 12:
            for t in range(half, half + rest):
                self.beat(t)
        else:
            lax.fori_loop(half, half + rest, lambda t, c: (self.beat(t), c)[1], 0)

        for way in (0, 1):

            @pl.when(me != (self.n - 1 if way == 0 else 0))
            def _(way=way):
                for piece in range(self.pieces):
                    self.copy(way, piece).wait_send()


def mm(a, b, da, db):
    return lax.dot_general(
        a.astype(BF), b.astype(BF), (((da,), (db,)), ((), ())), preferred_element_type=F32
    )


def exact(a, b, da=1, db=0):
    return lax.dot_general(
        a, b, (((da,), (db,)), ((), ())), precision=HIGH, preferred_element_type=F32
    )


def softplus(v):
    return jnp.maximum(v, 0.0) + jnp.log1p(jnp.exp(-jnp.abs(v)))


def head_mask(width, heads_first):
    shape = (LANES, width) if heads_first else (width, LANES)
    head = lax.broadcasted_iota(jnp.int32, shape, 0 if heads_first else 1)
    column = lax.broadcasted_iota(jnp.int32, shape, 1 if heads_first else 0)
    return (column // HDIM == head).astype(F32)


def decays(raw, bias, decay_log):
    length = raw.shape[0]
    step = softplus(raw + bias)
    rate = jnp.exp(decay_log)
    row = lax.broadcasted_iota(jnp.int32, (length, length), 0)
    col = lax.broadcasted_iota(jnp.int32, (length, length), 1)
    lower = (row >= col).astype(F32)
    cumulative = exact(lower, -step * rate)
    return step, rate, cumulative, row, col, lower


def front_kernel(
    sizes, heads,
    own, w_in_h, w_mix_h, w_step, conv_in, conv_mix, bias, log, grad,
    sum_in, sum_mix, raw_ref, state_ref, back_ref, decay_ref, xs,
    w_in, w_mix, wst, xg, blocks, mid, wide_in, wide_mix, hal_o, hal_i, vec,
    w_sem, near_s, near_r, far_s, far_r, relay_s, relay_r, swap_s, swap_r, cross_s, cross_r, hal_sem,
):
    D, S, C = sizes["dp"], sizes["seq"], sizes["chan"]
    mine, me, ch = lax.axis_index("dp"), lax.axis_index("seq"), lax.axis_index("chan")
    rows, model = own.shape
    length, width = sum_in.shape
    mixed = sum_mix.shape[1]
    taps = conv_in.shape[0]
    cols = model // (D * S)
    half = mixed // 2
    barrier = pltpu.get_barrier_semaphore()
    total = greet_all(barrier, "dp", D) + greet_all(barrier, "seq", S) + greet_all(barrier, "chan", C)
    weights = [
        pltpu.make_async_copy(h, v, w_sem.at[i])
        for i, (h, v) in enumerate(((w_in_h, w_in), (w_mix_h, w_mix)))
    ]
    for copy in weights:
        copy.start()
    for d in range(D):
        for k in range(S):
            at = (d * S + k) * cols
            blocks[d, k] = own[:, at : at + cols]
    pieces = C
    cut = model // pieces
    sides = C // 2
    side, low = lax.div(ch, 2), lax.rem(ch, 2)
    partner = ch + 1 - 2 * low

    def block(c, p):
        return xg.at[pl.ds(pl.multiple_of(c * rows, rows), rows), pl.ds(p * cut, cut)]

    def mine_at(p):
        return own.at[:, pl.ds(p * cut, cut)]

    def near(c, p):
        return rcopy(mine_at(p), block(c, p), near_s.at[p], near_r.at[p], chan=partner)

    def far(to, c, slot, p):
        return rcopy(
            mine_at(p), block(c, p), far_s.at[to, p], far_r.at[slot, p], chan=2 * to + low
        )

    def relay(source, lane, p):
        c = 2 * source + lane
        return rcopy(block(c, p), block(c, p), relay_s.at[source, p], relay_r.at[source, p], chan=partner)

    def swap(q, landing, slot):
        return rcopy(blocks.at[q], mid.at[landing], swap_s.at[q], swap_r.at[slot], dp=q)

    def cross(q, landing, slot):
        return rcopy(mid.at[:, q], xs.at[landing], cross_s.at[q], cross_r.at[slot], seq=q)

    pl.semaphore_wait(barrier, total)
    for p in range(pieces):
        for d in range(1, sides):
            far(lax.rem(side + d, sides), ch, side, p).start()
        near(ch, p).start()
    each(D, lambda d: swap(lax.rem(mine + d, D), mine, mine).start())
    mid[mine] = blocks[mine]
    xg[pl.ds(pl.multiple_of(ch * rows, rows), rows), :] = own[...]
    wst[...] = jnp.zeros(wst.shape, BF)
    wst[0:heads, :] = w_step[...]
    vec[...] = jnp.zeros(vec.shape, F32)
    vec[0:1, 0:heads] = bias[...]
    vec[1:2, 0:heads] = log[...]

    def pass_on(p):
        for d in range(1, sides):
            source = lax.rem(side + d, sides)
            far(source, ch, source, p).wait_recv()
            relay(source, low, p).start()

    def project(p):
        near(partner, p).wait_recv()
        for d in range(1, sides):
            source = lax.rem(side + d, sides)
            relay(source, 1 - low, p).wait_recv()
        piece = slice(p * cut, (p + 1) * cut)
        x = xg[:, piece]
        inner = mm(x, w_in[piece, :], 1, 0)
        mixer = mm(x, w_mix[piece, :], 1, 0)
        raw = mm(x, wst[:, piece], 1, 1)
        if p == 0:
            wide_in[PAD:, :], wide_mix[PAD:, :], raw_ref[...] = inner, mixer, raw
        else:
            wide_in[PAD:, :] = wide_in[PAD:, :] + inner
            wide_mix[PAD:, :] = wide_mix[PAD:, :] + mixer
            raw_ref[...] = raw_ref[...] + raw

    pass_on(0)
    for copy in weights:
        copy.wait()
    for p in range(pieces):
        if p + 1 < pieces:
            pass_on(p + 1)
        project(p)
        if p == pieces // 2:
            each(D, lambda d: swap(lax.rem(mine + d, D), mine, lax.rem(mine + d, D)).wait_recv())
            each(S, lambda d: cross(lax.rem(me + d, S), me, me).start())
            xs[me] = mid[:, me]
    inner_low = wide_in[PAD:, :].astype(BF)
    mixer_low = wide_mix[PAD:, :].astype(BF)
    hal_o[:, :width] = inner_low[length - PAD :, :]
    hal_o[:, width:] = mixer_low[length - PAD :, :]

    def halo():
        return rcopy(hal_o, hal_i, hal_sem.at[0], hal_sem.at[1], seq=lax.rem(me + 1, S))

    @pl.when(me < S - 1)
    def _():
        halo().start()

    wide_in[PAD:, :] = inner_low.astype(F32)
    wide_mix[PAD:, :] = mixer_low.astype(F32)
    wide_in[0:PAD, :] = jnp.zeros((PAD, width), F32)
    wide_mix[0:PAD, :] = jnp.zeros((PAD, mixed), F32)

    def convolved(wide, kernel, first, count):
        first = first + PAD - (taps - 1)
        total = kernel[0:1, :] * wide[pl.ds(first, count), :]
        for k in range(1, taps):
            total = total + kernel[k : k + 1, :] * wide[pl.ds(first + k, count), :]
        return total

    sum_in[PAD:, :] = convolved(wide_in, conv_in, PAD, length - PAD)
    sum_mix[PAD:, :] = convolved(wide_mix, conv_mix, PAD, length - PAD)
    step, rate, cumulative, row, col, lower = decays(raw_ref[...], vec[0:1, :], vec[1:2, :])
    last = cumulative[length - 1 : length, :]
    spread = head_mask(width, True)
    tail = exact(jnp.exp(last - cumulative) * step, spread)
    grown = exact(jnp.exp(cumulative), spread)
    pulled = grown * grad[...].astype(F32)
    row_decay = jnp.sum(head_mask(width, False) * jnp.exp(last), axis=1, keepdims=True)
    decay_ref[...] = jnp.broadcast_to(row_decay, decay_ref.shape)

    @pl.when(me > 0)
    def _():
        halo().wait_recv()
        wide_in[0:PAD, :] = hal_i[:, :width].astype(F32)
        wide_mix[0:PAD, :] = hal_i[:, width:].astype(F32)

    sum_in[0:PAD, :] = convolved(wide_in, conv_in, 0, PAD)
    sum_mix[0:PAD, :] = convolved(wide_mix, conv_mix, 0, PAD)
    mixer = sum_mix[...]
    mix = mixer * jax.nn.sigmoid(mixer)
    back_ref[...] = mm(pulled, mix[:, half:], 0, 0).astype(BF)
    inner = sum_in[...]
    act = inner * jax.nn.sigmoid(inner)
    state_ref[...] = mm(act * tail, mix[:, :half], 0, 0).astype(BF)

    @pl.when(me < S - 1)
    def _():
        halo().wait_send()

    for p in range(pieces):
        near(ch, p).wait_send()
        for d in range(1, sides):
            source = lax.rem(side + d, sides)
            far(source, ch, source, p).wait_send()
            relay(source, low, p).wait_send()
    each(D, lambda d: swap(lax.rem(mine + d, D), mine, mine).wait_send())

    def settle(d):
        q = lax.rem(me + d, S)
        cross(q, me, q).wait()

    each(S, settle)


def backward_kernel(
    heads, inner_ref, mixer_ref, raw_ref, bias_ref, log_ref, skip_ref, grad_ref, start_ref, end_ref,
    a_in_ref, a_mix_ref, step_ref, z_ref, y_ref, vec,
):
    length = raw_ref.shape[0]
    width = inner_ref.shape[1]
    spread = head_mask(width, True)
    spread_down = head_mask(width, False)
    vec[...] = jnp.zeros(vec.shape, F32)
    for i, ref in enumerate((bias_ref, log_ref, skip_ref)):
        vec[i : i + 1, 0:heads] = ref[...]
    bias, skips = vec[0:1, :], vec[2:3, :]
    start, end = start_ref[...].astype(F32), end_ref[...].astype(F32)
    inner, mixer = inner_ref[...], mixer_ref[...]
    inner_gate, mixer_gate = jax.nn.sigmoid(inner), jax.nn.sigmoid(mixer)
    act, mix = inner * inner_gate, mixer * mixer_gate
    half = mix.shape[1] // 2
    into, out_of = mix[:, :half], mix[:, half:]
    raw = raw_ref[...]
    step, rate, cumulative, row, col, lower = decays(raw, bias, vec[1:2, :])
    last = cumulative[length - 1 : length, :]
    step_wide = exact(step, spread)
    grown = exact(jnp.exp(cumulative), spread)
    fading = exact(jnp.exp(last - cumulative), spread)
    upstream_low = grad_ref[...]
    upstream = upstream_low.astype(F32)
    stepped_low = (act * step_wide).astype(BF)
    stepped = stepped_low.astype(F32)
    scores = mm(out_of, into, 1, 1)
    causal = row >= col
    across = cumulative.T
    score_grad = jnp.zeros((length, length), F32)
    for h in range(heads):
        cols = slice(h * HDIM, (h + 1) * HDIM)
        gap = cumulative[:, h : h + 1] - across[h : h + 1, :]
        decay = jnp.where(causal, jnp.exp(jnp.where(causal, gap, 0.0)), 0.0)
        weights = (decay * scores).astype(BF)
        grad_h, step_h = upstream_low[:, cols], stepped_low[:, cols]
        score_grad = score_grad + decay * mm(grad_h, step_h, 1, 1)
        z_ref[:, cols] = mm(weights, grad_h, 0, 0)
        y_ref[:, cols] = mm(weights, step_h, 1, 0)
    z = z_ref[...]
    carried = grown * mm(out_of, start, 1, 1)
    ending = fading * mm(into, end, 1, 1)
    act_grad = step_wide * (z + ending) + exact(jnp.broadcast_to(skips, (8, LANES)), spread)[0:1, :] * upstream
    to_heads = functools.partial(exact, b=spread, da=1, db=1)
    step_grad = to_heads(act * (z + ending))
    tail_term = to_heads(stepped * ending)
    sum_grad = to_heads(upstream * (y_ref[...] + carried) - stepped * z) - tail_term
    held = jnp.sum(start * end, axis=1, keepdims=True)
    overall = jnp.sum(tail_term, axis=0, keepdims=True) + jnp.exp(last) * jnp.sum(
        spread_down * held, axis=0, keepdims=True
    )
    decay_grad = exact(lower, sum_grad, 0, 0) + overall
    step_grad = (step_grad - rate * decay_grad) * jax.nn.sigmoid(raw + bias)
    out_grad = mm(score_grad, into, 1, 0) + mm(grown * upstream, start, 1, 0)
    into_grad = mm(score_grad, out_of, 0, 0) + mm(fading * stepped, end, 1, 0)
    inner_slope = inner_gate * (1.0 + inner * (1.0 - inner_gate))
    mixer_slope = mixer_gate * (1.0 + mixer * (1.0 - mixer_gate))
    a_in_ref[...] = act_grad * inner_slope
    a_mix_ref[:, :half] = into_grad * mixer_slope[:, :half]
    a_mix_ref[:, half:] = out_grad * mixer_slope[:, half:]
    step_ref[...] = step_grad


def rcopy(src, dst, send, recv, **where):
    return pltpu.make_async_remote_copy(
        src_ref=src, dst_ref=dst, send_sem=send, recv_sem=recv, device_id=where, device_id_type=MESH
    )


def greet_all(barrier, axis, n):
    me = lax.axis_index(axis)
    each(n, lambda d: signal_to(barrier, {axis: lax.rem(me + d, n)}))
    return n - 1


def mid_kernel(
    sizes, xs, state, back, decay, xc, start, end, scr0, scr1, gat_s, gat_r, *chain_sems
):
    n, chans = sizes["seq"], sizes["chan"]
    ch = lax.axis_index("chan")
    barrier = pltpu.get_barrier_semaphore()
    total = greet_line(barrier, n) + greet_all(barrier, "chan", chans)
    chain = Chain()
    chain.n, chain.ins, chain.outs = n, (state, back, decay), (start, end)
    chain.scratch = (scr0, scr1) + chain_sems
    pl.semaphore_wait(barrier, total)
    chain.start()

    def gather(q, landing, slot):
        return rcopy(xs, xc.at[:, :, landing], gat_s.at[q], gat_r.at[slot], chan=q)

    chain.beat(0)
    each(chans, lambda d: gather(lax.rem(ch + d, chans), ch, ch).start())
    xc[:, :, ch] = xs[...]
    chain.run()

    def settle_gather(d):
        q = lax.rem(ch + d, chans)
        gather(q, q, q).wait()

    each(chans, settle_gather)


def back_kernel(
    sizes, heads,
    a_in, a_mix, st, conv_in, conv_mix, w_in_h, w_mix_h, w_step, xc,
    p_i, o_dw, m_i, o_dws,
    w_in, w_mix, wst, pad_in, pad_mix, gin, gsm, hal_o, hal_i, gmp, gm_in, p_o, m_o,
    w_sem, hal_sem, z_r, c_r, u_s, d_s, x_s, c2_r, z2_r, x2_s, u2_s, d2_s,
    gm_s, gm_r, p_s, p_r, m_s, m_r,
):
    D, S, C = sizes["dp"], sizes["seq"], sizes["chan"]
    mine, me, ch = lax.axis_index("dp"), lax.axis_index("seq"), lax.axis_index("chan")
    length, width = a_in.shape
    mixed = a_mix.shape[1]
    taps = conv_in.shape[0]
    model = w_in.shape[0]
    rows = length // C
    parts = C
    barrier = pltpu.get_barrier_semaphore()
    total = greet_all(barrier, "dp", D) + greet_all(barrier, "chan", C) + greet_line(barrier, S)
    weights = [
        pltpu.make_async_copy(h, v, w_sem.at[i])
        for i, (h, v) in enumerate(((w_in_h, w_in), (w_mix_h, w_mix)))
    ]
    for copy in weights:
        copy.start()
    wst[...] = jnp.zeros(wst.shape, BF)
    wst[0:heads, :] = w_step[...]
    hal_o[:, :width] = a_in[0:8, :]
    hal_o[:, width:] = a_mix[0:8, :]
    pad_in[0:length, :] = a_in[...]
    pad_mix[0:length, :] = a_mix[...]
    pad_in[length:, :] = jnp.zeros((8, width), F32)
    pad_mix[length:, :] = jnp.zeros((8, mixed), F32)

    def spread_back(pad, kernel, first, count):
        total = None
        for k in range(taps):
            term = kernel[k : k + 1, :] * pad[pl.ds(first + taps - 1 - k, count), :]
            total = term if total is None else total + term
        return total.astype(BF)

    last = length - rows
    gin[me, mine, 0:last, :] = spread_back(pad_in, conv_in, 0, last)
    gmp[0:last, :] = spread_back(pad_mix, conv_mix, 0, last)
    gsm[me, mine, rows:, 0:LANES] = st[...].T[0:PAD, :].astype(BF)
    pl.semaphore_wait(barrier, total)

    def others():
        return [lax.rem(mine + e, D) for e in range(1, D)]

    def halo():
        return rcopy(hal_o, hal_i, hal_sem.at[0], hal_sem.at[1], seq=lax.rem(me + S - 1, S))

    @pl.when(me > 0)
    def _():
        halo().start()

    def part(p, e, k):
        return gin.at[k, e, pl.ds(p * rows, rows)]

    def zcopy(p, way, k):
        to = lax.rem(me + (1 if way == "up" else S - 1), S)
        send = (u_s if way == "up" else d_s).at[p, k]
        return rcopy(part(p, mine, k), part(p, mine, k), send, z_r.at[p, k], seq=to)

    def ccopy(p, k, e, to):
        return rcopy(part(p, e, k), part(p, e, k), x_s.at[p, to, k], c_r.at[p, e, k], dp=to)

    def zsmall(way, e, k):
        to = lax.rem(me + (1 if way == "up" else S - 1), S)
        send = (u2_s if way == "up" else d2_s).at[e, k]
        return rcopy(gsm.at[k, e], gsm.at[k, e], send, z2_r.at[e, k], seq=to)

    def csmall(e, to):
        return rcopy(gsm.at[me, e], gsm.at[me, e], x2_s.at[to], c2_r.at[e], dp=to)

    def onward(make, k):
        @pl.when(me < S - 1)
        def _():
            make("up", k).start()

        @pl.when(me > 0)
        def _():
            make("down", k).start()

    def own_part(p):
        onward(functools.partial(zcopy, p), me)
        for e in others():
            ccopy(p, me, mine, e).start()

    def forward(d, p):
        for way, k, there, more in (
            ("up", me - d, me >= d, me < S - 1),
            ("down", me + d, me + d < S, me > 0),
        ):

            @pl.when(there)
            def _(way=way, k=k):
                zcopy(p, way, k).wait_recv()

            @pl.when(there & more)
            def _(way=way, k=k):
                zcopy(p, way, k).start()

            @pl.when(there)
            def _(k=k):
                for e in others():
                    ccopy(p, k, mine, e).start()

    def own_small():
        for e in others():
            csmall(mine, e).start()
        onward(lambda way, k: zsmall(way, mine, k), me)

    def cross_small():
        for e in others():
            csmall(e, e).wait_recv()
            onward(lambda way, k, e=e: zsmall(way, e, k), me)

    def forward_small(d):
        for way, k, there, more in (
            ("up", me - d, me >= d, me < S - 1),
            ("down", me + d, me + d < S, me > 0),
        ):
            for e in [mine] + others():

                @pl.when(there)
                def _(way=way, k=k, e=e):
                    zsmall(way, e, k).wait_recv()

                @pl.when(there & more)
                def _(way=way, k=k, e=e):
                    zsmall(way, e, k).start()

    norm = 1.0 / math.sqrt(D * S * length)

    def columns_of(k):
        block = xc[k]
        return block.reshape(D * length, block.shape[-1])

    def weight_term(k, first=False):
        for e in others():
            for p in range(parts):
                ccopy(p, k, e, e).wait_recv()
        x = columns_of(k)
        term = norm * mm(x, gin[k].reshape(D * length, width), 0, 0)
        o_dw[...] = term if first else o_dw[...] + term

    def weight_terms(d):
        for k, there in ((me - d, me >= d), (me + d, me + d < S)):

            @pl.when(there)
            def _(k=k):
                weight_term(k)

    for p in range(parts - 1):
        own_part(p)

    @pl.when(me < S - 1)
    def _():
        halo().wait_recv()
        pad_in[length:, :] = hal_i[:, :width]
        pad_mix[length:, :] = hal_i[:, width:]

    gin[me, mine, last:, :] = spread_back(pad_in, conv_in, last, rows)
    gmp[last:, :] = spread_back(pad_mix, conv_mix, last, rows)
    own_part(parts - 1)

    def share_mix(q, landing, slot):
        return rcopy(gmp.at[pl.ds(q * rows, rows)], gm_in.at[landing], gm_s.at[q], gm_r.at[slot], chan=q)

    each(C, lambda d: share_mix(lax.rem(ch + d, C), ch, ch).start())
    for copy in weights:
        copy.wait()
    cut = model // parts

    def share_p(j, q, landing, slot):
        piece = pl.ds(j * cut, cut)
        return rcopy(
            p_o.at[q, :, piece], p_i.at[landing, :, piece], p_s.at[j, q], p_r.at[j, slot], chan=q
        )

    grads = gin[me, mine]
    mixes = gmp[...]
    steps = st[:, 0:PAD].astype(BF)

    def back_project(j):
        piece = slice(j * cut, (j + 1) * cut)
        out = mm(grads, w_in[piece, :], 1, 1) + mm(mixes, w_mix[piece, :], 1, 1)
        out = out + mm(steps, wst[:, piece], 1, 0)
        p_o[:, :, piece] = out.astype(BF).reshape(C, rows, cut)
        each(C, lambda d: share_p(j, lax.rem(ch + d, C), ch, ch).start())

    def finish_mix():
        gm_in[ch] = gmp[pl.ds(pl.multiple_of(ch * rows, rows), rows), :]
        each(C, lambda d: share_mix(lax.rem(ch + d, C), ch, lax.rem(ch + d, C)).wait_recv())
        mix = gm_in[0].astype(F32)
        for q in range(1, C):
            mix = mix + gm_in[q].astype(F32)
        gsm[me, mine, 0:rows, :] = mix.astype(BF)
        own_small()

    for j in range(parts):
        back_project(j)
        forward(1, j)
        if j == 0:
            finish_mix()
    weight_term(me, True)

    def hop(d):
        for p in range(parts):
            forward(d, p)
        if isinstance(d, int) and d == 2:
            cross_small()
        forward_small(d - 1)
        weight_terms(d - 1)

    hop(2)
    if S > 3:
        if S <= 12:
            for d in range(3, S):
                hop(d)
        else:
            lax.fori_loop(3, S, lambda d, c: (hop(d), c)[1], 0)
    forward_small(S - 1)

    mixer_columns = xc[:, :, ch].reshape(S * D * rows, xc.shape[-1])
    mixer_grads = gsm[:, :, 0:rows, :].reshape(S * D * rows, mixed)
    mixer_term = norm * mm(mixer_columns, mixer_grads, 0, 0)
    band = mixer_term.shape[0] // C
    for q in range(C):
        m_o[q] = mixer_term[q * band : (q + 1) * band, :].astype(BF)

    def share_m(q, landing, slot):
        return rcopy(m_o.at[q], m_i.at[landing], m_s.at[q], m_r.at[slot], chan=q)

    each(C, lambda d: share_m(lax.rem(ch + d, C), ch, ch).start())
    step_total = None
    for k in range(S) if S <= 12 else ():
        for e in range(D):
            x = xc[k, e].reshape(length, xc.shape[-1])
            term = mm(gsm[k, e, rows:, 0:LANES], x, 1, 0)
            step_total = term if step_total is None else step_total + term
    if step_total is None:

        def one(k, carry):
            for e in range(D):
                x = xc[k, e].reshape(length, xc.shape[-1])
                carry = carry + mm(gsm[k, e, rows:, 0:LANES], x, 1, 0)
            return carry

        step_total = lax.fori_loop(0, S, one, jnp.zeros((PAD, xc.shape[-1]), F32))
    o_dws[...] = (norm * step_total)[:heads, :]

    p_i[ch] = p_o[ch]
    for j in range(parts):
        each(C, lambda d, j=j: share_p(j, lax.rem(ch + d, C), ch, lax.rem(ch + d, C)).wait_recv())
    weight_terms(S - 1)
    m_i[ch] = m_o[ch]
    each(C, lambda d: share_m(lax.rem(ch + d, C), ch, lax.rem(ch + d, C)).wait_recv())

    @pl.when(me > 0)
    def _():
        halo().wait_send()

    def settle_chan(d):
        q = lax.rem(ch + d, C)
        share_mix(q, ch, ch).wait_send()
        share_m(q, ch, ch).wait_send()
        for j in range(parts):
            share_p(j, q, ch, ch).wait_send()

    each(C, settle_chan)

    def settle_line(k):
        for e in others():
            for p in range(parts):
                ccopy(p, k, mine, e).wait_send()
        for way, sent in (("up", (k <= me) & (me < S - 1)), ("down", (k >= me) & (me > 0))):

            @pl.when(sent)
            def _(way=way):
                for p in range(parts):
                    zcopy(p, way, k).wait_send()
                for e in [mine] + others():
                    zsmall(way, e, k).wait_send()

    settle_line(0)
    each(S, settle_line)
    for e in others():
        csmall(mine, e).wait_send()


def finish_kernel(parts, dw, mixes, dws, o_ig, o_dw, o_dwm, o_dws, ig, dwm, sems):
    copies = [
        pltpu.make_async_copy(a, b, sems.at[i])
        for i, (a, b) in enumerate(((dw, o_dw), (dws, o_dws), (ig, o_ig), (dwm, o_dwm)))
    ]
    copies[0].start()
    copies[1].start()
    total = parts[0].astype(F32)
    for q in range(1, parts.shape[0]):
        total = total + parts[q].astype(F32)
    ig[...] = total.astype(BF)
    copies[2].start()
    total = mixes[0].astype(F32)
    for q in range(1, mixes.shape[0]):
        total = total + mixes[q].astype(F32)
    dwm[...] = total
    copies[3].start()
    for copy in copies:
        copy.wait()


def local_call(kernel, out_shapes, scratch, name, *arrays):
    vmem = pl.BlockSpec(memory_space=pltpu.VMEM)
    return pl.pallas_call(
        kernel,
        out_shape=out_shapes,
        in_specs=[vmem] * len(arrays),
        out_specs=jax.tree.map(lambda unused: vmem, out_shapes),
        scratch_shapes=scratch,
        compiler_params=pltpu.CompilerParams(vmem_limit_bytes=LIMIT),
        name=name,
    )(*arrays)


def body(
    sizes,
    layer_input,
    inner_weight,
    mixer_weight,
    step_weight,
    conv_inner,
    conv_mixer,
    step_bias,
    decay_log,
    skip_gain,
    output_grad,
):
    own = layer_input[0]
    rows, model = own.shape
    chans, seqs, dps = sizes["chan"], sizes["seq"], sizes["dp"]
    groups = dps * seqs
    length = rows * chans
    width = inner_weight.shape[1]
    mixed = mixer_weight.shape[1]
    heads = step_bias.shape[0]
    cols = model // groups
    state_size = mixed // 2
    assert length == LANES and heads + conv_inner.shape[0] - 1 <= PAD
    upstream = output_grad[0]
    step_rows = step_weight.T
    bias, rates, skips = (v.reshape(1, heads) for v in (step_bias, decay_log, skip_gain))
    dma = pltpu.SemaphoreType.DMA
    vmem = pl.BlockSpec(memory_space=pltpu.VMEM)
    hbm = pl.BlockSpec(memory_space=pl.ANY)
    state_shape = jax.ShapeDtypeStruct((width, state_size), BF)
    inner_sum, mixer_sum, step_raw, state, back_state, decay, xs = pl.pallas_call(
        functools.partial(front_kernel, sizes, heads),
        out_shape=(
            jax.ShapeDtypeStruct((length, width), F32),
            jax.ShapeDtypeStruct((length, mixed), F32),
            jax.ShapeDtypeStruct((length, LANES), F32),
            state_shape,
            state_shape,
            jax.ShapeDtypeStruct((width, state_size), F32),
            jax.ShapeDtypeStruct((seqs, dps, rows, cols), BF),
        ),
        in_specs=[vmem] + [hbm] * 2 + [vmem] * 6,
        out_specs=(vmem,) * 7,
        scratch_shapes=[
            pltpu.VMEM((model, width), BF),
            pltpu.VMEM((model, mixed), BF),
            pltpu.VMEM((LANES, model), BF),
            pltpu.VMEM((length, model), BF),
            pltpu.VMEM((dps, seqs, rows, cols), BF),
            pltpu.VMEM((dps, seqs, rows, cols), BF),
            pltpu.VMEM((PAD + length, width), F32),
            pltpu.VMEM((PAD + length, mixed), F32),
            pltpu.VMEM((PAD, width + mixed), BF),
            pltpu.VMEM((PAD, width + mixed), BF),
            pltpu.VMEM((8, LANES), F32),
            dma((2,)),
            dma((chans,)), dma((chans,)),
            dma((chans // 2, chans)), dma((chans // 2, chans)),
            dma((chans // 2, chans)), dma((chans // 2, chans)),
            dma((dps,)), dma((dps,)), dma((seqs,)), dma((seqs,)), dma((2,)),
        ],
        compiler_params=pltpu.CompilerParams(
            collective_id=0, has_side_effects=True, vmem_limit_bytes=LIMIT
        ),
        name="front",
    )(own, inner_weight, mixer_weight, step_rows, conv_inner, conv_mixer, bias, rates, upstream)
    xc, start, end = pl.pallas_call(
        functools.partial(mid_kernel, sizes),
        out_shape=(
            jax.ShapeDtypeStruct((seqs, dps, chans, rows, cols), BF),
            state_shape,
            state_shape,
        ),
        in_specs=[vmem] * 4,
        out_specs=(vmem,) * 3,
        scratch_shapes=[
            pltpu.VMEM(state.shape, BF),
            pltpu.VMEM(state.shape, BF),
            dma((chans,)), dma((chans,)),
        ]
        + [dma((Chain.pieces,)) for unused in range(4)],
        compiler_params=pltpu.CompilerParams(
            collective_id=1, has_side_effects=True, vmem_limit_bytes=LIMIT
        ),
        name="middle",
    )(xs, state, back_state, decay)
    a_in, a_mix, steps = local_call(
        functools.partial(backward_kernel, heads),
        (
            jax.ShapeDtypeStruct((length, width), F32),
            jax.ShapeDtypeStruct((length, mixed), F32),
            jax.ShapeDtypeStruct((length, LANES), F32),
        ),
        [pltpu.VMEM((length, width), F32), pltpu.VMEM((length, width), F32), pltpu.VMEM((8, LANES), F32)],
        "backward",
        inner_sum, mixer_sum, step_raw, bias, rates, skips, upstream, start, end,
    )
    small = rows + PAD
    band = cols // chans
    parts, inner_grad, mix_parts, step_grad = pl.pallas_call(
        functools.partial(back_kernel, sizes, heads),
        out_shape=(
            jax.ShapeDtypeStruct((chans, rows, model), BF),
            jax.ShapeDtypeStruct((cols, width), F32),
            jax.ShapeDtypeStruct((chans, band, mixed), BF),
            jax.ShapeDtypeStruct((heads, cols), F32),
        ),
        in_specs=[vmem] * 5 + [hbm] * 2 + [vmem] * 2,
        out_specs=(vmem,) * 4,
        scratch_shapes=[
            pltpu.VMEM((model, width), BF),
            pltpu.VMEM((model, mixed), BF),
            pltpu.VMEM((PAD, model), BF),
            pltpu.VMEM((length + 8, width), F32),
            pltpu.VMEM((length + 8, mixed), F32),
            pltpu.VMEM((seqs, dps, length, width), BF),
            pltpu.VMEM((seqs, dps, small, mixed), BF),
            pltpu.VMEM((8, width + mixed), F32),
            pltpu.VMEM((8, width + mixed), F32),
            pltpu.VMEM((length, mixed), BF),
            pltpu.VMEM((chans, rows, mixed), BF),
            pltpu.VMEM((chans, rows, model), BF),
            pltpu.VMEM((chans, band, mixed), BF),
            dma((2,)), dma((2,)),
            dma((chans, seqs)), dma((chans, dps, seqs)),
            dma((chans, seqs)), dma((chans, seqs)), dma((chans, dps, seqs)),
            dma((dps,)), dma((dps, seqs)), dma((dps,)), dma((dps, seqs)), dma((dps, seqs)),
            dma((chans,)), dma((chans,)),
            dma((chans, chans)), dma((chans, chans)),
            dma((chans,)), dma((chans,)),
        ],
        compiler_params=pltpu.CompilerParams(
            collective_id=2, has_side_effects=True, vmem_limit_bytes=LIMIT
        ),
        name="back",
    )(a_in, a_mix, steps, conv_inner, conv_mixer, inner_weight, mixer_weight, step_rows, xc)
    input_grad, inner_grad, mixer_grad, step_grad = pl.pallas_call(
        finish_kernel,
        out_shape=(
            jax.ShapeDtypeStruct((rows, model), BF),
            jax.ShapeDtypeStruct((cols, width), F32),
            jax.ShapeDtypeStruct((band, mixed), F32),
            jax.ShapeDtypeStruct((heads, cols), F32),
        ),
        in_specs=[vmem] * 4,
        out_specs=(hbm,) * 4,
        scratch_shapes=[
            pltpu.VMEM((rows, model), BF),
            pltpu.VMEM((band, mixed), F32),
            dma((4,)),
        ],
        compiler_params=pltpu.CompilerParams(vmem_limit_bytes=LIMIT),
        name="finish",
    )(parts, inner_grad, mix_parts, step_grad)
    return input_grad[None], inner_grad, mixer_grad, step_grad.T


def solution(mesh):
    sizes = dict(mesh.shape)
    in_specs = (
        P("dp", ("seq", "chan"), None),
        P(None, "chan"),
        P(),
        P(None, "chan"),
        P(None, "chan"),
        P(),
        P("chan"),
        P("chan"),
        P("chan"),
        P("dp", "seq", "chan"),
    )
    out_specs = (
        P("dp", ("seq", "chan"), None),
        P(("dp", "seq"), "chan"),
        P(("dp", "seq", "chan"), None),
        P(("dp", "seq"), "chan"),
    )
    return jax.shard_map(
        functools.partial(body, sizes),
        mesh=mesh,
        in_specs=in_specs,
        out_specs=out_specs,
        check_vma=False,
    )
```

```python
import functools
import math
import types

import jax
import jax.numpy as jnp
from jax import lax
from jax.experimental import pallas as pl
from jax.experimental.pallas import tpu as pltpu
from jax.sharding import PartitionSpec as P

MESH = pl.DeviceIdType.MESH
HDIM = 64
PAD = 16
LANES = 128
LIMIT = 48 * 2**20
BF = jnp.bfloat16
F32 = jnp.float32
HIGH = lax.Precision.HIGHEST
PIECES = 10
LOADED = (
    "own", "w_in", "w_mix", "w_step", "conv_in", "conv_mix", "bias", "log", "skip", "grad",
)


def each(n, step):
    if n <= 12:
        for d in range(1, n):
            step(d)
    else:

        def one(d, carry):
            step(d)
            return carry

        lax.fori_loop(1, n, one, 0)


def signal_to(barrier, where):
    pl.semaphore_signal(barrier, inc=1, device_id=where, device_id_type=MESH)


def mm(a, b, da, db):
    return lax.dot_general(
        a.astype(BF), b.astype(BF), (((da,), (db,)), ((), ())), preferred_element_type=F32
    )


def exact(a, b, da=1, db=0):
    return lax.dot_general(
        a, b, (((da,), (db,)), ((), ())), precision=HIGH, preferred_element_type=F32
    )


def softplus(v):
    return jnp.maximum(v, 0.0) + jnp.log1p(jnp.exp(-jnp.abs(v)))


def head_mask(width, heads_first):
    shape = (LANES, width) if heads_first else (width, LANES)
    head = lax.broadcasted_iota(jnp.int32, shape, 0 if heads_first else 1)
    column = lax.broadcasted_iota(jnp.int32, shape, 1 if heads_first else 0)
    return (column // HDIM == head).astype(F32)


def decays(raw, bias, decay_log):
    length = raw.shape[0]
    step = softplus(raw + bias)
    rate = jnp.exp(decay_log)
    row = lax.broadcasted_iota(jnp.int32, (length, length), 0)
    col = lax.broadcasted_iota(jnp.int32, (length, length), 1)
    lower = (row >= col).astype(F32)
    cumulative = exact(lower, -step * rate)
    return step, rate, cumulative, row, col, lower


def rcopy(src, dst, send, recv, **where):
    return pltpu.make_async_remote_copy(
        src_ref=src, dst_ref=dst, send_sem=send, recv_sem=recv, device_id=where, device_id_type=MESH
    )


def greet_all(barrier, axis, n):
    me = lax.axis_index(axis)
    each(n, lambda d: signal_to(barrier, {axis: lax.rem(me + d, n)}))
    return n - 1


def convolved(wide, kernel, first, count):
    taps = kernel.shape[0]
    first = first + PAD - (taps - 1)
    total = kernel[0:1, :] * wide[pl.ds(first, count), :]
    for k in range(1, taps):
        total = total + kernel[k : k + 1, :] * wide[pl.ds(first + k, count), :]
    return total


def spread_back(pad, kernel, first, count):
    taps = kernel.shape[0]
    total = None
    for k in range(taps):
        term = kernel[k : k + 1, :] * pad[pl.ds(first + taps - 1 - k, count), :]
        total = term if total is None else total + term
    return total.astype(BF)


def layer_kernel(names, sizes, heads, *refs):
    r = types.SimpleNamespace(**dict(zip(names, refs, strict=True)))
    place = (lax.axis_index("dp"), lax.axis_index("seq"), lax.axis_index("chan"))
    D, S, C = sizes["dp"], sizes["seq"], sizes["chan"]
    barrier = pltpu.get_barrier_semaphore()
    total = greet_all(barrier, "dp", D) + greet_all(barrier, "seq", S) + greet_all(barrier, "chan", C)
    loads = {
        key: pltpu.make_async_copy(getattr(r, key + "_h"), getattr(r, key), r.load_sem.at[i])
        for i, key in enumerate(LOADED)
    }
    for copy in loads.values():
        copy.start()
    front(r, sizes, place, heads, loads, barrier, total)
    scan_back(r, sizes, place, heads)
    back(r, sizes, place, heads)


def front(r, sizes, place, heads, loads, barrier, total):
    D, S, C = sizes["dp"], sizes["seq"], sizes["chan"]
    mine, me, ch = place
    rows, model = r.own.shape
    length, width = r.sum_in.shape
    mixed = r.sum_mix.shape[1]
    cols = model // (D * S)
    half = mixed // 2
    pieces = C
    cut = model // pieces
    sides = C // 2
    side, low = lax.div(ch, 2), lax.rem(ch, 2)
    partner = ch + 1 - 2 * low

    def block(c, p):
        return r.xg.at[pl.ds(pl.multiple_of(c * rows, rows), rows), pl.ds(p * cut, cut)]

    def mine_at(p):
        return r.own.at[:, pl.ds(p * cut, cut)]

    def near(c, p):
        return rcopy(mine_at(p), block(c, p), r.near_s.at[p], r.near_r.at[p], chan=partner)

    def far(to, c, slot, p):
        return rcopy(
            mine_at(p), block(c, p), r.far_s.at[to, p], r.far_r.at[slot, p], chan=2 * to + low
        )

    def relay(source, lane, p):
        c = 2 * source + lane
        here = block(c, p)
        return rcopy(here, here, r.relay_s.at[source, p], r.relay_r.at[source, p], chan=partner)

    def swap(q, landing, slot):
        return rcopy(r.blocks.at[q], r.mid.at[landing], r.swap_s.at[q], r.swap_r.at[slot], dp=q)

    def cross(q, landing, slot):
        return rcopy(r.mid.at[:, q], r.xs.at[landing], r.cross_s.at[q], r.cross_r.at[slot], seq=q)

    loads["own"].wait()
    pl.semaphore_wait(barrier, total)
    for p in range(pieces):
        for d in range(1, sides):
            far(lax.rem(side + d, sides), ch, side, p).start()
        near(ch, p).start()
    for d in range(D):
        for k in range(S):
            at = (d * S + k) * cols
            r.blocks[d, k] = r.own[:, at : at + cols]
    each(D, lambda d: swap(lax.rem(mine + d, D), mine, mine).start())
    r.mid[mine] = r.blocks[mine]
    r.xg[pl.ds(pl.multiple_of(ch * rows, rows), rows), :] = r.own[...]
    r.wst[...] = jnp.zeros(r.wst.shape, BF)
    r.vec[...] = jnp.zeros(r.vec.shape, F32)
    for key in LOADED[1:]:
        loads[key].wait()
    r.wst[0:heads, :] = r.w_step[...]
    for i, ref in enumerate((r.bias, r.log, r.skip)):
        r.vec[i : i + 1, 0:heads] = ref[...]

    def pass_on(p):
        for d in range(1, sides):
            source = lax.rem(side + d, sides)
            far(source, ch, source, p).wait_recv()
            relay(source, low, p).start()

    def project(p):
        near(partner, p).wait_recv()
        for d in range(1, sides):
            source = lax.rem(side + d, sides)
            relay(source, 1 - low, p).wait_recv()
        piece = slice(p * cut, (p + 1) * cut)
        x = r.xg[:, piece]
        inner = mm(x, r.w_in[piece, :], 1, 0)
        mixer = mm(x, r.w_mix[piece, :], 1, 0)
        raw = mm(x, r.wst[:, piece], 1, 1)
        if p == 0:
            r.wide_in[PAD:, :], r.wide_mix[PAD:, :], r.raw[...] = inner, mixer, raw
        else:
            r.wide_in[PAD:, :] = r.wide_in[PAD:, :] + inner
            r.wide_mix[PAD:, :] = r.wide_mix[PAD:, :] + mixer
            r.raw[...] = r.raw[...] + raw

    pass_on(0)
    for p in range(pieces):
        if p + 1 < pieces:
            pass_on(p + 1)
        project(p)
        if p == pieces // 2:
            each(D, lambda d: swap(lax.rem(mine + d, D), mine, lax.rem(mine + d, D)).wait_recv())
            each(S, lambda d: cross(lax.rem(me + d, S), me, me).start())
            r.xs[me] = r.mid[:, me]
    inner_low = r.wide_in[PAD:, :].astype(BF)
    mixer_low = r.wide_mix[PAD:, :].astype(BF)
    r.fh_o[:, :width] = inner_low[length - PAD :, :]
    r.fh_o[:, width:] = mixer_low[length - PAD :, :]

    def halo():
        return rcopy(r.fh_o, r.fh_i, r.fh_sem.at[0], r.fh_sem.at[1], seq=lax.rem(me + 1, S))

    @pl.when(me < S - 1)
    def _():
        halo().start()

    r.wide_in[PAD:, :] = inner_low.astype(F32)
    r.wide_mix[PAD:, :] = mixer_low.astype(F32)
    r.wide_in[0:PAD, :] = jnp.zeros((PAD, width), F32)
    r.wide_mix[0:PAD, :] = jnp.zeros((PAD, mixed), F32)
    r.sum_in[PAD:, :] = convolved(r.wide_in, r.conv_in, PAD, length - PAD)
    r.sum_mix[PAD:, :] = convolved(r.wide_mix, r.conv_mix, PAD, length - PAD)
    step, rate, cumulative, row, col, lower = decays(r.raw[...], r.vec[0:1, :], r.vec[1:2, :])
    last = cumulative[length - 1 : length, :]
    spread = head_mask(width, True)
    r.cum[...] = cumulative
    step_wide = exact(step, spread)
    fading = exact(jnp.exp(last - cumulative), spread)
    grown = exact(jnp.exp(cumulative), spread)
    r.step_wide[...] = step_wide
    r.fading[...] = fading
    r.grown[...] = grown
    pulled = (grown * r.grad[...].astype(F32)).astype(BF)
    r.pulled[...] = pulled
    row_decay = jnp.sum(head_mask(width, False) * jnp.exp(last), axis=1, keepdims=True)
    r.decay[...] = jnp.broadcast_to(row_decay, r.decay.shape)

    @pl.when(me > 0)
    def _():
        halo().wait_recv()
        r.wide_in[0:PAD, :] = r.fh_i[:, :width].astype(F32)
        r.wide_mix[0:PAD, :] = r.fh_i[:, width:].astype(F32)

    r.sum_in[0:PAD, :] = convolved(r.wide_in, r.conv_in, 0, PAD)
    r.sum_mix[0:PAD, :] = convolved(r.wide_mix, r.conv_mix, 0, PAD)
    mixer = r.sum_mix[...]
    mix = mixer * jax.nn.sigmoid(mixer)
    r.mix[...] = mix.astype(BF)
    r.back_term[...] = mm(pulled, mix[:, half:], 0, 0).astype(BF)
    inner = r.sum_in[...]
    act = inner * jax.nn.sigmoid(inner)
    r.act[...] = act
    r.state_term[...] = mm(act * (fading * step_wide), mix[:, :half], 0, 0).astype(BF)

    @pl.when(me < S - 1)
    def _():
        halo().wait_send()

    for p in range(pieces):
        near(ch, p).wait_send()
        for d in range(1, sides):
            source = lax.rem(side + d, sides)
            far(source, ch, source, p).wait_send()
            relay(source, low, p).wait_send()
    each(D, lambda d: swap(lax.rem(mine + d, D), mine, mine).wait_send())

    def settle(d):
        q = lax.rem(me + d, S)
        cross(q, me, q).wait()

    each(S, settle)


def scan_back(r, sizes, place, heads):
    S, C = sizes["seq"], sizes["chan"]
    mine, me, ch = place
    length, width = r.sum_in.shape
    half = r.sum_mix.shape[1] // 2
    pieces, lag = PIECES, PIECES // 2
    size = width // pieces
    terms, outs, scratch = (r.state_term, r.back_term), (r.start, r.end), (r.scr0, r.scr1)
    spots = (me, S - 1 - me)

    def carry(way, piece, first=False):
        part = pl.ds(pl.multiple_of(piece * size, size), size)
        to = lax.rem(me + 1, S) if way == 0 else lax.rem(me + S - 1, S)
        source = terms[way] if first else scratch[way]
        sems = r.chain_s.at[way, piece], r.chain_r.at[way, piece]
        return rcopy(source.at[part], outs[way].at[part], *sems, seq=to)

    for way in (0, 1):

        @pl.when(spots[way] == 0)
        def _(way=way):
            for piece in range(pieces):
                carry(way, piece, True).start()
            outs[way][...] = jnp.zeros(outs[way].shape, BF)

    def beat(t):
        for way in (0, 1):
            spot = spots[way]
            piece = t - lag * (spot - 1)

            @pl.when((piece >= 0) & (piece < pieces) & (spot > 0) & (spot < S - 1))
            def _(way=way, piece=piece):
                carry(way, piece).wait_recv()
                part = pl.ds(pl.multiple_of(piece * size, size), size)
                before = outs[way][part, :].astype(F32)
                term = terms[way][part, :].astype(F32)
                scratch[way][part, :] = (r.decay[part, :] * before + term).astype(BF)
                carry(way, piece).start()

    def gather(q, landing, slot):
        return rcopy(r.xs, r.xc.at[:, :, landing], r.gat_s.at[q], r.gat_r.at[slot], chan=q)

    each(C, lambda d: gather(lax.rem(ch + d, C), ch, ch).start())
    r.xc[:, :, ch] = r.xs[...]

    spread = head_mask(width, True)
    cumulative = r.cum[...]
    across = cumulative.T
    row = lax.broadcasted_iota(jnp.int32, (length, length), 0)
    col = lax.broadcasted_iota(jnp.int32, (length, length), 1)
    causal = row >= col
    lower = causal.astype(F32)
    into, out_of = r.mix[:, :half], r.mix[:, half:]
    scores = mm(out_of, into, 1, 1)
    act = r.act[...]
    stepped_low = (act * r.step_wide[...]).astype(BF)
    r.stepped[...] = stepped_low

    def head(h):
        cols = slice(h * HDIM, (h + 1) * HDIM)
        gap = cumulative[:, h : h + 1] - across[h : h + 1, :]
        decay = jnp.where(causal, jnp.exp(jnp.where(causal, gap, 0.0)), 0.0)
        weights = (decay * scores).astype(BF)
        grad_h, step_h = r.grad[:, cols], r.stepped[:, cols]
        term = decay * mm(grad_h, step_h, 1, 1)
        r.score_grad[...] = term if h == 0 else r.score_grad[...] + term
        r.z[:, cols] = mm(weights, grad_h, 0, 0)
        r.y[:, cols] = mm(weights, step_h, 1, 0)

    beats = pieces + lag * max(S - 3, 0)
    early = heads // 2
    for h in range(early):
        head(h)
    if beats <= 24:
        for t in range(beats):
            beat(t)
            if early + t < heads:
                head(early + t)
    else:
        for h in range(early, heads):
            head(h)
        lax.fori_loop(0, beats, lambda t, c: (beat(t), c)[1], 0)

    upstream = r.grad[...].astype(F32)
    stepped = r.stepped[...].astype(F32)
    step_wide = r.step_wide[...]
    skip_wide = exact(jnp.broadcast_to(r.vec[2:3, :], (8, LANES)), spread)[0:1, :]
    inner, mixer = r.sum_in[...], r.sum_mix[...]
    inner_gate, mixer_gate = jax.nn.sigmoid(inner), jax.nn.sigmoid(mixer)
    inner_slope = inner_gate * (1.0 + inner * (1.0 - inner_gate))
    mixer_slope = mixer_gate * (1.0 + mixer * (1.0 - mixer_gate))
    to_heads = functools.partial(exact, b=spread, da=1, db=1)
    z = r.z[...]
    r.slope_in[...] = inner_slope
    r.slope_mix[...] = mixer_slope
    r.local[...] = (step_wide * z + skip_wide * upstream) * inner_slope
    local_step = to_heads(r.act[...] * z)
    local_sum = to_heads(upstream * r.y[...] - stepped * z)
    score_grad = r.score_grad[...]
    out_local = mm(score_grad, into, 1, 0)
    into_local = mm(score_grad, out_of, 0, 0)
    faded = (r.fading[...] * stepped).astype(BF)

    for way in (0, 1):

        @pl.when(spots[way] == S - 1)
        def _(way=way):
            for piece in range(pieces):
                carry(way, piece).wait_recv()

    start, end = r.start[...], r.end[...]
    carried = r.grown[...] * mm(out_of, start, 1, 1)
    ending = r.fading[...] * mm(into, end, 1, 1)
    r.pad_in[0:length, :] = r.local[...] + (r.step_wide[...] * ending) * r.slope_in[...]
    r.pad_mix[0:length, :half] = (into_local + mm(faded, end, 1, 0)) * r.slope_mix[:, :half]
    r.pad_mix[0:length, half:] = (out_local + mm(r.pulled[...], start, 1, 0)) * r.slope_mix[:, half:]
    step_grad = local_step + to_heads(r.act[...] * ending)
    tail_term = to_heads(stepped * ending)
    sum_grad = local_sum + to_heads(upstream * carried) - tail_term
    held = jnp.sum(start.astype(F32) * end.astype(F32), axis=1, keepdims=True)
    last = cumulative[length - 1 : length, :]
    overall = jnp.sum(tail_term, axis=0, keepdims=True) + jnp.exp(last) * jnp.sum(
        head_mask(width, False) * held, axis=0, keepdims=True
    )
    decay_grad = exact(lower, sum_grad, 0, 0) + overall
    rate = jnp.exp(r.vec[1:2, :])
    step_grad = (step_grad - rate * decay_grad) * jax.nn.sigmoid(r.raw[...] + r.vec[0:1, :])
    r.steps[...] = step_grad.astype(BF)

    for way in (0, 1):

        @pl.when(spots[way] < S - 1)
        def _(way=way):
            for piece in range(pieces):
                carry(way, piece).wait_send()

    def settle_gather(d):
        q = lax.rem(ch + d, C)
        gather(q, q, q).wait()

    each(C, settle_gather)


def back(r, sizes, place, heads):
    D, S, C = sizes["dp"], sizes["seq"], sizes["chan"]
    mine, me, ch = place
    length, width = r.sum_in.shape
    mixed = r.sum_mix.shape[1]
    model = r.w_in.shape[0]
    rows = length // C
    parts = C
    r.hal_o[:, :width] = r.pad_in[0:8, :]
    r.hal_o[:, width:] = r.pad_mix[0:8, :]
    r.pad_in[length:, :] = jnp.zeros((8, width), F32)
    r.pad_mix[length:, :] = jnp.zeros((8, mixed), F32)
    last = length - rows
    r.gin[me, mine, 0:last, :] = spread_back(r.pad_in, r.conv_in, 0, last)
    r.gmp[0:last, :] = spread_back(r.pad_mix, r.conv_mix, 0, last)
    r.gsm[me, mine, rows:, 0:LANES] = r.steps[...].astype(F32).T[0:PAD, :].astype(BF)

    def others():
        return [lax.rem(mine + e, D) for e in range(1, D)]

    def halo():
        return rcopy(r.hal_o, r.hal_i, r.hal_sem.at[0], r.hal_sem.at[1], seq=lax.rem(me + S - 1, S))

    @pl.when(me > 0)
    def _():
        halo().start()

    def part(p, e, k):
        return r.gin.at[k, e, pl.ds(p * rows, rows)]

    def zcopy(p, way, k):
        to = lax.rem(me + (1 if way == "up" else S - 1), S)
        send = (r.u_s if way == "up" else r.d_s).at[p, k]
        return rcopy(part(p, mine, k), part(p, mine, k), send, r.z_r.at[p, k], seq=to)

    def ccopy(p, k, e, to):
        return rcopy(part(p, e, k), part(p, e, k), r.x_s.at[p, to, k], r.c_r.at[p, e, k], dp=to)

    def zsmall(way, e, k):
        to = lax.rem(me + (1 if way == "up" else S - 1), S)
        send = (r.u2_s if way == "up" else r.d2_s).at[e, k]
        return rcopy(r.gsm.at[k, e], r.gsm.at[k, e], send, r.z2_r.at[e, k], seq=to)

    def csmall(e, to):
        return rcopy(r.gsm.at[me, e], r.gsm.at[me, e], r.x2_s.at[to], r.c2_r.at[e], dp=to)

    def onward(make, k):
        @pl.when(me < S - 1)
        def _():
            make("up", k).start()

        @pl.when(me > 0)
        def _():
            make("down", k).start()

    def own_part(p):
        onward(functools.partial(zcopy, p), me)
        for e in others():
            ccopy(p, me, mine, e).start()

    def forward(d, p):
        for way, k, there, more in (
            ("up", me - d, me >= d, me < S - 1),
            ("down", me + d, me + d < S, me > 0),
        ):

            @pl.when(there)
            def _(way=way, k=k):
                zcopy(p, way, k).wait_recv()

            @pl.when(there & more)
            def _(way=way, k=k):
                zcopy(p, way, k).start()

            @pl.when(there)
            def _(k=k):
                for e in others():
                    ccopy(p, k, mine, e).start()

    def own_small():
        for e in others():
            csmall(mine, e).start()
        onward(lambda way, k: zsmall(way, mine, k), me)

    def cross_small():
        for e in others():
            csmall(e, e).wait_recv()
            onward(lambda way, k, e=e: zsmall(way, e, k), me)

    def forward_small(d):
        for way, k, there, more in (
            ("up", me - d, me >= d, me < S - 1),
            ("down", me + d, me + d < S, me > 0),
        ):
            for e in [mine] + others():

                @pl.when(there)
                def _(way=way, k=k, e=e):
                    zsmall(way, e, k).wait_recv()

                @pl.when(there & more)
                def _(way=way, k=k, e=e):
                    zsmall(way, e, k).start()

    norm = 1.0 / math.sqrt(D * S * length)

    def columns_of(k):
        block = r.xc[k]
        return block.reshape(D * length, block.shape[-1])

    def weight_term(k, first=False):
        for e in others():
            for p in range(parts):
                ccopy(p, k, e, e).wait_recv()
        x = columns_of(k)
        term = norm * mm(x, r.gin[k].reshape(D * length, width), 0, 0)
        r.o_dw[...] = term if first else r.o_dw[...] + term

    def weight_terms(d):
        for k, there in ((me - d, me >= d), (me + d, me + d < S)):

            @pl.when(there)
            def _(k=k):
                weight_term(k)

    for p in range(parts - 1):
        own_part(p)

    @pl.when(me < S - 1)
    def _():
        halo().wait_recv()
        r.pad_in[length:, :] = r.hal_i[:, :width]
        r.pad_mix[length:, :] = r.hal_i[:, width:]

    r.gin[me, mine, last:, :] = spread_back(r.pad_in, r.conv_in, last, rows)
    r.gmp[last:, :] = spread_back(r.pad_mix, r.conv_mix, last, rows)
    own_part(parts - 1)

    def share_mix(q, landing, slot):
        return rcopy(r.gmp.at[pl.ds(q * rows, rows)], r.gm_in.at[landing], r.gm_s.at[q], r.gm_r.at[slot], chan=q)

    each(C, lambda d: share_mix(lax.rem(ch + d, C), ch, ch).start())
    cut = model // parts

    def share_p(j, q, landing, slot):
        piece = pl.ds(j * cut, cut)
        return rcopy(
            r.p_o.at[q, :, piece], r.p_i.at[landing, :, piece], r.p_s.at[j, q], r.p_r.at[j, slot], chan=q
        )

    grads = r.gin[me, mine]
    mixes = r.gmp[...]
    steps = r.steps[:, 0:PAD]

    def back_project(j):
        piece = slice(j * cut, (j + 1) * cut)
        out = mm(grads, r.w_in[piece, :], 1, 1) + mm(mixes, r.w_mix[piece, :], 1, 1)
        out = out + mm(steps, r.wst[0:PAD, piece], 1, 0)
        r.p_o[:, :, piece] = out.astype(BF).reshape(C, rows, cut)
        each(C, lambda d: share_p(j, lax.rem(ch + d, C), ch, ch).start())

    def finish_mix():
        r.gm_in[ch] = r.gmp[pl.ds(pl.multiple_of(ch * rows, rows), rows), :]
        each(C, lambda d: share_mix(lax.rem(ch + d, C), ch, lax.rem(ch + d, C)).wait_recv())
        mix = r.gm_in[0].astype(F32)
        for q in range(1, C):
            mix = mix + r.gm_in[q].astype(F32)
        r.gsm[me, mine, 0:rows, :] = mix.astype(BF)
        own_small()

    for j in range(parts):
        back_project(j)
        forward(1, j)
        if j == 0:
            finish_mix()
    weight_term(me, True)

    def hop(d):
        for p in range(parts):
            forward(d, p)
        if isinstance(d, int) and d == 2:
            cross_small()
        forward_small(d - 1)
        weight_terms(d - 1)

    hop(2)
    if S > 3:
        if S <= 12:
            for d in range(3, S):
                hop(d)
        else:
            lax.fori_loop(3, S, lambda d, c: (hop(d), c)[1], 0)
    forward_small(S - 1)

    mixer_columns = r.xc[:, :, ch].reshape(S * D * rows, r.xc.shape[-1])
    mixer_grads = r.gsm[:, :, 0:rows, :].reshape(S * D * rows, mixed)
    mixer_term = norm * mm(mixer_columns, mixer_grads, 0, 0)
    band = mixer_term.shape[0] // C
    for q in range(C):
        r.m_o[q] = mixer_term[q * band : (q + 1) * band, :].astype(BF)

    def share_m(q, landing, slot):
        return rcopy(r.m_o.at[q], r.m_i.at[landing], r.m_s.at[q], r.m_r.at[slot], chan=q)

    each(C, lambda d: share_m(lax.rem(ch + d, C), ch, ch).start())
    step_total = None
    for k in range(S) if S <= 12 else ():
        for e in range(D):
            x = r.xc[k, e].reshape(length, r.xc.shape[-1])
            term = mm(r.gsm[k, e, rows:, 0:LANES], x, 1, 0)
            step_total = term if step_total is None else step_total + term
    if step_total is None:

        def one(k, carry):
            for e in range(D):
                x = r.xc[k, e].reshape(length, r.xc.shape[-1])
                carry = carry + mm(r.gsm[k, e, rows:, 0:LANES], x, 1, 0)
            return carry

        step_total = lax.fori_loop(0, S, one, jnp.zeros((PAD, r.xc.shape[-1]), F32))
    r.o_dws[...] = (norm * step_total)[:heads, :]

    r.p_i[ch] = r.p_o[ch]
    for j in range(parts):
        each(C, lambda d, j=j: share_p(j, lax.rem(ch + d, C), ch, lax.rem(ch + d, C)).wait_recv())
    weight_terms(S - 1)
    r.m_i[ch] = r.m_o[ch]
    each(C, lambda d: share_m(lax.rem(ch + d, C), ch, lax.rem(ch + d, C)).wait_recv())

    @pl.when(me > 0)
    def _():
        halo().wait_send()

    def settle_chan(d):
        q = lax.rem(ch + d, C)
        share_mix(q, ch, ch).wait_send()
        share_m(q, ch, ch).wait_send()
        for j in range(parts):
            share_p(j, q, ch, ch).wait_send()

    each(C, settle_chan)

    def settle_line(k):
        for e in others():
            for p in range(parts):
                ccopy(p, k, mine, e).wait_send()
        for way, sent in (("up", (k <= me) & (me < S - 1)), ("down", (k >= me) & (me > 0))):

            @pl.when(sent)
            def _(way=way):
                for p in range(parts):
                    zcopy(p, way, k).wait_send()
                for e in [mine] + others():
                    zsmall(way, e, k).wait_send()

    settle_line(0)
    each(S, settle_line)
    for e in others():
        csmall(mine, e).wait_send()


def finish_kernel(parts, dw, mixes, dws, o_ig, o_dw, o_dwm, o_dws, ig, dwm, sems):
    copies = [
        pltpu.make_async_copy(a, b, sems.at[i])
        for i, (a, b) in enumerate(((dw, o_dw), (dws, o_dws), (ig, o_ig), (dwm, o_dwm)))
    ]
    copies[0].start()
    copies[1].start()
    total = parts[0].astype(F32)
    for q in range(1, parts.shape[0]):
        total = total + parts[q].astype(F32)
    ig[...] = total.astype(BF)
    copies[2].start()
    total = mixes[0].astype(F32)
    for q in range(1, mixes.shape[0]):
        total = total + mixes[q].astype(F32)
    dwm[...] = total
    copies[3].start()
    for copy in copies:
        copy.wait()


def body(
    sizes,
    layer_input,
    inner_weight,
    mixer_weight,
    step_weight,
    conv_inner,
    conv_mixer,
    step_bias,
    decay_log,
    skip_gain,
    output_grad,
):
    own = layer_input[0]
    rows, model = own.shape
    chans, seqs, dps = sizes["chan"], sizes["seq"], sizes["dp"]
    groups = dps * seqs
    length = rows * chans
    width = inner_weight.shape[1]
    mixed = mixer_weight.shape[1]
    heads = step_bias.shape[0]
    cols = model // groups
    state_size = mixed // 2
    assert width % PIECES == 0 and chans % 2 == 0 and seqs > 2
    assert length == LANES and heads + conv_inner.shape[0] - 1 <= PAD
    upstream = output_grad[0]
    step_rows = step_weight.T
    bias, rates, skips = (v.reshape(1, heads) for v in (step_bias, decay_log, skip_gain))
    dma = pltpu.SemaphoreType.DMA
    vmem = pl.BlockSpec(memory_space=pltpu.VMEM)
    hbm = pl.BlockSpec(memory_space=pltpu.HBM)
    small = rows + PAD
    band = cols // chans

    def low(*shape):
        return pltpu.VMEM(shape, BF)

    def full(*shape):
        return pltpu.VMEM(shape, F32)

    inputs = dict(
        own=own, w_in=inner_weight, w_mix=mixer_weight, w_step=step_rows, conv_in=conv_inner,
        conv_mix=conv_mixer, bias=bias, log=rates, skip=skips, grad=upstream,
    )
    outputs = dict(
        p_i=jax.ShapeDtypeStruct((chans, rows, model), BF),
        o_dw=jax.ShapeDtypeStruct((cols, width), F32),
        m_i=jax.ShapeDtypeStruct((chans, band, mixed), BF),
        o_dws=jax.ShapeDtypeStruct((heads, cols), F32),
    )
    scratch = {key: pltpu.VMEM(v.shape, v.dtype) for key, v in inputs.items()}
    scratch |= dict(
        wst=low(LANES, model), xg=low(length, model),
        blocks=low(dps, seqs, rows, cols), mid=low(dps, seqs, rows, cols),
        xs=low(seqs, dps, rows, cols), xc=low(seqs, dps, chans, rows, cols),
        wide_in=full(PAD + length, width), wide_mix=full(PAD + length, mixed),
        fh_o=low(PAD, width + mixed), fh_i=low(PAD, width + mixed), vec=full(8, LANES),
        sum_in=full(length, width), sum_mix=full(length, mixed), raw=full(length, LANES),
        cum=full(length, LANES), step_wide=full(length, width), fading=full(length, width),
        grown=full(length, width), pulled=low(length, width), decay=full(width, state_size),
        mix=low(length, mixed), act=full(length, width), stepped=low(length, width),
        state_term=low(width, state_size), back_term=low(width, state_size),
        start=low(width, state_size), end=low(width, state_size),
        scr0=low(width, state_size), scr1=low(width, state_size),
        z=full(length, width), y=full(length, width), score_grad=full(length, length),
        local=full(length, width), slope_in=full(length, width), slope_mix=full(length, mixed),
        steps=low(length, LANES),
        pad_in=full(length + 8, width), pad_mix=full(length + 8, mixed),
        gin=low(seqs, dps, length, width), gsm=low(seqs, dps, small, mixed),
        hal_o=full(8, width + mixed), hal_i=full(8, width + mixed),
        gmp=low(length, mixed), gm_in=low(chans, rows, mixed),
        p_o=low(chans, rows, model), m_o=low(chans, band, mixed),
        load_sem=dma((len(LOADED),)), fh_sem=dma((2,)), hal_sem=dma((2,)),
        near_s=dma((chans,)), near_r=dma((chans,)),
        far_s=dma((chans // 2, chans)), far_r=dma((chans // 2, chans)),
        relay_s=dma((chans // 2, chans)), relay_r=dma((chans // 2, chans)),
        swap_s=dma((dps,)), swap_r=dma((dps,)), cross_s=dma((seqs,)), cross_r=dma((seqs,)),
        gat_s=dma((chans,)), gat_r=dma((chans,)),
        chain_s=dma((2, PIECES)), chain_r=dma((2, PIECES)),
        z_r=dma((chans, seqs)), c_r=dma((chans, dps, seqs)),
        u_s=dma((chans, seqs)), d_s=dma((chans, seqs)), x_s=dma((chans, dps, seqs)),
        c2_r=dma((dps,)), z2_r=dma((dps, seqs)), x2_s=dma((dps,)),
        u2_s=dma((dps, seqs)), d2_s=dma((dps, seqs)),
        gm_s=dma((chans,)), gm_r=dma((chans,)),
        p_s=dma((chans, chans)), p_r=dma((chans, chans)), m_s=dma((chans,)), m_r=dma((chans,)),
    )
    names = [key + "_h" for key in inputs] + list(outputs) + list(scratch)
    parts, inner_grad, mix_parts, step_grad = pl.pallas_call(
        functools.partial(layer_kernel, names, sizes, heads),
        out_shape=tuple(outputs.values()),
        in_specs=[hbm] * len(inputs),
        out_specs=(vmem,) * len(outputs),
        scratch_shapes=list(scratch.values()),
        compiler_params=pltpu.CompilerParams(
            collective_id=0, has_side_effects=True, vmem_limit_bytes=LIMIT
        ),
        name="layer",
    )(*inputs.values())
    input_grad, inner_grad, mixer_grad, step_grad = pl.pallas_call(
        finish_kernel,
        out_shape=(
            jax.ShapeDtypeStruct((rows, model), BF),
            jax.ShapeDtypeStruct((cols, width), F32),
            jax.ShapeDtypeStruct((band, mixed), F32),
            jax.ShapeDtypeStruct((heads, cols), F32),
        ),
        in_specs=[vmem] * 4,
        out_specs=(pl.BlockSpec(memory_space=pl.ANY),) * 4,
        scratch_shapes=[
            pltpu.VMEM((rows, model), BF),
            pltpu.VMEM((band, mixed), F32),
            dma((4,)),
        ],
        compiler_params=pltpu.CompilerParams(vmem_limit_bytes=LIMIT),
        name="finish",
    )(parts, inner_grad, mix_parts, step_grad)
    return input_grad[None], inner_grad, mixer_grad, step_grad.T


def solution(mesh):
    sizes = dict(mesh.shape)
    in_specs = (
        P("dp", ("seq", "chan"), None),
        P(None, "chan"),
        P(),
        P(None, "chan"),
        P(None, "chan"),
        P(),
        P("chan"),
        P("chan"),
        P("chan"),
        P("dp", "seq", "chan"),
    )
    out_specs = (
        P("dp", ("seq", "chan"), None),
        P(("dp", "seq"), "chan"),
        P(("dp", "seq", "chan"), None),
        P(("dp", "seq"), "chan"),
    )
    return jax.shard_map(
        functools.partial(body, sizes),
        mesh=mesh,
        in_specs=in_specs,
        out_specs=out_specs,
        check_vma=False,
    )
```

```python
import functools
import math
import types

import jax
import jax.numpy as jnp
from jax import lax
from jax.experimental import pallas as pl
from jax.experimental.pallas import tpu as pltpu
from jax.sharding import PartitionSpec as P

MESH = pl.DeviceIdType.MESH
HDIM = 64
PAD = 16
LANES = 128
LIMIT = 48 * 2**20
BF = jnp.bfloat16
F32 = jnp.float32
HIGH = lax.Precision.HIGHEST
PIECES = 10
LOADED = (
    "own", "w_in", "w_mix", "w_step", "conv_in", "conv_mix", "bias", "log", "skip", "grad",
)


def each(n, step):
    if n <= 12:
        for d in range(1, n):
            step(d)
    else:

        def one(d, carry):
            step(d)
            return carry

        lax.fori_loop(1, n, one, 0)


def signal_to(barrier, where):
    pl.semaphore_signal(barrier, inc=1, device_id=where, device_id_type=MESH)


def mm(a, b, da, db):
    return lax.dot_general(
        a.astype(BF), b.astype(BF), (((da,), (db,)), ((), ())), preferred_element_type=F32
    )


def exact(a, b, da=1, db=0):
    return lax.dot_general(
        a, b, (((da,), (db,)), ((), ())), precision=HIGH, preferred_element_type=F32
    )


def softplus(v):
    return jnp.maximum(v, 0.0) + jnp.log1p(jnp.exp(-jnp.abs(v)))


def head_mask(width, heads_first):
    shape = (LANES, width) if heads_first else (width, LANES)
    head = lax.broadcasted_iota(jnp.int32, shape, 0 if heads_first else 1)
    column = lax.broadcasted_iota(jnp.int32, shape, 1 if heads_first else 0)
    return (column // HDIM == head).astype(F32)


def decays(raw, bias, decay_log):
    length = raw.shape[0]
    step = softplus(raw + bias)
    rate = jnp.exp(decay_log)
    row = lax.broadcasted_iota(jnp.int32, (length, length), 0)
    col = lax.broadcasted_iota(jnp.int32, (length, length), 1)
    lower = (row >= col).astype(F32)
    cumulative = exact(lower, -step * rate)
    return step, rate, cumulative, row, col, lower


def rcopy(src, dst, send, recv, **where):
    return pltpu.make_async_remote_copy(
        src_ref=src, dst_ref=dst, send_sem=send, recv_sem=recv, device_id=where, device_id_type=MESH
    )


def greet_all(barrier, axis, n):
    me = lax.axis_index(axis)
    each(n, lambda d: signal_to(barrier, {axis: lax.rem(me + d, n)}))
    return n - 1


def convolved(wide, kernel, first, count):
    taps = kernel.shape[0]
    first = first + PAD - (taps - 1)
    total = kernel[0:1, :] * wide[pl.ds(first, count), :]
    for k in range(1, taps):
        total = total + kernel[k : k + 1, :] * wide[pl.ds(first + k, count), :]
    return total


def spread_back(pad, kernel, first, count):
    taps = kernel.shape[0]
    total = None
    for k in range(taps):
        term = kernel[k : k + 1, :] * pad[pl.ds(first + taps - 1 - k, count), :]
        total = term if total is None else total + term
    return total.astype(BF)


def layer_kernel(names, sizes, heads, *refs):
    r = types.SimpleNamespace(**dict(zip(names, refs, strict=True)))
    place = (lax.axis_index("dp"), lax.axis_index("seq"), lax.axis_index("chan"))
    D, S, C = sizes["dp"], sizes["seq"], sizes["chan"]
    barrier = pltpu.get_barrier_semaphore()
    total = greet_all(barrier, "dp", D) + greet_all(barrier, "seq", S) + greet_all(barrier, "chan", C)
    loads = {
        key: pltpu.make_async_copy(getattr(r, key + "_h"), getattr(r, key), r.load_sem.at[i])
        for i, key in enumerate(LOADED)
    }
    for copy in loads.values():
        copy.start()
    front(r, sizes, place, heads, loads, barrier, total)
    scan_back(r, sizes, place, heads)
    back(r, sizes, place, heads)


def front(r, sizes, place, heads, loads, barrier, total):
    D, S, C = sizes["dp"], sizes["seq"], sizes["chan"]
    mine, me, ch = place
    rows, model = r.own.shape
    length, width = r.sum_in.shape
    mixed = r.sum_mix.shape[1]
    cols = model // (D * S)
    half = mixed // 2
    pieces = C
    cut = model // pieces
    sides = C // 2
    side, low = lax.div(ch, 2), lax.rem(ch, 2)
    partner = ch + 1 - 2 * low

    def block(c, p):
        return r.xg.at[pl.ds(pl.multiple_of(c * rows, rows), rows), pl.ds(p * cut, cut)]

    def mine_at(p):
        return r.own.at[:, pl.ds(p * cut, cut)]

    def near(c, p):
        return rcopy(mine_at(p), block(c, p), r.near_s.at[p], r.near_r.at[p], chan=partner)

    def far(to, c, slot, p):
        return rcopy(
            mine_at(p), block(c, p), r.far_s.at[to, p], r.far_r.at[slot, p], chan=2 * to + low
        )

    def relay(source, lane, p):
        c = 2 * source + lane
        here = block(c, p)
        return rcopy(here, here, r.relay_s.at[source, p], r.relay_r.at[source, p], chan=partner)

    def swap(q, landing, slot):
        return rcopy(r.blocks.at[q], r.mid.at[landing], r.swap_s.at[q], r.swap_r.at[slot], dp=q)

    def cross(q, landing, slot):
        return rcopy(r.mid.at[:, q], r.xs.at[landing], r.cross_s.at[q], r.cross_r.at[slot], seq=q)

    loads["own"].wait()
    pl.semaphore_wait(barrier, total)
    for p in range(pieces):
        for d in range(1, sides):
            far(lax.rem(side + d, sides), ch, side, p).start()
        near(ch, p).start()
    for d in range(D):
        for k in range(S):
            at = (d * S + k) * cols
            r.blocks[d, k] = r.own[:, at : at + cols]
    each(D, lambda d: swap(lax.rem(mine + d, D), mine, mine).start())
    r.mid[mine] = r.blocks[mine]
    r.xg[pl.ds(pl.multiple_of(ch * rows, rows), rows), :] = r.own[...]
    r.wst[...] = jnp.zeros(r.wst.shape, BF)
    r.vec[...] = jnp.zeros(r.vec.shape, F32)
    for key in LOADED[1:]:
        loads[key].wait()
    r.wst[0:heads, :] = r.w_step[...]
    for i, ref in enumerate((r.bias, r.log, r.skip)):
        r.vec[i : i + 1, 0:heads] = ref[...]

    def pass_on(p):
        for d in range(1, sides):
            source = lax.rem(side + d, sides)
            far(source, ch, source, p).wait_recv()
            relay(source, low, p).start()

    def project(p):
        near(partner, p).wait_recv()
        for d in range(1, sides):
            source = lax.rem(side + d, sides)
            relay(source, 1 - low, p).wait_recv()
        piece = slice(p * cut, (p + 1) * cut)
        x = r.xg[:, piece]
        inner = mm(x, r.w_in[piece, :], 1, 0)
        mixer = mm(x, r.w_mix[piece, :], 1, 0)
        raw = mm(x, r.wst[:, piece], 1, 1)
        if p == 0:
            r.wide_in[PAD:, :], r.wide_mix[PAD:, :], r.raw[...] = inner, mixer, raw
        else:
            r.wide_in[PAD:, :] = r.wide_in[PAD:, :] + inner
            r.wide_mix[PAD:, :] = r.wide_mix[PAD:, :] + mixer
            r.raw[...] = r.raw[...] + raw

    pass_on(0)
    for p in range(pieces):
        if p + 1 < pieces:
            pass_on(p + 1)
        project(p)
        if p == pieces // 2:
            each(D, lambda d: swap(lax.rem(mine + d, D), mine, lax.rem(mine + d, D)).wait_recv())
            each(S, lambda d: cross(lax.rem(me + d, S), me, me).start())
            r.xs[me] = r.mid[:, me]
    inner_low = r.wide_in[PAD:, :].astype(BF)
    mixer_low = r.wide_mix[PAD:, :].astype(BF)
    r.fh_o[:, :width] = inner_low[length - PAD :, :]
    r.fh_o[:, width:] = mixer_low[length - PAD :, :]

    def halo():
        return rcopy(r.fh_o, r.fh_i, r.fh_sem.at[0], r.fh_sem.at[1], seq=lax.rem(me + 1, S))

    @pl.when(me < S - 1)
    def _():
        halo().start()

    r.wide_in[PAD:, :] = inner_low.astype(F32)
    r.wide_mix[PAD:, :] = mixer_low.astype(F32)
    r.wide_in[0:PAD, :] = jnp.zeros((PAD, width), F32)
    r.wide_mix[0:PAD, :] = jnp.zeros((PAD, mixed), F32)
    r.sum_in[PAD:, :] = convolved(r.wide_in, r.conv_in, PAD, length - PAD)
    r.sum_mix[PAD:, :] = convolved(r.wide_mix, r.conv_mix, PAD, length - PAD)
    step, rate, cumulative, row, col, lower = decays(r.raw[...], r.vec[0:1, :], r.vec[1:2, :])
    last = cumulative[length - 1 : length, :]
    spread = head_mask(width, True)
    r.cum[...] = cumulative
    step_wide = exact(step, spread)
    fading = exact(jnp.exp(last - cumulative), spread)
    grown = exact(jnp.exp(cumulative), spread)
    r.step_wide[...] = step_wide
    r.fading[...] = fading
    r.grown[...] = grown
    pulled = (grown * r.grad[...].astype(F32)).astype(BF)
    r.pulled[...] = pulled
    row_decay = jnp.sum(head_mask(width, False) * jnp.exp(last), axis=1, keepdims=True)
    r.decay[...] = jnp.broadcast_to(row_decay, r.decay.shape)

    @pl.when(me > 0)
    def _():
        halo().wait_recv()
        r.wide_in[0:PAD, :] = r.fh_i[:, :width].astype(F32)
        r.wide_mix[0:PAD, :] = r.fh_i[:, width:].astype(F32)

    r.sum_in[0:PAD, :] = convolved(r.wide_in, r.conv_in, 0, PAD)
    r.sum_mix[0:PAD, :] = convolved(r.wide_mix, r.conv_mix, 0, PAD)
    mixer = r.sum_mix[...]
    mix = mixer * jax.nn.sigmoid(mixer)
    r.mix[...] = mix.astype(BF)
    r.back_term[...] = mm(pulled, mix[:, half:], 0, 0).astype(BF)
    inner = r.sum_in[...]
    act = inner * jax.nn.sigmoid(inner)
    r.act[...] = act
    r.state_term[...] = mm(act * (fading * step_wide), mix[:, :half], 0, 0).astype(BF)

    @pl.when(me < S - 1)
    def _():
        halo().wait_send()

    for p in range(pieces):
        near(ch, p).wait_send()
        for d in range(1, sides):
            source = lax.rem(side + d, sides)
            far(source, ch, source, p).wait_send()
            relay(source, low, p).wait_send()
    each(D, lambda d: swap(lax.rem(mine + d, D), mine, mine).wait_send())

    def settle(d):
        q = lax.rem(me + d, S)
        cross(q, me, q).wait()

    each(S, settle)


def scan_back(r, sizes, place, heads):
    S, C = sizes["seq"], sizes["chan"]
    mine, me, ch = place
    length, width = r.sum_in.shape
    half = r.sum_mix.shape[1] // 2
    pieces, lag = PIECES, PIECES // 2
    size = width // pieces
    terms, outs, scratch = (r.state_term, r.back_term), (r.start, r.end), (r.scr0, r.scr1)
    spots = (me, S - 1 - me)

    def carry(way, piece, first=False):
        part = pl.ds(pl.multiple_of(piece * size, size), size)
        to = lax.rem(me + 1, S) if way == 0 else lax.rem(me + S - 1, S)
        source = terms[way] if first else scratch[way]
        sems = r.chain_s.at[way, piece], r.chain_r.at[way, piece]
        return rcopy(source.at[part], outs[way].at[part], *sems, seq=to)

    for way in (0, 1):

        @pl.when(spots[way] == 0)
        def _(way=way):
            for piece in range(pieces):
                carry(way, piece, True).start()
            outs[way][...] = jnp.zeros(outs[way].shape, BF)

    def beat(t):
        for way in (0, 1):
            spot = spots[way]
            piece = t - lag * (spot - 1)

            @pl.when((piece >= 0) & (piece < pieces) & (spot > 0) & (spot < S - 1))
            def _(way=way, piece=piece):
                carry(way, piece).wait_recv()
                part = pl.ds(pl.multiple_of(piece * size, size), size)
                before = outs[way][part, :].astype(F32)
                term = terms[way][part, :].astype(F32)
                scratch[way][part, :] = (r.decay[part, :] * before + term).astype(BF)
                carry(way, piece).start()

    def gather(q, landing, slot):
        return rcopy(r.xs, r.xc.at[:, :, landing], r.gat_s.at[q], r.gat_r.at[slot], chan=q)

    each(C, lambda d: gather(lax.rem(ch + d, C), ch, ch).start())
    r.xc[:, :, ch] = r.xs[...]

    spread = head_mask(width, True)
    cumulative = r.cum[...]
    across = cumulative.T
    row = lax.broadcasted_iota(jnp.int32, (length, length), 0)
    col = lax.broadcasted_iota(jnp.int32, (length, length), 1)
    causal = row >= col
    lower = causal.astype(F32)
    into, out_of = r.mix[:, :half], r.mix[:, half:]
    scores = mm(out_of, into, 1, 1)
    act = r.act[...]
    stepped_low = (act * r.step_wide[...]).astype(BF)
    r.stepped[...] = stepped_low

    def head(h):
        cols = slice(h * HDIM, (h + 1) * HDIM)
        gap = cumulative[:, h : h + 1] - across[h : h + 1, :]
        decay = jnp.where(causal, jnp.exp(jnp.where(causal, gap, 0.0)), 0.0)
        weights = (decay * scores).astype(BF)
        grad_h, step_h = r.grad[:, cols], r.stepped[:, cols]
        term = decay * mm(grad_h, step_h, 1, 1)
        r.score_grad[...] = term if h == 0 else r.score_grad[...] + term
        r.z[:, cols] = mm(weights, grad_h, 0, 0)
        r.y[:, cols] = mm(weights, step_h, 1, 0)

    beats = pieces + lag * max(S - 3, 0)
    early = heads // 2
    for h in range(early):
        head(h)
    if beats <= 24:
        for t in range(beats):
            beat(t)
            if early + t < heads:
                head(early + t)
    else:
        for h in range(early, heads):
            head(h)
        lax.fori_loop(0, beats, lambda t, c: (beat(t), c)[1], 0)

    upstream = r.grad[...].astype(F32)
    stepped = r.stepped[...].astype(F32)
    step_wide = r.step_wide[...]
    skip_wide = exact(jnp.broadcast_to(r.vec[2:3, :], (8, LANES)), spread)[0:1, :]
    inner, mixer = r.sum_in[...], r.sum_mix[...]
    inner_gate, mixer_gate = jax.nn.sigmoid(inner), jax.nn.sigmoid(mixer)
    inner_slope = inner_gate * (1.0 + inner * (1.0 - inner_gate))
    mixer_slope = mixer_gate * (1.0 + mixer * (1.0 - mixer_gate))
    to_heads = functools.partial(exact, b=spread, da=1, db=1)
    z = r.z[...]
    r.slope_in[...] = inner_slope
    r.slope_mix[...] = mixer_slope
    r.local[...] = (step_wide * z + skip_wide * upstream) * inner_slope
    local_step = to_heads(r.act[...] * z)
    local_sum = to_heads(upstream * r.y[...] - stepped * z)
    score_grad = r.score_grad[...]
    out_local = mm(score_grad, into, 1, 0)
    into_local = mm(score_grad, out_of, 0, 0)
    faded = (r.fading[...] * stepped).astype(BF)

    for way in (0, 1):

        @pl.when(spots[way] == S - 1)
        def _(way=way):
            for piece in range(pieces):
                carry(way, piece).wait_recv()

    start, end = r.start[...], r.end[...]
    carried = r.grown[...] * mm(out_of, start, 1, 1)
    ending = r.fading[...] * mm(into, end, 1, 1)
    r.pad_in[0:length, :] = r.local[...] + (r.step_wide[...] * ending) * r.slope_in[...]
    r.pad_mix[0:length, :half] = (into_local + mm(faded, end, 1, 0)) * r.slope_mix[:, :half]
    r.pad_mix[0:length, half:] = (out_local + mm(r.pulled[...], start, 1, 0)) * r.slope_mix[:, half:]
    step_grad = local_step + to_heads(r.act[...] * ending)
    tail_term = to_heads(stepped * ending)
    sum_grad = local_sum + to_heads(upstream * carried) - tail_term
    held = jnp.sum(start.astype(F32) * end.astype(F32), axis=1, keepdims=True)
    last = cumulative[length - 1 : length, :]
    overall = jnp.sum(tail_term, axis=0, keepdims=True) + jnp.exp(last) * jnp.sum(
        head_mask(width, False) * held, axis=0, keepdims=True
    )
    decay_grad = exact(lower, sum_grad, 0, 0) + overall
    rate = jnp.exp(r.vec[1:2, :])
    step_grad = (step_grad - rate * decay_grad) * jax.nn.sigmoid(r.raw[...] + r.vec[0:1, :])
    r.steps[...] = step_grad.astype(BF)

    for way in (0, 1):

        @pl.when(spots[way] < S - 1)
        def _(way=way):
            for piece in range(pieces):
                carry(way, piece).wait_send()

    def settle_gather(d):
        q = lax.rem(ch + d, C)
        gather(q, q, q).wait()

    each(C, settle_gather)


def back(r, sizes, place, heads):
    D, S, C = sizes["dp"], sizes["seq"], sizes["chan"]
    mine, me, ch = place
    length, width = r.sum_in.shape
    mixed = r.sum_mix.shape[1]
    model = r.w_in.shape[0]
    rows = length // C
    parts = C
    r.hal_o[:, :width] = r.pad_in[0:8, :]
    r.hal_o[:, width:] = r.pad_mix[0:8, :]
    r.pad_in[length:, :] = jnp.zeros((8, width), F32)
    r.pad_mix[length:, :] = jnp.zeros((8, mixed), F32)
    last = length - rows
    r.gin[me, mine, 0:last, :] = spread_back(r.pad_in, r.conv_in, 0, last)
    r.gmp[0:last, :] = spread_back(r.pad_mix, r.conv_mix, 0, last)
    r.gsm[me, mine, rows:, 0:LANES] = r.steps[...].astype(F32).T[0:PAD, :].astype(BF)

    def others():
        return [lax.rem(mine + e, D) for e in range(1, D)]

    def halo():
        return rcopy(r.hal_o, r.hal_i, r.hal_sem.at[0], r.hal_sem.at[1], seq=lax.rem(me + S - 1, S))

    @pl.when(me > 0)
    def _():
        halo().start()

    def part(p, e, k):
        return r.gin.at[k, e, pl.ds(p * rows, rows)]

    def zcopy(p, way, k):
        to = lax.rem(me + (1 if way == "up" else S - 1), S)
        send = (r.u_s if way == "up" else r.d_s).at[p, k]
        return rcopy(part(p, mine, k), part(p, mine, k), send, r.z_r.at[p, k], seq=to)

    def ccopy(p, k, e, to):
        return rcopy(part(p, e, k), part(p, e, k), r.x_s.at[p, to, k], r.c_r.at[p, e, k], dp=to)

    def zsmall(way, e, k):
        to = lax.rem(me + (1 if way == "up" else S - 1), S)
        send = (r.u2_s if way == "up" else r.d2_s).at[e, k]
        return rcopy(r.gsm.at[k, e], r.gsm.at[k, e], send, r.z2_r.at[e, k], seq=to)

    def csmall(e, to):
        return rcopy(r.gsm.at[me, e], r.gsm.at[me, e], r.x2_s.at[to], r.c2_r.at[e], dp=to)

    def onward(make, k):
        @pl.when(me < S - 1)
        def _():
            make("up", k).start()

        @pl.when(me > 0)
        def _():
            make("down", k).start()

    def own_part(p):
        onward(functools.partial(zcopy, p), me)
        for e in others():
            ccopy(p, me, mine, e).start()

    def forward(d, p):
        for way, k, there, more in (
            ("up", me - d, me >= d, me < S - 1),
            ("down", me + d, me + d < S, me > 0),
        ):

            @pl.when(there)
            def _(way=way, k=k):
                zcopy(p, way, k).wait_recv()

            @pl.when(there & more)
            def _(way=way, k=k):
                zcopy(p, way, k).start()

            @pl.when(there)
            def _(k=k):
                for e in others():
                    ccopy(p, k, mine, e).start()

    def own_small():
        for e in others():
            csmall(mine, e).start()
        onward(lambda way, k: zsmall(way, mine, k), me)

    def cross_small():
        for e in others():
            csmall(e, e).wait_recv()
            onward(lambda way, k, e=e: zsmall(way, e, k), me)

    def forward_small(d):
        for way, k, there, more in (
            ("up", me - d, me >= d, me < S - 1),
            ("down", me + d, me + d < S, me > 0),
        ):
            for e in [mine] + others():

                @pl.when(there)
                def _(way=way, k=k, e=e):
                    zsmall(way, e, k).wait_recv()

                @pl.when(there & more)
                def _(way=way, k=k, e=e):
                    zsmall(way, e, k).start()

    norm = 1.0 / math.sqrt(D * S * length)

    def columns_of(k):
        block = r.xc[k]
        return block.reshape(D * length, block.shape[-1])

    def weight_term(k, first=False):
        for e in others():
            for p in range(parts):
                ccopy(p, k, e, e).wait_recv()
        x = columns_of(k)
        term = norm * mm(x, r.gin[k].reshape(D * length, width), 0, 0)
        r.o_dw[...] = term if first else r.o_dw[...] + term

    def weight_terms(d):
        for k, there in ((me - d, me >= d), (me + d, me + d < S)):

            @pl.when(there)
            def _(k=k):
                weight_term(k)

    for p in range(parts - 1):
        own_part(p)

    @pl.when(me < S - 1)
    def _():
        halo().wait_recv()
        r.pad_in[length:, :] = r.hal_i[:, :width]
        r.pad_mix[length:, :] = r.hal_i[:, width:]

    r.gin[me, mine, last:, :] = spread_back(r.pad_in, r.conv_in, last, rows)
    r.gmp[last:, :] = spread_back(r.pad_mix, r.conv_mix, last, rows)
    own_part(parts - 1)

    def share_mix(q, landing, slot):
        return rcopy(r.gmp.at[pl.ds(q * rows, rows)], r.gm_in.at[landing], r.gm_s.at[q], r.gm_r.at[slot], chan=q)

    each(C, lambda d: share_mix(lax.rem(ch + d, C), ch, ch).start())
    cut = model // parts

    def share_p(j, q, landing, slot):
        piece = pl.ds(j * cut, cut)
        return rcopy(
            r.p_o.at[q, :, piece], r.p_i.at[landing, :, piece], r.p_s.at[j, q], r.p_r.at[j, slot], chan=q
        )

    grads = r.gin[me, mine]
    mixes = r.gmp[...]
    steps = r.steps[:, 0:PAD]

    def back_project(j):
        piece = slice(j * cut, (j + 1) * cut)
        out = mm(grads, r.w_in[piece, :], 1, 1) + mm(mixes, r.w_mix[piece, :], 1, 1)
        out = out + mm(steps, r.wst[0:PAD, piece], 1, 0)
        r.p_o[:, :, piece] = out.astype(BF).reshape(C, rows, cut)
        each(C, lambda d: share_p(j, lax.rem(ch + d, C), ch, ch).start())

    def finish_mix():
        r.gm_in[ch] = r.gmp[pl.ds(pl.multiple_of(ch * rows, rows), rows), :]
        each(C, lambda d: share_mix(lax.rem(ch + d, C), ch, lax.rem(ch + d, C)).wait_recv())
        mix = r.gm_in[0].astype(F32)
        for q in range(1, C):
            mix = mix + r.gm_in[q].astype(F32)
        r.gsm[me, mine, 0:rows, :] = mix.astype(BF)
        own_small()

    for j in range(parts):
        back_project(j)
        forward(1, j)
        if j == 0:
            finish_mix()
    weight_term(me, True)

    def hop(d):
        for p in range(parts):
            forward(d, p)
        if isinstance(d, int) and d == 2:
            cross_small()
        forward_small(d - 1)
        weight_terms(d - 1)

    hop(2)
    if S > 3:
        if S <= 12:
            for d in range(3, S):
                hop(d)
        else:
            lax.fori_loop(3, S, lambda d, c: (hop(d), c)[1], 0)
    forward_small(S - 1)

    mixer_columns = r.xc[:, :, ch].reshape(S * D * rows, r.xc.shape[-1])
    mixer_grads = r.gsm[:, :, 0:rows, :].reshape(S * D * rows, mixed)
    mixer_term = norm * mm(mixer_columns, mixer_grads, 0, 0)
    band = mixer_term.shape[0] // C
    for q in range(C):
        r.m_o[q] = mixer_term[q * band : (q + 1) * band, :].astype(BF)

    def share_m(q, landing, slot):
        return rcopy(r.m_o.at[q], r.m_i.at[landing], r.m_s.at[q], r.m_r.at[slot], chan=q)

    each(C, lambda d: share_m(lax.rem(ch + d, C), ch, ch).start())
    step_total = None
    for k in range(S) if S <= 12 else ():
        for e in range(D):
            x = r.xc[k, e].reshape(length, r.xc.shape[-1])
            term = mm(r.gsm[k, e, rows:, 0:LANES], x, 1, 0)
            step_total = term if step_total is None else step_total + term
    if step_total is None:

        def one(k, carry):
            for e in range(D):
                x = r.xc[k, e].reshape(length, r.xc.shape[-1])
                carry = carry + mm(r.gsm[k, e, rows:, 0:LANES], x, 1, 0)
            return carry

        step_total = lax.fori_loop(0, S, one, jnp.zeros((PAD, r.xc.shape[-1]), F32))
    r.o_dws[...] = (norm * step_total)[:heads, :]

    r.p_i[ch] = r.p_o[ch]
    for j in range(parts):
        each(C, lambda d, j=j: share_p(j, lax.rem(ch + d, C), ch, lax.rem(ch + d, C)).wait_recv())
    weight_terms(S - 1)
    r.m_i[ch] = r.m_o[ch]
    each(C, lambda d: share_m(lax.rem(ch + d, C), ch, lax.rem(ch + d, C)).wait_recv())

    @pl.when(me > 0)
    def _():
        halo().wait_send()

    def settle_chan(d):
        q = lax.rem(ch + d, C)
        share_mix(q, ch, ch).wait_send()
        share_m(q, ch, ch).wait_send()
        for j in range(parts):
            share_p(j, q, ch, ch).wait_send()

    each(C, settle_chan)

    def settle_line(k):
        for e in others():
            for p in range(parts):
                ccopy(p, k, mine, e).wait_send()
        for way, sent in (("up", (k <= me) & (me < S - 1)), ("down", (k >= me) & (me > 0))):

            @pl.when(sent)
            def _(way=way):
                for p in range(parts):
                    zcopy(p, way, k).wait_send()
                for e in [mine] + others():
                    zsmall(way, e, k).wait_send()

    settle_line(0)
    each(S, settle_line)
    for e in others():
        csmall(mine, e).wait_send()


def finish_kernel(parts, dw, mixes, dws, o_ig, o_dw, o_dwm, o_dws, ig, dwm, sems):
    copies = [
        pltpu.make_async_copy(a, b, sems.at[i])
        for i, (a, b) in enumerate(((dw, o_dw), (dws, o_dws), (ig, o_ig), (dwm, o_dwm)))
    ]
    copies[0].start()
    copies[1].start()
    total = parts[0].astype(F32)
    for q in range(1, parts.shape[0]):
        total = total + parts[q].astype(F32)
    ig[...] = total.astype(BF)
    copies[2].start()
    total = mixes[0].astype(F32)
    for q in range(1, mixes.shape[0]):
        total = total + mixes[q].astype(F32)
    dwm[...] = total
    copies[3].start()
    for copy in copies:
        copy.wait()


def body(
    sizes,
    layer_input,
    inner_weight,
    mixer_weight,
    step_weight,
    conv_inner,
    conv_mixer,
    step_bias,
    decay_log,
    skip_gain,
    output_grad,
):
    own = layer_input[0]
    rows, model = own.shape
    chans, seqs, dps = sizes["chan"], sizes["seq"], sizes["dp"]
    groups = dps * seqs
    length = rows * chans
    width = inner_weight.shape[1]
    mixed = mixer_weight.shape[1]
    heads = step_bias.shape[0]
    cols = model // groups
    state_size = mixed // 2
    assert width % PIECES == 0 and chans % 2 == 0 and seqs > 2
    assert length == LANES and heads + conv_inner.shape[0] - 1 <= PAD
    upstream = output_grad[0]
    step_rows = step_weight.T
    bias, rates, skips = (v.reshape(1, heads) for v in (step_bias, decay_log, skip_gain))
    dma = pltpu.SemaphoreType.DMA
    vmem = pl.BlockSpec(memory_space=pltpu.VMEM)
    hbm = pl.BlockSpec(memory_space=pltpu.HBM)
    small = rows + PAD
    band = cols // chans

    def low(*shape):
        return pltpu.VMEM(shape, BF)

    def full(*shape):
        return pltpu.VMEM(shape, F32)

    inputs = dict(
        own=own, w_in=inner_weight, w_mix=mixer_weight, w_step=step_rows, conv_in=conv_inner,
        conv_mix=conv_mixer, bias=bias, log=rates, skip=skips, grad=upstream,
    )
    outputs = dict(
        p_i=jax.ShapeDtypeStruct((chans, rows, model), BF),
        o_dw=jax.ShapeDtypeStruct((cols, width), F32),
        m_i=jax.ShapeDtypeStruct((chans, band, mixed), BF),
        o_dws=jax.ShapeDtypeStruct((heads, cols), F32),
    )
    scratch = {key: pltpu.VMEM(v.shape, v.dtype) for key, v in inputs.items()}
    scratch |= dict(
        wst=low(LANES, model), xg=low(length, model),
        blocks=low(dps, seqs, rows, cols), mid=low(dps, seqs, rows, cols),
        xs=low(seqs, dps, rows, cols), xc=low(seqs, dps, chans, rows, cols),
        wide_in=full(PAD + length, width), wide_mix=full(PAD + length, mixed),
        fh_o=low(PAD, width + mixed), fh_i=low(PAD, width + mixed), vec=full(8, LANES),
        sum_in=full(length, width), sum_mix=full(length, mixed), raw=full(length, LANES),
        cum=full(length, LANES), step_wide=full(length, width), fading=full(length, width),
        grown=full(length, width), pulled=low(length, width), decay=full(width, state_size),
        mix=low(length, mixed), act=full(length, width), stepped=low(length, width),
        state_term=low(width, state_size), back_term=low(width, state_size),
        start=low(width, state_size), end=low(width, state_size),
        scr0=low(width, state_size), scr1=low(width, state_size),
        z=full(length, width), y=full(length, width), score_grad=full(length, length),
        local=full(length, width), slope_in=full(length, width), slope_mix=full(length, mixed),
        steps=low(length, LANES),
        pad_in=full(length + 8, width), pad_mix=full(length + 8, mixed),
        gin=low(seqs, dps, length, width), gsm=low(seqs, dps, small, mixed),
        hal_o=full(8, width + mixed), hal_i=full(8, width + mixed),
        gmp=low(length, mixed), gm_in=low(chans, rows, mixed),
        p_o=low(chans, rows, model), m_o=low(chans, band, mixed),
        load_sem=dma((len(LOADED),)), fh_sem=dma((2,)), hal_sem=dma((2,)),
        near_s=dma((chans,)), near_r=dma((chans,)),
        far_s=dma((chans // 2, chans)), far_r=dma((chans // 2, chans)),
        relay_s=dma((chans // 2, chans)), relay_r=dma((chans // 2, chans)),
        swap_s=dma((dps,)), swap_r=dma((dps,)), cross_s=dma((seqs,)), cross_r=dma((seqs,)),
        gat_s=dma((chans,)), gat_r=dma((chans,)),
        chain_s=dma((2, PIECES)), chain_r=dma((2, PIECES)),
        z_r=dma((chans, seqs)), c_r=dma((chans, dps, seqs)),
        u_s=dma((chans, seqs)), d_s=dma((chans, seqs)), x_s=dma((chans, dps, seqs)),
        c2_r=dma((dps,)), z2_r=dma((dps, seqs)), x2_s=dma((dps,)),
        u2_s=dma((dps, seqs)), d2_s=dma((dps, seqs)),
        gm_s=dma((chans,)), gm_r=dma((chans,)),
        p_s=dma((chans, chans)), p_r=dma((chans, chans)), m_s=dma((chans,)), m_r=dma((chans,)),
    )
    names = [key + "_h" for key in inputs] + list(outputs) + list(scratch)
    parts, inner_grad, mix_parts, step_grad = pl.pallas_call(
        functools.partial(layer_kernel, names, sizes, heads),
        out_shape=tuple(outputs.values()),
        in_specs=[hbm] * len(inputs),
        out_specs=(vmem,) * len(outputs),
        scratch_shapes=list(scratch.values()),
        compiler_params=pltpu.CompilerParams(
            collective_id=0, has_side_effects=True, vmem_limit_bytes=LIMIT
        ),
        name="layer",
    )(*(pltpu.with_memory_space_constraint(v, pltpu.HBM) for v in inputs.values()))
    input_grad, inner_grad, mixer_grad, step_grad = pl.pallas_call(
        finish_kernel,
        out_shape=(
            jax.ShapeDtypeStruct((rows, model), BF),
            jax.ShapeDtypeStruct((cols, width), F32),
            jax.ShapeDtypeStruct((band, mixed), F32),
            jax.ShapeDtypeStruct((heads, cols), F32),
        ),
        in_specs=[vmem] * 4,
        out_specs=(pl.BlockSpec(memory_space=pl.ANY),) * 4,
        scratch_shapes=[
            pltpu.VMEM((rows, model), BF),
            pltpu.VMEM((band, mixed), F32),
            dma((4,)),
        ],
        compiler_params=pltpu.CompilerParams(vmem_limit_bytes=LIMIT),
        name="finish",
    )(parts, inner_grad, mix_parts, step_grad)
    return input_grad[None], inner_grad, mixer_grad, step_grad.T


def solution(mesh):
    sizes = dict(mesh.shape)
    in_specs = (
        P("dp", ("seq", "chan"), None),
        P(None, "chan"),
        P(),
        P(None, "chan"),
        P(None, "chan"),
        P(),
        P("chan"),
        P("chan"),
        P("chan"),
        P("dp", "seq", "chan"),
    )
    out_specs = (
        P("dp", ("seq", "chan"), None),
        P(("dp", "seq"), "chan"),
        P(("dp", "seq", "chan"), None),
        P(("dp", "seq"), "chan"),
    )
    return jax.shard_map(
        functools.partial(body, sizes),
        mesh=mesh,
        in_specs=in_specs,
        out_specs=out_specs,
        check_vma=False,
    )
```

```python
import functools
import math
import types

import jax
import jax.numpy as jnp
from jax import lax
from jax.experimental import pallas as pl
from jax.experimental.pallas import tpu as pltpu
from jax.sharding import PartitionSpec as P

MESH = pl.DeviceIdType.MESH
HDIM = 64
PAD = 16
LANES = 128
LIMIT = 48 * 2**20
BF = jnp.bfloat16
F32 = jnp.float32
HIGH = lax.Precision.HIGHEST
PIECES = 10
LOADED = (
    "own", "w_in", "w_mix", "w_step", "conv_in", "conv_mix", "bias", "log", "skip", "grad",
)


def each(n, step):
    if n <= 12:
        for d in range(1, n):
            step(d)
    else:

        def one(d, carry):
            step(d)
            return carry

        lax.fori_loop(1, n, one, 0)


def signal_to(barrier, where):
    pl.semaphore_signal(barrier, inc=1, device_id=where, device_id_type=MESH)


def mm(a, b, da, db):
    return lax.dot_general(
        a.astype(BF), b.astype(BF), (((da,), (db,)), ((), ())), preferred_element_type=F32
    )


def exact(a, b, da=1, db=0):
    return lax.dot_general(
        a, b, (((da,), (db,)), ((), ())), precision=HIGH, preferred_element_type=F32
    )


def softplus(v):
    return jnp.maximum(v, 0.0) + jnp.log1p(jnp.exp(-jnp.abs(v)))


def head_mask(width, heads_first):
    shape = (LANES, width) if heads_first else (width, LANES)
    head = lax.broadcasted_iota(jnp.int32, shape, 0 if heads_first else 1)
    column = lax.broadcasted_iota(jnp.int32, shape, 1 if heads_first else 0)
    return (column // HDIM == head).astype(F32)


def decays(raw, bias, decay_log):
    length = raw.shape[0]
    step = softplus(raw + bias)
    rate = jnp.exp(decay_log)
    row = lax.broadcasted_iota(jnp.int32, (length, length), 0)
    col = lax.broadcasted_iota(jnp.int32, (length, length), 1)
    lower = (row >= col).astype(F32)
    cumulative = exact(lower, -step * rate)
    return step, rate, cumulative, row, col, lower


def rcopy(src, dst, send, recv, **where):
    return pltpu.make_async_remote_copy(
        src_ref=src, dst_ref=dst, send_sem=send, recv_sem=recv, device_id=where, device_id_type=MESH
    )


def greet_all(barrier, axis, n):
    me = lax.axis_index(axis)
    each(n, lambda d: signal_to(barrier, {axis: lax.rem(me + d, n)}))
    return n - 1


def convolved(wide, kernel, first, count):
    taps = kernel.shape[0]
    first = first + PAD - (taps - 1)
    total = kernel[0:1, :] * wide[pl.ds(first, count), :]
    for k in range(1, taps):
        total = total + kernel[k : k + 1, :] * wide[pl.ds(first + k, count), :]
    return total


def spread_back(pad, kernel, first, count):
    taps = kernel.shape[0]
    total = None
    for k in range(taps):
        term = kernel[k : k + 1, :] * pad[pl.ds(first + taps - 1 - k, count), :]
        total = term if total is None else total + term
    return total.astype(BF)


def layer_kernel(names, sizes, heads, *refs):
    r = types.SimpleNamespace(**dict(zip(names, refs, strict=True)))
    place = (lax.axis_index("dp"), lax.axis_index("seq"), lax.axis_index("chan"))
    D, S, C = sizes["dp"], sizes["seq"], sizes["chan"]
    barrier = pltpu.get_barrier_semaphore()
    total = greet_all(barrier, "dp", D) + greet_all(barrier, "seq", S) + greet_all(barrier, "chan", C)
    after = lax.rem(place[1] + 1, S)

    @pl.when(place[2] == C - 1)
    def _():
        for c in range(C):
            signal_to(barrier, {"seq": after, "chan": jnp.int32(c)})

    total += 1
    loads = {
        key: pltpu.make_async_copy(getattr(r, key + "_h"), getattr(r, key), r.load_sem.at[i])
        for i, key in enumerate(LOADED)
    }
    for copy in loads.values():
        copy.start()
    front(r, sizes, place, heads, loads, barrier, total)
    scan_back(r, sizes, place, heads)
    back(r, sizes, place, heads)


def front(r, sizes, place, heads, loads, barrier, total):
    D, S, C = sizes["dp"], sizes["seq"], sizes["chan"]
    mine, me, ch = place
    rows, model = r.own.shape
    length, width = r.sum_in.shape
    mixed = r.sum_mix.shape[1]
    cols = model // (D * S)
    half = mixed // 2
    pieces = C
    cut = model // pieces
    sides = C // 2
    side, low = lax.div(ch, 2), lax.rem(ch, 2)
    partner = ch + 1 - 2 * low

    def block(c, p):
        return r.xg.at[pl.ds(pl.multiple_of(c * rows, rows), rows), pl.ds(p * cut, cut)]

    def mine_at(p):
        return r.own.at[:, pl.ds(p * cut, cut)]

    def near(c, p):
        return rcopy(mine_at(p), block(c, p), r.near_s.at[p], r.near_r.at[p], chan=partner)

    def far(to, c, slot, p):
        return rcopy(
            mine_at(p), block(c, p), r.far_s.at[to, p], r.far_r.at[slot, p], chan=2 * to + low
        )

    def relay(source, lane, p):
        c = 2 * source + lane
        here = block(c, p)
        return rcopy(here, here, r.relay_s.at[source, p], r.relay_r.at[source, p], chan=partner)

    def swap(q, landing, slot):
        return rcopy(r.blocks.at[q], r.mid.at[landing], r.swap_s.at[q], r.swap_r.at[slot], dp=q)

    def cross(q, landing, slot):
        return rcopy(r.mid.at[:, q], r.xs.at[landing], r.cross_s.at[q], r.cross_r.at[slot], seq=q)

    loads["own"].wait()
    pl.semaphore_wait(barrier, total)
    for p in range(pieces):
        for d in range(1, sides):
            far(lax.rem(side + d, sides), ch, side, p).start()
        near(ch, p).start()
    for d in range(D):
        for k in range(S):
            at = (d * S + k) * cols
            r.blocks[d, k] = r.own[:, at : at + cols]
    each(D, lambda d: swap(lax.rem(mine + d, D), mine, mine).start())
    r.mid[mine] = r.blocks[mine]
    r.xg[pl.ds(pl.multiple_of(ch * rows, rows), rows), :] = r.own[...]
    r.wst[...] = jnp.zeros(r.wst.shape, BF)
    r.vec[...] = jnp.zeros(r.vec.shape, F32)
    for key in LOADED[1:]:
        loads[key].wait()
    r.wst[0:heads, :] = r.w_step[...]
    for i, ref in enumerate((r.bias, r.log, r.skip)):
        r.vec[i : i + 1, 0:heads] = ref[...]

    def pass_on(p):
        for d in range(1, sides):
            source = lax.rem(side + d, sides)
            far(source, ch, source, p).wait_recv()
            relay(source, low, p).start()

    def project(p):
        near(partner, p).wait_recv()
        for d in range(1, sides):
            source = lax.rem(side + d, sides)
            relay(source, 1 - low, p).wait_recv()
        piece = slice(p * cut, (p + 1) * cut)
        x = r.xg[:, piece]
        inner = mm(x, r.w_in[piece, :], 1, 0)
        mixer = mm(x, r.w_mix[piece, :], 1, 0)
        raw = mm(x, r.wst[:, piece], 1, 1)
        if p == 0:
            r.wide_in[PAD:, :], r.wide_mix[PAD:, :], r.raw[...] = inner, mixer, raw
        else:
            r.wide_in[PAD:, :] = r.wide_in[PAD:, :] + inner
            r.wide_mix[PAD:, :] = r.wide_mix[PAD:, :] + mixer
            r.raw[...] = r.raw[...] + raw

    pass_on(0)
    for p in range(pieces):
        if p + 1 < pieces:
            pass_on(p + 1)
        project(p)
        if p == pieces // 2:
            each(D, lambda d: swap(lax.rem(mine + d, D), mine, lax.rem(mine + d, D)).wait_recv())
            each(S, lambda d: cross(lax.rem(me + d, S), me, me).start())
            r.xs[me] = r.mid[:, me]
    inner_low = r.wide_in[PAD:, :].astype(BF)
    mixer_low = r.wide_mix[PAD:, :].astype(BF)
    r.fh_o[:, :width] = inner_low[length - PAD :, :]
    r.fh_o[:, width:] = mixer_low[length - PAD :, :]

    def halo():
        return rcopy(r.fh_o, r.fh_i, r.fh_sem.at[0], r.fh_sem.at[1], seq=lax.rem(me + 1, S))

    @pl.when(me < S - 1)
    def _():
        halo().start()

    r.wide_in[PAD:, :] = inner_low.astype(F32)
    r.wide_mix[PAD:, :] = mixer_low.astype(F32)
    r.wide_in[0:PAD, :] = jnp.zeros((PAD, width), F32)
    r.wide_mix[0:PAD, :] = jnp.zeros((PAD, mixed), F32)
    r.sum_in[PAD:, :] = convolved(r.wide_in, r.conv_in, PAD, length - PAD)
    r.sum_mix[PAD:, :] = convolved(r.wide_mix, r.conv_mix, PAD, length - PAD)
    step, rate, cumulative, row, col, lower = decays(r.raw[...], r.vec[0:1, :], r.vec[1:2, :])
    last = cumulative[length - 1 : length, :]
    spread = head_mask(width, True)
    r.cum[...] = cumulative
    step_wide = exact(step, spread)
    fading = exact(jnp.exp(last - cumulative), spread)
    grown = exact(jnp.exp(cumulative), spread)
    r.step_wide[...] = step_wide
    r.fading[...] = fading
    r.grown[...] = grown
    pulled = (grown * r.grad[...].astype(F32)).astype(BF)
    r.pulled[...] = pulled
    row_decay = jnp.sum(head_mask(width, False) * jnp.exp(last), axis=1, keepdims=True)
    r.decay[...] = jnp.broadcast_to(row_decay, r.decay.shape)

    @pl.when(me > 0)
    def _():
        halo().wait_recv()
        r.wide_in[0:PAD, :] = r.fh_i[:, :width].astype(F32)
        r.wide_mix[0:PAD, :] = r.fh_i[:, width:].astype(F32)

    r.sum_in[0:PAD, :] = convolved(r.wide_in, r.conv_in, 0, PAD)
    r.sum_mix[0:PAD, :] = convolved(r.wide_mix, r.conv_mix, 0, PAD)
    mixer = r.sum_mix[...]
    mix = mixer * jax.nn.sigmoid(mixer)
    r.mix[...] = mix.astype(BF)
    r.back_term[...] = mm(pulled, mix[:, half:], 0, 0).astype(BF)
    inner = r.sum_in[...]
    act = inner * jax.nn.sigmoid(inner)
    r.act[...] = act
    r.state_term[...] = mm(act * (fading * step_wide), mix[:, :half], 0, 0).astype(BF)

    @pl.when(me < S - 1)
    def _():
        halo().wait_send()

    for p in range(pieces):
        near(ch, p).wait_send()
        for d in range(1, sides):
            source = lax.rem(side + d, sides)
            far(source, ch, source, p).wait_send()
            relay(source, low, p).wait_send()
    each(D, lambda d: swap(lax.rem(mine + d, D), mine, mine).wait_send())

    def settle(d):
        q = lax.rem(me + d, S)
        cross(q, me, q).wait()

    each(S, settle)


def scan_back(r, sizes, place, heads):
    S, C = sizes["seq"], sizes["chan"]
    mine, me, ch = place
    length, width = r.sum_in.shape
    half = r.sum_mix.shape[1] // 2
    pieces, lag = PIECES, PIECES // 2
    size = width // pieces
    terms, outs, scratch = (r.state_term, r.back_term), (r.start, r.end), (r.scr0, r.scr1)
    spots = (me, S - 1 - me)

    def carry(way, piece, first=False):
        part = pl.ds(pl.multiple_of(piece * size, size), size)
        to = lax.rem(me + 1, S) if way == 0 else lax.rem(me + S - 1, S)
        source = terms[way] if first else scratch[way]
        sems = r.chain_s.at[way, piece], r.chain_r.at[way, piece]
        return rcopy(source.at[part], outs[way].at[part], *sems, seq=to)

    for way in (0, 1):

        @pl.when(spots[way] == 0)
        def _(way=way):
            for piece in range(pieces):
                carry(way, piece, True).start()
            outs[way][...] = jnp.zeros(outs[way].shape, BF)

    def beat(t):
        for way in (0, 1):
            spot = spots[way]
            piece = t - lag * (spot - 1)

            @pl.when((piece >= 0) & (piece < pieces) & (spot > 0) & (spot < S - 1))
            def _(way=way, piece=piece):
                carry(way, piece).wait_recv()
                part = pl.ds(pl.multiple_of(piece * size, size), size)
                before = outs[way][part, :].astype(F32)
                term = terms[way][part, :].astype(F32)
                scratch[way][part, :] = (r.decay[part, :] * before + term).astype(BF)
                carry(way, piece).start()

    def gather(q, landing, slot):
        return rcopy(r.xs, r.xc.at[:, :, landing], r.gat_s.at[q], r.gat_r.at[slot], chan=q)

    each(C, lambda d: gather(lax.rem(ch + d, C), ch, ch).start())
    r.xc[:, :, ch] = r.xs[...]

    spread = head_mask(width, True)
    cumulative = r.cum[...]
    across = cumulative.T
    row = lax.broadcasted_iota(jnp.int32, (length, length), 0)
    col = lax.broadcasted_iota(jnp.int32, (length, length), 1)
    causal = row >= col
    lower = causal.astype(F32)
    into, out_of = r.mix[:, :half], r.mix[:, half:]
    scores = mm(out_of, into, 1, 1)
    act = r.act[...]
    stepped_low = (act * r.step_wide[...]).astype(BF)
    r.stepped[...] = stepped_low

    def head(h):
        cols = slice(h * HDIM, (h + 1) * HDIM)
        gap = cumulative[:, h : h + 1] - across[h : h + 1, :]
        decay = jnp.where(causal, jnp.exp(jnp.where(causal, gap, 0.0)), 0.0)
        weights = (decay * scores).astype(BF)
        grad_h, step_h = r.grad[:, cols], r.stepped[:, cols]
        term = decay * mm(grad_h, step_h, 1, 1)
        r.score_grad[...] = term if h == 0 else r.score_grad[...] + term
        r.z[:, cols] = mm(weights, grad_h, 0, 0)
        r.y[:, cols] = mm(weights, step_h, 1, 0)

    beats = pieces + lag * max(S - 3, 0)
    early = heads // 2
    for h in range(early):
        head(h)
    if beats <= 24:
        for t in range(beats):
            beat(t)
            if early + t < heads:
                head(early + t)
    else:
        for h in range(early, heads):
            head(h)
        lax.fori_loop(0, beats, lambda t, c: (beat(t), c)[1], 0)

    upstream = r.grad[...].astype(F32)
    stepped = r.stepped[...].astype(F32)
    step_wide = r.step_wide[...]
    skip_wide = exact(jnp.broadcast_to(r.vec[2:3, :], (8, LANES)), spread)[0:1, :]
    inner, mixer = r.sum_in[...], r.sum_mix[...]
    inner_gate, mixer_gate = jax.nn.sigmoid(inner), jax.nn.sigmoid(mixer)
    inner_slope = inner_gate * (1.0 + inner * (1.0 - inner_gate))
    mixer_slope = mixer_gate * (1.0 + mixer * (1.0 - mixer_gate))
    to_heads = functools.partial(exact, b=spread, da=1, db=1)
    z = r.z[...]
    r.slope_in[...] = inner_slope
    r.slope_mix[...] = mixer_slope
    r.local[...] = (step_wide * z + skip_wide * upstream) * inner_slope
    local_step = to_heads(r.act[...] * z)
    local_sum = to_heads(upstream * r.y[...] - stepped * z)
    score_grad = r.score_grad[...]
    out_local = mm(score_grad, into, 1, 0)
    into_local = mm(score_grad, out_of, 0, 0)
    faded = (r.fading[...] * stepped).astype(BF)

    for way in (0, 1):

        @pl.when(spots[way] == S - 1)
        def _(way=way):
            for piece in range(pieces):
                carry(way, piece).wait_recv()

    start, end = r.start[...], r.end[...]
    carried = r.grown[...] * mm(out_of, start, 1, 1)
    ending = r.fading[...] * mm(into, end, 1, 1)
    r.pad_in[0:length, :] = r.local[...] + (r.step_wide[...] * ending) * r.slope_in[...]
    r.pad_mix[0:length, :half] = (into_local + mm(faded, end, 1, 0)) * r.slope_mix[:, :half]
    r.pad_mix[0:length, half:] = (out_local + mm(r.pulled[...], start, 1, 0)) * r.slope_mix[:, half:]
    step_grad = local_step + to_heads(r.act[...] * ending)
    tail_term = to_heads(stepped * ending)
    sum_grad = local_sum + to_heads(upstream * carried) - tail_term
    held = jnp.sum(start.astype(F32) * end.astype(F32), axis=1, keepdims=True)
    last = cumulative[length - 1 : length, :]
    overall = jnp.sum(tail_term, axis=0, keepdims=True) + jnp.exp(last) * jnp.sum(
        head_mask(width, False) * held, axis=0, keepdims=True
    )
    decay_grad = exact(lower, sum_grad, 0, 0) + overall
    rate = jnp.exp(r.vec[1:2, :])
    step_grad = (step_grad - rate * decay_grad) * jax.nn.sigmoid(r.raw[...] + r.vec[0:1, :])
    r.steps[...] = step_grad.astype(BF)

    for way in (0, 1):

        @pl.when(spots[way] < S - 1)
        def _(way=way):
            for piece in range(pieces):
                carry(way, piece).wait_send()

    def settle_gather(d):
        q = lax.rem(ch + d, C)
        gather(q, q, q).wait()

    each(C, settle_gather)


def back(r, sizes, place, heads):
    D, S, C = sizes["dp"], sizes["seq"], sizes["chan"]
    mine, me, ch = place
    length, width = r.sum_in.shape
    mixed = r.sum_mix.shape[1]
    model = r.w_in.shape[0]
    rows = length // C
    parts = C
    mixes_low = r.pad_mix[0:length, :].astype(BF)
    r.am[0:length, :] = mixes_low
    r.am[length:, :] = jnp.zeros((PAD, mixed), BF)

    def share_mix(q, landing, slot):
        some = r.am.at[pl.ds(pl.multiple_of(q * rows, rows), rows + PAD)]
        return rcopy(some, r.gm_in.at[landing], r.gm_s.at[q], r.gm_r.at[slot], chan=q)

    def mix_tail(slot):
        return rcopy(
            r.am.at[pl.ds(0, PAD)], r.mt_in.at[slot], r.mt_s.at[0], r.mt_r.at[slot],
            seq=lax.rem(me + S - 1, S), chan=jnp.int32(C - 1),
        )

    each(C, lambda d: share_mix(lax.rem(ch + d, C), ch, ch).start())

    @pl.when(me > 0)
    def _():
        mix_tail(ch).start()

    r.hal_o[:, :width] = r.pad_in[0:8, :]
    r.hal_o[:, width:] = r.pad_mix[0:8, :]

    def halo():
        return rcopy(r.hal_o, r.hal_i, r.hal_sem.at[0], r.hal_sem.at[1], seq=lax.rem(me + S - 1, S))

    @pl.when(me > 0)
    def _():
        halo().start()

    r.pad_in[length:, :] = jnp.zeros((8, width), F32)
    r.pad_mix[length:, :] = jnp.zeros((8, mixed), F32)
    last = length - rows

    def others():
        return [lax.rem(mine + e, D) for e in range(1, D)]

    def part(p, e, k):
        return r.gin.at[k, e, pl.ds(p * rows, rows)]

    def zcopy(p, way, k):
        to = lax.rem(me + (1 if way == "up" else S - 1), S)
        send = (r.u_s if way == "up" else r.d_s).at[p, k]
        return rcopy(part(p, mine, k), part(p, mine, k), send, r.z_r.at[p, k], seq=to)

    def ccopy(p, k, e, to):
        return rcopy(part(p, e, k), part(p, e, k), r.x_s.at[p, to, k], r.c_r.at[p, e, k], dp=to)

    def small_to(e, k, q):
        return rcopy(r.gsm.at[k, e], r.gsm.at[k, e], r.z2_s.at[e, q], r.z2_r.at[e, k], seq=q)

    def csmall(e, to):
        return rcopy(r.gsm.at[me, e], r.gsm.at[me, e], r.x2_s.at[to], r.c2_r.at[e], dp=to)

    def onward(make, k):
        @pl.when(me < S - 1)
        def _():
            make("up", k).start()

        @pl.when(me > 0)
        def _():
            make("down", k).start()

    def own_part(p):
        onward(functools.partial(zcopy, p), me)
        for e in others():
            ccopy(p, me, mine, e).start()

    def forward(d, p):
        for way, k, there, more in (
            ("up", me - d, me >= d, me < S - 1),
            ("down", me + d, me + d < S, me > 0),
        ):

            @pl.when(there)
            def _(way=way, k=k):
                zcopy(p, way, k).wait_recv()

            @pl.when(there & more)
            def _(way=way, k=k):
                zcopy(p, way, k).start()

            @pl.when(there)
            def _(k=k):
                for e in others():
                    ccopy(p, k, mine, e).start()

    def send_small(e):
        each(S, lambda d: small_to(e, me, lax.rem(me + d, S)).start())

    def cross_small():
        for e in others():
            csmall(e, e).wait_recv()
            send_small(e)

    norm = 1.0 / math.sqrt(D * S * length)

    def columns_of(k):
        block = r.xc[k]
        return block.reshape(D * length, block.shape[-1])

    def weight_term(k, first=False):
        for e in others():
            for p in range(parts):
                ccopy(p, k, e, e).wait_recv()
        x = columns_of(k)
        term = norm * mm(x, r.gin[k].reshape(D * length, width), 0, 0)
        r.o_dw[...] = term if first else r.o_dw[...] + term

    def weight_terms(d):
        for k, there in ((me - d, me >= d), (me + d, me + d < S)):

            @pl.when(there)
            def _(k=k):
                weight_term(k)

    for p in range(parts - 1):
        piece = slice(p * rows, (p + 1) * rows)
        r.gin[me, mine, piece, :] = spread_back(r.pad_in, r.conv_in, p * rows, rows)
        own_part(p)
    r.gmp[0:last, :] = spread_back(r.pad_mix, r.conv_mix, 0, last)
    r.gsm[me, mine, rows:, 0:LANES] = r.steps[...].astype(F32).T[0:PAD, :].astype(BF)
    own_rows = pl.ds(pl.multiple_of(ch * rows, rows), rows + PAD)
    r.gm_in[ch] = r.am[own_rows, :]

    @pl.when(me < S - 1)
    def _():
        halo().wait_recv()
        r.pad_in[length:, :] = r.hal_i[:, :width]
        r.pad_mix[length:, :] = r.hal_i[:, width:]

    r.gin[me, mine, last:, :] = spread_back(r.pad_in, r.conv_in, last, rows)
    own_part(parts - 1)
    r.gmp[last:, :] = spread_back(r.pad_mix, r.conv_mix, last, rows)
    each(C, lambda d: share_mix(lax.rem(ch + d, C), ch, lax.rem(ch + d, C)).wait_recv())
    mix = r.gm_in[0].astype(F32)
    for q in range(1, C):
        mix = mix + r.gm_in[q].astype(F32)
    r.gmt[...] = mix

    @pl.when((me < S - 1) & (ch == C - 1))
    def _():
        for q in range(C):
            mix_tail(q).wait_recv()
        tail = r.mt_in[0].astype(F32)
        for q in range(1, C):
            tail = tail + r.mt_in[q].astype(F32)
        r.gmt[rows:, :] = tail

    r.gsm[me, mine, 0:rows, :] = spread_back(r.gmt, r.conv_mix, 0, rows)
    for e in others():
        csmall(mine, e).start()
    send_small(mine)
    cut = model // parts

    def share_p(j, q, landing, slot):
        piece = pl.ds(j * cut, cut)
        return rcopy(
            r.p_o.at[q, :, piece], r.p_i.at[landing, :, piece], r.p_s.at[j, q], r.p_r.at[j, slot], chan=q
        )

    grads = r.gin[me, mine]
    mixes = r.gmp[...]
    steps = r.steps[:, 0:PAD]

    def back_project(j):
        piece = slice(j * cut, (j + 1) * cut)
        out = mm(grads, r.w_in[piece, :], 1, 1) + mm(mixes, r.w_mix[piece, :], 1, 1)
        out = out + mm(steps, r.wst[0:PAD, piece], 1, 0)
        r.p_o[:, :, piece] = out.astype(BF).reshape(C, rows, cut)
        each(C, lambda d: share_p(j, lax.rem(ch + d, C), ch, ch).start())

    for j in range(parts):
        if j == parts - 1:
            cross_small()
        back_project(j)
        forward(1, j)
    weight_term(me, True)

    def hop(d):
        for p in range(parts):
            forward(d, p)

    hop(2)
    for e in [mine] + others():
        each(S, lambda d, e=e: small_to(e, lax.rem(me + d, S), lax.rem(me + d, S)).wait_recv())

    mixer_columns = r.xc[:, :, ch].reshape(S * D * rows, r.xc.shape[-1])
    mixer_grads = r.gsm[:, :, 0:rows, :].reshape(S * D * rows, mixed)
    mixer_term = norm * mm(mixer_columns, mixer_grads, 0, 0)
    band = mixer_term.shape[0] // C
    for q in range(C):
        r.m_o[q] = mixer_term[q * band : (q + 1) * band, :].astype(BF)

    def share_m(q, landing, slot):
        return rcopy(r.m_o.at[q], r.m_i.at[landing], r.m_s.at[q], r.m_r.at[slot], chan=q)

    each(C, lambda d: share_m(lax.rem(ch + d, C), ch, ch).start())
    step_total = None
    for k in range(S) if S <= 12 else ():
        for e in range(D):
            x = r.xc[k, e].reshape(length, r.xc.shape[-1])
            term = mm(r.gsm[k, e, rows:, 0:LANES], x, 1, 0)
            step_total = term if step_total is None else step_total + term
    if step_total is None:

        def one(k, carry):
            for e in range(D):
                x = r.xc[k, e].reshape(length, r.xc.shape[-1])
                carry = carry + mm(r.gsm[k, e, rows:, 0:LANES], x, 1, 0)
            return carry

        step_total = lax.fori_loop(0, S, one, jnp.zeros((PAD, r.xc.shape[-1]), F32))
    r.o_dws[...] = (norm * step_total)[:heads, :]

    if S <= 12:
        for d in range(3, S):
            hop(d)
    else:
        lax.fori_loop(3, S, lambda d, c: (hop(d), c)[1], 0)
    r.p_i[ch] = r.p_o[ch]
    r.m_i[ch] = r.m_o[ch]
    for j in range(parts):
        each(C, lambda d, j=j: share_p(j, lax.rem(ch + d, C), ch, lax.rem(ch + d, C)).wait_recv())
    each(S, weight_terms)
    each(C, lambda d: share_m(lax.rem(ch + d, C), ch, lax.rem(ch + d, C)).wait_recv())

    @pl.when(me > 0)
    def _():
        halo().wait_send()
        mix_tail(ch).wait_send()

    def settle_chan(d):
        q = lax.rem(ch + d, C)
        share_mix(q, ch, ch).wait_send()
        share_m(q, ch, ch).wait_send()
        for j in range(parts):
            share_p(j, q, ch, ch).wait_send()

    each(C, settle_chan)

    def settle_line(k):
        for e in others():
            for p in range(parts):
                ccopy(p, k, mine, e).wait_send()
        for way, sent in (("up", (k <= me) & (me < S - 1)), ("down", (k >= me) & (me > 0))):

            @pl.when(sent)
            def _(way=way):
                for p in range(parts):
                    zcopy(p, way, k).wait_send()

    settle_line(0)
    each(S, settle_line)
    for e in others():
        csmall(mine, e).wait_send()
    for e in [mine] + others():
        each(S, lambda d, e=e: small_to(e, me, lax.rem(me + d, S)).wait_send())


def finish_kernel(parts, dw, mixes, dws, o_ig, o_dw, o_dwm, o_dws, ig, dwm, sems):
    copies = [
        pltpu.make_async_copy(a, b, sems.at[i])
        for i, (a, b) in enumerate(((dw, o_dw), (dws, o_dws), (ig, o_ig), (dwm, o_dwm)))
    ]
    copies[0].start()
    copies[1].start()
    total = parts[0].astype(F32)
    for q in range(1, parts.shape[0]):
        total = total + parts[q].astype(F32)
    ig[...] = total.astype(BF)
    copies[2].start()
    total = mixes[0].astype(F32)
    for q in range(1, mixes.shape[0]):
        total = total + mixes[q].astype(F32)
    dwm[...] = total
    copies[3].start()
    for copy in copies:
        copy.wait()


def body(
    sizes,
    layer_input,
    inner_weight,
    mixer_weight,
    step_weight,
    conv_inner,
    conv_mixer,
    step_bias,
    decay_log,
    skip_gain,
    output_grad,
):
    own = layer_input[0]
    rows, model = own.shape
    chans, seqs, dps = sizes["chan"], sizes["seq"], sizes["dp"]
    groups = dps * seqs
    length = rows * chans
    width = inner_weight.shape[1]
    mixed = mixer_weight.shape[1]
    heads = step_bias.shape[0]
    cols = model // groups
    state_size = mixed // 2
    assert width % PIECES == 0 and chans % 2 == 0 and seqs > 2
    assert length == LANES and heads + conv_inner.shape[0] - 1 <= PAD
    upstream = output_grad[0]
    step_rows = step_weight.T
    bias, rates, skips = (v.reshape(1, heads) for v in (step_bias, decay_log, skip_gain))
    dma = pltpu.SemaphoreType.DMA
    vmem = pl.BlockSpec(memory_space=pltpu.VMEM)
    hbm = pl.BlockSpec(memory_space=pltpu.HBM)
    small = rows + PAD
    band = cols // chans

    def low(*shape):
        return pltpu.VMEM(shape, BF)

    def full(*shape):
        return pltpu.VMEM(shape, F32)

    inputs = dict(
        own=own, w_in=inner_weight, w_mix=mixer_weight, w_step=step_rows, conv_in=conv_inner,
        conv_mix=conv_mixer, bias=bias, log=rates, skip=skips, grad=upstream,
    )
    outputs = dict(
        p_i=jax.ShapeDtypeStruct((chans, rows, model), BF),
        o_dw=jax.ShapeDtypeStruct((cols, width), F32),
        m_i=jax.ShapeDtypeStruct((chans, band, mixed), BF),
        o_dws=jax.ShapeDtypeStruct((heads, cols), F32),
    )
    scratch = {key: pltpu.VMEM(v.shape, v.dtype) for key, v in inputs.items()}
    scratch |= dict(
        wst=low(LANES, model), xg=low(length, model),
        blocks=low(dps, seqs, rows, cols), mid=low(dps, seqs, rows, cols),
        xs=low(seqs, dps, rows, cols), xc=low(seqs, dps, chans, rows, cols),
        wide_in=full(PAD + length, width), wide_mix=full(PAD + length, mixed),
        fh_o=low(PAD, width + mixed), fh_i=low(PAD, width + mixed), vec=full(8, LANES),
        sum_in=full(length, width), sum_mix=full(length, mixed), raw=full(length, LANES),
        cum=full(length, LANES), step_wide=full(length, width), fading=full(length, width),
        grown=full(length, width), pulled=low(length, width), decay=full(width, state_size),
        mix=low(length, mixed), act=full(length, width), stepped=low(length, width),
        state_term=low(width, state_size), back_term=low(width, state_size),
        start=low(width, state_size), end=low(width, state_size),
        scr0=low(width, state_size), scr1=low(width, state_size),
        z=full(length, width), y=full(length, width), score_grad=full(length, length),
        local=full(length, width), slope_in=full(length, width), slope_mix=full(length, mixed),
        steps=low(length, LANES),
        pad_in=full(length + 8, width), pad_mix=full(length + 8, mixed),
        gin=low(seqs, dps, length, width), gsm=low(seqs, dps, small, mixed),
        hal_o=full(8, width + mixed), hal_i=full(8, width + mixed),
        gmp=low(length, mixed), gm_in=low(chans, small, mixed), gmt=full(small, mixed),
        am=low(length + PAD, mixed), mt_in=low(chans, PAD, mixed),
        p_o=low(chans, rows, model), m_o=low(chans, band, mixed),
        load_sem=dma((len(LOADED),)), fh_sem=dma((2,)), hal_sem=dma((2,)),
        near_s=dma((chans,)), near_r=dma((chans,)),
        far_s=dma((chans // 2, chans)), far_r=dma((chans // 2, chans)),
        relay_s=dma((chans // 2, chans)), relay_r=dma((chans // 2, chans)),
        swap_s=dma((dps,)), swap_r=dma((dps,)), cross_s=dma((seqs,)), cross_r=dma((seqs,)),
        gat_s=dma((chans,)), gat_r=dma((chans,)),
        chain_s=dma((2, PIECES)), chain_r=dma((2, PIECES)),
        z_r=dma((chans, seqs)), c_r=dma((chans, dps, seqs)),
        u_s=dma((chans, seqs)), d_s=dma((chans, seqs)), x_s=dma((chans, dps, seqs)),
        c2_r=dma((dps,)), z2_r=dma((dps, seqs)), x2_s=dma((dps,)),
        z2_s=dma((dps, seqs)), mt_s=dma((1,)), mt_r=dma((chans,)),
        gm_s=dma((chans,)), gm_r=dma((chans,)),
        p_s=dma((chans, chans)), p_r=dma((chans, chans)), m_s=dma((chans,)), m_r=dma((chans,)),
    )
    names = [key + "_h" for key in inputs] + list(outputs) + list(scratch)
    parts, inner_grad, mix_parts, step_grad = pl.pallas_call(
        functools.partial(layer_kernel, names, sizes, heads),
        out_shape=tuple(outputs.values()),
        in_specs=[hbm] * len(inputs),
        out_specs=(vmem,) * len(outputs),
        scratch_shapes=list(scratch.values()),
        compiler_params=pltpu.CompilerParams(
            collective_id=0, has_side_effects=True, vmem_limit_bytes=LIMIT
        ),
        name="layer",
    )(*(pltpu.with_memory_space_constraint(v, pltpu.HBM) for v in inputs.values()))
    input_grad, inner_grad, mixer_grad, step_grad = pl.pallas_call(
        finish_kernel,
        out_shape=(
            jax.ShapeDtypeStruct((rows, model), BF),
            jax.ShapeDtypeStruct((cols, width), F32),
            jax.ShapeDtypeStruct((band, mixed), F32),
            jax.ShapeDtypeStruct((heads, cols), F32),
        ),
        in_specs=[vmem] * 4,
        out_specs=(pl.BlockSpec(memory_space=pl.ANY),) * 4,
        scratch_shapes=[
            pltpu.VMEM((rows, model), BF),
            pltpu.VMEM((band, mixed), F32),
            dma((4,)),
        ],
        compiler_params=pltpu.CompilerParams(vmem_limit_bytes=LIMIT),
        name="finish",
    )(parts, inner_grad, mix_parts, step_grad)
    return input_grad[None], inner_grad, mixer_grad, step_grad.T


def solution(mesh):
    sizes = dict(mesh.shape)
    in_specs = (
        P("dp", ("seq", "chan"), None),
        P(None, "chan"),
        P(),
        P(None, "chan"),
        P(None, "chan"),
        P(),
        P("chan"),
        P("chan"),
        P("chan"),
        P("dp", "seq", "chan"),
    )
    out_specs = (
        P("dp", ("seq", "chan"), None),
        P(("dp", "seq"), "chan"),
        P(("dp", "seq", "chan"), None),
        P(("dp", "seq"), "chan"),
    )
    return jax.shard_map(
        functools.partial(body, sizes),
        mesh=mesh,
        in_specs=in_specs,
        out_specs=out_specs,
        check_vma=False,
    )
```

```python
import functools
import math
import types

import jax
import jax.numpy as jnp
from jax import lax
from jax.experimental import pallas as pl
from jax.experimental.pallas import tpu as pltpu
from jax.sharding import PartitionSpec as P

MESH = pl.DeviceIdType.MESH
HDIM = 64
PAD = 16
LANES = 128
LIMIT = 48 * 2**20
BF = jnp.bfloat16
F32 = jnp.float32
HIGH = lax.Precision.HIGHEST
PIECES = 10
LOADED = (
    "own", "w_in", "w_mix", "w_step", "conv_in", "conv_mix", "bias", "log", "skip", "grad",
)


def each(n, step):
    if n <= 12:
        for d in range(1, n):
            step(d)
    else:

        def one(d, carry):
            step(d)
            return carry

        lax.fori_loop(1, n, one, 0)


def signal_to(barrier, where):
    pl.semaphore_signal(barrier, inc=1, device_id=where, device_id_type=MESH)


def mm(a, b, da, db):
    return lax.dot_general(
        a.astype(BF), b.astype(BF), (((da,), (db,)), ((), ())), preferred_element_type=F32
    )


def exact(a, b, da=1, db=0):
    return lax.dot_general(
        a, b, (((da,), (db,)), ((), ())), precision=HIGH, preferred_element_type=F32
    )


def softplus(v):
    return jnp.maximum(v, 0.0) + jnp.log1p(jnp.exp(-jnp.abs(v)))


def head_mask(width, heads_first):
    shape = (LANES, width) if heads_first else (width, LANES)
    head = lax.broadcasted_iota(jnp.int32, shape, 0 if heads_first else 1)
    column = lax.broadcasted_iota(jnp.int32, shape, 1 if heads_first else 0)
    return (column // HDIM == head).astype(F32)


def decays(raw, bias, decay_log):
    length = raw.shape[0]
    step = softplus(raw + bias)
    rate = jnp.exp(decay_log)
    row = lax.broadcasted_iota(jnp.int32, (length, length), 0)
    col = lax.broadcasted_iota(jnp.int32, (length, length), 1)
    lower = (row >= col).astype(F32)
    cumulative = exact(lower, -step * rate)
    return step, rate, cumulative, row, col, lower


def rcopy(src, dst, send, recv, **where):
    return pltpu.make_async_remote_copy(
        src_ref=src, dst_ref=dst, send_sem=send, recv_sem=recv, device_id=where, device_id_type=MESH
    )


def greet_all(barrier, axis, n):
    me = lax.axis_index(axis)
    each(n, lambda d: signal_to(barrier, {axis: lax.rem(me + d, n)}))
    return n - 1


def convolved(wide, kernel, first, count):
    taps = kernel.shape[0]
    first = first + PAD - (taps - 1)
    total = kernel[0:1, :] * wide[pl.ds(first, count), :]
    for k in range(1, taps):
        total = total + kernel[k : k + 1, :] * wide[pl.ds(first + k, count), :]
    return total


def spread_back(pad, kernel, first, count, cols=slice(None)):
    taps = kernel.shape[0]
    total = None
    for k in range(taps):
        term = kernel[k : k + 1, cols] * pad[pl.ds(first + taps - 1 - k, count), cols]
        total = term if total is None else total + term
    return total.astype(BF)


def layer_kernel(names, sizes, heads, *refs):
    r = types.SimpleNamespace(**dict(zip(names, refs, strict=True)))
    place = (lax.axis_index("dp"), lax.axis_index("seq"), lax.axis_index("chan"))
    D, S, C = sizes["dp"], sizes["seq"], sizes["chan"]
    barrier = pltpu.get_barrier_semaphore()
    total = greet_all(barrier, "dp", D) + greet_all(barrier, "seq", S) + greet_all(barrier, "chan", C)
    after = lax.rem(place[1] + 1, S)

    @pl.when(place[2] == C - 1)
    def _():
        for c in range(C):
            signal_to(barrier, {"seq": after, "chan": jnp.int32(c)})

    total += 1 + (D - 1) * (S - 1)
    for e in range(1, D):
        far = lax.rem(place[0] + e, D)
        each(S, lambda d, far=far: signal_to(barrier, {"dp": far, "seq": lax.rem(place[1] + d, S)}))
    loads = {
        key: pltpu.make_async_copy(getattr(r, key + "_h"), getattr(r, key), r.load_sem.at[i])
        for i, key in enumerate(LOADED)
    }
    for copy in loads.values():
        copy.start()
    crossed = front(r, sizes, place, heads, loads, barrier, total)
    rear(r, sizes, place, heads, crossed)


def front(r, sizes, place, heads, loads, barrier, total):
    D, S, C = sizes["dp"], sizes["seq"], sizes["chan"]
    mine, me, ch = place
    rows, model = r.own.shape
    length, width = r.sum_in.shape
    mixed = r.sum_mix.shape[1]
    cols = model // (D * S)
    half = mixed // 2
    pieces = C
    cut = model // pieces
    sides = C // 2
    side, low = lax.div(ch, 2), lax.rem(ch, 2)
    partner = ch + 1 - 2 * low

    def block(c, p):
        return r.xg.at[pl.ds(pl.multiple_of(c * rows, rows), rows), pl.ds(p * cut, cut)]

    def mine_at(p):
        return r.own.at[:, pl.ds(p * cut, cut)]

    def near(c, p):
        return rcopy(mine_at(p), block(c, p), r.near_s.at[p], r.near_r.at[p], chan=partner)

    def far(to, c, slot, p):
        return rcopy(
            mine_at(p), block(c, p), r.far_s.at[to, p], r.far_r.at[slot, p], chan=2 * to + low
        )

    def relay(source, lane, p):
        c = 2 * source + lane
        here = block(c, p)
        return rcopy(here, here, r.relay_s.at[source, p], r.relay_r.at[source, p], chan=partner)

    def swap(q, landing, slot):
        return rcopy(r.blocks.at[q], r.mid.at[landing], r.swap_s.at[q], r.swap_r.at[slot], dp=q)

    def cross(q, landing, slot):
        return rcopy(r.mid.at[:, q], r.xs.at[landing], r.cross_s.at[q], r.cross_r.at[slot], seq=q)

    loads["own"].wait()
    pl.semaphore_wait(barrier, total)
    for p in range(pieces):
        for d in range(1, sides):
            far(lax.rem(side + d, sides), ch, side, p).start()
        near(ch, p).start()
    for d in range(D):
        for k in range(S):
            at = (d * S + k) * cols
            r.blocks[d, k] = r.own[:, at : at + cols]
    each(D, lambda d: swap(lax.rem(mine + d, D), mine, mine).start())
    r.mid[mine] = r.blocks[mine]
    r.xg[pl.ds(pl.multiple_of(ch * rows, rows), rows), :] = r.own[...]
    r.wst[...] = jnp.zeros(r.wst.shape, BF)
    r.vec[...] = jnp.zeros(r.vec.shape, F32)
    for key in LOADED[1:]:
        loads[key].wait()
    r.wst[0:heads, :] = r.w_step[...]
    for i, ref in enumerate((r.bias, r.log, r.skip)):
        r.vec[i : i + 1, 0:heads] = ref[...]

    def pass_on(p):
        for d in range(1, sides):
            source = lax.rem(side + d, sides)
            far(source, ch, source, p).wait_recv()
            relay(source, low, p).start()

    def project(p):
        near(partner, p).wait_recv()
        for d in range(1, sides):
            source = lax.rem(side + d, sides)
            relay(source, 1 - low, p).wait_recv()
        piece = slice(p * cut, (p + 1) * cut)
        x = r.xg[:, piece]
        inner = mm(x, r.w_in[piece, :], 1, 0)
        mixer = mm(x, r.w_mix[piece, :], 1, 0)
        raw = mm(x, r.wst[:, piece], 1, 1)
        if p == 0:
            r.wide_in[PAD:, :], r.wide_mix[PAD:, :], r.raw[...] = inner, mixer, raw
        else:
            r.wide_in[PAD:, :] = r.wide_in[PAD:, :] + inner
            r.wide_mix[PAD:, :] = r.wide_mix[PAD:, :] + mixer
            r.raw[...] = r.raw[...] + raw

    pass_on(0)
    for p in range(pieces):
        if p + 1 < pieces:
            pass_on(p + 1)
        project(p)
        if p == 0:
            each(D, lambda d: swap(lax.rem(mine + d, D), mine, lax.rem(mine + d, D)).wait_recv())
            each(S, lambda d: cross(lax.rem(me + d, S), me, me).start())
            r.xs[me] = r.mid[:, me]
    inner_low = r.wide_in[PAD:, :].astype(BF)
    mixer_low = r.wide_mix[PAD:, :].astype(BF)
    r.fh_o[:, :width] = inner_low[length - PAD :, :]
    r.fh_o[:, width:] = mixer_low[length - PAD :, :]

    def halo():
        return rcopy(r.fh_o, r.fh_i, r.fh_sem.at[0], r.fh_sem.at[1], seq=lax.rem(me + 1, S))

    @pl.when(me < S - 1)
    def _():
        halo().start()

    r.wide_in[PAD:, :] = inner_low.astype(F32)
    r.wide_mix[PAD:, :] = mixer_low.astype(F32)
    r.wide_in[0:PAD, :] = jnp.zeros((PAD, width), F32)
    r.wide_mix[0:PAD, :] = jnp.zeros((PAD, mixed), F32)
    r.sum_in[PAD:, :] = convolved(r.wide_in, r.conv_in, PAD, length - PAD)
    r.sum_mix[PAD:, :] = convolved(r.wide_mix, r.conv_mix, PAD, length - PAD)
    step, rate, cumulative, row, col, lower = decays(r.raw[...], r.vec[0:1, :], r.vec[1:2, :])
    last = cumulative[length - 1 : length, :]
    spread = head_mask(width, True)
    r.cum[...] = cumulative
    step_wide = exact(step, spread)
    fading = exact(jnp.exp(last - cumulative), spread)
    grown = exact(jnp.exp(cumulative), spread)
    r.step_wide[...] = step_wide
    r.fading[...] = fading
    r.grown[...] = grown
    pulled = (grown * r.grad[...].astype(F32)).astype(BF)
    r.pulled[...] = pulled
    row_decay = jnp.sum(head_mask(width, False) * jnp.exp(last), axis=1, keepdims=True)
    r.decay[...] = jnp.broadcast_to(row_decay, r.decay.shape)

    @pl.when(me > 0)
    def _():
        halo().wait_recv()
        r.wide_in[0:PAD, :] = r.fh_i[:, :width].astype(F32)
        r.wide_mix[0:PAD, :] = r.fh_i[:, width:].astype(F32)

    r.sum_in[0:PAD, :] = convolved(r.wide_in, r.conv_in, 0, PAD)
    r.sum_mix[0:PAD, :] = convolved(r.wide_mix, r.conv_mix, 0, PAD)
    mixer = r.sum_mix[...]
    mix = mixer * jax.nn.sigmoid(mixer)
    r.mix[...] = mix.astype(BF)
    r.back_term[...] = mm(pulled, mix[:, half:], 0, 0).astype(BF)
    inner = r.sum_in[...]
    act = inner * jax.nn.sigmoid(inner)
    r.act[...] = act
    r.state_term[...] = mm(act * (fading * step_wide), mix[:, :half], 0, 0).astype(BF)

    @pl.when(me < S - 1)
    def _():
        halo().wait_send()

    for p in range(pieces):
        near(ch, p).wait_send()
        for d in range(1, sides):
            source = lax.rem(side + d, sides)
            far(source, ch, source, p).wait_send()
            relay(source, low, p).wait_send()
    each(D, lambda d: swap(lax.rem(mine + d, D), mine, mine).wait_send())

    def settle(d):
        q = lax.rem(me + d, S)
        cross(q, me, q).wait()

    return lambda: each(S, settle)


def rear(r, sizes, place, heads, crossed):
    D, S, C = sizes["dp"], sizes["seq"], sizes["chan"]
    mine, me, ch = place
    length, width = r.sum_in.shape
    mixed = r.sum_mix.shape[1]
    half = mixed // 2
    model = r.w_in.shape[0]
    rows = length // C
    pieces, lag = PIECES, PIECES // 2
    size = width // pieces
    strips = width // LANES
    per = pieces // strips
    parts = C
    cut = model // parts
    terms, outs, scratch = (r.state_term, r.back_term), (r.start, r.end), (r.scr0, r.scr1)
    spots = (me, S - 1 - me)
    above, below = lax.rem(me + 1, S), lax.rem(me + S - 1, S)
    others = [lax.rem(mine + e, D) for e in range(1, D)]

    def carry(way, piece, first=False):
        part = pl.ds(pl.multiple_of(piece * size, size), size)
        source = terms[way] if first else scratch[way]
        sems = r.chain_s.at[way, piece], r.chain_r.at[way, piece]
        return rcopy(source.at[part], outs[way].at[part], *sems, seq=above if way == 0 else below)

    for way in (1, 0):

        @pl.when(spots[way] == 0)
        def _(way=way):
            for piece in range(pieces):
                carry(way, piece, True).start()
            outs[way][...] = jnp.zeros(outs[way].shape, BF)

    def beat(t):
        for way in (1, 0):
            spot = spots[way]
            piece = t - lag * (spot - 1)

            @pl.when((piece >= 0) & (piece < pieces) & (spot > 0) & (spot < S - 1))
            def _(way=way, piece=piece):
                carry(way, piece).wait_recv()
                part = pl.ds(pl.multiple_of(piece * size, size), size)
                before = outs[way][part, :].astype(F32)
                term = terms[way][part, :].astype(F32)
                scratch[way][part, :] = (r.decay[part, :] * before + term).astype(BF)
                carry(way, piece).start()

    def gather(q, landing, slot):
        return rcopy(r.xs, r.xc.at[:, :, landing], r.gat_s.at[q], r.gat_r.at[slot], chan=q)

    spread = head_mask(width, True)
    cumulative = r.cum[...]
    across = cumulative.T
    row = lax.broadcasted_iota(jnp.int32, (length, length), 0)
    col = lax.broadcasted_iota(jnp.int32, (length, length), 1)
    causal = row >= col
    lower = causal.astype(F32)
    into, out_of = r.mix[:, :half], r.mix[:, half:]
    scores = mm(out_of, into, 1, 1)
    r.stepped[...] = (r.act[...] * r.step_wide[...]).astype(BF)
    inner = r.sum_in[...]
    gate = jax.nn.sigmoid(inner)
    r.slope_in[...] = gate * (1.0 + inner * (1.0 - gate))
    skip_wide = exact(jnp.broadcast_to(r.vec[2:3, :], (8, LANES)), spread)
    r.skips[...] = skip_wide
    r.pad_in[length:, :] = jnp.zeros((8, width), F32)
    r.pad_mix[length:, :] = jnp.zeros((8, mixed), F32)

    def head(h):
        cols = slice(h * HDIM, (h + 1) * HDIM)
        gap = cumulative[:, h : h + 1] - across[h : h + 1, :]
        decay = jnp.where(causal, jnp.exp(jnp.where(causal, gap, 0.0)), 0.0)
        weights = (decay * scores).astype(BF)
        grad_h, step_h = r.grad[:, cols], r.stepped[:, cols]
        term = decay * mm(grad_h, step_h, 1, 1)
        r.score_grad[...] = term if h == 0 else r.score_grad[...] + term
        r.z[:, cols] = mm(weights, grad_h, 0, 0)
        r.y[:, cols] = mm(weights, step_h, 1, 0)

    def strip(j):
        return slice(j * LANES, (j + 1) * LANES)

    def halo(j):
        return rcopy(r.hal_o.at[j], r.hal_i.at[j], r.hal_s.at[j], r.hal_r.at[j], seq=below)

    def strip_sum(j):
        cols = strip(j)

        @pl.when(spots[1] == S - 1)
        def _():
            for piece in range(j * per, (j + 1) * per):
                carry(1, piece).wait_recv()

        ending = r.fading[:, cols] * mm(into, r.end[cols, :], 1, 1)
        r.ending[:, cols] = ending
        direct = r.skips[0:1, cols] * r.grad[:, cols].astype(F32)
        total = (r.step_wide[:, cols] * (r.z[:, cols] + ending) + direct) * r.slope_in[:, cols]
        r.pad_in[0:length, cols] = total
        r.hal_o[j] = total[0:8, :]

        @pl.when(me > 0)
        def _():
            halo(j).start()

    def part(p, e, k):
        return r.gin.at[k, e, :, pl.ds(p * LANES, LANES)]

    def zcopy(p, way, k):
        send = (r.u_s if way == "up" else r.d_s).at[p, k]
        here = part(p, mine, k)
        return rcopy(here, here, send, r.z_r.at[p, k], seq=above if way == "up" else below)

    def ccopy(p, k, e, to):
        return rcopy(part(p, e, k), part(p, e, k), r.x_s.at[p, to, k], r.c_r.at[p, e, k], dp=to)

    def strip_out(j):
        cols = strip(j)

        @pl.when(me < S - 1)
        def _():
            halo(j).wait_recv()
            r.pad_in[length:, cols] = r.hal_i[j]

        r.gin[me, mine, :, cols] = spread_back(r.pad_in, r.conv_in, 0, length, cols)
        for e in others:
            ccopy(j, me, mine, e).start()

    def strip_along(j):
        @pl.when(me < S - 1)
        def _():
            zcopy(j, "up", me).start()

        @pl.when(me > 0)
        def _():
            zcopy(j, "down", me).start()

    beats = pieces + lag * max(S - 3, 0)
    early = heads // 2
    for h in range(early):
        head(h)
    near = spots[1] <= 1
    crossed()
    each(C, lambda d: gather(lax.rem(ch + d, C), ch, ch).start())
    r.xc[:, :, ch] = r.xs[...]
    if beats <= 24:
        sums = {per * j + per - 1: j for j in range(strips)}
        late = {lag + t: j for t, j in sums.items()}
        for t in range(max(beats, heads - early)):
            beat(t)
            if early + t < heads:
                head(early + t)
            if t in sums:
                pl.when(near)(functools.partial(strip_sum, sums[t]))
            if t in late:
                pl.when(near)(functools.partial(strip_out, late[t]))
                pl.when(spots[1] == 2)(functools.partial(strip_sum, late[t]))
        for j in range(strips):
            pl.when(spots[1] > 2)(functools.partial(strip_sum, j))
            pl.when(spots[1] > 1)(functools.partial(strip_out, j))
            strip_along(j)
    else:
        for h in range(early, heads):
            head(h)
        lax.fori_loop(0, beats, lambda t, c: (beat(t), c)[1], 0)
        for j in range(strips):
            strip_sum(j)
        for j in range(strips):
            strip_out(j)
            strip_along(j)

    @pl.when(spots[0] == S - 1)
    def _():
        for piece in range(pieces):
            carry(0, piece).wait_recv()

    start, end = r.start[...], r.end[...]
    score_grad = r.score_grad[...]
    mixer = r.sum_mix[...]
    gate = jax.nn.sigmoid(mixer)
    mixer_slope = gate * (1.0 + mixer * (1.0 - gate))
    faded = (r.fading[...] * r.stepped[...].astype(F32)).astype(BF)
    into_grad = mm(score_grad, out_of, 0, 0) + mm(faded, end, 1, 0)
    out_grad = mm(score_grad, into, 1, 0) + mm(r.pulled[...], start, 1, 0)
    r.pad_mix[0:length, :half] = into_grad * mixer_slope[:, :half]
    r.pad_mix[0:length, half:] = out_grad * mixer_slope[:, half:]
    r.am[0:length, :] = r.pad_mix[0:length, :].astype(BF)
    r.am[length:, :] = jnp.zeros((PAD, mixed), BF)
    r.halm_o[...] = r.pad_mix[0:8, :]

    def share_mix(q, landing, slot):
        some = r.am.at[pl.ds(pl.multiple_of(q * rows, rows), rows + PAD)]
        return rcopy(some, r.gm_in.at[landing], r.gm_s.at[q], r.gm_r.at[slot], chan=q)

    def mix_tail(slot):
        return rcopy(
            r.am.at[pl.ds(0, PAD)], r.mt_in.at[slot], r.mt_s.at[0], r.mt_r.at[slot],
            seq=below, chan=jnp.int32(C - 1),
        )

    def mix_halo():
        return rcopy(r.halm_o, r.halm_i, r.halm_s.at[0], r.halm_s.at[1], seq=below)

    each(C, lambda d: share_mix(lax.rem(ch + d, C), ch, ch).start())

    @pl.when(me > 0)
    def _():
        mix_tail(ch).start()
        mix_halo().start()

    r.gm_in[ch] = r.am[pl.ds(pl.multiple_of(ch * rows, rows), rows + PAD), :]
    r.gmp[...] = spread_back(r.pad_mix, r.conv_mix, 0, length)

    upstream = r.grad[...].astype(F32)
    stepped = r.stepped[...].astype(F32)
    ending = r.ending[...]
    carried = r.grown[...] * mm(out_of, start, 1, 1)
    to_heads = functools.partial(exact, b=spread, da=1, db=1)
    z = r.z[...]
    step_grad = to_heads(r.act[...] * (z + ending))
    tail_term = to_heads(stepped * ending)
    sum_grad = to_heads(upstream * (r.y[...] + carried) - stepped * z) - tail_term
    held = jnp.sum(start.astype(F32) * end.astype(F32), axis=1, keepdims=True)
    last = cumulative[length - 1 : length, :]
    overall = jnp.sum(tail_term, axis=0, keepdims=True) + jnp.exp(last) * jnp.sum(
        head_mask(width, False) * held, axis=0, keepdims=True
    )
    decay_grad = exact(lower, sum_grad, 0, 0) + overall
    rate = jnp.exp(r.vec[1:2, :])
    step_grad = (step_grad - rate * decay_grad) * jax.nn.sigmoid(r.raw[...] + r.vec[0:1, :])
    steps = step_grad.astype(BF)
    r.gsm[me, mine, rows:, 0:LANES] = step_grad.T[0:PAD, :].astype(BF)
    steps = steps[:, 0:PAD]

    each(C, lambda d: share_mix(lax.rem(ch + d, C), ch, lax.rem(ch + d, C)).wait_recv())
    mix = r.gm_in[0].astype(F32)
    for q in range(1, C):
        mix = mix + r.gm_in[q].astype(F32)
    r.gmt[...] = mix

    @pl.when((me < S - 1) & (ch == C - 1))
    def _():
        for q in range(C):
            mix_tail(q).wait_recv()
        tail = r.mt_in[0].astype(F32)
        for q in range(1, C):
            tail = tail + r.mt_in[q].astype(F32)
        r.gmt[rows:, :] = tail

    r.gsm[me, mine, 0:rows, :] = spread_back(r.gmt, r.conv_mix, 0, rows)

    def small_to(e, k, to, q):
        here = r.gsm.at[k, e]
        return rcopy(here, here, r.z2_s.at[to, q], r.z2_r.at[e, k], dp=to, seq=q)

    def small_all(do):
        each(S, lambda d: do(mine, lax.rem(me + d, S)))
        for e in others:
            do(e, me)
            each(S, lambda d, e=e: do(e, lax.rem(me + d, S)))

    small_all(lambda e, q: small_to(mine, me, e, q).start())

    def forward(p, way, d):
        k = me - d if way == "up" else me + d
        there = (k >= 0) if way == "up" else (k < S)
        more = (me < S - 1) if way == "up" else (me > 0)

        @pl.when(there)
        def _():
            zcopy(p, way, k).wait_recv()

        @pl.when(there & more)
        def _():
            zcopy(p, way, k).start()

        @pl.when(there)
        def _():
            for e in others:
                ccopy(p, k, mine, e).start()

    def hop(way, d):
        for p in range(strips):
            forward(p, way, d)

    def share_p(j, q, landing, slot):
        piece = pl.ds(j * cut, cut)
        return rcopy(
            r.p_o.at[q, :, piece], r.p_i.at[landing, :, piece], r.p_s.at[j, q], r.p_r.at[j, slot], chan=q
        )

    grads = r.gin[me, mine]
    mixes = r.gmp[...]

    def send_p(j, final):
        def one(d):
            q = lax.rem(ch + d, C)

            @pl.when((q == C - 1) if final else (q < C - 1))
            def _():
                share_p(j, q, ch, ch).start()

        each(C, one)

    for j in range(parts):
        piece = slice(j * cut, (j + 1) * cut)
        out = mm(grads, r.w_in[piece, :], 1, 1) + mm(mixes, r.w_mix[piece, :], 1, 1)
        out = out + mm(steps, r.wst[0:PAD, piece], 1, 0)
        r.p_o[:, :, piece] = out.astype(BF).reshape(C, rows, cut)
        r.p_last[:, piece] = out[length - PAD :, :]
        send_p(j, False)
        forward(j, "down", 1)
    for p in range(parts, strips):
        forward(p, "down", 1)

    @pl.when(me < S - 1)
    def _():
        mix_halo().wait_recv()
        r.pad_mix[length:, :] = r.halm_i[...]
        final = spread_back(r.pad_mix, r.conv_mix, length - PAD, PAD)
        change = final.astype(F32) - r.gmp[length - PAD :, :].astype(F32)
        fixed = r.p_last[...] + mm(change, r.w_mix[...], 1, 1)
        r.p_o[C - 1, rows - PAD :, :] = fixed.astype(BF)

    for j in range(parts):
        send_p(j, True)
    hop("up", 1)
    hop("down", 2)
    hop("up", 2)
    small_all(lambda e, q: small_to(e, q, e, q).wait_recv())

    norm = 1.0 / math.sqrt(D * S * length)
    columns = r.xc.shape[-1]

    def settle_gather(d):
        q = lax.rem(ch + d, C)
        gather(q, q, q).wait()

    each(C, settle_gather)
    mixer_columns = r.xc[:, :, ch].reshape(S * D * rows, columns)
    mixer_grads = r.gsm[:, :, 0:rows, :].reshape(S * D * rows, mixed)
    mixer_term = norm * mm(mixer_columns, mixer_grads, 0, 0)
    band = columns // C
    for q in range(C):
        r.m_o[q] = mixer_term[q * band : (q + 1) * band, :].astype(BF)

    def share_m(q, landing, slot):
        return rcopy(r.m_o.at[q], r.m_i.at[landing], r.m_s.at[q], r.m_r.at[slot], chan=q)

    each(C, lambda d: share_m(lax.rem(ch + d, C), ch, ch).start())
    if S <= 12:
        for d in range(3, S):
            hop("down", d)
            hop("up", d)
    else:
        lax.fori_loop(3, S, lambda d, c: (hop("down", d), hop("up", d), c)[2], 0)

    def step_term(k, total):
        for e in range(D):
            x = r.xc[k, e].reshape(length, columns)
            total = total + mm(r.gsm[k, e, rows:, 0:LANES], x, 1, 0)
        return total

    step_total = jnp.zeros((PAD, columns), F32)
    if S <= 12:
        for k in range(S):
            step_total = step_term(k, step_total)
    else:
        step_total = lax.fori_loop(0, S, step_term, step_total)
    r.o_dws[...] = (norm * step_total)[:heads, :]

    def weight_term(k, first=False):
        for e in others:
            for p in range(strips):
                ccopy(p, k, e, e).wait_recv()
        x = r.xc[k].reshape(D * length, columns)
        term = norm * mm(x, r.gin[k].reshape(D * length, width), 0, 0)
        r.o_dw[...] = term if first else r.o_dw[...] + term

    def weight_terms(d):
        for k, there in ((me + d, me + d < S), (me - d, me >= d)):
            pl.when(there)(functools.partial(weight_term, k))

    weight_term(me, True)
    each(S, weight_terms)
    r.p_i[ch] = r.p_o[ch]
    r.m_i[ch] = r.m_o[ch]
    for j in range(parts):
        each(C, lambda d, j=j: share_p(j, lax.rem(ch + d, C), ch, lax.rem(ch + d, C)).wait_recv())
    each(C, lambda d: share_m(lax.rem(ch + d, C), ch, lax.rem(ch + d, C)).wait_recv())

    for way in (0, 1):

        @pl.when(spots[way] < S - 1)
        def _(way=way):
            for piece in range(pieces):
                carry(way, piece).wait_send()

    @pl.when(me > 0)
    def _():
        for j in range(strips):
            halo(j).wait_send()
        mix_halo().wait_send()
        mix_tail(ch).wait_send()

    def settle_chan(d):
        q = lax.rem(ch + d, C)
        share_mix(q, ch, ch).wait_send()
        share_m(q, ch, ch).wait_send()
        for j in range(parts):
            share_p(j, q, ch, ch).wait_send()

    each(C, settle_chan)

    def settle_line(k):
        for e in others:
            for p in range(strips):
                ccopy(p, k, mine, e).wait_send()
        for way, sent in (("up", (k <= me) & (me < S - 1)), ("down", (k >= me) & (me > 0))):

            @pl.when(sent)
            def _(way=way):
                for p in range(strips):
                    zcopy(p, way, k).wait_send()

    settle_line(0)
    each(S, settle_line)
    small_all(lambda e, q: small_to(mine, me, e, q).wait_send())


def finish_kernel(parts, dw, mixes, dws, o_ig, o_dw, o_dwm, o_dws, ig, dwm, sems):
    copies = [
        pltpu.make_async_copy(a, b, sems.at[i])
        for i, (a, b) in enumerate(((dw, o_dw), (dws, o_dws), (ig, o_ig), (dwm, o_dwm)))
    ]
    copies[0].start()
    copies[1].start()
    total = parts[0].astype(F32)
    for q in range(1, parts.shape[0]):
        total = total + parts[q].astype(F32)
    ig[...] = total.astype(BF)
    copies[2].start()
    total = mixes[0].astype(F32)
    for q in range(1, mixes.shape[0]):
        total = total + mixes[q].astype(F32)
    dwm[...] = total
    copies[3].start()
    for copy in copies:
        copy.wait()


def body(
    sizes,
    layer_input,
    inner_weight,
    mixer_weight,
    step_weight,
    conv_inner,
    conv_mixer,
    step_bias,
    decay_log,
    skip_gain,
    output_grad,
):
    own = layer_input[0]
    rows, model = own.shape
    chans, seqs, dps = sizes["chan"], sizes["seq"], sizes["dp"]
    groups = dps * seqs
    length = rows * chans
    width = inner_weight.shape[1]
    mixed = mixer_weight.shape[1]
    heads = step_bias.shape[0]
    cols = model // groups
    state_size = mixed // 2
    assert width % PIECES == 0 and chans % 2 == 0 and seqs > 2
    assert width % LANES == 0 and PIECES % (width // LANES) == 0
    assert length == LANES and heads + conv_inner.shape[0] - 1 <= PAD
    upstream = output_grad[0]
    step_rows = step_weight.T
    bias, rates, skips = (v.reshape(1, heads) for v in (step_bias, decay_log, skip_gain))
    dma = pltpu.SemaphoreType.DMA
    vmem = pl.BlockSpec(memory_space=pltpu.VMEM)
    hbm = pl.BlockSpec(memory_space=pltpu.HBM)
    small = rows + PAD
    strips = width // LANES
    band = cols // chans

    def low(*shape):
        return pltpu.VMEM(shape, BF)

    def full(*shape):
        return pltpu.VMEM(shape, F32)

    inputs = dict(
        own=own, w_in=inner_weight, w_mix=mixer_weight, w_step=step_rows, conv_in=conv_inner,
        conv_mix=conv_mixer, bias=bias, log=rates, skip=skips, grad=upstream,
    )
    outputs = dict(
        p_i=jax.ShapeDtypeStruct((chans, rows, model), BF),
        o_dw=jax.ShapeDtypeStruct((cols, width), F32),
        m_i=jax.ShapeDtypeStruct((chans, band, mixed), BF),
        o_dws=jax.ShapeDtypeStruct((heads, cols), F32),
    )
    scratch = {key: pltpu.VMEM(v.shape, v.dtype) for key, v in inputs.items()}
    scratch |= dict(
        wst=low(LANES, model), xg=low(length, model),
        blocks=low(dps, seqs, rows, cols), mid=low(dps, seqs, rows, cols),
        xs=low(seqs, dps, rows, cols), xc=low(seqs, dps, chans, rows, cols),
        wide_in=full(PAD + length, width), wide_mix=full(PAD + length, mixed),
        fh_o=low(PAD, width + mixed), fh_i=low(PAD, width + mixed), vec=full(8, LANES),
        sum_in=full(length, width), sum_mix=full(length, mixed), raw=full(length, LANES),
        cum=full(length, LANES), step_wide=full(length, width), fading=full(length, width),
        grown=full(length, width), pulled=low(length, width), decay=full(width, state_size),
        mix=low(length, mixed), act=full(length, width), stepped=low(length, width),
        state_term=low(width, state_size), back_term=low(width, state_size),
        start=low(width, state_size), end=low(width, state_size),
        scr0=low(width, state_size), scr1=low(width, state_size),
        z=full(length, width), y=full(length, width), score_grad=full(length, length),
        slope_in=full(length, width),
        pad_in=full(length + 8, width), pad_mix=full(length + 8, mixed),
        gin=low(seqs, dps, length, width), gsm=low(seqs, dps, small, mixed),
        hal_o=full(strips, 8, LANES), hal_i=full(strips, 8, LANES),
        halm_o=full(8, mixed), halm_i=full(8, mixed), p_last=full(PAD, model),
        skips=full(8, width), ending=full(length, width),
        gmp=low(length, mixed), gm_in=low(chans, small, mixed), gmt=full(small, mixed),
        am=low(length + PAD, mixed), mt_in=low(chans, PAD, mixed),
        p_o=low(chans, rows, model), m_o=low(chans, band, mixed),
        load_sem=dma((len(LOADED),)), fh_sem=dma((2,)), halm_s=dma((2,)),
        hal_s=dma((strips,)), hal_r=dma((strips,)),
        near_s=dma((chans,)), near_r=dma((chans,)),
        far_s=dma((chans // 2, chans)), far_r=dma((chans // 2, chans)),
        relay_s=dma((chans // 2, chans)), relay_r=dma((chans // 2, chans)),
        swap_s=dma((dps,)), swap_r=dma((dps,)), cross_s=dma((seqs,)), cross_r=dma((seqs,)),
        gat_s=dma((chans,)), gat_r=dma((chans,)),
        chain_s=dma((2, PIECES)), chain_r=dma((2, PIECES)),
        z_r=dma((strips, seqs)), c_r=dma((strips, dps, seqs)),
        u_s=dma((strips, seqs)), d_s=dma((strips, seqs)), x_s=dma((strips, dps, seqs)),
        z2_r=dma((dps, seqs)),
        z2_s=dma((dps, seqs)), mt_s=dma((1,)), mt_r=dma((chans,)),
        gm_s=dma((chans,)), gm_r=dma((chans,)),
        p_s=dma((chans, chans)), p_r=dma((chans, chans)), m_s=dma((chans,)), m_r=dma((chans,)),
    )
    names = [key + "_h" for key in inputs] + list(outputs) + list(scratch)
    parts, inner_grad, mix_parts, step_grad = pl.pallas_call(
        functools.partial(layer_kernel, names, sizes, heads),
        out_shape=tuple(outputs.values()),
        in_specs=[hbm] * len(inputs),
        out_specs=(vmem,) * len(outputs),
        scratch_shapes=list(scratch.values()),
        compiler_params=pltpu.CompilerParams(
            collective_id=0, has_side_effects=True, vmem_limit_bytes=LIMIT
        ),
        name="layer",
    )(*(pltpu.with_memory_space_constraint(v, pltpu.HBM) for v in inputs.values()))
    input_grad, inner_grad, mixer_grad, step_grad = pl.pallas_call(
        finish_kernel,
        out_shape=(
            jax.ShapeDtypeStruct((rows, model), BF),
            jax.ShapeDtypeStruct((cols, width), F32),
            jax.ShapeDtypeStruct((band, mixed), F32),
            jax.ShapeDtypeStruct((heads, cols), F32),
        ),
        in_specs=[vmem] * 4,
        out_specs=(pl.BlockSpec(memory_space=pl.ANY),) * 4,
        scratch_shapes=[
            pltpu.VMEM((rows, model), BF),
            pltpu.VMEM((band, mixed), F32),
            dma((4,)),
        ],
        compiler_params=pltpu.CompilerParams(vmem_limit_bytes=LIMIT),
        name="finish",
    )(parts, inner_grad, mix_parts, step_grad)
    return input_grad[None], inner_grad, mixer_grad, step_grad.T


def solution(mesh):
    sizes = dict(mesh.shape)
    in_specs = (
        P("dp", ("seq", "chan"), None),
        P(None, "chan"),
        P(),
        P(None, "chan"),
        P(None, "chan"),
        P(),
        P("chan"),
        P("chan"),
        P("chan"),
        P("dp", "seq", "chan"),
    )
    out_specs = (
        P("dp", ("seq", "chan"), None),
        P(("dp", "seq"), "chan"),
        P(("dp", "seq", "chan"), None),
        P(("dp", "seq"), "chan"),
    )
    return jax.shard_map(
        functools.partial(body, sizes),
        mesh=mesh,
        in_specs=in_specs,
        out_specs=out_specs,
        check_vma=False,
    )
```

```python
import functools
import math
import types

import jax
import jax.numpy as jnp
from jax import lax
from jax.experimental import pallas as pl
from jax.experimental.pallas import tpu as pltpu
from jax.sharding import PartitionSpec as P

MESH = pl.DeviceIdType.MESH
HDIM = 64
PAD = 16
LANES = 128
LIMIT = 48 * 2**20
BF = jnp.bfloat16
F32 = jnp.float32
HIGH = lax.Precision.HIGHEST
PIECES = 10
LOADED = (
    "own", "w_in", "w_mix", "w_step", "conv_in", "conv_mix", "bias", "log", "skip", "grad",
)


def each(n, step):
    if n <= 12:
        for d in range(1, n):
            step(d)
    else:

        def one(d, carry):
            step(d)
            return carry

        lax.fori_loop(1, n, one, 0)


def signal_to(barrier, where):
    pl.semaphore_signal(barrier, inc=1, device_id=where, device_id_type=MESH)


def mm(a, b, da, db):
    return lax.dot_general(
        a.astype(BF), b.astype(BF), (((da,), (db,)), ((), ())), preferred_element_type=F32
    )


def exact(a, b, da=1, db=0):
    return lax.dot_general(
        a, b, (((da,), (db,)), ((), ())), precision=HIGH, preferred_element_type=F32
    )


def softplus(v):
    return jnp.maximum(v, 0.0) + jnp.log1p(jnp.exp(-jnp.abs(v)))


def head_mask(width, heads_first):
    shape = (LANES, width) if heads_first else (width, LANES)
    head = lax.broadcasted_iota(jnp.int32, shape, 0 if heads_first else 1)
    column = lax.broadcasted_iota(jnp.int32, shape, 1 if heads_first else 0)
    return (column // HDIM == head).astype(F32)


def decays(raw, bias, decay_log):
    length = raw.shape[0]
    step = softplus(raw + bias)
    rate = jnp.exp(decay_log)
    row = lax.broadcasted_iota(jnp.int32, (length, length), 0)
    col = lax.broadcasted_iota(jnp.int32, (length, length), 1)
    lower = (row >= col).astype(F32)
    cumulative = exact(lower, -step * rate)
    return step, rate, cumulative, row, col, lower


def rcopy(src, dst, send, recv, **where):
    return pltpu.make_async_remote_copy(
        src_ref=src, dst_ref=dst, send_sem=send, recv_sem=recv, device_id=where, device_id_type=MESH
    )


def greet_all(barrier, axis, n):
    me = lax.axis_index(axis)
    each(n, lambda d: signal_to(barrier, {axis: lax.rem(me + d, n)}))
    return n - 1


def convolved(wide, kernel, first, count):
    taps = kernel.shape[0]
    first = first + PAD - (taps - 1)
    total = kernel[0:1, :] * wide[pl.ds(first, count), :]
    for k in range(1, taps):
        total = total + kernel[k : k + 1, :] * wide[pl.ds(first + k, count), :]
    return total


def spread_back(pad, kernel, first, count, cols=slice(None)):
    taps = kernel.shape[0]
    total = None
    for k in range(taps):
        term = kernel[k : k + 1, cols] * pad[pl.ds(first + taps - 1 - k, count), cols]
        total = term if total is None else total + term
    return total.astype(BF)


def layer_kernel(names, sizes, heads, *refs):
    r = types.SimpleNamespace(**dict(zip(names, refs, strict=True)))
    place = (lax.axis_index("dp"), lax.axis_index("seq"), lax.axis_index("chan"))
    D, S, C = sizes["dp"], sizes["seq"], sizes["chan"]
    barrier = pltpu.get_barrier_semaphore()
    total = greet_all(barrier, "dp", D) + greet_all(barrier, "seq", S) + greet_all(barrier, "chan", C)
    after = lax.rem(place[1] + 1, S)

    @pl.when(place[2] == C - 1)
    def _():
        for c in range(C):
            signal_to(barrier, {"seq": after, "chan": jnp.int32(c)})

    total += 1 + (D - 1) * (S - 1)
    for e in range(1, D):
        far = lax.rem(place[0] + e, D)
        each(S, lambda d, far=far: signal_to(barrier, {"dp": far, "seq": lax.rem(place[1] + d, S)}))
    loads = {
        key: pltpu.make_async_copy(getattr(r, key + "_h"), getattr(r, key), r.load_sem.at[i])
        for i, key in enumerate(LOADED)
    }
    for copy in loads.values():
        copy.start()
    crossed = front(r, sizes, place, heads, loads, barrier, total)
    rear(r, sizes, place, heads, crossed)


def front(r, sizes, place, heads, loads, barrier, total):
    D, S, C = sizes["dp"], sizes["seq"], sizes["chan"]
    mine, me, ch = place
    rows, model = r.own.shape
    length, width = r.sum_in.shape
    mixed = r.sum_mix.shape[1]
    cols = model // (D * S)
    half = mixed // 2
    pieces = C
    cut = model // pieces
    sides = C // 2
    side, low = lax.div(ch, 2), lax.rem(ch, 2)
    partner = ch + 1 - 2 * low

    def block(c, p):
        return r.xg.at[pl.ds(pl.multiple_of(c * rows, rows), rows), pl.ds(p * cut, cut)]

    def mine_at(p):
        return r.own.at[:, pl.ds(p * cut, cut)]

    def near(c, p):
        return rcopy(mine_at(p), block(c, p), r.near_s.at[p], r.near_r.at[p], chan=partner)

    def far(to, c, slot, p):
        return rcopy(
            mine_at(p), block(c, p), r.far_s.at[to, p], r.far_r.at[slot, p], chan=2 * to + low
        )

    def relay(source, lane, p):
        c = 2 * source + lane
        here = block(c, p)
        return rcopy(here, here, r.relay_s.at[source, p], r.relay_r.at[source, p], chan=partner)

    def swap(q, landing, slot):
        return rcopy(r.blocks.at[q], r.mid.at[landing], r.swap_s.at[q], r.swap_r.at[slot], dp=q)

    def cross(q, landing, slot):
        return rcopy(r.mid.at[:, q], r.xs.at[landing], r.cross_s.at[q], r.cross_r.at[slot], seq=q)

    loads["own"].wait()
    pl.semaphore_wait(barrier, total)
    for p in range(pieces):
        for d in range(1, sides):
            far(lax.rem(side + d, sides), ch, side, p).start()
        near(ch, p).start()
    for d in range(D):
        for k in range(S):
            at = (d * S + k) * cols
            r.blocks[d, k] = r.own[:, at : at + cols]
    each(D, lambda d: swap(lax.rem(mine + d, D), mine, mine).start())
    r.mid[mine] = r.blocks[mine]
    r.xg[pl.ds(pl.multiple_of(ch * rows, rows), rows), :] = r.own[...]
    r.wst[...] = jnp.zeros(r.wst.shape, BF)
    r.vec[...] = jnp.zeros(r.vec.shape, F32)
    for key in LOADED[1:]:
        loads[key].wait()
    r.wst[0:heads, :] = r.w_step[...]
    for i, ref in enumerate((r.bias, r.log, r.skip)):
        r.vec[i : i + 1, 0:heads] = ref[...]

    def pass_on(p):
        for d in range(1, sides):
            source = lax.rem(side + d, sides)
            far(source, ch, source, p).wait_recv()
            relay(source, low, p).start()

    def project(p):
        near(partner, p).wait_recv()
        for d in range(1, sides):
            source = lax.rem(side + d, sides)
            relay(source, 1 - low, p).wait_recv()
        piece = slice(p * cut, (p + 1) * cut)
        x = r.xg[:, piece]
        inner = mm(x, r.w_in[piece, :], 1, 0)
        mixer = mm(x, r.w_mix[piece, :], 1, 0)
        raw = mm(x, r.wst[:, piece], 1, 1)
        if p == 0:
            r.wide_in[PAD:, :], r.wide_mix[PAD:, :], r.raw[...] = inner, mixer, raw
        else:
            r.wide_in[PAD:, :] = r.wide_in[PAD:, :] + inner
            r.wide_mix[PAD:, :] = r.wide_mix[PAD:, :] + mixer
            r.raw[...] = r.raw[...] + raw

    pass_on(0)
    for p in range(pieces):
        if p + 1 < pieces:
            pass_on(p + 1)
        project(p)
        if p == 0:
            each(D, lambda d: swap(lax.rem(mine + d, D), mine, lax.rem(mine + d, D)).wait_recv())
            each(S, lambda d: cross(lax.rem(me + d, S), me, me).start())
            r.xs[me] = r.mid[:, me]
    inner_low = r.wide_in[PAD:, :].astype(BF)
    mixer_low = r.wide_mix[PAD:, :].astype(BF)
    r.fh_o[:, :width] = inner_low[length - PAD :, :]
    r.fh_o[:, width:] = mixer_low[length - PAD :, :]

    def halo():
        return rcopy(r.fh_o, r.fh_i, r.fh_sem.at[0], r.fh_sem.at[1], seq=lax.rem(me + 1, S))

    @pl.when(me < S - 1)
    def _():
        halo().start()

    r.wide_in[PAD:, :] = inner_low.astype(F32)
    r.wide_mix[PAD:, :] = mixer_low.astype(F32)
    r.wide_in[0:PAD, :] = jnp.zeros((PAD, width), F32)
    r.wide_mix[0:PAD, :] = jnp.zeros((PAD, mixed), F32)
    r.sum_in[PAD:, :] = convolved(r.wide_in, r.conv_in, PAD, length - PAD)
    r.sum_mix[PAD:, :] = convolved(r.wide_mix, r.conv_mix, PAD, length - PAD)
    step, rate, cumulative, row, col, lower = decays(r.raw[...], r.vec[0:1, :], r.vec[1:2, :])
    last = cumulative[length - 1 : length, :]
    spread = head_mask(width, True)
    r.cum[...] = cumulative
    step_wide = exact(step, spread)
    fading = exact(jnp.exp(last - cumulative), spread)
    grown = exact(jnp.exp(cumulative), spread)
    r.step_wide[...] = step_wide
    r.fading[...] = fading
    r.grown[...] = grown
    pulled = (grown * r.grad[...].astype(F32)).astype(BF)
    r.pulled[...] = pulled
    row_decay = jnp.sum(head_mask(width, False) * jnp.exp(last), axis=1, keepdims=True)
    r.decay[...] = jnp.broadcast_to(row_decay, r.decay.shape)

    @pl.when(me > 0)
    def _():
        halo().wait_recv()
        r.wide_in[0:PAD, :] = r.fh_i[:, :width].astype(F32)
        r.wide_mix[0:PAD, :] = r.fh_i[:, width:].astype(F32)

    r.sum_in[0:PAD, :] = convolved(r.wide_in, r.conv_in, 0, PAD)
    r.sum_mix[0:PAD, :] = convolved(r.wide_mix, r.conv_mix, 0, PAD)
    mixer = r.sum_mix[...]
    mix = mixer * jax.nn.sigmoid(mixer)
    r.mix[...] = mix.astype(BF)
    r.back_term[...] = mm(pulled, mix[:, half:], 0, 0).astype(BF)
    inner = r.sum_in[...]
    act = inner * jax.nn.sigmoid(inner)
    r.act[...] = act
    r.state_term[...] = mm(act * (fading * step_wide), mix[:, :half], 0, 0).astype(BF)

    @pl.when(me < S - 1)
    def _():
        halo().wait_send()

    for p in range(pieces):
        near(ch, p).wait_send()
        for d in range(1, sides):
            source = lax.rem(side + d, sides)
            far(source, ch, source, p).wait_send()
            relay(source, low, p).wait_send()
    each(D, lambda d: swap(lax.rem(mine + d, D), mine, mine).wait_send())

    def settle(d):
        q = lax.rem(me + d, S)
        cross(q, me, q).wait()

    return lambda: each(S, settle)


def rear(r, sizes, place, heads, crossed):
    D, S, C = sizes["dp"], sizes["seq"], sizes["chan"]
    mine, me, ch = place
    length, width = r.sum_in.shape
    mixed = r.sum_mix.shape[1]
    half = mixed // 2
    model = r.w_in.shape[0]
    rows = length // C
    pieces, lag = PIECES, PIECES // 2
    size = width // pieces
    strips = width // LANES
    per = pieces // strips
    parts = C
    cut = model // parts
    terms, outs, scratch = (r.state_term, r.back_term), (r.start, r.end), (r.scr0, r.scr1)
    spots = (me, S - 1 - me)
    above, below = lax.rem(me + 1, S), lax.rem(me + S - 1, S)
    others = [lax.rem(mine + e, D) for e in range(1, D)]

    def carry(way, piece, first=False):
        part = pl.ds(pl.multiple_of(piece * size, size), size)
        source = terms[way] if first else scratch[way]
        sems = r.chain_s.at[way, piece], r.chain_r.at[way, piece]
        return rcopy(source.at[part], outs[way].at[part], *sems, seq=above if way == 0 else below)

    for way in (1, 0):

        @pl.when(spots[way] == 0)
        def _(way=way):
            for piece in range(pieces):
                carry(way, piece, True).start()
            outs[way][...] = jnp.zeros(outs[way].shape, BF)

    def beat(t):
        for way in (1, 0):
            spot = spots[way]
            piece = t - lag * (spot - 1)

            @pl.when((piece >= 0) & (piece < pieces) & (spot > 0) & (spot < S - 1))
            def _(way=way, piece=piece):
                carry(way, piece).wait_recv()
                part = pl.ds(pl.multiple_of(piece * size, size), size)
                before = outs[way][part, :].astype(F32)
                term = terms[way][part, :].astype(F32)
                scratch[way][part, :] = (r.decay[part, :] * before + term).astype(BF)
                carry(way, piece).start()

    def gather(q, landing, slot):
        return rcopy(r.xs, r.xc.at[:, :, landing], r.gat_s.at[q], r.gat_r.at[slot], chan=q)

    spread = head_mask(width, True)
    cumulative = r.cum[...]
    across = cumulative.T
    row = lax.broadcasted_iota(jnp.int32, (length, length), 0)
    col = lax.broadcasted_iota(jnp.int32, (length, length), 1)
    causal = row >= col
    lower = causal.astype(F32)
    into, out_of = r.mix[:, :half], r.mix[:, half:]
    scores = mm(out_of, into, 1, 1)
    r.stepped[...] = (r.act[...] * r.step_wide[...]).astype(BF)
    inner = r.sum_in[...]
    gate = jax.nn.sigmoid(inner)
    r.slope_in[...] = gate * (1.0 + inner * (1.0 - gate))
    skip_wide = exact(jnp.broadcast_to(r.vec[2:3, :], (8, LANES)), spread)
    r.skips[...] = skip_wide
    r.pad_in[length:, :] = jnp.zeros((8, width), F32)
    r.pad_mix[length:, :] = jnp.zeros((8, mixed), F32)

    def head(h):
        cols = slice(h * HDIM, (h + 1) * HDIM)
        gap = cumulative[:, h : h + 1] - across[h : h + 1, :]
        decay = jnp.where(causal, jnp.exp(jnp.where(causal, gap, 0.0)), 0.0)
        weights = (decay * scores).astype(BF)
        grad_h, step_h = r.grad[:, cols], r.stepped[:, cols]
        term = decay * mm(grad_h, step_h, 1, 1)
        r.score_grad[...] = term if h == 0 else r.score_grad[...] + term
        r.z[:, cols] = mm(weights, grad_h, 0, 0)
        r.y[:, cols] = mm(weights, step_h, 1, 0)

    def strip(j):
        return slice(j * LANES, (j + 1) * LANES)

    def halo(j):
        return rcopy(r.hal_o.at[j], r.hal_i.at[j], r.hal_s.at[j], r.hal_r.at[j], seq=below)

    def strip_sum(j):
        cols = strip(j)

        @pl.when(spots[1] == S - 1)
        def _():
            for piece in range(j * per, (j + 1) * per):
                carry(1, piece).wait_recv()

        ending = r.fading[:, cols] * mm(into, r.end[cols, :], 1, 1)
        r.ending[:, cols] = ending
        direct = r.skips[0:1, cols] * r.grad[:, cols].astype(F32)
        total = (r.step_wide[:, cols] * (r.z[:, cols] + ending) + direct) * r.slope_in[:, cols]
        r.pad_in[0:length, cols] = total
        r.hal_o[j] = total[0:8, :]

        @pl.when(me > 0)
        def _():
            halo(j).start()

    def part(p, e, k):
        return r.gin.at[k, e, :, pl.ds(p * LANES, LANES)]

    def zcopy(p, way, k, e=mine):
        send = (r.u_s if way == "up" else r.d_s).at[p, e, k]
        here = part(p, e, k)
        return rcopy(here, here, send, r.z_r.at[p, e, k], seq=above if way == "up" else below)

    def ccopy(p, k, e, to):
        return rcopy(part(p, e, k), part(p, e, k), r.x_s.at[p, to, k], r.c_r.at[p, e, k], dp=to)

    def strip_out(j):
        cols = strip(j)

        @pl.when(me < S - 1)
        def _():
            halo(j).wait_recv()
            r.pad_in[length:, cols] = r.hal_i[j]

        r.gin[me, mine, :, cols] = spread_back(r.pad_in, r.conv_in, 0, length, cols)
        for e in others:
            ccopy(j, me, mine, e).start()

    def strip_along(j):
        @pl.when(me < S - 1)
        def _():
            zcopy(j, "up", me).start()

        @pl.when(me > 0)
        def _():
            zcopy(j, "down", me).start()

    beats = pieces + lag * max(S - 3, 0)
    early = heads // 2
    for h in range(early):
        head(h)
    near = spots[1] <= 1
    crossed()
    each(C, lambda d: gather(lax.rem(ch + d, C), ch, ch).start())
    r.xc[:, :, ch] = r.xs[...]
    if beats <= 24:
        sums = {per * j + per - 1: j for j in range(strips)}
        late = {lag + t: j for t, j in sums.items()}
        for t in range(max(beats, heads - early)):
            beat(t)
            if early + t < heads:
                head(early + t)
            if t in sums:
                pl.when(near)(functools.partial(strip_sum, sums[t]))
            if t in late:
                pl.when(near)(functools.partial(strip_out, late[t]))
                pl.when(spots[1] == 2)(functools.partial(strip_sum, late[t]))
            if t - 2 in late:
                pl.when(spots[1] == 2)(functools.partial(strip_out, late[t - 2]))
        done = max(beats, heads - early) - 2
        for j in range(strips):
            pl.when(spots[1] > 2)(functools.partial(strip_sum, j))
            left = spots[1] > 2 if [t for t in late if late[t] == j][0] < done else spots[1] > 1
            pl.when(left)(functools.partial(strip_out, j))
            strip_along(j)
    else:
        for h in range(early, heads):
            head(h)
        lax.fori_loop(0, beats, lambda t, c: (beat(t), c)[1], 0)
        for j in range(strips):
            strip_sum(j)
        for j in range(strips):
            strip_out(j)
            strip_along(j)

    @pl.when(me == S - 1)
    def _():
        for p in range(strips):
            for e in others:
                ccopy(p, me, e, e).wait_recv()
                zcopy(p, "down", me, e).start()

    @pl.when(spots[0] == S - 1)
    def _():
        for piece in range(pieces):
            carry(0, piece).wait_recv()

    start, end = r.start[...], r.end[...]
    score_grad = r.score_grad[...]
    mixer = r.sum_mix[...]
    gate = jax.nn.sigmoid(mixer)
    mixer_slope = gate * (1.0 + mixer * (1.0 - gate))
    faded = (r.fading[...] * r.stepped[...].astype(F32)).astype(BF)
    into_grad = mm(score_grad, out_of, 0, 0) + mm(faded, end, 1, 0)
    out_grad = mm(score_grad, into, 1, 0) + mm(r.pulled[...], start, 1, 0)
    r.pad_mix[0:length, :half] = into_grad * mixer_slope[:, :half]
    r.pad_mix[0:length, half:] = out_grad * mixer_slope[:, half:]
    r.am[0:length, :] = r.pad_mix[0:length, :].astype(BF)
    r.am[length:, :] = jnp.zeros((PAD, mixed), BF)
    r.halm_o[...] = r.pad_mix[0:8, :]

    def share_mix(q, landing, slot):
        some = r.am.at[pl.ds(pl.multiple_of(q * rows, rows), rows + PAD)]
        return rcopy(some, r.gm_in.at[landing], r.gm_s.at[q], r.gm_r.at[slot], chan=q)

    def mix_tail(slot):
        return rcopy(
            r.am.at[pl.ds(0, PAD)], r.mt_in.at[slot], r.mt_s.at[0], r.mt_r.at[slot],
            seq=below, chan=jnp.int32(C - 1),
        )

    def mix_halo():
        return rcopy(r.halm_o, r.halm_i, r.halm_s.at[0], r.halm_s.at[1], seq=below)

    each(C, lambda d: share_mix(lax.rem(ch + d, C), ch, ch).start())

    @pl.when(me > 0)
    def _():
        mix_tail(ch).start()
        mix_halo().start()

    r.gm_in[ch] = r.am[pl.ds(pl.multiple_of(ch * rows, rows), rows + PAD), :]
    r.gmp[...] = spread_back(r.pad_mix, r.conv_mix, 0, length)

    upstream = r.grad[...].astype(F32)
    stepped = r.stepped[...].astype(F32)
    ending = r.ending[...]
    carried = r.grown[...] * mm(out_of, start, 1, 1)
    to_heads = functools.partial(exact, b=spread, da=1, db=1)
    z = r.z[...]
    step_grad = to_heads(r.act[...] * (z + ending))
    tail_term = to_heads(stepped * ending)
    sum_grad = to_heads(upstream * (r.y[...] + carried) - stepped * z) - tail_term
    held = jnp.sum(start.astype(F32) * end.astype(F32), axis=1, keepdims=True)
    last = cumulative[length - 1 : length, :]
    overall = jnp.sum(tail_term, axis=0, keepdims=True) + jnp.exp(last) * jnp.sum(
        head_mask(width, False) * held, axis=0, keepdims=True
    )
    decay_grad = exact(lower, sum_grad, 0, 0) + overall
    rate = jnp.exp(r.vec[1:2, :])
    step_grad = (step_grad - rate * decay_grad) * jax.nn.sigmoid(r.raw[...] + r.vec[0:1, :])
    steps = step_grad.astype(BF)
    r.gsm[me, mine, rows:, 0:LANES] = step_grad.T[0:PAD, :].astype(BF)
    steps = steps[:, 0:PAD]

    each(C, lambda d: share_mix(lax.rem(ch + d, C), ch, lax.rem(ch + d, C)).wait_recv())
    mix = r.gm_in[0].astype(F32)
    for q in range(1, C):
        mix = mix + r.gm_in[q].astype(F32)
    r.gmt[...] = mix

    @pl.when((me < S - 1) & (ch == C - 1))
    def _():
        for q in range(C):
            mix_tail(q).wait_recv()
        tail = r.mt_in[0].astype(F32)
        for q in range(1, C):
            tail = tail + r.mt_in[q].astype(F32)
        r.gmt[rows:, :] = tail

    r.gsm[me, mine, 0:rows, :] = spread_back(r.gmt, r.conv_mix, 0, rows)

    def small_to(e, k, to, q):
        here = r.gsm.at[k, e]
        return rcopy(here, here, r.z2_s.at[to, q], r.z2_r.at[e, k], dp=to, seq=q)

    def small_all(do):
        each(S, lambda d: do(mine, lax.rem(me + d, S)))
        for e in others:
            do(e, me)
            each(S, lambda d, e=e: do(e, lax.rem(me + d, S)))

    small_all(lambda e, q: small_to(mine, me, e, q).start())

    def forward(p, way, d):
        k = me - d if way == "up" else me + d
        there = (k >= 0) if way == "up" else (k < S)
        more = (me < S - 1) if way == "up" else (me > 0)

        for e in [mine] + (others if way == "down" else []):
            here = there if e is mine else k == S - 1

            @pl.when(here)
            def _(e=e):
                zcopy(p, way, k, e).wait_recv()

            @pl.when(here & more)
            def _(e=e):
                zcopy(p, way, k, e).start()

        @pl.when(there & (k < S - 1))
        def _():
            for e in others:
                ccopy(p, k, mine, e).start()

    def hop(d):
        for p in range(strips):
            forward(p, "up", d)
            forward(p, "down", d)

    def share_p(j, q, landing, slot):
        piece = pl.ds(j * cut, cut)
        return rcopy(
            r.p_o.at[q, :, piece], r.p_i.at[landing, :, piece], r.p_s.at[j, q], r.p_r.at[j, slot], chan=q
        )

    grads = r.gin[me, mine]
    mixes = r.gmp[...]

    def send_p(j, final):
        def one(d):
            q = lax.rem(ch + d, C)

            @pl.when((q == C - 1) if final else (q < C - 1))
            def _():
                share_p(j, q, ch, ch).start()

        each(C, one)

    for j in range(parts):
        piece = slice(j * cut, (j + 1) * cut)
        out = mm(grads, r.w_in[piece, :], 1, 1) + mm(mixes, r.w_mix[piece, :], 1, 1)
        out = out + mm(steps, r.wst[0:PAD, piece], 1, 0)
        r.p_o[:, :, piece] = out.astype(BF).reshape(C, rows, cut)
        r.p_last[:, piece] = out[length - PAD :, :]
        send_p(j, False)
        forward(j, "up", 1)
        forward(j, "down", 1)
    for p in range(parts, strips):
        forward(p, "up", 1)
        forward(p, "down", 1)

    @pl.when(me < S - 1)
    def _():
        mix_halo().wait_recv()
        r.pad_mix[length:, :] = r.halm_i[...]
        final = spread_back(r.pad_mix, r.conv_mix, length - PAD, PAD)
        change = final.astype(F32) - r.gmp[length - PAD :, :].astype(F32)
        fixed = r.p_last[...] + mm(change, r.w_mix[...], 1, 1)
        r.p_o[C - 1, rows - PAD :, :] = fixed.astype(BF)

    for j in range(parts):
        send_p(j, True)
    hop(2)
    small_all(lambda e, q: small_to(e, q, e, q).wait_recv())

    norm = 1.0 / math.sqrt(D * S * length)
    columns = r.xc.shape[-1]

    def settle_gather(d):
        q = lax.rem(ch + d, C)
        gather(q, q, q).wait()

    each(C, settle_gather)
    mixer_columns = r.xc[:, :, ch].reshape(S * D * rows, columns)
    mixer_grads = r.gsm[:, :, 0:rows, :].reshape(S * D * rows, mixed)
    mixer_term = norm * mm(mixer_columns, mixer_grads, 0, 0)
    band = columns // C
    for q in range(C):
        r.m_o[q] = mixer_term[q * band : (q + 1) * band, :].astype(BF)

    def share_m(q, landing, slot):
        return rcopy(r.m_o.at[q], r.m_i.at[landing], r.m_s.at[q], r.m_r.at[slot], chan=q)

    each(C, lambda d: share_m(lax.rem(ch + d, C), ch, ch).start())
    if S <= 12:
        for d in range(3, S):
            hop(d)
    else:
        lax.fori_loop(3, S, lambda d, c: (hop(d), c)[1], 0)

    def step_term(k, total):
        for e in range(D):
            x = r.xc[k, e].reshape(length, columns)
            total = total + mm(r.gsm[k, e, rows:, 0:LANES], x, 1, 0)
        return total

    step_total = jnp.zeros((PAD, columns), F32)
    if S <= 12:
        for k in range(S):
            step_total = step_term(k, step_total)
    else:
        step_total = lax.fori_loop(0, S, step_term, step_total)
    r.o_dws[...] = (norm * step_total)[:heads, :]

    def weight_term(k, first=False):
        @pl.when(k < S - 1)
        def _():
            for e in others:
                for p in range(strips):
                    ccopy(p, k, e, e).wait_recv()

        x = r.xc[k].reshape(D * length, columns)
        term = norm * mm(x, r.gin[k].reshape(D * length, width), 0, 0)
        r.o_dw[...] = term if first else r.o_dw[...] + term

    def weight_terms(d):
        for k, there in ((me + d, me + d < S), (me - d, me >= d)):
            pl.when(there)(functools.partial(weight_term, k))

    weight_term(me, True)
    each(S, weight_terms)
    r.p_i[ch] = r.p_o[ch]
    r.m_i[ch] = r.m_o[ch]
    for j in range(parts):
        each(C, lambda d, j=j: share_p(j, lax.rem(ch + d, C), ch, lax.rem(ch + d, C)).wait_recv())
    each(C, lambda d: share_m(lax.rem(ch + d, C), ch, lax.rem(ch + d, C)).wait_recv())

    for way in (0, 1):

        @pl.when(spots[way] < S - 1)
        def _(way=way):
            for piece in range(pieces):
                carry(way, piece).wait_send()

    @pl.when(me > 0)
    def _():
        for j in range(strips):
            halo(j).wait_send()
        mix_halo().wait_send()
        mix_tail(ch).wait_send()

    def settle_chan(d):
        q = lax.rem(ch + d, C)
        share_mix(q, ch, ch).wait_send()
        share_m(q, ch, ch).wait_send()
        for j in range(parts):
            share_p(j, q, ch, ch).wait_send()

    each(C, settle_chan)

    def settle_line(k):
        @pl.when((k < S - 1) | (me == S - 1))
        def _():
            for e in others:
                for p in range(strips):
                    ccopy(p, k, mine, e).wait_send()

        for way, e, sent in [
            ("up", mine, (k <= me) & (me < S - 1)), ("down", mine, (k >= me) & (me > 0))
        ] + [("down", e, (k == S - 1) & (me > 0)) for e in others]:

            @pl.when(sent)
            def _(way=way, e=e):
                for p in range(strips):
                    zcopy(p, way, k, e).wait_send()

    settle_line(0)
    each(S, settle_line)
    small_all(lambda e, q: small_to(mine, me, e, q).wait_send())


def finish_kernel(parts, dw, mixes, dws, o_ig, o_dw, o_dwm, o_dws, ig, dwm, sems):
    copies = [
        pltpu.make_async_copy(a, b, sems.at[i])
        for i, (a, b) in enumerate(((dw, o_dw), (dws, o_dws), (ig, o_ig), (dwm, o_dwm)))
    ]
    copies[0].start()
    copies[1].start()
    total = parts[0].astype(F32)
    for q in range(1, parts.shape[0]):
        total = total + parts[q].astype(F32)
    ig[...] = total.astype(BF)
    copies[2].start()
    total = mixes[0].astype(F32)
    for q in range(1, mixes.shape[0]):
        total = total + mixes[q].astype(F32)
    dwm[...] = total
    copies[3].start()
    for copy in copies:
        copy.wait()


def body(
    sizes,
    layer_input,
    inner_weight,
    mixer_weight,
    step_weight,
    conv_inner,
    conv_mixer,
    step_bias,
    decay_log,
    skip_gain,
    output_grad,
):
    own = layer_input[0]
    rows, model = own.shape
    chans, seqs, dps = sizes["chan"], sizes["seq"], sizes["dp"]
    groups = dps * seqs
    length = rows * chans
    width = inner_weight.shape[1]
    mixed = mixer_weight.shape[1]
    heads = step_bias.shape[0]
    cols = model // groups
    state_size = mixed // 2
    assert width % PIECES == 0 and chans % 2 == 0 and seqs > 2
    assert width % LANES == 0 and PIECES % (width // LANES) == 0
    assert length == LANES and heads + conv_inner.shape[0] - 1 <= PAD
    upstream = output_grad[0]
    step_rows = step_weight.T
    bias, rates, skips = (v.reshape(1, heads) for v in (step_bias, decay_log, skip_gain))
    dma = pltpu.SemaphoreType.DMA
    vmem = pl.BlockSpec(memory_space=pltpu.VMEM)
    hbm = pl.BlockSpec(memory_space=pltpu.HBM)
    small = rows + PAD
    strips = width // LANES
    band = cols // chans

    def low(*shape):
        return pltpu.VMEM(shape, BF)

    def full(*shape):
        return pltpu.VMEM(shape, F32)

    inputs = dict(
        own=own, w_in=inner_weight, w_mix=mixer_weight, w_step=step_rows, conv_in=conv_inner,
        conv_mix=conv_mixer, bias=bias, log=rates, skip=skips, grad=upstream,
    )
    outputs = dict(
        p_i=jax.ShapeDtypeStruct((chans, rows, model), BF),
        o_dw=jax.ShapeDtypeStruct((cols, width), F32),
        m_i=jax.ShapeDtypeStruct((chans, band, mixed), BF),
        o_dws=jax.ShapeDtypeStruct((heads, cols), F32),
    )
    scratch = {key: pltpu.VMEM(v.shape, v.dtype) for key, v in inputs.items()}
    scratch |= dict(
        wst=low(LANES, model), xg=low(length, model),
        blocks=low(dps, seqs, rows, cols), mid=low(dps, seqs, rows, cols),
        xs=low(seqs, dps, rows, cols), xc=low(seqs, dps, chans, rows, cols),
        wide_in=full(PAD + length, width), wide_mix=full(PAD + length, mixed),
        fh_o=low(PAD, width + mixed), fh_i=low(PAD, width + mixed), vec=full(8, LANES),
        sum_in=full(length, width), sum_mix=full(length, mixed), raw=full(length, LANES),
        cum=full(length, LANES), step_wide=full(length, width), fading=full(length, width),
        grown=full(length, width), pulled=low(length, width), decay=full(width, state_size),
        mix=low(length, mixed), act=full(length, width), stepped=low(length, width),
        state_term=low(width, state_size), back_term=low(width, state_size),
        start=low(width, state_size), end=low(width, state_size),
        scr0=low(width, state_size), scr1=low(width, state_size),
        z=full(length, width), y=full(length, width), score_grad=full(length, length),
        slope_in=full(length, width),
        pad_in=full(length + 8, width), pad_mix=full(length + 8, mixed),
        gin=low(seqs, dps, length, width), gsm=low(seqs, dps, small, mixed),
        hal_o=full(strips, 8, LANES), hal_i=full(strips, 8, LANES),
        halm_o=full(8, mixed), halm_i=full(8, mixed), p_last=full(PAD, model),
        skips=full(8, width), ending=full(length, width),
        gmp=low(length, mixed), gm_in=low(chans, small, mixed), gmt=full(small, mixed),
        am=low(length + PAD, mixed), mt_in=low(chans, PAD, mixed),
        p_o=low(chans, rows, model), m_o=low(chans, band, mixed),
        load_sem=dma((len(LOADED),)), fh_sem=dma((2,)), halm_s=dma((2,)),
        hal_s=dma((strips,)), hal_r=dma((strips,)),
        near_s=dma((chans,)), near_r=dma((chans,)),
        far_s=dma((chans // 2, chans)), far_r=dma((chans // 2, chans)),
        relay_s=dma((chans // 2, chans)), relay_r=dma((chans // 2, chans)),
        swap_s=dma((dps,)), swap_r=dma((dps,)), cross_s=dma((seqs,)), cross_r=dma((seqs,)),
        gat_s=dma((chans,)), gat_r=dma((chans,)),
        chain_s=dma((2, PIECES)), chain_r=dma((2, PIECES)),
        z_r=dma((strips, dps, seqs)), c_r=dma((strips, dps, seqs)),
        u_s=dma((strips, dps, seqs)), d_s=dma((strips, dps, seqs)),
        x_s=dma((strips, dps, seqs)),
        z2_r=dma((dps, seqs)),
        z2_s=dma((dps, seqs)), mt_s=dma((1,)), mt_r=dma((chans,)),
        gm_s=dma((chans,)), gm_r=dma((chans,)),
        p_s=dma((chans, chans)), p_r=dma((chans, chans)), m_s=dma((chans,)), m_r=dma((chans,)),
    )
    names = [key + "_h" for key in inputs] + list(outputs) + list(scratch)
    parts, inner_grad, mix_parts, step_grad = pl.pallas_call(
        functools.partial(layer_kernel, names, sizes, heads),
        out_shape=tuple(outputs.values()),
        in_specs=[hbm] * len(inputs),
        out_specs=(vmem,) * len(outputs),
        scratch_shapes=list(scratch.values()),
        compiler_params=pltpu.CompilerParams(
            collective_id=0, has_side_effects=True, vmem_limit_bytes=LIMIT
        ),
        name="layer",
    )(*(pltpu.with_memory_space_constraint(v, pltpu.HBM) for v in inputs.values()))
    input_grad, inner_grad, mixer_grad, step_grad = pl.pallas_call(
        finish_kernel,
        out_shape=(
            jax.ShapeDtypeStruct((rows, model), BF),
            jax.ShapeDtypeStruct((cols, width), F32),
            jax.ShapeDtypeStruct((band, mixed), F32),
            jax.ShapeDtypeStruct((heads, cols), F32),
        ),
        in_specs=[vmem] * 4,
        out_specs=(pl.BlockSpec(memory_space=pl.ANY),) * 4,
        scratch_shapes=[
            pltpu.VMEM((rows, model), BF),
            pltpu.VMEM((band, mixed), F32),
            dma((4,)),
        ],
        compiler_params=pltpu.CompilerParams(vmem_limit_bytes=LIMIT),
        name="finish",
    )(parts, inner_grad, mix_parts, step_grad)
    return input_grad[None], inner_grad, mixer_grad, step_grad.T


def solution(mesh):
    sizes = dict(mesh.shape)
    in_specs = (
        P("dp", ("seq", "chan"), None),
        P(None, "chan"),
        P(),
        P(None, "chan"),
        P(None, "chan"),
        P(),
        P("chan"),
        P("chan"),
        P("chan"),
        P("dp", "seq", "chan"),
    )
    out_specs = (
        P("dp", ("seq", "chan"), None),
        P(("dp", "seq"), "chan"),
        P(("dp", "seq", "chan"), None),
        P(("dp", "seq"), "chan"),
    )
    return jax.shard_map(
        functools.partial(body, sizes),
        mesh=mesh,
        in_specs=in_specs,
        out_specs=out_specs,
        check_vma=False,
    )
```

```python
import functools
import math
import types

import jax
import jax.numpy as jnp
from jax import lax
from jax.experimental import pallas as pl
from jax.experimental.pallas import tpu as pltpu
from jax.sharding import PartitionSpec as P

MESH = pl.DeviceIdType.MESH
HDIM = 64
PAD = 16
LANES = 128
LIMIT = 48 * 2**20
BF = jnp.bfloat16
F32 = jnp.float32
PIECES = 10
LOADED = (
    "own", "w_in", "w_mix", "w_step", "conv_in", "conv_mix", "bias", "log", "skip", "grad",
)


def each(n, step):
    if n <= 12:
        for d in range(1, n):
            step(d)
    else:

        def one(d, carry):
            step(d)
            return carry

        lax.fori_loop(1, n, one, 0)


def signal_to(barrier, where):
    pl.semaphore_signal(barrier, inc=1, device_id=where, device_id_type=MESH)


def mm(a, b, da, db):
    return lax.dot_general(
        a.astype(BF), b.astype(BF), (((da,), (db,)), ((), ())), preferred_element_type=F32
    )


def thirds(v):
    high = v.astype(BF)
    rest = v - high.astype(F32)
    middle = rest.astype(BF)
    return high, middle, (rest - middle.astype(F32)).astype(BF)


def exact(a, b, da=1, db=0):
    high, middle, low = thirds(a)
    return mm(high, b, da, db) + (mm(middle, b, da, db) + mm(low, b, da, db))


def exact_left(a, b, da=1, db=0):
    high, middle, low = thirds(b)
    return mm(a, high, da, db) + (mm(a, middle, da, db) + mm(a, low, da, db))


def softplus(v):
    return jnp.maximum(v, 0.0) + jnp.log1p(jnp.exp(-jnp.abs(v)))


def head_mask(width, heads_first):
    shape = (LANES, width) if heads_first else (width, LANES)
    head = lax.broadcasted_iota(jnp.int32, shape, 0 if heads_first else 1)
    column = lax.broadcasted_iota(jnp.int32, shape, 1 if heads_first else 0)
    return (column // HDIM == head).astype(F32)


def decays(raw, bias, decay_log):
    length = raw.shape[0]
    step = softplus(raw + bias)
    rate = jnp.exp(decay_log)
    row = lax.broadcasted_iota(jnp.int32, (length, length), 0)
    col = lax.broadcasted_iota(jnp.int32, (length, length), 1)
    lower = (row >= col).astype(F32)
    cumulative = exact_left(lower, -step * rate)
    return step, rate, cumulative, row, col, lower


def rcopy(src, dst, send, recv, **where):
    return pltpu.make_async_remote_copy(
        src_ref=src, dst_ref=dst, send_sem=send, recv_sem=recv, device_id=where, device_id_type=MESH
    )


def greet_all(barrier, axis, n):
    me = lax.axis_index(axis)
    each(n, lambda d: signal_to(barrier, {axis: lax.rem(me + d, n)}))
    return n - 1


def convolved(wide, kernel, first, count):
    taps = kernel.shape[0]
    first = first + PAD - (taps - 1)
    total = kernel[0:1, :] * wide[pl.ds(first, count), :]
    for k in range(1, taps):
        total = total + kernel[k : k + 1, :] * wide[pl.ds(first + k, count), :]
    return total


def spread_back(pad, kernel, first, count, cols=slice(None)):
    taps = kernel.shape[0]
    total = None
    for k in range(taps):
        term = kernel[k : k + 1, cols] * pad[pl.ds(first + taps - 1 - k, count), cols]
        total = term if total is None else total + term
    return total.astype(BF)


def layer_kernel(names, sizes, heads, *refs):
    r = types.SimpleNamespace(**dict(zip(names, refs, strict=True)))
    place = (lax.axis_index("dp"), lax.axis_index("seq"), lax.axis_index("chan"))
    D, S, C = sizes["dp"], sizes["seq"], sizes["chan"]
    barrier = pltpu.get_barrier_semaphore()
    total = greet_all(barrier, "dp", D) + greet_all(barrier, "seq", S) + greet_all(barrier, "chan", C)
    after = lax.rem(place[1] + 1, S)

    @pl.when(place[2] == C - 1)
    def _():
        for c in range(C):
            signal_to(barrier, {"seq": after, "chan": jnp.int32(c)})

    total += 1 + (D - 1) * (S - 1)
    for e in range(1, D):
        far = lax.rem(place[0] + e, D)
        each(S, lambda d, far=far: signal_to(barrier, {"dp": far, "seq": lax.rem(place[1] + d, S)}))
    loads = {
        key: pltpu.make_async_copy(getattr(r, key + "_h"), getattr(r, key), r.load_sem.at[i])
        for i, key in enumerate(LOADED)
    }
    for copy in loads.values():
        copy.start()
    crossed = front(r, sizes, place, heads, loads, barrier, total)
    rear(r, sizes, place, heads, crossed)


def front(r, sizes, place, heads, loads, barrier, total):
    D, S, C = sizes["dp"], sizes["seq"], sizes["chan"]
    mine, me, ch = place
    rows, model = r.own.shape
    length, width = r.sum_in.shape
    mixed = r.sum_mix.shape[1]
    cols = model // (D * S)
    half = mixed // 2
    pieces = C
    cut = model // pieces
    sides = C // 2
    side, low = lax.div(ch, 2), lax.rem(ch, 2)
    partner = ch + 1 - 2 * low

    def block(c, p):
        return r.xg.at[pl.ds(pl.multiple_of(c * rows, rows), rows), pl.ds(p * cut, cut)]

    def mine_at(p):
        return r.own.at[:, pl.ds(p * cut, cut)]

    def near(c, p):
        return rcopy(mine_at(p), block(c, p), r.near_s.at[0], r.near_r.at[p], chan=partner)

    def far(to, c, slot, p):
        return rcopy(
            mine_at(p), block(c, p), r.far_s.at[to], r.far_r.at[slot, p], chan=2 * to + low
        )

    def relay(source, lane, p):
        c = 2 * source + lane
        here = block(c, p)
        return rcopy(here, here, r.relay_s.at[source], r.relay_r.at[source, p], chan=partner)

    def column(e, q, landing_e, landing_q):
        return rcopy(
            r.blocks.at[e, q], r.xs.at[landing_q, landing_e],
            r.cross_s.at[e, q], r.cross_r.at[landing_e, landing_q], dp=e, seq=q,
        )

    def columns_all(do):
        each(S, lambda d: do(mine, lax.rem(me + d, S)))
        for d in range(1, D):
            e = lax.rem(mine + d, D)
            do(e, me)
            each(S, lambda d, e=e: do(e, lax.rem(me + d, S)))

    loads["own"].wait()
    pl.semaphore_wait(barrier, total)
    for p in range(pieces):
        for d in range(1, sides):
            far(lax.rem(side + d, sides), ch, side, p).start()
        near(ch, p).start()
    for d in range(D):
        for k in range(S):
            at = (d * S + k) * cols
            r.blocks[d, k] = r.own[:, at : at + cols]
    columns_all(lambda e, q: column(e, q, mine, me).start())
    r.xs[me, mine] = r.blocks[mine, me]
    r.xg[pl.ds(pl.multiple_of(ch * rows, rows), rows), :] = r.own[...]
    r.wst[...] = jnp.zeros(r.wst.shape, BF)
    r.vec[...] = jnp.zeros(r.vec.shape, F32)
    for key in LOADED[1:]:
        loads[key].wait()
    r.wst[0:heads, :] = r.w_step[...]
    for i, ref in enumerate((r.bias, r.log, r.skip)):
        r.vec[i : i + 1, 0:heads] = ref[...]

    def pass_on(p):
        for d in range(1, sides):
            source = lax.rem(side + d, sides)
            far(source, ch, source, p).wait_recv()
            relay(source, low, p).start()

    def project(p):
        near(partner, p).wait_recv()
        for d in range(1, sides):
            source = lax.rem(side + d, sides)
            relay(source, 1 - low, p).wait_recv()
        piece = slice(p * cut, (p + 1) * cut)
        x = r.xg[:, piece]
        inner = mm(x, r.w_in[piece, :], 1, 0)
        mixer = mm(x, r.w_mix[piece, :], 1, 0)
        raw = mm(x, r.wst[:, piece], 1, 1)
        if p == 0:
            r.wide_in[PAD:, :], r.wide_mix[PAD:, :], r.raw[...] = inner, mixer, raw
        else:
            r.wide_in[PAD:, :] = r.wide_in[PAD:, :] + inner
            r.wide_mix[PAD:, :] = r.wide_mix[PAD:, :] + mixer
            r.raw[...] = r.raw[...] + raw

    pass_on(0)
    for p in range(pieces):
        if p + 1 < pieces:
            pass_on(p + 1)
        project(p)
    inner_low = r.wide_in[PAD:, :].astype(BF)
    mixer_low = r.wide_mix[PAD:, :].astype(BF)
    r.fh_o[:, :width] = inner_low[length - PAD :, :]
    r.fh_o[:, width:] = mixer_low[length - PAD :, :]

    def halo():
        return rcopy(r.fh_o, r.fh_i, r.fh_sem.at[0], r.fh_sem.at[1], seq=lax.rem(me + 1, S))

    @pl.when(me < S - 1)
    def _():
        halo().start()

    r.wide_in[PAD:, :] = inner_low.astype(F32)
    r.wide_mix[PAD:, :] = mixer_low.astype(F32)
    r.wide_in[0:PAD, :] = jnp.zeros((PAD, width), F32)
    r.wide_mix[0:PAD, :] = jnp.zeros((PAD, mixed), F32)
    r.sum_in[PAD:, :] = convolved(r.wide_in, r.conv_in, PAD, length - PAD)
    r.sum_mix[PAD:, :] = convolved(r.wide_mix, r.conv_mix, PAD, length - PAD)
    step, rate, cumulative, row, col, lower = decays(r.raw[...], r.vec[0:1, :], r.vec[1:2, :])
    last = cumulative[length - 1 : length, :]
    spread = head_mask(width, True)
    r.cum[...] = cumulative
    step_wide = exact(step, spread)
    fading = exact(jnp.exp(last - cumulative), spread)
    grown = exact(jnp.exp(cumulative), spread)
    r.step_wide[...] = step_wide
    r.fading[...] = fading
    r.grown[...] = grown
    pulled = (grown * r.grad[...].astype(F32)).astype(BF)
    r.pulled[...] = pulled
    row_decay = jnp.sum(head_mask(width, False) * jnp.exp(last), axis=1, keepdims=True)
    r.decay[...] = jnp.broadcast_to(row_decay, r.decay.shape)

    @pl.when(me > 0)
    def _():
        halo().wait_recv()
        r.wide_in[0:PAD, :] = r.fh_i[:, :width].astype(F32)
        r.wide_mix[0:PAD, :] = r.fh_i[:, width:].astype(F32)

    r.sum_in[0:PAD, :] = convolved(r.wide_in, r.conv_in, 0, PAD)
    r.sum_mix[0:PAD, :] = convolved(r.wide_mix, r.conv_mix, 0, PAD)
    mixer = r.sum_mix[...]
    mix = mixer * jax.nn.sigmoid(mixer)
    r.mix[...] = mix.astype(BF)
    r.back_term[...] = mm(pulled, mix[:, half:], 0, 0).astype(BF)
    inner = r.sum_in[...]
    act = inner * jax.nn.sigmoid(inner)
    r.act[...] = act
    r.state_term[...] = mm(act * (fading * step_wide), mix[:, :half], 0, 0).astype(BF)

    @pl.when(me < S - 1)
    def _():
        halo().wait_send()

    def sent(sem):
        rcopy(r.own, r.own, sem, r.near_r.at[0], chan=partner).wait_send()

    sent(r.near_s.at[0])
    for d in range(1, sides):
        source = lax.rem(side + d, sides)
        sent(r.far_s.at[source])
        sent(r.relay_s.at[source])
    return lambda: columns_all(lambda e, q: column(e, q, e, q).wait())


def rear(r, sizes, place, heads, crossed):
    D, S, C = sizes["dp"], sizes["seq"], sizes["chan"]
    mine, me, ch = place
    length, width = r.sum_in.shape
    mixed = r.sum_mix.shape[1]
    half = mixed // 2
    model = r.w_in.shape[0]
    rows = length // C
    pieces, lag = PIECES, PIECES // 2
    size = width // pieces
    strips = width // LANES
    per = pieces // strips
    parts = C
    cut = model // parts
    terms, outs, scratch = (r.state_term, r.back_term), (r.start, r.end), (r.scr0, r.scr1)
    spots = (me, S - 1 - me)
    above, below = lax.rem(me + 1, S), lax.rem(me + S - 1, S)
    others = [lax.rem(mine + e, D) for e in range(1, D)]

    def carry(way, piece, first=False):
        part = pl.ds(pl.multiple_of(piece * size, size), size)
        source = terms[way] if first else scratch[way]
        sems = r.chain_s.at[way], r.chain_r.at[way, piece]
        return rcopy(source.at[part], outs[way].at[part], *sems, seq=above if way == 0 else below)

    for way in (1, 0):

        @pl.when(spots[way] == 0)
        def _(way=way):
            for piece in range(pieces):
                carry(way, piece, True).start()
            outs[way][...] = jnp.zeros(outs[way].shape, BF)

    def beat(t):
        for way in (1, 0):
            spot = spots[way]
            piece = t - lag * (spot - 1)

            @pl.when((piece >= 0) & (piece < pieces) & (spot > 0) & (spot < S - 1))
            def _(way=way, piece=piece):
                carry(way, piece).wait_recv()
                part = pl.ds(pl.multiple_of(piece * size, size), size)
                before = outs[way][part, :].astype(F32)
                term = terms[way][part, :].astype(F32)
                scratch[way][part, :] = (r.decay[part, :] * before + term).astype(BF)
                carry(way, piece).start()

    def gather(q, landing, slot):
        return rcopy(r.xs, r.xc.at[:, :, landing], r.gat_s.at[q], r.gat_r.at[slot], chan=q)

    spread = head_mask(width, True)
    cumulative = r.cum[...]
    across = cumulative.T
    row = lax.broadcasted_iota(jnp.int32, (length, length), 0)
    col = lax.broadcasted_iota(jnp.int32, (length, length), 1)
    causal = row >= col
    lower = causal.astype(F32)
    into, out_of = r.mix[:, :half], r.mix[:, half:]
    scores = mm(out_of, into, 1, 1)
    r.stepped[...] = (r.act[...] * r.step_wide[...]).astype(BF)
    inner = r.sum_in[...]
    gate = jax.nn.sigmoid(inner)
    r.slope_in[...] = gate * (1.0 + inner * (1.0 - gate))
    skip_wide = exact(jnp.broadcast_to(r.vec[2:3, :], (8, LANES)), spread)
    r.skips[...] = skip_wide
    r.pad_in[length:, :] = jnp.zeros((8, width), F32)
    r.pad_mix[length:, :] = jnp.zeros((8, mixed), F32)

    def head(h):
        cols = slice(h * HDIM, (h + 1) * HDIM)
        gap = cumulative[:, h : h + 1] - across[h : h + 1, :]
        decay = jnp.where(causal, jnp.exp(jnp.where(causal, gap, 0.0)), 0.0)
        weights = (decay * scores).astype(BF)
        grad_h, step_h = r.grad[:, cols], r.stepped[:, cols]
        term = decay * mm(grad_h, step_h, 1, 1)
        r.score_grad[...] = term if h == 0 else r.score_grad[...] + term
        r.z[:, cols] = mm(weights, grad_h, 0, 0)
        r.y[:, cols] = mm(weights, step_h, 1, 0)

    def strip(j):
        return slice(j * LANES, (j + 1) * LANES)

    def halo(j):
        return rcopy(r.hal_o.at[j], r.hal_i.at[j], r.hal_s.at[0], r.hal_r.at[j], seq=below)

    def strip_sum(j):
        cols = strip(j)

        @pl.when(spots[1] == S - 1)
        def _():
            for piece in range(j * per, (j + 1) * per):
                carry(1, piece).wait_recv()

        ending = r.fading[:, cols] * mm(into, r.end[cols, :], 1, 1)
        r.ending[:, cols] = ending
        direct = r.skips[0:1, cols] * r.grad[:, cols].astype(F32)
        total = (r.step_wide[:, cols] * (r.z[:, cols] + ending) + direct) * r.slope_in[:, cols]
        r.pad_in[0:length, cols] = total
        r.hal_o[j] = total[0:8, :]

        @pl.when(me > 0)
        def _():
            halo(j).start()

    def part(p, e, k):
        return r.gin.at[k, e, :, pl.ds(p * LANES, LANES)]

    def zcopy(p, way, k):
        send = (r.u_s if way == "up" else r.d_s).at[k]
        here = part(p, mine, k)
        return rcopy(here, here, send, r.z_r.at[p, k], seq=above if way == "up" else below)

    def ccopy(p, k, e, to):
        return rcopy(part(p, e, k), part(p, e, k), r.x_s.at[to, k], r.c_r.at[e, k], dp=to)

    def strip_out(j):
        cols = strip(j)

        @pl.when(me < S - 1)
        def _():
            halo(j).wait_recv()
            r.pad_in[length:, cols] = r.hal_i[j]

        r.gin[me, mine, :, cols] = spread_back(r.pad_in, r.conv_in, 0, length, cols)
        for e in others:
            ccopy(j, me, mine, e).start()

    def strip_along(j):
        @pl.when(me < S - 1)
        def _():
            zcopy(j, "up", me).start()

        @pl.when(me > 0)
        def _():
            zcopy(j, "down", me).start()

    beats = pieces + lag * max(S - 3, 0)
    early = heads // 2
    for h in range(early):
        head(h)
    near = spots[1] <= 1
    crossed()
    each(C, lambda d: gather(lax.rem(ch + d, C), ch, ch).start())
    r.xc[:, :, ch] = r.xs[...]
    if beats <= 24:
        sums = {per * j + per - 1: j for j in range(strips)}
        late = {lag + t: j for t, j in sums.items()}
        for t in range(max(beats, heads - early)):
            beat(t)
            if early + t < heads:
                head(early + t)
            if t in sums:
                pl.when(near)(functools.partial(strip_sum, sums[t]))
            if t in late:
                pl.when(near)(functools.partial(strip_out, late[t]))
                pl.when(spots[1] == 2)(functools.partial(strip_sum, late[t]))
        for j in range(strips):
            pl.when(spots[1] > 2)(functools.partial(strip_sum, j))
            pl.when(spots[1] > 1)(functools.partial(strip_out, j))
            strip_along(j)
    else:
        for h in range(early, heads):
            head(h)
        lax.fori_loop(0, beats, lambda t, c: (beat(t), c)[1], 0)
        for j in range(strips):
            strip_sum(j)
        for j in range(strips):
            strip_out(j)
            strip_along(j)

    @pl.when(spots[0] == S - 1)
    def _():
        for piece in range(pieces):
            carry(0, piece).wait_recv()

    start, end = r.start[...], r.end[...]
    score_grad = r.score_grad[...]
    mixer = r.sum_mix[...]
    gate = jax.nn.sigmoid(mixer)
    mixer_slope = gate * (1.0 + mixer * (1.0 - gate))
    faded = (r.fading[...] * r.stepped[...].astype(F32)).astype(BF)
    into_grad = mm(score_grad, out_of, 0, 0) + mm(faded, end, 1, 0)
    out_grad = mm(score_grad, into, 1, 0) + mm(r.pulled[...], start, 1, 0)
    r.pad_mix[0:length, :half] = into_grad * mixer_slope[:, :half]
    r.pad_mix[0:length, half:] = out_grad * mixer_slope[:, half:]
    r.am[0:length, :] = r.pad_mix[0:length, :].astype(BF)
    r.am[length:, :] = jnp.zeros((PAD, mixed), BF)
    r.halm_o[...] = r.pad_mix[0:8, :]

    def share_mix(q, landing, slot):
        some = r.am.at[pl.ds(pl.multiple_of(q * rows, rows), rows + PAD)]
        return rcopy(some, r.gm_in.at[landing], r.gm_s.at[q], r.gm_r.at[slot], chan=q)

    def mix_tail(slot):
        return rcopy(
            r.am.at[pl.ds(0, PAD)], r.mt_in.at[slot], r.mt_s.at[0], r.mt_r.at[slot],
            seq=below, chan=jnp.int32(C - 1),
        )

    def mix_halo():
        return rcopy(r.halm_o, r.halm_i, r.halm_s.at[0], r.halm_s.at[1], seq=below)

    each(C, lambda d: share_mix(lax.rem(ch + d, C), ch, ch).start())

    @pl.when(me > 0)
    def _():
        mix_tail(ch).start()
        mix_halo().start()

    r.gm_in[ch] = r.am[pl.ds(pl.multiple_of(ch * rows, rows), rows + PAD), :]
    r.gmp[...] = spread_back(r.pad_mix, r.conv_mix, 0, length)

    def forward(p, way, d):
        k = me - d if way == "up" else me + d
        there = (k >= 0) if way == "up" else (k < S)
        more = (me < S - 1) if way == "up" else (me > 0)

        @pl.when(there)
        def _():
            zcopy(p, way, k).wait_recv()

        @pl.when(there & more)
        def _():
            zcopy(p, way, k).start()

        @pl.when(there)
        def _():
            for e in others:
                ccopy(p, k, mine, e).start()

    def both(p, d):
        forward(p, "up", d)
        forward(p, "down", d)

    def hop(d):
        for p in range(strips):
            both(p, d)

    upstream = r.grad[...].astype(F32)
    stepped = r.stepped[...].astype(F32)
    ending = r.ending[...]
    carried = r.grown[...] * mm(out_of, start, 1, 1)
    to_heads = functools.partial(exact, b=spread, da=1, db=1)
    z = r.z[...]
    step_grad = to_heads(r.act[...] * (z + ending))
    tail_term = to_heads(stepped * ending)
    sum_grad = to_heads(upstream * (r.y[...] + carried) - stepped * z) - tail_term
    held = jnp.sum(start.astype(F32) * end.astype(F32), axis=1, keepdims=True)
    last = cumulative[length - 1 : length, :]
    overall = jnp.sum(tail_term, axis=0, keepdims=True) + jnp.exp(last) * jnp.sum(
        head_mask(width, False) * held, axis=0, keepdims=True
    )
    decay_grad = exact_left(lower, sum_grad, 0, 0) + overall
    rate = jnp.exp(r.vec[1:2, :])
    step_grad = (step_grad - rate * decay_grad) * jax.nn.sigmoid(r.raw[...] + r.vec[0:1, :])
    steps = step_grad.astype(BF)
    r.gsm[me, mine, rows:, 0:LANES] = step_grad.T[0:PAD, :].astype(BF)
    steps = steps[:, 0:PAD]

    both(0, 1)

    each(C, lambda d: share_mix(lax.rem(ch + d, C), ch, lax.rem(ch + d, C)).wait_recv())
    mix = r.gm_in[0].astype(F32)
    for q in range(1, C):
        mix = mix + r.gm_in[q].astype(F32)
    r.gmt[...] = mix

    @pl.when((me < S - 1) & (ch == C - 1))
    def _():
        for q in range(C):
            mix_tail(q).wait_recv()
        tail = r.mt_in[0].astype(F32)
        for q in range(1, C):
            tail = tail + r.mt_in[q].astype(F32)
        r.gmt[rows:, :] = tail

    r.gsm[me, mine, 0:rows, :] = spread_back(r.gmt, r.conv_mix, 0, rows)

    def small_to(e, k, to, q):
        here = r.gsm.at[k, e]
        return rcopy(here, here, r.z2_s.at[to, q], r.z2_r.at[e, k], dp=to, seq=q)

    def small_all(do):
        each(S, lambda d: do(mine, lax.rem(me + d, S)))
        for e in others:
            do(e, me)
            each(S, lambda d, e=e: do(e, lax.rem(me + d, S)))

    small_all(lambda e, q: small_to(mine, me, e, q).start())

    both(1, 1)

    def share_p(j, q, landing, slot):
        piece = pl.ds(j * cut, cut)
        return rcopy(
            r.p_o.at[q, :, piece], r.p_i.at[landing, :, piece], r.p_s.at[q], r.p_r.at[slot], chan=q
        )

    def whole_p(q):
        return rcopy(r.p_o.at[q], r.p_i.at[q], r.p_s.at[q], r.p_r.at[q], chan=q)

    grads = r.gin[me, mine]
    mixes = r.gmp[...]

    def send_p(j, final):
        def one(d):
            q = lax.rem(ch + d, C)

            @pl.when((q == C - 1) if final else (q < C - 1))
            def _():
                share_p(j, q, ch, ch).start()

        each(C, one)

    for j in range(parts):
        piece = slice(j * cut, (j + 1) * cut)
        out = mm(grads, r.w_in[piece, :], 1, 1) + mm(mixes, r.w_mix[piece, :], 1, 1)
        out = out + mm(steps, r.wst[0:PAD, piece], 1, 0)
        r.p_o[:, :, piece] = out.astype(BF).reshape(C, rows, cut)
        r.p_last[:, piece] = out[length - PAD :, :]
        send_p(j, False)
        if j + 2 < strips:
            both(j + 2, 1)
    for p in range(parts + 2, strips):
        both(p, 1)

    @pl.when(me < S - 1)
    def _():
        mix_halo().wait_recv()
        r.pad_mix[length:, :] = r.halm_i[...]
        final = spread_back(r.pad_mix, r.conv_mix, length - PAD, PAD)
        change = final.astype(F32) - r.gmp[length - PAD :, :].astype(F32)
        fixed = r.p_last[...] + mm(change, r.w_mix[...], 1, 1)
        r.p_o[C - 1, rows - PAD :, :] = fixed.astype(BF)

    for j in range(parts):
        send_p(j, True)
    hop(2)
    small_all(lambda e, q: small_to(e, q, e, q).wait_recv())

    norm = 1.0 / math.sqrt(D * S * length)
    columns = r.xc.shape[-1]

    def settle_gather(d):
        q = lax.rem(ch + d, C)
        gather(q, q, q).wait()

    each(C, settle_gather)
    mixer_columns = r.xc[:, :, ch].reshape(S * D * rows, columns)
    mixer_grads = r.gsm[:, :, 0:rows, :].reshape(S * D * rows, mixed)
    mixer_term = norm * mm(mixer_columns, mixer_grads, 0, 0)
    band = columns // C
    for q in range(C):
        r.m_o[q] = mixer_term[q * band : (q + 1) * band, :].astype(BF)

    def share_m(q, landing, slot):
        return rcopy(r.m_o.at[q], r.m_i.at[landing], r.m_s.at[q], r.m_r.at[slot], chan=q)

    each(C, lambda d: share_m(lax.rem(ch + d, C), ch, ch).start())
    if S <= 12:
        for d in range(3, S):
            hop(d)
    else:
        lax.fori_loop(3, S, lambda d, c: (hop(d), c)[1], 0)

    def step_term(k, total):
        for e in range(D):
            x = r.xc[k, e].reshape(length, columns)
            total = total + mm(r.gsm[k, e, rows:, 0:LANES], x, 1, 0)
        return total

    step_total = jnp.zeros((PAD, columns), F32)
    if S <= 12:
        for k in range(S):
            step_total = step_term(k, step_total)
    else:
        step_total = lax.fori_loop(0, S, step_term, step_total)
    r.o_dws[...] = (norm * step_total)[:heads, :]

    def whole(k, e, send, recv):
        return rcopy(r.gin.at[k, e], r.gin.at[k, e], send, recv, seq=above)

    def weight_term(k, first=False):
        for e in others:
            whole(k, e, r.x_s.at[e, k], r.c_r.at[e, k]).wait_recv()
        x = r.xc[k].reshape(D * length, columns)
        term = norm * mm(x, r.gin[k].reshape(D * length, width), 0, 0)
        r.o_dw[...] = term if first else r.o_dw[...] + term

    def weight_terms(d):
        for k, there in ((me + d, me + d < S), (me - d, me >= d)):
            pl.when(there)(functools.partial(weight_term, k))

    weight_term(me, True)
    each(S, weight_terms)
    r.p_i[ch] = r.p_o[ch]
    r.m_i[ch] = r.m_o[ch]
    each(C, lambda d: whole_p(lax.rem(ch + d, C)).wait_recv())
    each(C, lambda d: share_m(lax.rem(ch + d, C), ch, lax.rem(ch + d, C)).wait_recv())

    for way in (0, 1):

        @pl.when(spots[way] < S - 1)
        def _(way=way):
            rcopy(terms[way], outs[way], r.chain_s.at[way], r.chain_r.at[way, 0], seq=above).wait_send()

    @pl.when(me > 0)
    def _():
        rcopy(r.hal_o, r.hal_i, r.hal_s.at[0], r.hal_r.at[0], seq=below).wait_send()
        mix_halo().wait_send()
        mix_tail(ch).wait_send()

    def settle_chan(d):
        q = lax.rem(ch + d, C)
        share_mix(q, ch, ch).wait_send()
        share_m(q, ch, ch).wait_send()
        whole_p(q).wait_send()

    each(C, settle_chan)

    def settle_line(k):
        for e in others:
            whole(k, mine, r.x_s.at[e, k], r.c_r.at[mine, k]).wait_send()
        for way, sent in (("up", (k <= me) & (me < S - 1)), ("down", (k >= me) & (me > 0))):

            @pl.when(sent)
            def _(way=way):
                whole(k, mine, (r.u_s if way == "up" else r.d_s).at[k], r.z_r.at[0, k]).wait_send()

    settle_line(0)
    each(S, settle_line)
    small_all(lambda e, q: small_to(mine, me, e, q).wait_send())


def finish_kernel(parts, dw, mixes, dws, o_ig, o_dw, o_dwm, o_dws, ig, dwm, sems):
    copies = [
        pltpu.make_async_copy(a, b, sems.at[i])
        for i, (a, b) in enumerate(((dw, o_dw), (dws, o_dws), (ig, o_ig), (dwm, o_dwm)))
    ]
    copies[0].start()
    copies[1].start()
    total = parts[0].astype(F32)
    for q in range(1, parts.shape[0]):
        total = total + parts[q].astype(F32)
    ig[...] = total.astype(BF)
    copies[2].start()
    total = mixes[0].astype(F32)
    for q in range(1, mixes.shape[0]):
        total = total + mixes[q].astype(F32)
    dwm[...] = total
    copies[3].start()
    for copy in copies:
        copy.wait()


def body(
    sizes,
    layer_input,
    inner_weight,
    mixer_weight,
    step_weight,
    conv_inner,
    conv_mixer,
    step_bias,
    decay_log,
    skip_gain,
    output_grad,
):
    own = layer_input[0]
    rows, model = own.shape
    chans, seqs, dps = sizes["chan"], sizes["seq"], sizes["dp"]
    groups = dps * seqs
    length = rows * chans
    width = inner_weight.shape[1]
    mixed = mixer_weight.shape[1]
    heads = step_bias.shape[0]
    cols = model // groups
    state_size = mixed // 2
    assert width % PIECES == 0 and chans % 2 == 0 and seqs > 2
    assert width % LANES == 0 and PIECES % (width // LANES) == 0
    assert length == LANES and heads + conv_inner.shape[0] - 1 <= PAD
    upstream = output_grad[0]
    step_rows = step_weight.T
    bias, rates, skips = (v.reshape(1, heads) for v in (step_bias, decay_log, skip_gain))
    dma = pltpu.SemaphoreType.DMA
    vmem = pl.BlockSpec(memory_space=pltpu.VMEM)
    hbm = pl.BlockSpec(memory_space=pltpu.HBM)
    small = rows + PAD
    strips = width // LANES
    band = cols // chans

    def low(*shape):
        return pltpu.VMEM(shape, BF)

    def full(*shape):
        return pltpu.VMEM(shape, F32)

    inputs = dict(
        own=own, w_in=inner_weight, w_mix=mixer_weight, w_step=step_rows, conv_in=conv_inner,
        conv_mix=conv_mixer, bias=bias, log=rates, skip=skips, grad=upstream,
    )
    outputs = dict(
        p_i=jax.ShapeDtypeStruct((chans, rows, model), BF),
        o_dw=jax.ShapeDtypeStruct((cols, width), F32),
        m_i=jax.ShapeDtypeStruct((chans, band, mixed), BF),
        o_dws=jax.ShapeDtypeStruct((heads, cols), F32),
    )
    scratch = {key: pltpu.VMEM(v.shape, v.dtype) for key, v in inputs.items()}
    scratch |= dict(
        wst=low(LANES, model), xg=low(length, model),
        blocks=low(dps, seqs, rows, cols),
        xs=low(seqs, dps, rows, cols), xc=low(seqs, dps, chans, rows, cols),
        wide_in=full(PAD + length, width), wide_mix=full(PAD + length, mixed),
        fh_o=low(PAD, width + mixed), fh_i=low(PAD, width + mixed), vec=full(8, LANES),
        sum_in=full(length, width), sum_mix=full(length, mixed), raw=full(length, LANES),
        cum=full(length, LANES), step_wide=full(length, width), fading=full(length, width),
        grown=full(length, width), pulled=low(length, width), decay=full(width, state_size),
        mix=low(length, mixed), act=full(length, width), stepped=low(length, width),
        state_term=low(width, state_size), back_term=low(width, state_size),
        start=low(width, state_size), end=low(width, state_size),
        scr0=low(width, state_size), scr1=low(width, state_size),
        z=full(length, width), y=full(length, width), score_grad=full(length, length),
        slope_in=full(length, width),
        pad_in=full(length + 8, width), pad_mix=full(length + 8, mixed),
        gin=low(seqs, dps, length, width), gsm=low(seqs, dps, small, mixed),
        hal_o=full(strips, 8, LANES), hal_i=full(strips, 8, LANES),
        halm_o=full(8, mixed), halm_i=full(8, mixed), p_last=full(PAD, model),
        skips=full(8, width), ending=full(length, width),
        gmp=low(length, mixed), gm_in=low(chans, small, mixed), gmt=full(small, mixed),
        am=low(length + PAD, mixed), mt_in=low(chans, PAD, mixed),
        p_o=low(chans, rows, model), m_o=low(chans, band, mixed),
        load_sem=dma((len(LOADED),)), fh_sem=dma((2,)), halm_s=dma((2,)),
        hal_s=dma((1,)), hal_r=dma((strips,)),
        near_s=dma((1,)), near_r=dma((chans,)),
        far_s=dma((chans // 2,)), far_r=dma((chans // 2, chans)),
        relay_s=dma((chans // 2,)), relay_r=dma((chans // 2, chans)),
        cross_s=dma((dps, seqs)), cross_r=dma((dps, seqs)),
        gat_s=dma((chans,)), gat_r=dma((chans,)),
        chain_s=dma((2,)), chain_r=dma((2, PIECES)),
        z_r=dma((strips, seqs)), c_r=dma((dps, seqs)),
        u_s=dma((seqs,)), d_s=dma((seqs,)), x_s=dma((dps, seqs)),
        z2_r=dma((dps, seqs)),
        z2_s=dma((dps, seqs)), mt_s=dma((1,)), mt_r=dma((chans,)),
        gm_s=dma((chans,)), gm_r=dma((chans,)),
        p_s=dma((chans,)), p_r=dma((chans,)), m_s=dma((chans,)), m_r=dma((chans,)),
    )
    names = [key + "_h" for key in inputs] + list(outputs) + list(scratch)
    parts, inner_grad, mix_parts, step_grad = pl.pallas_call(
        functools.partial(layer_kernel, names, sizes, heads),
        out_shape=tuple(outputs.values()),
        in_specs=[hbm] * len(inputs),
        out_specs=(vmem,) * len(outputs),
        scratch_shapes=list(scratch.values()),
        compiler_params=pltpu.CompilerParams(
            collective_id=0, has_side_effects=True, vmem_limit_bytes=LIMIT
        ),
        name="layer",
    )(*(pltpu.with_memory_space_constraint(v, pltpu.HBM) for v in inputs.values()))
    input_grad, inner_grad, mixer_grad, step_grad = pl.pallas_call(
        finish_kernel,
        out_shape=(
            jax.ShapeDtypeStruct((rows, model), BF),
            jax.ShapeDtypeStruct((cols, width), F32),
            jax.ShapeDtypeStruct((band, mixed), F32),
            jax.ShapeDtypeStruct((heads, cols), F32),
        ),
        in_specs=[vmem] * 4,
        out_specs=(pl.BlockSpec(memory_space=pl.ANY),) * 4,
        scratch_shapes=[
            pltpu.VMEM((rows, model), BF),
            pltpu.VMEM((band, mixed), F32),
            dma((4,)),
        ],
        compiler_params=pltpu.CompilerParams(vmem_limit_bytes=LIMIT),
        name="finish",
    )(parts, inner_grad, mix_parts, step_grad)
    return input_grad[None], inner_grad, mixer_grad, step_grad.T


def solution(mesh):
    sizes = dict(mesh.shape)
    in_specs = (
        P("dp", ("seq", "chan"), None),
        P(None, "chan"),
        P(),
        P(None, "chan"),
        P(None, "chan"),
        P(),
        P("chan"),
        P("chan"),
        P("chan"),
        P("dp", "seq", "chan"),
    )
    out_specs = (
        P("dp", ("seq", "chan"), None),
        P(("dp", "seq"), "chan"),
        P(("dp", "seq", "chan"), None),
        P(("dp", "seq"), "chan"),
    )
    return jax.shard_map(
        functools.partial(body, sizes),
        mesh=mesh,
        in_specs=in_specs,
        out_specs=out_specs,
        check_vma=False,
    )
```

```python
import functools
import math
import types

import jax
import jax.numpy as jnp
from jax import lax
from jax.experimental import pallas as pl
from jax.experimental.pallas import tpu as pltpu
from jax.sharding import PartitionSpec as P

MESH = pl.DeviceIdType.MESH
HDIM = 64
PAD = 16
LANES = 128
LIMIT = 48 * 2**20
BF = jnp.bfloat16
F32 = jnp.float32
PIECES = 10
LOADED = (
    "own", "w_in", "w_mix", "w_step", "conv_in", "conv_mix", "bias", "log", "skip", "grad",
)


def each(n, step):
    if n <= 12:
        for d in range(1, n):
            step(d)
    else:

        def one(d, carry):
            step(d)
            return carry

        lax.fori_loop(1, n, one, 0)


def signal_to(barrier, where):
    pl.semaphore_signal(barrier, inc=1, device_id=where, device_id_type=MESH)


def mm(a, b, da, db):
    return lax.dot_general(
        a.astype(BF), b.astype(BF), (((da,), (db,)), ((), ())), preferred_element_type=F32
    )


def thirds(v):
    high = v.astype(BF)
    rest = v - high.astype(F32)
    middle = rest.astype(BF)
    return high, middle, (rest - middle.astype(F32)).astype(BF)


def exact(a, b, da=1, db=0):
    high, middle, low = thirds(a)
    return mm(high, b, da, db) + (mm(middle, b, da, db) + mm(low, b, da, db))


def exact_left(a, b, da=1, db=0):
    high, middle, low = thirds(b)
    return mm(a, high, da, db) + (mm(a, middle, da, db) + mm(a, low, da, db))


def softplus(v):
    return jnp.maximum(v, 0.0) + jnp.log1p(jnp.exp(-jnp.abs(v)))


def head_mask(width, heads_first):
    shape = (LANES, width) if heads_first else (width, LANES)
    head = lax.broadcasted_iota(jnp.int32, shape, 0 if heads_first else 1)
    column = lax.broadcasted_iota(jnp.int32, shape, 1 if heads_first else 0)
    return (column // HDIM == head).astype(F32)


def decays(raw, bias, decay_log):
    length = raw.shape[0]
    step = softplus(raw + bias)
    rate = jnp.exp(decay_log)
    row = lax.broadcasted_iota(jnp.int32, (length, length), 0)
    col = lax.broadcasted_iota(jnp.int32, (length, length), 1)
    lower = (row >= col).astype(F32)
    cumulative = exact_left(lower, -step * rate)
    return step, rate, cumulative, row, col, lower


def rcopy(src, dst, send, recv, **where):
    return pltpu.make_async_remote_copy(
        src_ref=src, dst_ref=dst, send_sem=send, recv_sem=recv, device_id=where, device_id_type=MESH
    )


def greet_all(barrier, axis, n):
    me = lax.axis_index(axis)
    each(n, lambda d: signal_to(barrier, {axis: lax.rem(me + d, n)}))
    return n - 1


def convolved(wide, kernel, first, count):
    taps = kernel.shape[0]
    first = first + PAD - (taps - 1)
    total = kernel[0:1, :] * wide[pl.ds(first, count), :]
    for k in range(1, taps):
        total = total + kernel[k : k + 1, :] * wide[pl.ds(first + k, count), :]
    return total


def spread_back(pad, kernel, first, count, cols=slice(None)):
    taps = kernel.shape[0]
    total = None
    for k in range(taps):
        term = kernel[k : k + 1, cols] * pad[pl.ds(first + taps - 1 - k, count), cols]
        total = term if total is None else total + term
    return total.astype(BF)


def layer_kernel(names, sizes, heads, *refs):
    r = types.SimpleNamespace(**dict(zip(names, refs, strict=True)))
    place = (lax.axis_index("dp"), lax.axis_index("seq"), lax.axis_index("chan"))
    D, S, C = sizes["dp"], sizes["seq"], sizes["chan"]
    barrier = pltpu.get_barrier_semaphore()
    total = greet_all(barrier, "dp", D) + greet_all(barrier, "seq", S) + greet_all(barrier, "chan", C)
    after = lax.rem(place[1] + 1, S)

    @pl.when(place[2] == C - 1)
    def _():
        for c in range(C):
            signal_to(barrier, {"seq": after, "chan": jnp.int32(c)})

    total += 1 + (D - 1) * (S - 1)
    for e in range(1, D):
        far = lax.rem(place[0] + e, D)
        each(S, lambda d, far=far: signal_to(barrier, {"dp": far, "seq": lax.rem(place[1] + d, S)}))
    loads = {
        key: pltpu.make_async_copy(getattr(r, key + "_h"), getattr(r, key), r.load_sem.at[i])
        for i, key in enumerate(LOADED)
    }
    for copy in loads.values():
        copy.start()
    crossed = front(r, sizes, place, heads, loads, barrier, total)
    rear(r, sizes, place, heads, crossed)


def front(r, sizes, place, heads, loads, barrier, total):
    D, S, C = sizes["dp"], sizes["seq"], sizes["chan"]
    mine, me, ch = place
    rows, model = r.own.shape
    length, width = r.sum_in.shape
    mixed = r.sum_mix.shape[1]
    cols = model // (D * S)
    half = mixed // 2
    splits = 2
    high = rows // 2
    cut = model // splits
    pieces = [(1, k) for k in range(splits)] + [(0, k) for k in range(splits)]
    sides = C // 2
    side, low = lax.div(ch, 2), lax.rem(ch, 2)
    partner = ch + 1 - 2 * low

    def block(c, p):
        part, k = pieces[p]
        first = pl.multiple_of(c * rows + part * high, high)
        return r.xg.at[pl.ds(first, high), pl.ds(k * cut, cut)]

    def mine_at(p):
        part, k = pieces[p]
        return r.own.at[pl.ds(part * high, high), pl.ds(k * cut, cut)]

    def near(c, p):
        return rcopy(mine_at(p), block(c, p), r.near_s.at[0], r.near_r.at[p], chan=partner)

    def far(to, c, slot, p):
        return rcopy(
            mine_at(p), block(c, p), r.far_s.at[to], r.far_r.at[slot, p], chan=2 * to + low
        )

    def relay(source, lane, p):
        c = 2 * source + lane
        here = block(c, p)
        return rcopy(here, here, r.relay_s.at[source], r.relay_r.at[source, p], chan=partner)

    def column(e, q, landing_e, landing_q):
        return rcopy(
            r.blocks.at[e, q], r.xs.at[landing_q, landing_e],
            r.cross_s.at[e, q], r.cross_r.at[landing_e, landing_q], dp=e, seq=q,
        )

    def columns_all(do):
        each(S, lambda d: do(mine, lax.rem(me + d, S)))
        for d in range(1, D):
            e = lax.rem(mine + d, D)
            do(e, me)
            each(S, lambda d, e=e: do(e, lax.rem(me + d, S)))

    loads["own"].wait()
    pl.semaphore_wait(barrier, total)
    for p in range(len(pieces)):
        for d in range(1, sides):
            far(lax.rem(side + d, sides), ch, side, p).start()
        near(ch, p).start()
    for d in range(D):
        for k in range(S):
            at = (d * S + k) * cols
            r.blocks[d, k] = r.own[:, at : at + cols]
    columns_all(lambda e, q: column(e, q, mine, me).start())
    r.xs[me, mine] = r.blocks[mine, me]
    r.xg[pl.ds(pl.multiple_of(ch * rows, rows), rows), :] = r.own[...]
    r.wst[...] = jnp.zeros(r.wst.shape, BF)
    r.vec[...] = jnp.zeros(r.vec.shape, F32)
    for key in LOADED[1:]:
        loads[key].wait()
    r.wst[0:heads, :] = r.w_step[...]
    for i, ref in enumerate((r.bias, r.log, r.skip)):
        r.vec[i : i + 1, 0:heads] = ref[...]

    def pass_on(p):
        for d in range(1, sides):
            source = lax.rem(side + d, sides)
            far(source, ch, source, p).wait_recv()
            relay(source, low, p).start()

    def project(p):
        near(partner, p).wait_recv()
        for d in range(1, sides):
            source = lax.rem(side + d, sides)
            relay(source, 1 - low, p).wait_recv()
        part, k = pieces[p]
        piece = slice(k * cut, (k + 1) * cut)
        x = jnp.concatenate([r.xg[c * rows + part * high : c * rows + (part + 1) * high, piece] for c in range(C)])
        inner = mm(x, r.w_in[piece, :], 1, 0)
        mixer = mm(x, r.w_mix[piece, :], 1, 0)
        raw = mm(x, r.wst[:, piece], 1, 1)
        for c in range(C):
            at = c * rows + part * high
            here = slice(c * high, (c + 1) * high)
            for ref, pad, term in ((r.wide_in, PAD, inner), (r.wide_mix, PAD, mixer), (r.raw, 0, raw)):
                old = ref[pad + at : pad + at + high, :] if k else 0.0
                ref[pad + at : pad + at + high, :] = old + term[here, :]

    def halo():
        return rcopy(r.fh_o, r.fh_i, r.fh_sem.at[0], r.fh_sem.at[1], seq=lax.rem(me + 1, S))

    pass_on(0)
    for p in range(len(pieces)):
        if p + 1 < len(pieces):
            pass_on(p + 1)
        project(p)
        if p == splits - 1:
            r.fh_o[:, :width] = r.wide_in[length:, :].astype(BF)
            r.fh_o[:, width:] = r.wide_mix[length:, :].astype(BF)
            pl.when(me < S - 1)(lambda: halo().start())
    inner_low = r.wide_in[PAD:, :].astype(BF)
    mixer_low = r.wide_mix[PAD:, :].astype(BF)
    r.wide_in[PAD:, :] = inner_low.astype(F32)
    r.wide_mix[PAD:, :] = mixer_low.astype(F32)
    r.wide_in[0:PAD, :] = jnp.zeros((PAD, width), F32)
    r.wide_mix[0:PAD, :] = jnp.zeros((PAD, mixed), F32)
    r.sum_in[PAD:, :] = convolved(r.wide_in, r.conv_in, PAD, length - PAD)
    r.sum_mix[PAD:, :] = convolved(r.wide_mix, r.conv_mix, PAD, length - PAD)
    step, rate, cumulative, row, col, lower = decays(r.raw[...], r.vec[0:1, :], r.vec[1:2, :])
    last = cumulative[length - 1 : length, :]
    spread = head_mask(width, True)
    r.cum[...] = cumulative
    step_wide = exact(step, spread)
    fading = exact(jnp.exp(last - cumulative), spread)
    grown = exact(jnp.exp(cumulative), spread)
    r.step_wide[...] = step_wide
    r.fading[...] = fading
    r.grown[...] = grown
    pulled = (grown * r.grad[...].astype(F32)).astype(BF)
    r.pulled[...] = pulled
    row_decay = jnp.sum(head_mask(width, False) * jnp.exp(last), axis=1, keepdims=True)
    r.decay[...] = jnp.broadcast_to(row_decay, r.decay.shape)

    @pl.when(me > 0)
    def _():
        halo().wait_recv()
        r.wide_in[0:PAD, :] = r.fh_i[:, :width].astype(F32)
        r.wide_mix[0:PAD, :] = r.fh_i[:, width:].astype(F32)

    r.sum_in[0:PAD, :] = convolved(r.wide_in, r.conv_in, 0, PAD)
    r.sum_mix[0:PAD, :] = convolved(r.wide_mix, r.conv_mix, 0, PAD)
    mixer = r.sum_mix[...]
    mix = mixer * jax.nn.sigmoid(mixer)
    r.mix[...] = mix.astype(BF)
    r.back_term[...] = mm(pulled, mix[:, half:], 0, 0).astype(BF)
    inner = r.sum_in[...]
    act = inner * jax.nn.sigmoid(inner)
    r.act[...] = act
    r.state_term[...] = mm(act * (fading * step_wide), mix[:, :half], 0, 0).astype(BF)

    @pl.when(me < S - 1)
    def _():
        halo().wait_send()

    def sent(sem):
        rcopy(r.own, r.own, sem, r.near_r.at[0], chan=partner).wait_send()

    sent(r.near_s.at[0])
    for d in range(1, sides):
        source = lax.rem(side + d, sides)
        sent(r.far_s.at[source])
        sent(r.relay_s.at[source])
    return lambda: columns_all(lambda e, q: column(e, q, e, q).wait())


def rear(r, sizes, place, heads, crossed):
    D, S, C = sizes["dp"], sizes["seq"], sizes["chan"]
    mine, me, ch = place
    length, width = r.sum_in.shape
    mixed = r.sum_mix.shape[1]
    half = mixed // 2
    model = r.w_in.shape[0]
    rows = length // C
    pieces, lag = PIECES, PIECES // 2
    size = width // pieces
    strips = width // LANES
    per = pieces // strips
    parts = C
    cut = model // parts
    terms, outs, scratch = (r.state_term, r.back_term), (r.start, r.end), (r.scr0, r.scr1)
    spots = (me, S - 1 - me)
    above, below = lax.rem(me + 1, S), lax.rem(me + S - 1, S)
    others = [lax.rem(mine + e, D) for e in range(1, D)]

    def carry(way, piece, first=False):
        part = pl.ds(pl.multiple_of(piece * size, size), size)
        source = terms[way] if first else scratch[way]
        sems = r.chain_s.at[way], r.chain_r.at[way, piece]
        return rcopy(source.at[part], outs[way].at[part], *sems, seq=above if way == 0 else below)

    for way in (1, 0):

        @pl.when(spots[way] == 0)
        def _(way=way):
            for piece in range(pieces):
                carry(way, piece, True).start()
            outs[way][...] = jnp.zeros(outs[way].shape, BF)

    def beat(t):
        for way in (1, 0):
            spot = spots[way]
            piece = t - lag * (spot - 1)

            @pl.when((piece >= 0) & (piece < pieces) & (spot > 0) & (spot < S - 1))
            def _(way=way, piece=piece):
                carry(way, piece).wait_recv()
                part = pl.ds(pl.multiple_of(piece * size, size), size)
                before = outs[way][part, :].astype(F32)
                term = terms[way][part, :].astype(F32)
                scratch[way][part, :] = (r.decay[part, :] * before + term).astype(BF)
                carry(way, piece).start()

    def gather(q, landing, slot):
        return rcopy(r.xs, r.xc.at[:, :, landing], r.gat_s.at[q], r.gat_r.at[slot], chan=q)

    spread = head_mask(width, True)
    cumulative = r.cum[...]
    across = cumulative.T
    row = lax.broadcasted_iota(jnp.int32, (length, length), 0)
    col = lax.broadcasted_iota(jnp.int32, (length, length), 1)
    causal = row >= col
    lower = causal.astype(F32)
    into, out_of = r.mix[:, :half], r.mix[:, half:]
    scores = mm(out_of, into, 1, 1)
    r.stepped[...] = (r.act[...] * r.step_wide[...]).astype(BF)
    inner = r.sum_in[...]
    gate = jax.nn.sigmoid(inner)
    r.slope_in[...] = gate * (1.0 + inner * (1.0 - gate))
    skip_wide = exact(jnp.broadcast_to(r.vec[2:3, :], (8, LANES)), spread)
    r.skips[...] = skip_wide
    r.pad_in[length:, :] = jnp.zeros((8, width), F32)
    r.pad_mix[length:, :] = jnp.zeros((8, mixed), F32)

    def head(h):
        cols = slice(h * HDIM, (h + 1) * HDIM)
        gap = cumulative[:, h : h + 1] - across[h : h + 1, :]
        decay = jnp.where(causal, jnp.exp(jnp.where(causal, gap, 0.0)), 0.0)
        weights = (decay * scores).astype(BF)
        grad_h, step_h = r.grad[:, cols], r.stepped[:, cols]
        term = decay * mm(grad_h, step_h, 1, 1)
        r.score_grad[...] = term if h == 0 else r.score_grad[...] + term
        r.z[:, cols] = mm(weights, grad_h, 0, 0)
        r.y[:, cols] = mm(weights, step_h, 1, 0)

    def strip(j):
        return slice(j * LANES, (j + 1) * LANES)

    def halo(j):
        return rcopy(r.hal_o.at[j], r.hal_i.at[j], r.hal_s.at[0], r.hal_r.at[j], seq=below)

    def strip_sum(j):
        cols = strip(j)

        @pl.when(spots[1] == S - 1)
        def _():
            for piece in range(j * per, (j + 1) * per):
                carry(1, piece).wait_recv()

        ending = r.fading[:, cols] * mm(into, r.end[cols, :], 1, 1)
        r.ending[:, cols] = ending
        direct = r.skips[0:1, cols] * r.grad[:, cols].astype(F32)
        total = (r.step_wide[:, cols] * (r.z[:, cols] + ending) + direct) * r.slope_in[:, cols]
        r.pad_in[0:length, cols] = total
        r.hal_o[j] = total[0:8, :]

        @pl.when(me > 0)
        def _():
            halo(j).start()

    def part(p, e, k):
        return r.gin.at[k, e, :, pl.ds(p * LANES, LANES)]

    def zcopy(p, way, k):
        send = (r.u_s if way == "up" else r.d_s).at[k]
        here = part(p, mine, k)
        return rcopy(here, here, send, r.z_r.at[p, k], seq=above if way == "up" else below)

    def ccopy(p, k, e, to):
        return rcopy(part(p, e, k), part(p, e, k), r.x_s.at[to, k], r.c_r.at[e, k], dp=to)

    def strip_out(j):
        cols = strip(j)

        @pl.when(me < S - 1)
        def _():
            halo(j).wait_recv()
            r.pad_in[length:, cols] = r.hal_i[j]

        r.gin[me, mine, :, cols] = spread_back(r.pad_in, r.conv_in, 0, length, cols)
        for e in others:
            ccopy(j, me, mine, e).start()

    def strip_up(j):
        zcopy(j, "up", me).start()

    def strip_early(j):
        strip_out(j)
        strip_up(j)

    def strip_along(j, sent):
        @pl.when((me < S - 1) & (spots[1] != 2) if sent else me < S - 1)
        def _():
            strip_up(j)

        @pl.when(me > 0)
        def _():
            zcopy(j, "down", me).start()

    beats = pieces + lag * max(S - 3, 0)
    early = heads // 2
    for h in range(early):
        head(h)
    near = spots[1] <= 1
    crossed()
    each(C, lambda d: gather(lax.rem(ch + d, C), ch, ch).start())
    r.xc[:, :, ch] = r.xs[...]
    if beats <= 24:
        sums = {per * j + per - 1: j for j in range(strips)}
        late = {lag + t: j for t, j in sums.items()}
        for t in range(max(beats, heads - early)):
            beat(t)
            if early + t < heads:
                head(early + t)
            if t in sums:
                pl.when(near)(functools.partial(strip_sum, sums[t]))
            if t in late:
                pl.when(near)(functools.partial(strip_out, late[t]))
                pl.when(spots[1] == 2)(functools.partial(strip_sum, late[t]))
            if t - 2 in late:
                pl.when(spots[1] == 2)(functools.partial(strip_early, late[t - 2]))
        done = {j: t + 2 < max(beats, heads - early) for t, j in late.items()}
        for j in range(strips):
            pl.when(spots[1] > 2)(functools.partial(strip_sum, j))
            pl.when(spots[1] > (2 if done[j] else 1))(functools.partial(strip_out, j))
            strip_along(j, done[j])
    else:
        for h in range(early, heads):
            head(h)
        lax.fori_loop(0, beats, lambda t, c: (beat(t), c)[1], 0)
        for j in range(strips):
            strip_sum(j)
        for j in range(strips):
            strip_out(j)
            strip_along(j, False)

    @pl.when(spots[0] == S - 1)
    def _():
        for piece in range(pieces):
            carry(0, piece).wait_recv()

    start, end = r.start[...], r.end[...]
    score_grad = r.score_grad[...]
    mixer = r.sum_mix[...]
    gate = jax.nn.sigmoid(mixer)
    mixer_slope = gate * (1.0 + mixer * (1.0 - gate))
    faded = (r.fading[...] * r.stepped[...].astype(F32)).astype(BF)
    into_grad = mm(score_grad, out_of, 0, 0) + mm(faded, end, 1, 0)
    out_grad = mm(score_grad, into, 1, 0) + mm(r.pulled[...], start, 1, 0)
    r.pad_mix[0:length, :half] = into_grad * mixer_slope[:, :half]
    r.pad_mix[0:length, half:] = out_grad * mixer_slope[:, half:]
    r.am[0:length, :] = r.pad_mix[0:length, :].astype(BF)
    r.am[length:, :] = jnp.zeros((PAD, mixed), BF)
    r.halm_o[...] = r.pad_mix[0:8, :]

    def share_mix(q, landing, slot):
        some = r.am.at[pl.ds(pl.multiple_of(q * rows, rows), rows + PAD)]
        return rcopy(some, r.gm_in.at[landing], r.gm_s.at[q], r.gm_r.at[slot], chan=q)

    def mix_tail(slot):
        return rcopy(
            r.am.at[pl.ds(0, PAD)], r.mt_in.at[slot], r.mt_s.at[0], r.mt_r.at[slot],
            seq=below, chan=jnp.int32(C - 1),
        )

    def mix_halo():
        return rcopy(r.halm_o, r.halm_i, r.halm_s.at[0], r.halm_s.at[1], seq=below)

    each(C, lambda d: share_mix(lax.rem(ch + d, C), ch, ch).start())

    @pl.when(me > 0)
    def _():
        mix_tail(ch).start()
        mix_halo().start()

    r.gm_in[ch] = r.am[pl.ds(pl.multiple_of(ch * rows, rows), rows + PAD), :]
    r.gmp[...] = spread_back(r.pad_mix, r.conv_mix, 0, length)

    def forward(p, way, d):
        k = me - d if way == "up" else me + d
        there = (k >= 0) if way == "up" else (k < S)
        more = (me < S - 1) if way == "up" else (me > 0)

        @pl.when(there)
        def _():
            zcopy(p, way, k).wait_recv()

        @pl.when(there & more)
        def _():
            zcopy(p, way, k).start()

        @pl.when(there)
        def _():
            for e in others:
                ccopy(p, k, mine, e).start()

    def both(p, d):
        forward(p, "up", d)
        forward(p, "down", d)

    def hop(d):
        for p in range(strips):
            both(p, d)

    upstream = r.grad[...].astype(F32)
    stepped = r.stepped[...].astype(F32)
    ending = r.ending[...]
    carried = r.grown[...] * mm(out_of, start, 1, 1)
    to_heads = functools.partial(exact, b=spread, da=1, db=1)
    z = r.z[...]
    step_grad = to_heads(r.act[...] * (z + ending))
    tail_term = to_heads(stepped * ending)
    sum_grad = to_heads(upstream * (r.y[...] + carried) - stepped * z) - tail_term
    held = jnp.sum(start.astype(F32) * end.astype(F32), axis=1, keepdims=True)
    last = cumulative[length - 1 : length, :]
    overall = jnp.sum(tail_term, axis=0, keepdims=True) + jnp.exp(last) * jnp.sum(
        head_mask(width, False) * held, axis=0, keepdims=True
    )
    decay_grad = exact_left(lower, sum_grad, 0, 0) + overall
    rate = jnp.exp(r.vec[1:2, :])
    step_grad = (step_grad - rate * decay_grad) * jax.nn.sigmoid(r.raw[...] + r.vec[0:1, :])
    steps = step_grad.astype(BF)
    r.gsm[me, mine, rows:, 0:LANES] = step_grad.T[0:PAD, :].astype(BF)
    steps = steps[:, 0:PAD]

    each(C, lambda d: share_mix(lax.rem(ch + d, C), ch, lax.rem(ch + d, C)).wait_recv())
    mix = r.gm_in[0].astype(F32)
    for q in range(1, C):
        mix = mix + r.gm_in[q].astype(F32)
    r.gmt[...] = mix

    @pl.when((me < S - 1) & (ch == C - 1))
    def _():
        for q in range(C):
            mix_tail(q).wait_recv()
        tail = r.mt_in[0].astype(F32)
        for q in range(1, C):
            tail = tail + r.mt_in[q].astype(F32)
        r.gmt[rows:, :] = tail

    r.gsm[me, mine, 0:rows, :] = spread_back(r.gmt, r.conv_mix, 0, rows)

    def small_to(e, k, to, q):
        here = r.gsm.at[k, e]
        return rcopy(here, here, r.z2_s.at[to, q], r.z2_r.at[e, k], dp=to, seq=q)

    def small_all(do):
        each(S, lambda d: do(mine, lax.rem(me + d, S)))
        for e in others:
            do(e, me)
            each(S, lambda d, e=e: do(e, lax.rem(me + d, S)))


    both(0, 1)

    def share_p(j, q, landing, slot):
        piece = pl.ds(j * cut, cut)
        return rcopy(
            r.p_o.at[q, :, piece], r.p_i.at[landing, :, piece], r.p_s.at[q], r.p_r.at[slot], chan=q
        )

    def whole_p(q):
        return rcopy(r.p_o.at[q], r.p_i.at[q], r.p_s.at[q], r.p_r.at[q], chan=q)

    grads = r.gin[me, mine]
    mixes = r.gmp[...]

    def send_p(j, final):
        def one(d):
            q = lax.rem(ch + d, C)

            @pl.when((q == C - 1) if final else (q < C - 1))
            def _():
                share_p(j, q, ch, ch).start()

        each(C, one)

    for j in range(parts):
        piece = slice(j * cut, (j + 1) * cut)
        out = mm(grads, r.w_in[piece, :], 1, 1) + mm(mixes, r.w_mix[piece, :], 1, 1)
        out = out + mm(steps, r.wst[0:PAD, piece], 1, 0)
        r.p_o[:, :, piece] = out.astype(BF).reshape(C, rows, cut)
        r.p_last[:, piece] = out[length - PAD :, :]
        send_p(j, False)
        if j + 1 < strips:
            both(j + 1, 1)
        if j == 1:
            small_all(lambda e, q: small_to(mine, me, e, q).start())
    for p in range(parts + 1, strips):
        both(p, 1)

    @pl.when(me < S - 1)
    def _():
        mix_halo().wait_recv()
        r.pad_mix[length:, :] = r.halm_i[...]
        final = spread_back(r.pad_mix, r.conv_mix, length - PAD, PAD)
        change = final.astype(F32) - r.gmp[length - PAD :, :].astype(F32)
        fixed = r.p_last[...] + mm(change, r.w_mix[...], 1, 1)
        r.p_o[C - 1, rows - PAD :, :] = fixed.astype(BF)

    for j in range(parts):
        send_p(j, True)
    hop(2)
    small_all(lambda e, q: small_to(e, q, e, q).wait_recv())

    norm = 1.0 / math.sqrt(D * S * length)
    columns = r.xc.shape[-1]

    def settle_gather(d):
        q = lax.rem(ch + d, C)
        gather(q, q, q).wait()

    each(C, settle_gather)
    mixer_columns = r.xc[:, :, ch].reshape(S * D * rows, columns)
    mixer_grads = r.gsm[:, :, 0:rows, :].reshape(S * D * rows, mixed)
    mixer_term = norm * mm(mixer_columns, mixer_grads, 0, 0)
    band = columns // C
    for q in range(C):
        r.m_o[q] = mixer_term[q * band : (q + 1) * band, :].astype(BF)

    def share_m(q, landing, slot):
        return rcopy(r.m_o.at[q], r.m_i.at[landing], r.m_s.at[q], r.m_r.at[slot], chan=q)

    each(C, lambda d: share_m(lax.rem(ch + d, C), ch, ch).start())
    if S <= 12:
        for d in range(3, S):
            hop(d)
    else:
        lax.fori_loop(3, S, lambda d, c: (hop(d), c)[1], 0)

    def step_term(k, total):
        for e in range(D):
            x = r.xc[k, e].reshape(length, columns)
            total = total + mm(r.gsm[k, e, rows:, 0:LANES], x, 1, 0)
        return total

    step_total = jnp.zeros((PAD, columns), F32)
    if S <= 12:
        for k in range(S):
            step_total = step_term(k, step_total)
    else:
        step_total = lax.fori_loop(0, S, step_term, step_total)
    r.o_dws[...] = (norm * step_total)[:heads, :]

    def whole(k, e, send, recv):
        return rcopy(r.gin.at[k, e], r.gin.at[k, e], send, recv, seq=above)

    def weight_term(k, first=False):
        for e in others:
            whole(k, e, r.x_s.at[e, k], r.c_r.at[e, k]).wait_recv()
        x = r.xc[k].reshape(D * length, columns)
        term = norm * mm(x, r.gin[k].reshape(D * length, width), 0, 0)
        r.o_dw[...] = term if first else r.o_dw[...] + term

    def weight_terms(d):
        for k, there in ((me + d, me + d < S), (me - d, me >= d)):
            pl.when(there)(functools.partial(weight_term, k))

    weight_term(me, True)
    each(S, weight_terms)
    r.p_i[ch] = r.p_o[ch]
    r.m_i[ch] = r.m_o[ch]
    each(C, lambda d: whole_p(lax.rem(ch + d, C)).wait_recv())
    each(C, lambda d: share_m(lax.rem(ch + d, C), ch, lax.rem(ch + d, C)).wait_recv())

    for way in (0, 1):

        @pl.when(spots[way] < S - 1)
        def _(way=way):
            rcopy(terms[way], outs[way], r.chain_s.at[way], r.chain_r.at[way, 0], seq=above).wait_send()

    @pl.when(me > 0)
    def _():
        rcopy(r.hal_o, r.hal_i, r.hal_s.at[0], r.hal_r.at[0], seq=below).wait_send()
        mix_halo().wait_send()
        mix_tail(ch).wait_send()

    def settle_chan(d):
        q = lax.rem(ch + d, C)
        share_mix(q, ch, ch).wait_send()
        share_m(q, ch, ch).wait_send()
        whole_p(q).wait_send()

    each(C, settle_chan)

    def settle_line(k):
        for e in others:
            whole(k, mine, r.x_s.at[e, k], r.c_r.at[mine, k]).wait_send()
        for way, sent in (("up", (k <= me) & (me < S - 1)), ("down", (k >= me) & (me > 0))):

            @pl.when(sent)
            def _(way=way):
                whole(k, mine, (r.u_s if way == "up" else r.d_s).at[k], r.z_r.at[0, k]).wait_send()

    settle_line(0)
    each(S, settle_line)
    small_all(lambda e, q: small_to(mine, me, e, q).wait_send())


def finish_kernel(parts, dw, mixes, dws, o_ig, o_dw, o_dwm, o_dws, ig, dwm, sems):
    copies = [
        pltpu.make_async_copy(a, b, sems.at[i])
        for i, (a, b) in enumerate(((dw, o_dw), (dws, o_dws), (ig, o_ig), (dwm, o_dwm)))
    ]
    copies[0].start()
    copies[1].start()
    total = parts[0].astype(F32)
    for q in range(1, parts.shape[0]):
        total = total + parts[q].astype(F32)
    ig[...] = total.astype(BF)
    copies[2].start()
    total = mixes[0].astype(F32)
    for q in range(1, mixes.shape[0]):
        total = total + mixes[q].astype(F32)
    dwm[...] = total
    copies[3].start()
    for copy in copies:
        copy.wait()


def body(
    sizes,
    layer_input,
    inner_weight,
    mixer_weight,
    step_weight,
    conv_inner,
    conv_mixer,
    step_bias,
    decay_log,
    skip_gain,
    output_grad,
):
    own = layer_input[0]
    rows, model = own.shape
    chans, seqs, dps = sizes["chan"], sizes["seq"], sizes["dp"]
    groups = dps * seqs
    length = rows * chans
    width = inner_weight.shape[1]
    mixed = mixer_weight.shape[1]
    heads = step_bias.shape[0]
    cols = model // groups
    state_size = mixed // 2
    assert width % PIECES == 0 and chans % 2 == 0 and seqs > 2
    assert rows == 2 * PAD and width % LANES == 0 and PIECES % (width // LANES) == 0
    assert length == LANES and heads + conv_inner.shape[0] - 1 <= PAD
    upstream = output_grad[0]
    step_rows = step_weight.T
    bias, rates, skips = (v.reshape(1, heads) for v in (step_bias, decay_log, skip_gain))
    dma = pltpu.SemaphoreType.DMA
    vmem = pl.BlockSpec(memory_space=pltpu.VMEM)
    hbm = pl.BlockSpec(memory_space=pltpu.HBM)
    small = rows + PAD
    strips = width // LANES
    band = cols // chans

    def low(*shape):
        return pltpu.VMEM(shape, BF)

    def full(*shape):
        return pltpu.VMEM(shape, F32)

    inputs = dict(
        own=own, w_in=inner_weight, w_mix=mixer_weight, w_step=step_rows, conv_in=conv_inner,
        conv_mix=conv_mixer, bias=bias, log=rates, skip=skips, grad=upstream,
    )
    outputs = dict(
        p_i=jax.ShapeDtypeStruct((chans, rows, model), BF),
        o_dw=jax.ShapeDtypeStruct((cols, width), F32),
        m_i=jax.ShapeDtypeStruct((chans, band, mixed), BF),
        o_dws=jax.ShapeDtypeStruct((heads, cols), F32),
    )
    scratch = {key: pltpu.VMEM(v.shape, v.dtype) for key, v in inputs.items()}
    scratch |= dict(
        wst=low(LANES, model), xg=low(length, model),
        blocks=low(dps, seqs, rows, cols),
        xs=low(seqs, dps, rows, cols), xc=low(seqs, dps, chans, rows, cols),
        wide_in=full(PAD + length, width), wide_mix=full(PAD + length, mixed),
        fh_o=low(PAD, width + mixed), fh_i=low(PAD, width + mixed), vec=full(8, LANES),
        sum_in=full(length, width), sum_mix=full(length, mixed), raw=full(length, LANES),
        cum=full(length, LANES), step_wide=full(length, width), fading=full(length, width),
        grown=full(length, width), pulled=low(length, width), decay=full(width, state_size),
        mix=low(length, mixed), act=full(length, width), stepped=low(length, width),
        state_term=low(width, state_size), back_term=low(width, state_size),
        start=low(width, state_size), end=low(width, state_size),
        scr0=low(width, state_size), scr1=low(width, state_size),
        z=full(length, width), y=full(length, width), score_grad=full(length, length),
        slope_in=full(length, width),
        pad_in=full(length + 8, width), pad_mix=full(length + 8, mixed),
        gin=low(seqs, dps, length, width), gsm=low(seqs, dps, small, mixed),
        hal_o=full(strips, 8, LANES), hal_i=full(strips, 8, LANES),
        halm_o=full(8, mixed), halm_i=full(8, mixed), p_last=full(PAD, model),
        skips=full(8, width), ending=full(length, width),
        gmp=low(length, mixed), gm_in=low(chans, small, mixed), gmt=full(small, mixed),
        am=low(length + PAD, mixed), mt_in=low(chans, PAD, mixed),
        p_o=low(chans, rows, model), m_o=low(chans, band, mixed),
        load_sem=dma((len(LOADED),)), fh_sem=dma((2,)), halm_s=dma((2,)),
        hal_s=dma((1,)), hal_r=dma((strips,)),
        near_s=dma((1,)), near_r=dma((chans,)),
        far_s=dma((chans // 2,)), far_r=dma((chans // 2, chans)),
        relay_s=dma((chans // 2,)), relay_r=dma((chans // 2, chans)),
        cross_s=dma((dps, seqs)), cross_r=dma((dps, seqs)),
        gat_s=dma((chans,)), gat_r=dma((chans,)),
        chain_s=dma((2,)), chain_r=dma((2, PIECES)),
        z_r=dma((strips, seqs)), c_r=dma((dps, seqs)),
        u_s=dma((seqs,)), d_s=dma((seqs,)), x_s=dma((dps, seqs)),
        z2_r=dma((dps, seqs)),
        z2_s=dma((dps, seqs)), mt_s=dma((1,)), mt_r=dma((chans,)),
        gm_s=dma((chans,)), gm_r=dma((chans,)),
        p_s=dma((chans,)), p_r=dma((chans,)), m_s=dma((chans,)), m_r=dma((chans,)),
    )
    names = [key + "_h" for key in inputs] + list(outputs) + list(scratch)
    parts, inner_grad, mix_parts, step_grad = pl.pallas_call(
        functools.partial(layer_kernel, names, sizes, heads),
        out_shape=tuple(outputs.values()),
        in_specs=[hbm] * len(inputs),
        out_specs=(vmem,) * len(outputs),
        scratch_shapes=list(scratch.values()),
        compiler_params=pltpu.CompilerParams(
            collective_id=0, has_side_effects=True, vmem_limit_bytes=LIMIT
        ),
        name="layer",
    )(*(pltpu.with_memory_space_constraint(v, pltpu.HBM) for v in inputs.values()))
    input_grad, inner_grad, mixer_grad, step_grad = pl.pallas_call(
        finish_kernel,
        out_shape=(
            jax.ShapeDtypeStruct((rows, model), BF),
            jax.ShapeDtypeStruct((cols, width), F32),
            jax.ShapeDtypeStruct((band, mixed), F32),
            jax.ShapeDtypeStruct((heads, cols), F32),
        ),
        in_specs=[vmem] * 4,
        out_specs=(pl.BlockSpec(memory_space=pl.ANY),) * 4,
        scratch_shapes=[
            pltpu.VMEM((rows, model), BF),
            pltpu.VMEM((band, mixed), F32),
            dma((4,)),
        ],
        compiler_params=pltpu.CompilerParams(vmem_limit_bytes=LIMIT),
        name="finish",
    )(parts, inner_grad, mix_parts, step_grad)
    return input_grad[None], inner_grad, mixer_grad, step_grad.T


def solution(mesh):
    sizes = dict(mesh.shape)
    in_specs = (
        P("dp", ("seq", "chan"), None),
        P(None, "chan"),
        P(),
        P(None, "chan"),
        P(None, "chan"),
        P(),
        P("chan"),
        P("chan"),
        P("chan"),
        P("dp", "seq", "chan"),
    )
    out_specs = (
        P("dp", ("seq", "chan"), None),
        P(("dp", "seq"), "chan"),
        P(("dp", "seq", "chan"), None),
        P(("dp", "seq"), "chan"),
    )
    return jax.shard_map(
        functools.partial(body, sizes),
        mesh=mesh,
        in_specs=in_specs,
        out_specs=out_specs,
        check_vma=False,
    )
```

```python
import functools
import math
import types

import jax
import jax.numpy as jnp
from jax import lax
from jax.experimental import pallas as pl
from jax.experimental.pallas import tpu as pltpu
from jax.sharding import PartitionSpec as P

MESH = pl.DeviceIdType.MESH
HDIM = 64
PAD = 16
LANES = 128
LIMIT = 48 * 2**20
BF = jnp.bfloat16
F32 = jnp.float32
PIECES = 10
LOADED = (
    "own", "w_in", "w_mix", "w_step", "conv_in", "conv_mix", "bias", "log", "skip", "grad",
)


def each(n, step):
    if n <= 12:
        for d in range(1, n):
            step(d)
    else:

        def one(d, carry):
            step(d)
            return carry

        lax.fori_loop(1, n, one, 0)


def signal_to(barrier, where):
    pl.semaphore_signal(barrier, inc=1, device_id=where, device_id_type=MESH)


def mm(a, b, da, db):
    return lax.dot_general(
        a.astype(BF), b.astype(BF), (((da,), (db,)), ((), ())), preferred_element_type=F32
    )


def thirds(v):
    high = v.astype(BF)
    rest = v - high.astype(F32)
    middle = rest.astype(BF)
    return high, middle, (rest - middle.astype(F32)).astype(BF)


def exact(a, b, da=1, db=0):
    high, middle, low = thirds(a)
    return mm(high, b, da, db) + (mm(middle, b, da, db) + mm(low, b, da, db))


def exact_left(a, b, da=1, db=0):
    high, middle, low = thirds(b)
    return mm(a, high, da, db) + (mm(a, middle, da, db) + mm(a, low, da, db))


def softplus(v):
    return jnp.maximum(v, 0.0) + jnp.log1p(jnp.exp(-jnp.abs(v)))


def head_mask(width, heads_first):
    shape = (LANES, width) if heads_first else (width, LANES)
    head = lax.broadcasted_iota(jnp.int32, shape, 0 if heads_first else 1)
    column = lax.broadcasted_iota(jnp.int32, shape, 1 if heads_first else 0)
    return (column // HDIM == head).astype(F32)


def decays(raw, bias, decay_log):
    length = raw.shape[0]
    step = softplus(raw + bias)
    rate = jnp.exp(decay_log)
    row = lax.broadcasted_iota(jnp.int32, (length, length), 0)
    col = lax.broadcasted_iota(jnp.int32, (length, length), 1)
    lower = (row >= col).astype(F32)
    cumulative = exact_left(lower, -step * rate)
    return step, rate, cumulative, row, col, lower


def rcopy(src, dst, send, recv, **where):
    return pltpu.make_async_remote_copy(
        src_ref=src, dst_ref=dst, send_sem=send, recv_sem=recv, device_id=where, device_id_type=MESH
    )


def greet_all(barrier, axis, n):
    me = lax.axis_index(axis)
    each(n, lambda d: signal_to(barrier, {axis: lax.rem(me + d, n)}))
    return n - 1


def convolved(wide, kernel, first, count):
    taps = kernel.shape[0]
    first = first + PAD - (taps - 1)
    total = kernel[0:1, :] * wide[pl.ds(first, count), :]
    for k in range(1, taps):
        total = total + kernel[k : k + 1, :] * wide[pl.ds(first + k, count), :]
    return total


def spread_back(pad, kernel, first, count, cols=slice(None)):
    taps = kernel.shape[0]
    total = None
    for k in range(taps):
        term = kernel[k : k + 1, cols] * pad[pl.ds(first + taps - 1 - k, count), cols]
        total = term if total is None else total + term
    return total.astype(BF)


def layer_kernel(names, sizes, heads, *refs):
    r = types.SimpleNamespace(**dict(zip(names, refs, strict=True)))
    place = (lax.axis_index("dp"), lax.axis_index("seq"), lax.axis_index("chan"))
    D, S, C = sizes["dp"], sizes["seq"], sizes["chan"]
    barrier = pltpu.get_barrier_semaphore()
    total = greet_all(barrier, "dp", D) + greet_all(barrier, "seq", S) + greet_all(barrier, "chan", C)
    after = lax.rem(place[1] + 1, S)

    @pl.when(place[2] == C - 1)
    def _():
        for c in range(C):
            signal_to(barrier, {"seq": after, "chan": jnp.int32(c)})

    total += 1 + (D - 1) * (S - 1)
    for e in range(1, D):
        far = lax.rem(place[0] + e, D)
        each(S, lambda d, far=far: signal_to(barrier, {"dp": far, "seq": lax.rem(place[1] + d, S)}))
    loads = {
        key: pltpu.make_async_copy(getattr(r, key + "_h"), getattr(r, key), r.load_sem.at[i])
        for i, key in enumerate(LOADED)
    }
    for copy in loads.values():
        copy.start()
    crossed = front(r, sizes, place, heads, loads, barrier, total)
    rear(r, sizes, place, heads, crossed)


def front(r, sizes, place, heads, loads, barrier, total):
    D, S, C = sizes["dp"], sizes["seq"], sizes["chan"]
    mine, me, ch = place
    rows, model = r.own.shape
    length, width = r.sum_in.shape
    mixed = r.sum_mix.shape[1]
    cols = model // (D * S)
    half = mixed // 2
    splits = 2
    high = rows // 2
    cut = model // splits
    pieces = [(1, k) for k in range(splits)] + [(0, k) for k in range(splits)]
    sides = C // 2
    side, low = lax.div(ch, 2), lax.rem(ch, 2)
    partner = ch + 1 - 2 * low

    def block(c, p):
        part, k = pieces[p]
        first = pl.multiple_of(c * rows + part * high, high)
        return r.xg.at[pl.ds(first, high), pl.ds(k * cut, cut)]

    def mine_at(p):
        part, k = pieces[p]
        return r.own.at[pl.ds(part * high, high), pl.ds(k * cut, cut)]

    def near(c, p):
        return rcopy(mine_at(p), block(c, p), r.near_s.at[0], r.near_r.at[p], chan=partner)

    def far(to, c, slot, p):
        return rcopy(
            mine_at(p), block(c, p), r.far_s.at[to], r.far_r.at[slot, p], chan=2 * to + low
        )

    def relay(source, lane, p):
        c = 2 * source + lane
        here = block(c, p)
        return rcopy(here, here, r.relay_s.at[source], r.relay_r.at[source, p], chan=partner)

    def column(e, q, landing_e, landing_q):
        return rcopy(
            r.blocks.at[e, q], r.xs.at[landing_q, landing_e],
            r.cross_s.at[e, q], r.cross_r.at[landing_e, landing_q], dp=e, seq=q,
        )

    def columns_all(do):
        each(S, lambda d: do(mine, lax.rem(me + d, S)))
        for d in range(1, D):
            e = lax.rem(mine + d, D)
            do(e, me)
            each(S, lambda d, e=e: do(e, lax.rem(me + d, S)))

    loads["own"].wait()
    pl.semaphore_wait(barrier, total)
    for p in range(len(pieces)):
        for d in range(1, sides):
            far(lax.rem(side + d, sides), ch, side, p).start()
        near(ch, p).start()
    for d in range(D):
        for k in range(S):
            at = (d * S + k) * cols
            r.blocks[d, k] = r.own[:, at : at + cols]
    columns_all(lambda e, q: column(e, q, mine, me).start())
    r.xs[me, mine] = r.blocks[mine, me]
    r.xg[pl.ds(pl.multiple_of(ch * rows, rows), rows), :] = r.own[...]
    r.wst[...] = jnp.zeros(r.wst.shape, BF)
    r.vec[...] = jnp.zeros(r.vec.shape, F32)
    for key in LOADED[1:]:
        loads[key].wait()
    r.wst[0:heads, :] = r.w_step[...]
    for i, ref in enumerate((r.bias, r.log, r.skip)):
        r.vec[i : i + 1, 0:heads] = ref[...]

    def pass_on(p):
        for d in range(1, sides):
            source = lax.rem(side + d, sides)
            far(source, ch, source, p).wait_recv()
            relay(source, low, p).start()

    def project(p):
        near(partner, p).wait_recv()
        for d in range(1, sides):
            source = lax.rem(side + d, sides)
            relay(source, 1 - low, p).wait_recv()
        part, k = pieces[p]
        piece = slice(k * cut, (k + 1) * cut)
        x = jnp.concatenate([r.xg[c * rows + part * high : c * rows + (part + 1) * high, piece] for c in range(C)])
        inner = mm(x, r.w_in[piece, :], 1, 0)
        mixer = mm(x, r.w_mix[piece, :], 1, 0)
        raw = mm(x, r.wst[:, piece], 1, 1)
        for c in range(C):
            at = c * rows + part * high
            here = slice(c * high, (c + 1) * high)
            for ref, pad, term in ((r.wide_in, PAD, inner), (r.wide_mix, PAD, mixer), (r.raw, 0, raw)):
                old = ref[pad + at : pad + at + high, :] if k else 0.0
                ref[pad + at : pad + at + high, :] = old + term[here, :]

    def halo():
        return rcopy(r.fh_o, r.fh_i, r.fh_sem.at[0], r.fh_sem.at[1], seq=lax.rem(me + 1, S))

    pass_on(0)
    for p in range(len(pieces)):
        if p + 1 < len(pieces):
            pass_on(p + 1)
        project(p)
        if p == splits - 1:
            r.fh_o[:, :width] = r.wide_in[length:, :].astype(BF)
            r.fh_o[:, width:] = r.wide_mix[length:, :].astype(BF)
            pl.when(me < S - 1)(lambda: halo().start())
    inner_low = r.wide_in[PAD:, :].astype(BF)
    mixer_low = r.wide_mix[PAD:, :].astype(BF)
    r.wide_in[PAD:, :] = inner_low.astype(F32)
    r.wide_mix[PAD:, :] = mixer_low.astype(F32)
    r.wide_in[0:PAD, :] = jnp.zeros((PAD, width), F32)
    r.wide_mix[0:PAD, :] = jnp.zeros((PAD, mixed), F32)
    r.sum_in[PAD:, :] = convolved(r.wide_in, r.conv_in, PAD, length - PAD)
    r.sum_mix[PAD:, :] = convolved(r.wide_mix, r.conv_mix, PAD, length - PAD)
    step, rate, cumulative, row, col, lower = decays(r.raw[...], r.vec[0:1, :], r.vec[1:2, :])
    last = cumulative[length - 1 : length, :]
    spread = head_mask(width, True)
    r.cum[...] = cumulative
    step_wide = exact(step, spread)
    fading = exact(jnp.exp(last - cumulative), spread)
    grown = exact(jnp.exp(cumulative), spread)
    r.step_wide[...] = step_wide
    r.fading[...] = fading
    r.grown[...] = grown
    pulled = (grown * r.grad[...].astype(F32)).astype(BF)
    r.pulled[...] = pulled
    row_decay = jnp.sum(head_mask(width, False) * jnp.exp(last), axis=1, keepdims=True)
    r.decay[...] = jnp.broadcast_to(row_decay, r.decay.shape)

    @pl.when(me > 0)
    def _():
        halo().wait_recv()
        r.wide_in[0:PAD, :] = r.fh_i[:, :width].astype(F32)
        r.wide_mix[0:PAD, :] = r.fh_i[:, width:].astype(F32)

    r.sum_in[0:PAD, :] = convolved(r.wide_in, r.conv_in, 0, PAD)
    r.sum_mix[0:PAD, :] = convolved(r.wide_mix, r.conv_mix, 0, PAD)
    mixer = r.sum_mix[...]
    mix = mixer * jax.nn.sigmoid(mixer)
    r.mix[...] = mix.astype(BF)
    r.back_term[...] = mm(pulled, mix[:, half:], 0, 0).astype(BF)
    inner = r.sum_in[...]
    act = inner * jax.nn.sigmoid(inner)
    r.act[...] = act
    r.state_term[...] = mm(act * (fading * step_wide), mix[:, :half], 0, 0).astype(BF)

    @pl.when(me < S - 1)
    def _():
        halo().wait_send()

    def sent(sem):
        rcopy(r.own, r.own, sem, r.near_r.at[0], chan=partner).wait_send()

    sent(r.near_s.at[0])
    for d in range(1, sides):
        source = lax.rem(side + d, sides)
        sent(r.far_s.at[source])
        sent(r.relay_s.at[source])
    return lambda: columns_all(lambda e, q: column(e, q, e, q).wait())


def rear(r, sizes, place, heads, crossed):
    D, S, C = sizes["dp"], sizes["seq"], sizes["chan"]
    mine, me, ch = place
    length, width = r.sum_in.shape
    mixed = r.sum_mix.shape[1]
    half = mixed // 2
    model = r.w_in.shape[0]
    rows = length // C
    pieces, lag = PIECES, PIECES // 2
    lags = (lag + 3, lag)
    size = width // pieces
    strips = width // LANES
    per = pieces // strips
    parts = C
    cut = model // parts
    terms, outs, scratch = (r.state_term, r.back_term), (r.start, r.end), (r.scr0, r.scr1)
    spots = (me, S - 1 - me)
    above, below = lax.rem(me + 1, S), lax.rem(me + S - 1, S)
    others = [lax.rem(mine + e, D) for e in range(1, D)]

    def carry(way, piece, first=False):
        part = pl.ds(pl.multiple_of(piece * size, size), size)
        source = terms[way] if first else scratch[way]
        sems = r.chain_s.at[way], r.chain_r.at[way, piece]
        return rcopy(source.at[part], outs[way].at[part], *sems, seq=above if way == 0 else below)

    for way in (1, 0):

        @pl.when(spots[way] == 0)
        def _(way=way):
            for piece in range(pieces):
                carry(way, piece, True).start()
            outs[way][...] = jnp.zeros(outs[way].shape, BF)

    def beat(t):
        for way in (1, 0):
            spot = spots[way]
            piece = t - lags[way] * (spot - 1)

            @pl.when((piece >= 0) & (piece < pieces) & (spot > 0) & (spot < S - 1))
            def _(way=way, piece=piece):
                carry(way, piece).wait_recv()
                part = pl.ds(pl.multiple_of(piece * size, size), size)
                before = outs[way][part, :].astype(F32)
                term = terms[way][part, :].astype(F32)
                scratch[way][part, :] = (r.decay[part, :] * before + term).astype(BF)
                carry(way, piece).start()

    def gather(q, landing, slot):
        return rcopy(r.xs, r.xc.at[:, :, landing], r.gat_s.at[q], r.gat_r.at[slot], chan=q)

    spread = head_mask(width, True)
    cumulative = r.cum[...]
    across = cumulative.T
    row = lax.broadcasted_iota(jnp.int32, (length, length), 0)
    col = lax.broadcasted_iota(jnp.int32, (length, length), 1)
    causal = row >= col
    lower = causal.astype(F32)
    into, out_of = r.mix[:, :half], r.mix[:, half:]
    scores = mm(out_of, into, 1, 1)
    r.stepped[...] = (r.act[...] * r.step_wide[...]).astype(BF)
    inner = r.sum_in[...]
    gate = jax.nn.sigmoid(inner)
    r.slope_in[...] = gate * (1.0 + inner * (1.0 - gate))
    skip_wide = exact(jnp.broadcast_to(r.vec[2:3, :], (8, LANES)), spread)
    r.skips[...] = skip_wide
    r.pad_in[length:, :] = jnp.zeros((8, width), F32)
    r.pad_mix[length:, :] = jnp.zeros((8, mixed), F32)

    def head(h):
        cols = slice(h * HDIM, (h + 1) * HDIM)
        gap = cumulative[:, h : h + 1] - across[h : h + 1, :]
        decay = jnp.where(causal, jnp.exp(jnp.where(causal, gap, 0.0)), 0.0)
        weights = (decay * scores).astype(BF)
        grad_h, step_h = r.grad[:, cols], r.stepped[:, cols]
        term = decay * mm(grad_h, step_h, 1, 1)
        r.score_grad[...] = term if h == 0 else r.score_grad[...] + term
        r.z[:, cols] = mm(weights, grad_h, 0, 0)
        r.y[:, cols] = mm(weights, step_h, 1, 0)

    def strip(j):
        return slice(j * LANES, (j + 1) * LANES)

    def halo(j):
        return rcopy(r.hal_o.at[j], r.hal_i.at[j], r.hal_s.at[0], r.hal_r.at[j], seq=below)

    def strip_sum(j):
        cols = strip(j)

        @pl.when(spots[1] == S - 1)
        def _():
            for piece in range(j * per, (j + 1) * per):
                carry(1, piece).wait_recv()

        ending = r.fading[:, cols] * mm(into, r.end[cols, :], 1, 1)
        r.ending[:, cols] = ending
        direct = r.skips[0:1, cols] * r.grad[:, cols].astype(F32)
        total = (r.step_wide[:, cols] * (r.z[:, cols] + ending) + direct) * r.slope_in[:, cols]
        r.pad_in[0:length, cols] = total
        r.hal_o[j] = total[0:8, :]

        @pl.when(me > 0)
        def _():
            halo(j).start()

    def part(p, e, k):
        return r.gin.at[k, e, :, pl.ds(p * LANES, LANES)]

    def zcopy(p, way, k):
        send = (r.u_s if way == "up" else r.d_s).at[k]
        here = part(p, mine, k)
        return rcopy(here, here, send, r.z_r.at[p, k], seq=above if way == "up" else below)

    def ccopy(p, k, e, to):
        return rcopy(part(p, e, k), part(p, e, k), r.x_s.at[to, k], r.c_r.at[e, k], dp=to)

    def strip_out(j):
        cols = strip(j)

        @pl.when(me < S - 1)
        def _():
            halo(j).wait_recv()
            r.pad_in[length:, cols] = r.hal_i[j]

        r.gin[me, mine, :, cols] = spread_back(r.pad_in, r.conv_in, 0, length, cols)
        for e in others:
            ccopy(j, me, mine, e).start()

    def strip_up(j):
        zcopy(j, "up", me).start()

    def strip_early(j):
        strip_out(j)
        strip_up(j)

    def strip_along(j, sent):
        @pl.when((me < S - 1) & (spots[1] != 2) if sent else me < S - 1)
        def _():
            strip_up(j)

        @pl.when(me > 0)
        def _():
            zcopy(j, "down", me).start()

    beats = pieces + lags[0] * max(S - 3, 0)
    early = heads // 2
    for h in range(early):
        head(h)
    near = spots[1] <= 1
    crossed()
    each(C, lambda d: gather(lax.rem(ch + d, C), ch, ch).start())
    r.xc[:, :, ch] = r.xs[...]
    if beats <= 24:
        sums = {per * j + per - 1: j for j in range(strips)}
        late = {lag + t: j for t, j in sums.items()}
        for t in range(max(beats, heads - early)):
            beat(t)
            if early + t < heads:
                head(early + t)
            if t in sums:
                pl.when(near)(functools.partial(strip_sum, sums[t]))
            if t in late:
                pl.when(near)(functools.partial(strip_out, late[t]))
                pl.when(spots[1] == 2)(functools.partial(strip_sum, late[t]))
            if t - 2 in late:
                pl.when(spots[1] == 2)(functools.partial(strip_early, late[t - 2]))
        done = {j: t + 2 < max(beats, heads - early) for t, j in late.items()}
        for j in range(strips):
            pl.when(spots[1] > 2)(functools.partial(strip_sum, j))
            pl.when(spots[1] > (2 if done[j] else 1))(functools.partial(strip_out, j))
            strip_along(j, done[j])
    else:
        for h in range(early, heads):
            head(h)
        lax.fori_loop(0, beats, lambda t, c: (beat(t), c)[1], 0)
        for j in range(strips):
            strip_sum(j)
        for j in range(strips):
            strip_out(j)
            strip_along(j, False)

    @pl.when(spots[0] == S - 1)
    def _():
        for piece in range(pieces):
            carry(0, piece).wait_recv()

    start, end = r.start[...], r.end[...]
    score_grad = r.score_grad[...]
    mixer = r.sum_mix[...]
    gate = jax.nn.sigmoid(mixer)
    mixer_slope = gate * (1.0 + mixer * (1.0 - gate))
    faded = (r.fading[...] * r.stepped[...].astype(F32)).astype(BF)
    into_grad = mm(score_grad, out_of, 0, 0) + mm(faded, end, 1, 0)
    out_grad = mm(score_grad, into, 1, 0) + mm(r.pulled[...], start, 1, 0)
    r.pad_mix[0:length, :half] = into_grad * mixer_slope[:, :half]
    r.pad_mix[0:length, half:] = out_grad * mixer_slope[:, half:]
    r.am[0:length, :] = r.pad_mix[0:length, :].astype(BF)
    r.am[length:, :] = jnp.zeros((PAD, mixed), BF)
    r.halm_o[...] = r.pad_mix[0:8, :]

    def share_mix(q, landing, slot):
        some = r.am.at[pl.ds(pl.multiple_of(q * rows, rows), rows + PAD)]
        return rcopy(some, r.gm_in.at[landing], r.gm_s.at[q], r.gm_r.at[slot], chan=q)

    def mix_tail(slot):
        return rcopy(
            r.am.at[pl.ds(0, PAD)], r.mt_in.at[slot], r.mt_s.at[0], r.mt_r.at[slot],
            seq=below, chan=jnp.int32(C - 1),
        )

    def mix_halo():
        return rcopy(r.halm_o, r.halm_i, r.halm_s.at[0], r.halm_s.at[1], seq=below)

    each(C, lambda d: share_mix(lax.rem(ch + d, C), ch, ch).start())

    @pl.when(me > 0)
    def _():
        mix_tail(ch).start()
        mix_halo().start()

    r.gm_in[ch] = r.am[pl.ds(pl.multiple_of(ch * rows, rows), rows + PAD), :]
    r.gmp[...] = spread_back(r.pad_mix, r.conv_mix, 0, length)

    def forward(p, way, d):
        k = me - d if way == "up" else me + d
        there = (k >= 0) if way == "up" else (k < S)
        more = (me < S - 1) if way == "up" else (me > 0)

        @pl.when(there)
        def _():
            zcopy(p, way, k).wait_recv()

        @pl.when(there & more)
        def _():
            zcopy(p, way, k).start()

        @pl.when(there)
        def _():
            for e in others:
                ccopy(p, k, mine, e).start()

    def both(p, d):
        forward(p, "up", d)
        forward(p, "down", d)

    def hop(d):
        for p in range(strips):
            both(p, d)

    upstream = r.grad[...].astype(F32)
    stepped = r.stepped[...].astype(F32)
    ending = r.ending[...]
    carried = r.grown[...] * mm(out_of, start, 1, 1)
    to_heads = functools.partial(exact, b=spread, da=1, db=1)
    z = r.z[...]
    step_grad = to_heads(r.act[...] * (z + ending))
    tail_term = to_heads(stepped * ending)
    sum_grad = to_heads(upstream * (r.y[...] + carried) - stepped * z) - tail_term
    held = jnp.sum(start.astype(F32) * end.astype(F32), axis=1, keepdims=True)
    last = cumulative[length - 1 : length, :]
    overall = jnp.sum(tail_term, axis=0, keepdims=True) + jnp.exp(last) * jnp.sum(
        head_mask(width, False) * held, axis=0, keepdims=True
    )
    decay_grad = exact_left(lower, sum_grad, 0, 0) + overall
    rate = jnp.exp(r.vec[1:2, :])
    step_grad = (step_grad - rate * decay_grad) * jax.nn.sigmoid(r.raw[...] + r.vec[0:1, :])
    steps = step_grad.astype(BF)
    r.gsm[me, mine, rows:, 0:LANES] = step_grad.T[0:PAD, :].astype(BF)
    steps = steps[:, 0:PAD]

    both(0, 1)

    each(C, lambda d: share_mix(lax.rem(ch + d, C), ch, lax.rem(ch + d, C)).wait_recv())
    mix = r.gm_in[0].astype(F32)
    for q in range(1, C):
        mix = mix + r.gm_in[q].astype(F32)
    r.gmt[...] = mix

    @pl.when((me < S - 1) & (ch == C - 1))
    def _():
        for q in range(C):
            mix_tail(q).wait_recv()
        tail = r.mt_in[0].astype(F32)
        for q in range(1, C):
            tail = tail + r.mt_in[q].astype(F32)
        r.gmt[rows:, :] = tail

    r.gsm[me, mine, 0:rows, :] = spread_back(r.gmt, r.conv_mix, 0, rows)

    def small_along(e, k, q):
        here = r.gsm.at[k, e]
        return rcopy(here, here, r.z2_s.at[e, q], r.z2_r.at[e, k], seq=q)

    def cross_small(to):
        here = r.gsm.at[me, mine]
        return rcopy(here, here, r.z2_s.at[to, me], r.z2_r.at[mine, me], dp=to)

    def crossed_small(e):
        here = r.gsm.at[me, e]
        return rcopy(here, here, r.z2_s.at[e, me], r.z2_r.at[e, me], dp=e)

    def send_small(e):
        each(S, lambda d: small_along(e, me, lax.rem(me + d, S)).start())

    def small_all(do):
        for e in [mine] + others:
            each(S, lambda d, e=e: do(e, lax.rem(me + d, S)))

    both(1, 1)
    both(2, 1)

    def share_p(j, q, landing, slot):
        piece = pl.ds(j * cut, cut)
        return rcopy(
            r.p_o.at[q, :, piece], r.p_i.at[landing, :, piece], r.p_s.at[q], r.p_r.at[slot], chan=q
        )

    def whole_p(q):
        return rcopy(r.p_o.at[q], r.p_i.at[q], r.p_s.at[q], r.p_r.at[q], chan=q)

    grads = r.gin[me, mine]
    mixes = r.gmp[...]

    def send_p(j, final):
        def one(d):
            q = lax.rem(ch + d, C)

            @pl.when((q == C - 1) if final else (q < C - 1))
            def _():
                share_p(j, q, ch, ch).start()

        each(C, one)

    for j in range(parts):
        piece = slice(j * cut, (j + 1) * cut)
        out = mm(grads, r.w_in[piece, :], 1, 1) + mm(mixes, r.w_mix[piece, :], 1, 1)
        out = out + mm(steps, r.wst[0:PAD, piece], 1, 0)
        r.p_o[:, :, piece] = out.astype(BF).reshape(C, rows, cut)
        r.p_last[:, piece] = out[length - PAD :, :]
        send_p(j, False)
        if j + 3 < strips:
            both(j + 3, 1)
        if j == 0:
            send_small(mine)
            for e in others:
                cross_small(e).start()
    for p in range(parts + 3, strips):
        both(p, 1)

    @pl.when(me < S - 1)
    def _():
        mix_halo().wait_recv()
        r.pad_mix[length:, :] = r.halm_i[...]
        final = spread_back(r.pad_mix, r.conv_mix, length - PAD, PAD)
        change = final.astype(F32) - r.gmp[length - PAD :, :].astype(F32)
        fixed = r.p_last[...] + mm(change, r.w_mix[...], 1, 1)
        r.p_o[C - 1, rows - PAD :, :] = fixed.astype(BF)

    for j in range(parts):
        send_p(j, True)
    for p in range(strips):
        both(p, 2)
        if p == strips // 2:
            for e in others:
                crossed_small(e).wait_recv()
                send_small(e)
    if S <= 12:
        for d in range(3, S):
            hop(d)
    else:
        lax.fori_loop(3, S, lambda d, c: (hop(d), c)[1], 0)
    small_all(lambda e, q: small_along(e, q, q).wait_recv())
    norm = 1.0 / math.sqrt(D * S * length)
    columns = r.xc.shape[-1]

    def settle_gather(d):
        q = lax.rem(ch + d, C)
        gather(q, q, q).wait()

    each(C, settle_gather)
    mixer_columns = r.xc[:, :, ch].reshape(S * D * rows, columns)
    mixer_grads = r.gsm[:, :, 0:rows, :].reshape(S * D * rows, mixed)
    mixer_term = norm * mm(mixer_columns, mixer_grads, 0, 0)
    band = columns // C
    for q in range(C):
        r.m_o[q] = mixer_term[q * band : (q + 1) * band, :].astype(BF)

    def share_m(q, landing, slot):
        return rcopy(r.m_o.at[q], r.m_i.at[landing], r.m_s.at[q], r.m_r.at[slot], chan=q)

    each(C, lambda d: share_m(lax.rem(ch + d, C), ch, ch).start())
    def step_term(k, total):
        for e in range(D):
            x = r.xc[k, e].reshape(length, columns)
            total = total + mm(r.gsm[k, e, rows:, 0:LANES], x, 1, 0)
        return total

    step_total = jnp.zeros((PAD, columns), F32)
    if S <= 12:
        for k in range(S):
            step_total = step_term(k, step_total)
    else:
        step_total = lax.fori_loop(0, S, step_term, step_total)
    r.o_dws[...] = (norm * step_total)[:heads, :]

    def whole(k, e, send, recv):
        return rcopy(r.gin.at[k, e], r.gin.at[k, e], send, recv, seq=above)

    def weight_term(k, first=False):
        for e in others:
            whole(k, e, r.x_s.at[e, k], r.c_r.at[e, k]).wait_recv()
        x = r.xc[k].reshape(D * length, columns)
        term = norm * mm(x, r.gin[k].reshape(D * length, width), 0, 0)
        r.o_dw[...] = term if first else r.o_dw[...] + term

    def weight_terms(d):
        for k, there in ((me + d, me + d < S), (me - d, me >= d)):
            pl.when(there)(functools.partial(weight_term, k))

    weight_term(me, True)
    each(S, weight_terms)
    r.p_i[ch] = r.p_o[ch]
    r.m_i[ch] = r.m_o[ch]
    each(C, lambda d: whole_p(lax.rem(ch + d, C)).wait_recv())
    each(C, lambda d: share_m(lax.rem(ch + d, C), ch, lax.rem(ch + d, C)).wait_recv())

    for way in (0, 1):

        @pl.when(spots[way] < S - 1)
        def _(way=way):
            rcopy(terms[way], outs[way], r.chain_s.at[way], r.chain_r.at[way, 0], seq=above).wait_send()

    @pl.when(me > 0)
    def _():
        rcopy(r.hal_o, r.hal_i, r.hal_s.at[0], r.hal_r.at[0], seq=below).wait_send()
        mix_halo().wait_send()
        mix_tail(ch).wait_send()

    def settle_chan(d):
        q = lax.rem(ch + d, C)
        share_mix(q, ch, ch).wait_send()
        share_m(q, ch, ch).wait_send()
        whole_p(q).wait_send()

    each(C, settle_chan)

    def settle_line(k):
        for e in others:
            whole(k, mine, r.x_s.at[e, k], r.c_r.at[mine, k]).wait_send()
        for way, sent in (("up", (k <= me) & (me < S - 1)), ("down", (k >= me) & (me > 0))):

            @pl.when(sent)
            def _(way=way):
                whole(k, mine, (r.u_s if way == "up" else r.d_s).at[k], r.z_r.at[0, k]).wait_send()

    settle_line(0)
    each(S, settle_line)
    small_all(lambda e, q: small_along(e, me, q).wait_send())
    for e in others:
        cross_small(e).wait_send()


def finish_kernel(parts, dw, mixes, dws, o_ig, o_dw, o_dwm, o_dws, ig, dwm, sems):
    copies = [
        pltpu.make_async_copy(a, b, sems.at[i])
        for i, (a, b) in enumerate(((dw, o_dw), (dws, o_dws), (ig, o_ig), (dwm, o_dwm)))
    ]
    copies[0].start()
    copies[1].start()
    total = parts[0].astype(F32)
    for q in range(1, parts.shape[0]):
        total = total + parts[q].astype(F32)
    ig[...] = total.astype(BF)
    copies[2].start()
    total = mixes[0].astype(F32)
    for q in range(1, mixes.shape[0]):
        total = total + mixes[q].astype(F32)
    dwm[...] = total
    copies[3].start()
    for copy in copies:
        copy.wait()


def body(
    sizes,
    layer_input,
    inner_weight,
    mixer_weight,
    step_weight,
    conv_inner,
    conv_mixer,
    step_bias,
    decay_log,
    skip_gain,
    output_grad,
):
    own = layer_input[0]
    rows, model = own.shape
    chans, seqs, dps = sizes["chan"], sizes["seq"], sizes["dp"]
    groups = dps * seqs
    length = rows * chans
    width = inner_weight.shape[1]
    mixed = mixer_weight.shape[1]
    heads = step_bias.shape[0]
    cols = model // groups
    state_size = mixed // 2
    assert width % PIECES == 0 and chans % 2 == 0 and seqs > 2
    assert rows == 2 * PAD and width % LANES == 0 and PIECES % (width // LANES) == 0
    assert length == LANES and heads + conv_inner.shape[0] - 1 <= PAD
    upstream = output_grad[0]
    step_rows = step_weight.T
    bias, rates, skips = (v.reshape(1, heads) for v in (step_bias, decay_log, skip_gain))
    dma = pltpu.SemaphoreType.DMA
    vmem = pl.BlockSpec(memory_space=pltpu.VMEM)
    hbm = pl.BlockSpec(memory_space=pltpu.HBM)
    small = rows + PAD
    strips = width // LANES
    band = cols // chans

    def low(*shape):
        return pltpu.VMEM(shape, BF)

    def full(*shape):
        return pltpu.VMEM(shape, F32)

    inputs = dict(
        own=own, w_in=inner_weight, w_mix=mixer_weight, w_step=step_rows, conv_in=conv_inner,
        conv_mix=conv_mixer, bias=bias, log=rates, skip=skips, grad=upstream,
    )
    outputs = dict(
        p_i=jax.ShapeDtypeStruct((chans, rows, model), BF),
        o_dw=jax.ShapeDtypeStruct((cols, width), F32),
        m_i=jax.ShapeDtypeStruct((chans, band, mixed), BF),
        o_dws=jax.ShapeDtypeStruct((heads, cols), F32),
    )
    scratch = {key: pltpu.VMEM(v.shape, v.dtype) for key, v in inputs.items()}
    scratch |= dict(
        wst=low(LANES, model), xg=low(length, model),
        blocks=low(dps, seqs, rows, cols),
        xs=low(seqs, dps, rows, cols), xc=low(seqs, dps, chans, rows, cols),
        wide_in=full(PAD + length, width), wide_mix=full(PAD + length, mixed),
        fh_o=low(PAD, width + mixed), fh_i=low(PAD, width + mixed), vec=full(8, LANES),
        sum_in=full(length, width), sum_mix=full(length, mixed), raw=full(length, LANES),
        cum=full(length, LANES), step_wide=full(length, width), fading=full(length, width),
        grown=full(length, width), pulled=low(length, width), decay=full(width, state_size),
        mix=low(length, mixed), act=full(length, width), stepped=low(length, width),
        state_term=low(width, state_size), back_term=low(width, state_size),
        start=low(width, state_size), end=low(width, state_size),
        scr0=low(width, state_size), scr1=low(width, state_size),
        z=full(length, width), y=full(length, width), score_grad=full(length, length),
        slope_in=full(length, width),
        pad_in=full(length + 8, width), pad_mix=full(length + 8, mixed),
        gin=low(seqs, dps, length, width), gsm=low(seqs, dps, small, mixed),
        hal_o=full(strips, 8, LANES), hal_i=full(strips, 8, LANES),
        halm_o=full(8, mixed), halm_i=full(8, mixed), p_last=full(PAD, model),
        skips=full(8, width), ending=full(length, width),
        gmp=low(length, mixed), gm_in=low(chans, small, mixed), gmt=full(small, mixed),
        am=low(length + PAD, mixed), mt_in=low(chans, PAD, mixed),
        p_o=low(chans, rows, model), m_o=low(chans, band, mixed),
        load_sem=dma((len(LOADED),)), fh_sem=dma((2,)), halm_s=dma((2,)),
        hal_s=dma((1,)), hal_r=dma((strips,)),
        near_s=dma((1,)), near_r=dma((chans,)),
        far_s=dma((chans // 2,)), far_r=dma((chans // 2, chans)),
        relay_s=dma((chans // 2,)), relay_r=dma((chans // 2, chans)),
        cross_s=dma((dps, seqs)), cross_r=dma((dps, seqs)),
        gat_s=dma((chans,)), gat_r=dma((chans,)),
        chain_s=dma((2,)), chain_r=dma((2, PIECES)),
        z_r=dma((strips, seqs)), c_r=dma((dps, seqs)),
        u_s=dma((seqs,)), d_s=dma((seqs,)), x_s=dma((dps, seqs)),
        z2_r=dma((dps, seqs)),
        z2_s=dma((dps, seqs)), mt_s=dma((1,)), mt_r=dma((chans,)),
        gm_s=dma((chans,)), gm_r=dma((chans,)),
        p_s=dma((chans,)), p_r=dma((chans,)), m_s=dma((chans,)), m_r=dma((chans,)),
    )
    names = [key + "_h" for key in inputs] + list(outputs) + list(scratch)
    parts, inner_grad, mix_parts, step_grad = pl.pallas_call(
        functools.partial(layer_kernel, names, sizes, heads),
        out_shape=tuple(outputs.values()),
        in_specs=[hbm] * len(inputs),
        out_specs=(vmem,) * len(outputs),
        scratch_shapes=list(scratch.values()),
        compiler_params=pltpu.CompilerParams(
            collective_id=0, has_side_effects=True, vmem_limit_bytes=LIMIT
        ),
        name="layer",
    )(*(pltpu.with_memory_space_constraint(v, pltpu.HBM) for v in inputs.values()))
    input_grad, inner_grad, mixer_grad, step_grad = pl.pallas_call(
        finish_kernel,
        out_shape=(
            jax.ShapeDtypeStruct((rows, model), BF),
            jax.ShapeDtypeStruct((cols, width), F32),
            jax.ShapeDtypeStruct((band, mixed), F32),
            jax.ShapeDtypeStruct((heads, cols), F32),
        ),
        in_specs=[vmem] * 4,
        out_specs=(pl.BlockSpec(memory_space=pl.ANY),) * 4,
        scratch_shapes=[
            pltpu.VMEM((rows, model), BF),
            pltpu.VMEM((band, mixed), F32),
            dma((4,)),
        ],
        compiler_params=pltpu.CompilerParams(vmem_limit_bytes=LIMIT),
        name="finish",
    )(parts, inner_grad, mix_parts, step_grad)
    return input_grad[None], inner_grad, mixer_grad, step_grad.T


def solution(mesh):
    sizes = dict(mesh.shape)
    in_specs = (
        P("dp", ("seq", "chan"), None),
        P(None, "chan"),
        P(),
        P(None, "chan"),
        P(None, "chan"),
        P(),
        P("chan"),
        P("chan"),
        P("chan"),
        P("dp", "seq", "chan"),
    )
    out_specs = (
        P("dp", ("seq", "chan"), None),
        P(("dp", "seq"), "chan"),
        P(("dp", "seq", "chan"), None),
        P(("dp", "seq"), "chan"),
    )
    return jax.shard_map(
        functools.partial(body, sizes),
        mesh=mesh,
        in_specs=in_specs,
        out_specs=out_specs,
        check_vma=False,
    )
```

```python
import functools
import math
import types

import jax
import jax.numpy as jnp
from jax import lax
from jax.experimental import pallas as pl
from jax.experimental.pallas import tpu as pltpu
from jax.sharding import PartitionSpec as P

MESH = pl.DeviceIdType.MESH
HDIM = 64
PAD = 16
LANES = 128
LIMIT = 48 * 2**20
BF = jnp.bfloat16
F32 = jnp.float32
PIECES = 10
LOADED = (
    "own", "w_in", "w_mix", "w_step", "conv_in", "conv_mix", "bias", "log", "skip", "grad",
)


def each(n, step):
    if n <= 12:
        for d in range(1, n):
            step(d)
    else:

        def one(d, carry):
            step(d)
            return carry

        lax.fori_loop(1, n, one, 0)


def signal_to(barrier, where):
    pl.semaphore_signal(barrier, inc=1, device_id=where, device_id_type=MESH)


def mm(a, b, da, db):
    return lax.dot_general(
        a.astype(BF), b.astype(BF), (((da,), (db,)), ((), ())), preferred_element_type=F32
    )


def thirds(v):
    high = v.astype(BF)
    rest = v - high.astype(F32)
    middle = rest.astype(BF)
    return high, middle, (rest - middle.astype(F32)).astype(BF)


def exact(a, b, da=1, db=0):
    high, middle, low = thirds(a)
    return mm(high, b, da, db) + (mm(middle, b, da, db) + mm(low, b, da, db))


def exact_left(a, b, da=1, db=0):
    high, middle, low = thirds(b)
    return mm(a, high, da, db) + (mm(a, middle, da, db) + mm(a, low, da, db))


def softplus(v):
    return jnp.maximum(v, 0.0) + jnp.log1p(jnp.exp(-jnp.abs(v)))


def head_mask(width, heads_first):
    shape = (LANES, width) if heads_first else (width, LANES)
    head = lax.broadcasted_iota(jnp.int32, shape, 0 if heads_first else 1)
    column = lax.broadcasted_iota(jnp.int32, shape, 1 if heads_first else 0)
    return (column // HDIM == head).astype(F32)


def decays(raw, bias, decay_log):
    length = raw.shape[0]
    step = softplus(raw + bias)
    rate = jnp.exp(decay_log)
    row = lax.broadcasted_iota(jnp.int32, (length, length), 0)
    col = lax.broadcasted_iota(jnp.int32, (length, length), 1)
    lower = (row >= col).astype(F32)
    cumulative = exact_left(lower, -step * rate)
    return step, rate, cumulative, row, col, lower


def rcopy(src, dst, send, recv, **where):
    return pltpu.make_async_remote_copy(
        src_ref=src, dst_ref=dst, send_sem=send, recv_sem=recv, device_id=where, device_id_type=MESH
    )


def greet_all(barrier, axis, n):
    me = lax.axis_index(axis)
    each(n, lambda d: signal_to(barrier, {axis: lax.rem(me + d, n)}))
    return n - 1


def convolved(wide, kernel, first, count):
    taps = kernel.shape[0]
    first = first + PAD - (taps - 1)
    total = kernel[0:1, :] * wide[pl.ds(first, count), :]
    for k in range(1, taps):
        total = total + kernel[k : k + 1, :] * wide[pl.ds(first + k, count), :]
    return total


def spread_back(pad, kernel, first, count, cols=slice(None)):
    taps = kernel.shape[0]
    total = None
    for k in range(taps):
        term = kernel[k : k + 1, cols] * pad[pl.ds(first + taps - 1 - k, count), cols]
        total = term if total is None else total + term
    return total.astype(BF)


def layer_kernel(names, sizes, heads, *refs):
    r = types.SimpleNamespace(**dict(zip(names, refs, strict=True)))
    place = (lax.axis_index("dp"), lax.axis_index("seq"), lax.axis_index("chan"))
    D, S, C = sizes["dp"], sizes["seq"], sizes["chan"]
    barrier = pltpu.get_barrier_semaphore()
    total = greet_all(barrier, "dp", D) + greet_all(barrier, "seq", S) + greet_all(barrier, "chan", C)
    after = lax.rem(place[1] + 1, S)

    @pl.when(place[2] == C - 1)
    def _():
        for c in range(C):
            signal_to(barrier, {"seq": after, "chan": jnp.int32(c)})

    total += 1 + (D - 1) * (S - 1)
    for e in range(1, D):
        far = lax.rem(place[0] + e, D)
        each(S, lambda d, far=far: signal_to(barrier, {"dp": far, "seq": lax.rem(place[1] + d, S)}))
    loads = {
        key: pltpu.make_async_copy(getattr(r, key + "_h"), getattr(r, key), r.load_sem.at[i])
        for i, key in enumerate(LOADED)
    }
    for copy in loads.values():
        copy.start()
    crossed = front(r, sizes, place, heads, loads, barrier, total)
    rear(r, sizes, place, heads, crossed)


def front(r, sizes, place, heads, loads, barrier, total):
    D, S, C = sizes["dp"], sizes["seq"], sizes["chan"]
    mine, me, ch = place
    rows, model = r.own.shape
    length, width = r.sum_in.shape
    mixed = r.sum_mix.shape[1]
    cols = model // (D * S)
    half = mixed // 2
    splits = 2
    high = rows // 2
    cut = model // splits
    pieces = [(1, k) for k in range(splits)] + [(0, k) for k in range(splits)]
    sides = C // 2
    side, low = lax.div(ch, 2), lax.rem(ch, 2)
    partner = ch + 1 - 2 * low

    def block(c, p):
        part, k = pieces[p]
        first = pl.multiple_of(c * rows + part * high, high)
        return r.xg.at[pl.ds(first, high), pl.ds(k * cut, cut)]

    def mine_at(p):
        part, k = pieces[p]
        return r.own.at[pl.ds(part * high, high), pl.ds(k * cut, cut)]

    def near(c, p):
        return rcopy(mine_at(p), block(c, p), r.near_s.at[0], r.near_r.at[p], chan=partner)

    def far(to, c, slot, p):
        return rcopy(
            mine_at(p), block(c, p), r.far_s.at[to], r.far_r.at[slot, p], chan=2 * to + low
        )

    def relay(source, lane, p):
        c = 2 * source + lane
        here = block(c, p)
        return rcopy(here, here, r.relay_s.at[source], r.relay_r.at[source, p], chan=partner)

    def column(e, q, landing_e, landing_q):
        return rcopy(
            r.blocks.at[e, q], r.xs.at[landing_q, landing_e],
            r.cross_s.at[e, q], r.cross_r.at[landing_e, landing_q], dp=e, seq=q,
        )

    def columns_all(do):
        each(S, lambda d: do(mine, lax.rem(me + d, S)))
        for d in range(1, D):
            e = lax.rem(mine + d, D)
            do(e, me)
            each(S, lambda d, e=e: do(e, lax.rem(me + d, S)))

    loads["own"].wait()
    pl.semaphore_wait(barrier, total)
    for p in range(len(pieces)):
        for d in range(1, sides):
            far(lax.rem(side + d, sides), ch, side, p).start()
        near(ch, p).start()
    for d in range(D):
        for k in range(S):
            at = (d * S + k) * cols
            r.blocks[d, k] = r.own[:, at : at + cols]
    columns_all(lambda e, q: column(e, q, mine, me).start())
    r.xs[me, mine] = r.blocks[mine, me]
    r.xg[pl.ds(pl.multiple_of(ch * rows, rows), rows), :] = r.own[...]
    r.wst[...] = jnp.zeros(r.wst.shape, BF)
    r.vec[...] = jnp.zeros(r.vec.shape, F32)
    for key in LOADED[1:]:
        loads[key].wait()
    r.wst[0:heads, :] = r.w_step[...]
    for i, ref in enumerate((r.bias, r.log, r.skip)):
        r.vec[i : i + 1, 0:heads] = ref[...]

    def pass_on(p):
        for d in range(1, sides):
            source = lax.rem(side + d, sides)
            far(source, ch, source, p).wait_recv()
            relay(source, low, p).start()

    def project(p):
        near(partner, p).wait_recv()
        for d in range(1, sides):
            source = lax.rem(side + d, sides)
            relay(source, 1 - low, p).wait_recv()
        part, k = pieces[p]
        piece = slice(k * cut, (k + 1) * cut)
        x = jnp.concatenate([r.xg[c * rows + part * high : c * rows + (part + 1) * high, piece] for c in range(C)])
        inner = mm(x, r.w_in[piece, :], 1, 0)
        mixer = mm(x, r.w_mix[piece, :], 1, 0)
        raw = mm(x, r.wst[:, piece], 1, 1)
        for c in range(C):
            at = c * rows + part * high
            here = slice(c * high, (c + 1) * high)
            for ref, pad, term in ((r.wide_in, PAD, inner), (r.wide_mix, PAD, mixer), (r.raw, 0, raw)):
                old = ref[pad + at : pad + at + high, :] if k else 0.0
                ref[pad + at : pad + at + high, :] = old + term[here, :]

    def halo():
        return rcopy(r.fh_o, r.fh_i, r.fh_sem.at[0], r.fh_sem.at[1], seq=lax.rem(me + 1, S))

    pass_on(0)
    for p in range(len(pieces)):
        if p + 1 < len(pieces):
            pass_on(p + 1)
        project(p)
        if p == splits - 1:
            r.fh_o[:, :width] = r.wide_in[length:, :].astype(BF)
            r.fh_o[:, width:] = r.wide_mix[length:, :].astype(BF)
            pl.when(me < S - 1)(lambda: halo().start())
    inner_low = r.wide_in[PAD:, :].astype(BF)
    mixer_low = r.wide_mix[PAD:, :].astype(BF)
    r.wide_in[PAD:, :] = inner_low.astype(F32)
    r.wide_mix[PAD:, :] = mixer_low.astype(F32)
    r.wide_in[0:PAD, :] = jnp.zeros((PAD, width), F32)
    r.wide_mix[0:PAD, :] = jnp.zeros((PAD, mixed), F32)
    r.sum_in[PAD:, :] = convolved(r.wide_in, r.conv_in, PAD, length - PAD)
    r.sum_mix[PAD:, :] = convolved(r.wide_mix, r.conv_mix, PAD, length - PAD)
    step, rate, cumulative, row, col, lower = decays(r.raw[...], r.vec[0:1, :], r.vec[1:2, :])
    last = cumulative[length - 1 : length, :]
    spread = head_mask(width, True)
    r.cum[...] = cumulative
    step_wide = exact(step, spread)
    fading = exact(jnp.exp(last - cumulative), spread)
    grown = exact(jnp.exp(cumulative), spread)
    r.step_wide[...] = step_wide
    r.fading[...] = fading
    r.grown[...] = grown
    pulled = (grown * r.grad[...].astype(F32)).astype(BF)
    r.pulled[...] = pulled
    row_decay = jnp.sum(head_mask(width, False) * jnp.exp(last), axis=1, keepdims=True)
    r.decay[...] = jnp.broadcast_to(row_decay, r.decay.shape)

    @pl.when(me > 0)
    def _():
        halo().wait_recv()
        r.wide_in[0:PAD, :] = r.fh_i[:, :width].astype(F32)
        r.wide_mix[0:PAD, :] = r.fh_i[:, width:].astype(F32)

    r.sum_in[0:PAD, :] = convolved(r.wide_in, r.conv_in, 0, PAD)
    r.sum_mix[0:PAD, :] = convolved(r.wide_mix, r.conv_mix, 0, PAD)
    mixer = r.sum_mix[...]
    mix = mixer * jax.nn.sigmoid(mixer)
    r.mix[...] = mix.astype(BF)
    r.back_term[...] = mm(pulled, mix[:, half:], 0, 0).astype(BF)
    inner = r.sum_in[...]
    act = inner * jax.nn.sigmoid(inner)
    r.act[...] = act
    r.state_term[...] = mm(act * (fading * step_wide), mix[:, :half], 0, 0).astype(BF)

    @pl.when(me < S - 1)
    def _():
        halo().wait_send()

    def sent(sem):
        rcopy(r.own, r.own, sem, r.near_r.at[0], chan=partner).wait_send()

    sent(r.near_s.at[0])
    for d in range(1, sides):
        source = lax.rem(side + d, sides)
        sent(r.far_s.at[source])
        sent(r.relay_s.at[source])
    return lambda: columns_all(lambda e, q: column(e, q, e, q).wait())


def rear(r, sizes, place, heads, crossed):
    D, S, C = sizes["dp"], sizes["seq"], sizes["chan"]
    mine, me, ch = place
    length, width = r.sum_in.shape
    mixed = r.sum_mix.shape[1]
    half = mixed // 2
    model = r.w_in.shape[0]
    rows = length // C
    pieces, lag = PIECES, PIECES // 2
    wait = lag + 3
    catch_up = {wait + i: [i] for i in range(2)}
    catch_up |= {wait + 2 + i: [2 * i + 2, 2 * i + 3] for i in range((pieces - 2) // 2)}
    size = width // pieces
    strips = width // LANES
    per = pieces // strips
    parts = C
    cut = model // parts
    terms, outs, scratch = (r.state_term, r.back_term), (r.start, r.end), (r.scr0, r.scr1)
    spots = (me, S - 1 - me)
    above, below = lax.rem(me + 1, S), lax.rem(me + S - 1, S)
    others = [lax.rem(mine + e, D) for e in range(1, D)]

    def carry(way, piece, first=False):
        part = pl.ds(pl.multiple_of(piece * size, size), size)
        source = terms[way] if first else scratch[way]
        sems = r.chain_s.at[way], r.chain_r.at[way, piece]
        return rcopy(source.at[part], outs[way].at[part], *sems, seq=above if way == 0 else below)

    for way in (1, 0):

        @pl.when(spots[way] == 0)
        def _(way=way):
            for piece in range(pieces):
                carry(way, piece, True).start()
            outs[way][...] = jnp.zeros(outs[way].shape, BF)

    def pass_state(way, piece):
        carry(way, piece).wait_recv()
        part = pl.ds(pl.multiple_of(piece * size, size), size)
        before = outs[way][part, :].astype(F32)
        term = terms[way][part, :].astype(F32)
        scratch[way][part, :] = (r.decay[part, :] * before + term).astype(BF)
        carry(way, piece).start()

    def beat(t):
        for way in (1, 0):
            spot = spots[way]
            piece = t - lag * (spot - 1)

            @pl.when((piece >= 0) & (piece < pieces) & (spot > 0) & (spot < S - 1))
            def _(way=way, piece=piece):
                pass_state(way, piece)

    def short_beat(t):
        beat_of = ((1, 1, [t]), (1, 2, [t - lag]), (0, 1, [t]), (0, 2, catch_up.get(t, [])))
        for way, spot, some in beat_of:
            some = [p for p in some if 0 <= p < pieces]
            if some:

                @pl.when(spots[way] == spot)
                def _(way=way, some=some):
                    for piece in some:
                        pass_state(way, piece)

    def gather(q, landing, slot):
        return rcopy(r.xs, r.xc.at[:, :, landing], r.gat_s.at[q], r.gat_r.at[slot], chan=q)

    spread = head_mask(width, True)
    cumulative = r.cum[...]
    across = cumulative.T
    row = lax.broadcasted_iota(jnp.int32, (length, length), 0)
    col = lax.broadcasted_iota(jnp.int32, (length, length), 1)
    causal = row >= col
    lower = causal.astype(F32)
    into, out_of = r.mix[:, :half], r.mix[:, half:]
    scores = mm(out_of, into, 1, 1)
    r.stepped[...] = (r.act[...] * r.step_wide[...]).astype(BF)
    inner = r.sum_in[...]
    gate = jax.nn.sigmoid(inner)
    r.slope_in[...] = gate * (1.0 + inner * (1.0 - gate))
    skip_wide = exact(jnp.broadcast_to(r.vec[2:3, :], (8, LANES)), spread)
    r.skips[...] = skip_wide
    r.pad_in[length:, :] = jnp.zeros((8, width), F32)
    r.pad_mix[length:, :] = jnp.zeros((8, mixed), F32)

    def head(h):
        cols = slice(h * HDIM, (h + 1) * HDIM)
        gap = cumulative[:, h : h + 1] - across[h : h + 1, :]
        decay = jnp.where(causal, jnp.exp(jnp.where(causal, gap, 0.0)), 0.0)
        weights = (decay * scores).astype(BF)
        grad_h, step_h = r.grad[:, cols], r.stepped[:, cols]
        term = decay * mm(grad_h, step_h, 1, 1)
        r.score_grad[...] = term if h == 0 else r.score_grad[...] + term
        r.z[:, cols] = mm(weights, grad_h, 0, 0)
        r.y[:, cols] = mm(weights, step_h, 1, 0)

    def strip(j):
        return slice(j * LANES, (j + 1) * LANES)

    def halo(j):
        return rcopy(r.hal_o.at[j], r.hal_i.at[j], r.hal_s.at[0], r.hal_r.at[j], seq=below)

    def strip_sum(j):
        cols = strip(j)

        @pl.when(spots[1] == S - 1)
        def _():
            for piece in range(j * per, (j + 1) * per):
                carry(1, piece).wait_recv()

        ending = r.fading[:, cols] * mm(into, r.end[cols, :], 1, 1)
        r.ending[:, cols] = ending
        direct = r.skips[0:1, cols] * r.grad[:, cols].astype(F32)
        total = (r.step_wide[:, cols] * (r.z[:, cols] + ending) + direct) * r.slope_in[:, cols]
        r.pad_in[0:length, cols] = total
        r.hal_o[j] = total[0:8, :]

        @pl.when(me > 0)
        def _():
            halo(j).start()

    def part(p, e, k):
        return r.gin.at[k, e, :, pl.ds(p * LANES, LANES)]

    def zcopy(p, way, k):
        send = (r.u_s if way == "up" else r.d_s).at[k]
        here = part(p, mine, k)
        return rcopy(here, here, send, r.z_r.at[p, k], seq=above if way == "up" else below)

    def ccopy(p, k, e, to):
        return rcopy(part(p, e, k), part(p, e, k), r.x_s.at[to, k], r.c_r.at[e, k], dp=to)

    def strip_out(j):
        cols = strip(j)

        @pl.when(me < S - 1)
        def _():
            halo(j).wait_recv()
            r.pad_in[length:, cols] = r.hal_i[j]

        r.gin[me, mine, :, cols] = spread_back(r.pad_in, r.conv_in, 0, length, cols)
        for e in others:
            ccopy(j, me, mine, e).start()

    def strip_up(j):
        zcopy(j, "up", me).start()

    def strip_early(j):
        strip_out(j)
        strip_up(j)

    def strip_along(j, sent):
        @pl.when((me < S - 1) & (spots[1] != 2) if sent else me < S - 1)
        def _():
            strip_up(j)

        @pl.when(me > 0)
        def _():
            zcopy(j, "down", me).start()

    beats = pieces + lag * max(S - 3, 0)
    early = heads // 2
    for h in range(early):
        head(h)
    near = spots[1] <= 1
    crossed()
    each(C, lambda d: gather(lax.rem(ch + d, C), ch, ch).start())
    r.xc[:, :, ch] = r.xs[...]
    if S == 4:
        sums = {per * j + per - 1: j for j in range(strips)}
        late = {lag + t: j for t, j in sums.items()}
        for t in range(max(beats, heads - early)):
            short_beat(t)
            if early + t < heads:
                head(early + t)
            if t in sums:
                pl.when(near)(functools.partial(strip_sum, sums[t]))
            if t in late:
                pl.when(near)(functools.partial(strip_out, late[t]))
                pl.when(spots[1] == 2)(functools.partial(strip_sum, late[t]))
            if t - 2 in late:
                pl.when(spots[1] == 2)(functools.partial(strip_early, late[t - 2]))
        done = {j: t + 2 < max(beats, heads - early) for t, j in late.items()}
        for j in range(strips):
            pl.when(spots[1] > 2)(functools.partial(strip_sum, j))
            pl.when(spots[1] > (2 if done[j] else 1))(functools.partial(strip_out, j))
            strip_along(j, done[j])
    else:
        for h in range(early, heads):
            head(h)
        lax.fori_loop(0, beats, lambda t, c: (beat(t), c)[1], 0)
        for j in range(strips):
            strip_sum(j)
        for j in range(strips):
            strip_out(j)
            strip_along(j, False)

    def forward(p, way, d):
        k = me - d if way == "up" else me + d
        there = (k >= 0) if way == "up" else (k < S)
        more = (me < S - 1) if way == "up" else (me > 0)

        @pl.when(there)
        def _():
            zcopy(p, way, k).wait_recv()

        @pl.when(there & more)
        def _():
            zcopy(p, way, k).start()

        @pl.when(there)
        def _():
            for e in others:
                ccopy(p, k, mine, e).start()

    def both(p, d):
        forward(p, "up", d)
        forward(p, "down", d)

    def hop(d):
        for p in range(strips):
            both(p, d)

    def soon(p):
        pl.when(spots[1] != 2)(lambda: both(p, 1))

    def later(p):
        pl.when(spots[1] == 2)(lambda: both(p, 1))

    @pl.when(spots[0] == S - 1)
    def _():
        for piece in range(pieces):
            carry(0, piece).wait_recv()

    soon(0)
    start, end = r.start[...], r.end[...]
    score_grad = r.score_grad[...]
    mixer = r.sum_mix[...]
    gate = jax.nn.sigmoid(mixer)
    mixer_slope = gate * (1.0 + mixer * (1.0 - gate))
    faded = (r.fading[...] * r.stepped[...].astype(F32)).astype(BF)
    into_grad = mm(score_grad, out_of, 0, 0) + mm(faded, end, 1, 0)
    out_grad = mm(score_grad, into, 1, 0) + mm(r.pulled[...], start, 1, 0)
    r.pad_mix[0:length, :half] = into_grad * mixer_slope[:, :half]
    r.pad_mix[0:length, half:] = out_grad * mixer_slope[:, half:]
    r.am[0:length, :] = r.pad_mix[0:length, :].astype(BF)
    r.am[length:, :] = jnp.zeros((PAD, mixed), BF)
    r.halm_o[...] = r.pad_mix[0:8, :]

    def share_mix(q, landing, slot):
        some = r.am.at[pl.ds(pl.multiple_of(q * rows, rows), rows + PAD)]
        return rcopy(some, r.gm_in.at[landing], r.gm_s.at[q], r.gm_r.at[slot], chan=q)

    def mix_tail(slot):
        return rcopy(
            r.am.at[pl.ds(0, PAD)], r.mt_in.at[slot], r.mt_s.at[0], r.mt_r.at[slot],
            seq=below, chan=jnp.int32(C - 1),
        )

    def mix_halo():
        return rcopy(r.halm_o, r.halm_i, r.halm_s.at[0], r.halm_s.at[1], seq=below)

    each(C, lambda d: share_mix(lax.rem(ch + d, C), ch, ch).start())

    @pl.when(me > 0)
    def _():
        mix_tail(ch).start()
        mix_halo().start()

    r.gm_in[ch] = r.am[pl.ds(pl.multiple_of(ch * rows, rows), rows + PAD), :]
    r.gmp[...] = spread_back(r.pad_mix, r.conv_mix, 0, length)

    soon(1)

    upstream = r.grad[...].astype(F32)
    stepped = r.stepped[...].astype(F32)
    ending = r.ending[...]
    carried = r.grown[...] * mm(out_of, start, 1, 1)
    to_heads = functools.partial(exact, b=spread, da=1, db=1)
    z = r.z[...]
    step_grad = to_heads(r.act[...] * (z + ending))
    tail_term = to_heads(stepped * ending)
    sum_grad = to_heads(upstream * (r.y[...] + carried) - stepped * z) - tail_term
    held = jnp.sum(start.astype(F32) * end.astype(F32), axis=1, keepdims=True)
    last = cumulative[length - 1 : length, :]
    overall = jnp.sum(tail_term, axis=0, keepdims=True) + jnp.exp(last) * jnp.sum(
        head_mask(width, False) * held, axis=0, keepdims=True
    )
    decay_grad = exact_left(lower, sum_grad, 0, 0) + overall
    rate = jnp.exp(r.vec[1:2, :])
    step_grad = (step_grad - rate * decay_grad) * jax.nn.sigmoid(r.raw[...] + r.vec[0:1, :])
    steps = step_grad.astype(BF)
    r.gsm[me, mine, rows:, 0:LANES] = step_grad.T[0:PAD, :].astype(BF)
    steps = steps[:, 0:PAD]

    soon(2)

    each(C, lambda d: share_mix(lax.rem(ch + d, C), ch, lax.rem(ch + d, C)).wait_recv())
    mix = r.gm_in[0].astype(F32)
    for q in range(1, C):
        mix = mix + r.gm_in[q].astype(F32)
    r.gmt[...] = mix

    @pl.when((me < S - 1) & (ch == C - 1))
    def _():
        for q in range(C):
            mix_tail(q).wait_recv()
        tail = r.mt_in[0].astype(F32)
        for q in range(1, C):
            tail = tail + r.mt_in[q].astype(F32)
        r.gmt[rows:, :] = tail

    r.gsm[me, mine, 0:rows, :] = spread_back(r.gmt, r.conv_mix, 0, rows)

    def small_along(e, k, q):
        here = r.gsm.at[k, e]
        return rcopy(here, here, r.z2_s.at[e, q], r.z2_r.at[e, k], seq=q)

    def cross_small(to):
        here = r.gsm.at[me, mine]
        return rcopy(here, here, r.z2_s.at[to, me], r.z2_r.at[mine, me], dp=to)

    def crossed_small(e):
        here = r.gsm.at[me, e]
        return rcopy(here, here, r.z2_s.at[e, me], r.z2_r.at[e, me], dp=e)

    def send_small(e):
        each(S, lambda d: small_along(e, me, lax.rem(me + d, S)).start())

    def small_all(do):
        for e in [mine] + others:
            each(S, lambda d, e=e: do(e, lax.rem(me + d, S)))

    for p in range(3, strips):
        soon(p)
    later(0)

    def share_p(j, q, landing, slot):
        piece = pl.ds(j * cut, cut)
        return rcopy(
            r.p_o.at[q, :, piece], r.p_i.at[landing, :, piece], r.p_s.at[q], r.p_r.at[slot], chan=q
        )

    def whole_p(q):
        return rcopy(r.p_o.at[q], r.p_i.at[q], r.p_s.at[q], r.p_r.at[q], chan=q)

    grads = r.gin[me, mine]
    mixes = r.gmp[...]

    def send_p(j, final):
        def one(d):
            q = lax.rem(ch + d, C)

            @pl.when((q == C - 1) if final else (q < C - 1))
            def _():
                share_p(j, q, ch, ch).start()

        each(C, one)

    for j in range(parts):
        piece = slice(j * cut, (j + 1) * cut)
        out = mm(grads, r.w_in[piece, :], 1, 1) + mm(mixes, r.w_mix[piece, :], 1, 1)
        out = out + mm(steps, r.wst[0:PAD, piece], 1, 0)
        r.p_o[:, :, piece] = out.astype(BF).reshape(C, rows, cut)
        r.p_last[:, piece] = out[length - PAD :, :]
        send_p(j, False)
        if j != 1:
            later(max(j, 1))
        if j == 0:
            send_small(mine)
            for e in others:
                cross_small(e).start()

    @pl.when(me < S - 1)
    def _():
        mix_halo().wait_recv()
        r.pad_mix[length:, :] = r.halm_i[...]
        final = spread_back(r.pad_mix, r.conv_mix, length - PAD, PAD)
        change = final.astype(F32) - r.gmp[length - PAD :, :].astype(F32)
        fixed = r.p_last[...] + mm(change, r.w_mix[...], 1, 1)
        r.p_o[C - 1, rows - PAD :, :] = fixed.astype(BF)

    for j in range(parts):
        send_p(j, True)
    for p in range(parts, strips):
        later(p)
    for p in range(strips):
        both(p, 2)
        if p == strips // 2:
            for e in others:
                crossed_small(e).wait_recv()
                send_small(e)
    if S <= 12:
        for d in range(3, S):
            hop(d)
    else:
        lax.fori_loop(3, S, lambda d, c: (hop(d), c)[1], 0)
    small_all(lambda e, q: small_along(e, q, q).wait_recv())
    norm = 1.0 / math.sqrt(D * S * length)
    columns = r.xc.shape[-1]

    def settle_gather(d):
        q = lax.rem(ch + d, C)
        gather(q, q, q).wait()

    each(C, settle_gather)
    mixer_columns = r.xc[:, :, ch].reshape(S * D * rows, columns)
    mixer_grads = r.gsm[:, :, 0:rows, :].reshape(S * D * rows, mixed)
    mixer_term = norm * mm(mixer_columns, mixer_grads, 0, 0)
    band = columns // C
    for q in range(C):
        r.m_o[q] = mixer_term[q * band : (q + 1) * band, :].astype(BF)

    def share_m(q, landing, slot):
        return rcopy(r.m_o.at[q], r.m_i.at[landing], r.m_s.at[q], r.m_r.at[slot], chan=q)

    each(C, lambda d: share_m(lax.rem(ch + d, C), ch, ch).start())
    def step_term(k, total):
        for e in range(D):
            x = r.xc[k, e].reshape(length, columns)
            total = total + mm(r.gsm[k, e, rows:, 0:LANES], x, 1, 0)
        return total

    step_total = jnp.zeros((PAD, columns), F32)
    if S <= 12:
        for k in range(S):
            step_total = step_term(k, step_total)
    else:
        step_total = lax.fori_loop(0, S, step_term, step_total)
    r.o_dws[...] = (norm * step_total)[:heads, :]

    def whole(k, e, send, recv):
        return rcopy(r.gin.at[k, e], r.gin.at[k, e], send, recv, seq=above)

    def weight_term(k, first=False):
        for e in others:
            whole(k, e, r.x_s.at[e, k], r.c_r.at[e, k]).wait_recv()
        x = r.xc[k].reshape(D * length, columns)
        term = norm * mm(x, r.gin[k].reshape(D * length, width), 0, 0)
        r.o_dw[...] = term if first else r.o_dw[...] + term

    def weight_terms(d):
        for k, there in ((me + d, me + d < S), (me - d, me >= d)):
            pl.when(there)(functools.partial(weight_term, k))

    weight_term(me, True)
    each(S, weight_terms)
    r.p_i[ch] = r.p_o[ch]
    r.m_i[ch] = r.m_o[ch]
    each(C, lambda d: whole_p(lax.rem(ch + d, C)).wait_recv())
    each(C, lambda d: share_m(lax.rem(ch + d, C), ch, lax.rem(ch + d, C)).wait_recv())

    for way in (0, 1):

        @pl.when(spots[way] < S - 1)
        def _(way=way):
            rcopy(terms[way], outs[way], r.chain_s.at[way], r.chain_r.at[way, 0], seq=above).wait_send()

    @pl.when(me > 0)
    def _():
        rcopy(r.hal_o, r.hal_i, r.hal_s.at[0], r.hal_r.at[0], seq=below).wait_send()
        mix_halo().wait_send()
        mix_tail(ch).wait_send()

    def settle_chan(d):
        q = lax.rem(ch + d, C)
        share_mix(q, ch, ch).wait_send()
        share_m(q, ch, ch).wait_send()
        whole_p(q).wait_send()

    each(C, settle_chan)

    def settle_line(k):
        for e in others:
            whole(k, mine, r.x_s.at[e, k], r.c_r.at[mine, k]).wait_send()
        for way, sent in (("up", (k <= me) & (me < S - 1)), ("down", (k >= me) & (me > 0))):

            @pl.when(sent)
            def _(way=way):
                whole(k, mine, (r.u_s if way == "up" else r.d_s).at[k], r.z_r.at[0, k]).wait_send()

    settle_line(0)
    each(S, settle_line)
    small_all(lambda e, q: small_along(e, me, q).wait_send())
    for e in others:
        cross_small(e).wait_send()


def finish_kernel(parts, dw, mixes, dws, o_ig, o_dw, o_dwm, o_dws, ig, dwm, sems):
    copies = [
        pltpu.make_async_copy(a, b, sems.at[i])
        for i, (a, b) in enumerate(((dw, o_dw), (dws, o_dws), (ig, o_ig), (dwm, o_dwm)))
    ]
    copies[0].start()
    copies[1].start()
    total = parts[0].astype(F32)
    for q in range(1, parts.shape[0]):
        total = total + parts[q].astype(F32)
    ig[...] = total.astype(BF)
    copies[2].start()
    total = mixes[0].astype(F32)
    for q in range(1, mixes.shape[0]):
        total = total + mixes[q].astype(F32)
    dwm[...] = total
    copies[3].start()
    for copy in copies:
        copy.wait()


def body(
    sizes,
    layer_input,
    inner_weight,
    mixer_weight,
    step_weight,
    conv_inner,
    conv_mixer,
    step_bias,
    decay_log,
    skip_gain,
    output_grad,
):
    own = layer_input[0]
    rows, model = own.shape
    chans, seqs, dps = sizes["chan"], sizes["seq"], sizes["dp"]
    groups = dps * seqs
    length = rows * chans
    width = inner_weight.shape[1]
    mixed = mixer_weight.shape[1]
    heads = step_bias.shape[0]
    cols = model // groups
    state_size = mixed // 2
    assert width % PIECES == 0 and chans % 2 == 0 and seqs > 2
    assert width > 3 * LANES and chans == 4 and rows == 2 * PAD and width % LANES == 0 and PIECES % (width // LANES) == 0
    assert length == LANES and heads + conv_inner.shape[0] - 1 <= PAD
    upstream = output_grad[0]
    step_rows = step_weight.T
    bias, rates, skips = (v.reshape(1, heads) for v in (step_bias, decay_log, skip_gain))
    dma = pltpu.SemaphoreType.DMA
    vmem = pl.BlockSpec(memory_space=pltpu.VMEM)
    hbm = pl.BlockSpec(memory_space=pltpu.HBM)
    small = rows + PAD
    strips = width // LANES
    band = cols // chans

    def low(*shape):
        return pltpu.VMEM(shape, BF)

    def full(*shape):
        return pltpu.VMEM(shape, F32)

    inputs = dict(
        own=own, w_in=inner_weight, w_mix=mixer_weight, w_step=step_rows, conv_in=conv_inner,
        conv_mix=conv_mixer, bias=bias, log=rates, skip=skips, grad=upstream,
    )
    outputs = dict(
        p_i=jax.ShapeDtypeStruct((chans, rows, model), BF),
        o_dw=jax.ShapeDtypeStruct((cols, width), F32),
        m_i=jax.ShapeDtypeStruct((chans, band, mixed), BF),
        o_dws=jax.ShapeDtypeStruct((heads, cols), F32),
    )
    scratch = {key: pltpu.VMEM(v.shape, v.dtype) for key, v in inputs.items()}
    scratch |= dict(
        wst=low(LANES, model), xg=low(length, model),
        blocks=low(dps, seqs, rows, cols),
        xs=low(seqs, dps, rows, cols), xc=low(seqs, dps, chans, rows, cols),
        wide_in=full(PAD + length, width), wide_mix=full(PAD + length, mixed),
        fh_o=low(PAD, width + mixed), fh_i=low(PAD, width + mixed), vec=full(8, LANES),
        sum_in=full(length, width), sum_mix=full(length, mixed), raw=full(length, LANES),
        cum=full(length, LANES), step_wide=full(length, width), fading=full(length, width),
        grown=full(length, width), pulled=low(length, width), decay=full(width, state_size),
        mix=low(length, mixed), act=full(length, width), stepped=low(length, width),
        state_term=low(width, state_size), back_term=low(width, state_size),
        start=low(width, state_size), end=low(width, state_size),
        scr0=low(width, state_size), scr1=low(width, state_size),
        z=full(length, width), y=full(length, width), score_grad=full(length, length),
        slope_in=full(length, width),
        pad_in=full(length + 8, width), pad_mix=full(length + 8, mixed),
        gin=low(seqs, dps, length, width), gsm=low(seqs, dps, small, mixed),
        hal_o=full(strips, 8, LANES), hal_i=full(strips, 8, LANES),
        halm_o=full(8, mixed), halm_i=full(8, mixed), p_last=full(PAD, model),
        skips=full(8, width), ending=full(length, width),
        gmp=low(length, mixed), gm_in=low(chans, small, mixed), gmt=full(small, mixed),
        am=low(length + PAD, mixed), mt_in=low(chans, PAD, mixed),
        p_o=low(chans, rows, model), m_o=low(chans, band, mixed),
        load_sem=dma((len(LOADED),)), fh_sem=dma((2,)), halm_s=dma((2,)),
        hal_s=dma((1,)), hal_r=dma((strips,)),
        near_s=dma((1,)), near_r=dma((chans,)),
        far_s=dma((chans // 2,)), far_r=dma((chans // 2, chans)),
        relay_s=dma((chans // 2,)), relay_r=dma((chans // 2, chans)),
        cross_s=dma((dps, seqs)), cross_r=dma((dps, seqs)),
        gat_s=dma((chans,)), gat_r=dma((chans,)),
        chain_s=dma((2,)), chain_r=dma((2, PIECES)),
        z_r=dma((strips, seqs)), c_r=dma((dps, seqs)),
        u_s=dma((seqs,)), d_s=dma((seqs,)), x_s=dma((dps, seqs)),
        z2_r=dma((dps, seqs)),
        z2_s=dma((dps, seqs)), mt_s=dma((1,)), mt_r=dma((chans,)),
        gm_s=dma((chans,)), gm_r=dma((chans,)),
        p_s=dma((chans,)), p_r=dma((chans,)), m_s=dma((chans,)), m_r=dma((chans,)),
    )
    names = [key + "_h" for key in inputs] + list(outputs) + list(scratch)
    parts, inner_grad, mix_parts, step_grad = pl.pallas_call(
        functools.partial(layer_kernel, names, sizes, heads),
        out_shape=tuple(outputs.values()),
        in_specs=[hbm] * len(inputs),
        out_specs=(vmem,) * len(outputs),
        scratch_shapes=list(scratch.values()),
        compiler_params=pltpu.CompilerParams(
            collective_id=0, has_side_effects=True, vmem_limit_bytes=LIMIT
        ),
        name="layer",
    )(*(pltpu.with_memory_space_constraint(v, pltpu.HBM) for v in inputs.values()))
    input_grad, inner_grad, mixer_grad, step_grad = pl.pallas_call(
        finish_kernel,
        out_shape=(
            jax.ShapeDtypeStruct((rows, model), BF),
            jax.ShapeDtypeStruct((cols, width), F32),
            jax.ShapeDtypeStruct((band, mixed), F32),
            jax.ShapeDtypeStruct((heads, cols), F32),
        ),
        in_specs=[vmem] * 4,
        out_specs=(pl.BlockSpec(memory_space=pl.ANY),) * 4,
        scratch_shapes=[
            pltpu.VMEM((rows, model), BF),
            pltpu.VMEM((band, mixed), F32),
            dma((4,)),
        ],
        compiler_params=pltpu.CompilerParams(vmem_limit_bytes=LIMIT),
        name="finish",
    )(parts, inner_grad, mix_parts, step_grad)
    return input_grad[None], inner_grad, mixer_grad, step_grad.T


def solution(mesh):
    sizes = dict(mesh.shape)
    in_specs = (
        P("dp", ("seq", "chan"), None),
        P(None, "chan"),
        P(),
        P(None, "chan"),
        P(None, "chan"),
        P(),
        P("chan"),
        P("chan"),
        P("chan"),
        P("dp", "seq", "chan"),
    )
    out_specs = (
        P("dp", ("seq", "chan"), None),
        P(("dp", "seq"), "chan"),
        P(("dp", "seq", "chan"), None),
        P(("dp", "seq"), "chan"),
    )
    return jax.shard_map(
        functools.partial(body, sizes),
        mesh=mesh,
        in_specs=in_specs,
        out_specs=out_specs,
        check_vma=False,
    )
```

```python
import functools
import math
import types

import jax
import jax.numpy as jnp
from jax import lax
from jax.experimental import pallas as pl
from jax.experimental.pallas import tpu as pltpu
from jax.sharding import PartitionSpec as P

MESH = pl.DeviceIdType.MESH
HDIM = 64
PAD = 16
LANES = 128
LIMIT = 48 * 2**20
BF = jnp.bfloat16
F32 = jnp.float32
PIECES = 10
LOADED = (
    "own", "w_in", "w_mix", "w_step", "conv_in", "conv_mix", "bias", "log", "skip", "grad",
)


def each(n, step):
    if n <= 12:
        for d in range(1, n):
            step(d)
    else:

        def one(d, carry):
            step(d)
            return carry

        lax.fori_loop(1, n, one, 0)


def signal_to(barrier, where):
    pl.semaphore_signal(barrier, inc=1, device_id=where, device_id_type=MESH)


def mm(a, b, da, db):
    return lax.dot_general(
        a.astype(BF), b.astype(BF), (((da,), (db,)), ((), ())), preferred_element_type=F32
    )


def thirds(v):
    high = v.astype(BF)
    rest = v - high.astype(F32)
    middle = rest.astype(BF)
    return high, middle, (rest - middle.astype(F32)).astype(BF)


def exact(a, b, da=1, db=0):
    high, middle, low = thirds(a)
    return mm(high, b, da, db) + (mm(middle, b, da, db) + mm(low, b, da, db))


def exact_left(a, b, da=1, db=0):
    high, middle, low = thirds(b)
    return mm(a, high, da, db) + (mm(a, middle, da, db) + mm(a, low, da, db))


def softplus(v):
    return jnp.maximum(v, 0.0) + jnp.log1p(jnp.exp(-jnp.abs(v)))


def head_mask(width, heads_first):
    shape = (LANES, width) if heads_first else (width, LANES)
    head = lax.broadcasted_iota(jnp.int32, shape, 0 if heads_first else 1)
    column = lax.broadcasted_iota(jnp.int32, shape, 1 if heads_first else 0)
    return (column // HDIM == head).astype(F32)


def decays(raw, bias, decay_log):
    length = raw.shape[0]
    step = softplus(raw + bias)
    rate = jnp.exp(decay_log)
    row = lax.broadcasted_iota(jnp.int32, (length, length), 0)
    col = lax.broadcasted_iota(jnp.int32, (length, length), 1)
    lower = (row >= col).astype(F32)
    cumulative = exact_left(lower, -step * rate)
    return step, rate, cumulative, row, col, lower


def rcopy(src, dst, send, recv, **where):
    return pltpu.make_async_remote_copy(
        src_ref=src, dst_ref=dst, send_sem=send, recv_sem=recv, device_id=where, device_id_type=MESH
    )


def greet_all(barrier, axis, n):
    me = lax.axis_index(axis)
    each(n, lambda d: signal_to(barrier, {axis: lax.rem(me + d, n)}))
    return n - 1


def convolved(wide, kernel, first, count):
    taps = kernel.shape[0]
    first = first + PAD - (taps - 1)
    total = kernel[0:1, :] * wide[pl.ds(first, count), :]
    for k in range(1, taps):
        total = total + kernel[k : k + 1, :] * wide[pl.ds(first + k, count), :]
    return total


def spread_back(pad, kernel, first, count, cols=slice(None)):
    taps = kernel.shape[0]
    total = None
    for k in range(taps):
        term = kernel[k : k + 1, cols] * pad[pl.ds(first + taps - 1 - k, count), cols]
        total = term if total is None else total + term
    return total.astype(BF)


def layer_kernel(names, sizes, heads, *refs):
    r = types.SimpleNamespace(**dict(zip(names, refs, strict=True)))
    place = (lax.axis_index("dp"), lax.axis_index("seq"), lax.axis_index("chan"))
    D, S, C = sizes["dp"], sizes["seq"], sizes["chan"]
    barrier = pltpu.get_barrier_semaphore()
    total = greet_all(barrier, "dp", D) + greet_all(barrier, "seq", S) + greet_all(barrier, "chan", C)
    after = lax.rem(place[1] + 1, S)

    @pl.when(place[2] == C - 1)
    def _():
        for c in range(C):
            signal_to(barrier, {"seq": after, "chan": jnp.int32(c)})

    total += 1 + (D - 1) * (S - 1)
    for e in range(1, D):
        far = lax.rem(place[0] + e, D)
        each(S, lambda d, far=far: signal_to(barrier, {"dp": far, "seq": lax.rem(place[1] + d, S)}))
    loads = {
        key: pltpu.make_async_copy(getattr(r, key + "_h"), getattr(r, key), r.load_sem.at[i])
        for i, key in enumerate(LOADED)
    }
    for copy in loads.values():
        copy.start()
    crossed = front(r, sizes, place, heads, loads, barrier, total)
    rear(r, sizes, place, heads, crossed)


def front(r, sizes, place, heads, loads, barrier, total):
    D, S, C = sizes["dp"], sizes["seq"], sizes["chan"]
    mine, me, ch = place
    rows, model = r.own.shape
    length, width = r.sum_in.shape
    mixed = r.sum_mix.shape[1]
    cols = model // (D * S)
    half = mixed // 2
    splits = 2
    high = rows // 2
    cut = model // splits
    pieces = [(1, k) for k in range(splits)] + [(0, k) for k in range(splits)]
    sides = C // 2
    side, low = lax.div(ch, 2), lax.rem(ch, 2)
    partner = ch + 1 - 2 * low

    def block(c, p):
        part, k = pieces[p]
        first = pl.multiple_of(c * rows + part * high, high)
        return r.xg.at[pl.ds(first, high), pl.ds(k * cut, cut)]

    def mine_at(p):
        part, k = pieces[p]
        return r.own.at[pl.ds(part * high, high), pl.ds(k * cut, cut)]

    def near(c, p):
        return rcopy(mine_at(p), block(c, p), r.near_s.at[0], r.near_r.at[p], chan=partner)

    def far(to, c, slot, p):
        return rcopy(
            mine_at(p), block(c, p), r.far_s.at[to], r.far_r.at[slot, p], chan=2 * to + low
        )

    def relay(source, lane, p):
        c = 2 * source + lane
        here = block(c, p)
        return rcopy(here, here, r.relay_s.at[source], r.relay_r.at[source, p], chan=partner)

    def column(e, q, landing_e, landing_q):
        return rcopy(
            r.blocks.at[e, q], r.xs.at[landing_q, landing_e],
            r.cross_s.at[e, q], r.cross_r.at[landing_e, landing_q], dp=e, seq=q,
        )

    def columns_all(do):
        each(S, lambda d: do(mine, lax.rem(me + d, S)))
        for d in range(1, D):
            e = lax.rem(mine + d, D)
            do(e, me)
            each(S, lambda d, e=e: do(e, lax.rem(me + d, S)))

    loads["own"].wait()
    pl.semaphore_wait(barrier, total)
    for p in range(len(pieces)):
        for d in range(1, sides):
            far(lax.rem(side + d, sides), ch, side, p).start()
        near(ch, p).start()
    for d in range(D):
        for k in range(S):
            at = (d * S + k) * cols
            r.blocks[d, k] = r.own[:, at : at + cols]
    columns_all(lambda e, q: column(e, q, mine, me).start())
    r.xs[me, mine] = r.blocks[mine, me]
    r.xg[pl.ds(pl.multiple_of(ch * rows, rows), rows), :] = r.own[...]
    r.wst[...] = jnp.zeros(r.wst.shape, BF)
    r.vec[...] = jnp.zeros(r.vec.shape, F32)
    for key in LOADED[1:]:
        loads[key].wait()
    r.wst[0:heads, :] = r.w_step[...]
    for i, ref in enumerate((r.bias, r.log, r.skip)):
        r.vec[i : i + 1, 0:heads] = ref[...]

    def pass_on(p):
        for d in range(1, sides):
            source = lax.rem(side + d, sides)
            far(source, ch, source, p).wait_recv()
            relay(source, low, p).start()

    def project(p):
        near(partner, p).wait_recv()
        for d in range(1, sides):
            source = lax.rem(side + d, sides)
            relay(source, 1 - low, p).wait_recv()
        part, k = pieces[p]
        piece = slice(k * cut, (k + 1) * cut)
        x = jnp.concatenate([r.xg[c * rows + part * high : c * rows + (part + 1) * high, piece] for c in range(C)])
        inner = mm(x, r.w_in[piece, :], 1, 0)
        mixer = mm(x, r.w_mix[piece, :], 1, 0)
        raw = mm(x, r.wst[:, piece], 1, 1)
        for c in range(C):
            at = c * rows + part * high
            here = slice(c * high, (c + 1) * high)
            for ref, pad, term in ((r.wide_in, PAD, inner), (r.wide_mix, PAD, mixer), (r.raw, 0, raw)):
                old = ref[pad + at : pad + at + high, :] if k else 0.0
                ref[pad + at : pad + at + high, :] = old + term[here, :]

    def halo():
        return rcopy(r.fh_o, r.fh_i, r.fh_sem.at[0], r.fh_sem.at[1], seq=lax.rem(me + 1, S))

    pass_on(0)
    for p in range(len(pieces)):
        if p + 1 < len(pieces):
            pass_on(p + 1)
        project(p)
        if p == splits - 1:
            r.fh_o[:, :width] = r.wide_in[length:, :].astype(BF)
            r.fh_o[:, width:] = r.wide_mix[length:, :].astype(BF)
            pl.when(me < S - 1)(lambda: halo().start())
    inner_low = r.wide_in[PAD:, :].astype(BF)
    mixer_low = r.wide_mix[PAD:, :].astype(BF)
    r.wide_in[PAD:, :] = inner_low.astype(F32)
    r.wide_mix[PAD:, :] = mixer_low.astype(F32)
    r.wide_in[0:PAD, :] = jnp.zeros((PAD, width), F32)
    r.wide_mix[0:PAD, :] = jnp.zeros((PAD, mixed), F32)
    r.sum_in[PAD:, :] = convolved(r.wide_in, r.conv_in, PAD, length - PAD)
    r.sum_mix[PAD:, :] = convolved(r.wide_mix, r.conv_mix, PAD, length - PAD)
    step, rate, cumulative, row, col, lower = decays(r.raw[...], r.vec[0:1, :], r.vec[1:2, :])
    last = cumulative[length - 1 : length, :]
    spread = head_mask(width, True)
    r.cum[...] = cumulative
    step_wide = exact(step, spread)
    fading = exact(jnp.exp(last - cumulative), spread)
    grown = exact(jnp.exp(cumulative), spread)
    r.step_wide[...] = step_wide
    r.fading[...] = fading
    r.grown[...] = grown
    pulled = (grown * r.grad[...].astype(F32)).astype(BF)
    r.pulled[...] = pulled
    row_decay = jnp.sum(head_mask(width, False) * jnp.exp(last), axis=1, keepdims=True)
    r.decay[...] = jnp.broadcast_to(row_decay, r.decay.shape)

    @pl.when(me > 0)
    def _():
        halo().wait_recv()
        r.wide_in[0:PAD, :] = r.fh_i[:, :width].astype(F32)
        r.wide_mix[0:PAD, :] = r.fh_i[:, width:].astype(F32)

    r.sum_in[0:PAD, :] = convolved(r.wide_in, r.conv_in, 0, PAD)
    r.sum_mix[0:PAD, :] = convolved(r.wide_mix, r.conv_mix, 0, PAD)
    mixer = r.sum_mix[...]
    mix = mixer * jax.nn.sigmoid(mixer)
    r.mix[...] = mix.astype(BF)
    r.back_term[...] = mm(pulled, mix[:, half:], 0, 0).astype(BF)
    inner = r.sum_in[...]
    act = inner * jax.nn.sigmoid(inner)
    r.act[...] = act
    r.state_term[...] = mm(act * (fading * step_wide), mix[:, :half], 0, 0).astype(BF)

    @pl.when(me < S - 1)
    def _():
        halo().wait_send()

    def sent(sem):
        rcopy(r.own, r.own, sem, r.near_r.at[0], chan=partner).wait_send()

    sent(r.near_s.at[0])
    for d in range(1, sides):
        source = lax.rem(side + d, sides)
        sent(r.far_s.at[source])
        sent(r.relay_s.at[source])
    return lambda: columns_all(lambda e, q: column(e, q, e, q).wait())


def rear(r, sizes, place, heads, crossed):
    D, S, C = sizes["dp"], sizes["seq"], sizes["chan"]
    mine, me, ch = place
    length, width = r.sum_in.shape
    mixed = r.sum_mix.shape[1]
    half = mixed // 2
    model = r.w_in.shape[0]
    rows = length // C
    pieces, lag = PIECES, PIECES // 2
    lags = (lag + 1, lag)
    size = width // pieces
    strips = width // LANES
    per = pieces // strips
    parts = C
    cut = model // parts
    terms, outs, scratch = (r.state_term, r.back_term), (r.start, r.end), (r.scr0, r.scr1)
    spots = (me, S - 1 - me)
    above, below = lax.rem(me + 1, S), lax.rem(me + S - 1, S)
    others = [lax.rem(mine + e, D) for e in range(1, D)]

    def carry(way, piece, first=False):
        part = pl.ds(pl.multiple_of(piece * size, size), size)
        source = terms[way] if first else scratch[way]
        sems = r.chain_s.at[way], r.chain_r.at[way, piece]
        return rcopy(source.at[part], outs[way].at[part], *sems, seq=above if way == 0 else below)

    for way in (1, 0):

        @pl.when(spots[way] == 0)
        def _(way=way):
            for piece in range(pieces):
                carry(way, piece, True).start()
            outs[way][...] = jnp.zeros(outs[way].shape, BF)

    def beat(t):
        for way in (1, 0):
            spot = spots[way]
            piece = t - lags[way] * (spot - 1)

            @pl.when((piece >= 0) & (piece < pieces) & (spot > 0) & (spot < S - 1))
            def _(way=way, piece=piece):
                carry(way, piece).wait_recv()
                part = pl.ds(pl.multiple_of(piece * size, size), size)
                before = outs[way][part, :].astype(F32)
                term = terms[way][part, :].astype(F32)
                scratch[way][part, :] = (r.decay[part, :] * before + term).astype(BF)
                carry(way, piece).start()

    def gather(q, landing, slot):
        return rcopy(r.xs, r.xc.at[:, :, landing], r.gat_s.at[q], r.gat_r.at[slot], chan=q)

    spread = head_mask(width, True)
    cumulative = r.cum[...]
    across = cumulative.T
    row = lax.broadcasted_iota(jnp.int32, (length, length), 0)
    col = lax.broadcasted_iota(jnp.int32, (length, length), 1)
    causal = row >= col
    lower = causal.astype(F32)
    into, out_of = r.mix[:, :half], r.mix[:, half:]
    scores = mm(out_of, into, 1, 1)
    r.stepped[...] = (r.act[...] * r.step_wide[...]).astype(BF)
    inner = r.sum_in[...]
    gate = jax.nn.sigmoid(inner)
    r.slope_in[...] = gate * (1.0 + inner * (1.0 - gate))
    skip_wide = exact(jnp.broadcast_to(r.vec[2:3, :], (8, LANES)), spread)
    r.skips[...] = skip_wide
    r.pad_in[length:, :] = jnp.zeros((8, width), F32)
    r.pad_mix[length:, :] = jnp.zeros((8, mixed), F32)

    def head(h):
        cols = slice(h * HDIM, (h + 1) * HDIM)
        gap = cumulative[:, h : h + 1] - across[h : h + 1, :]
        decay = jnp.where(causal, jnp.exp(jnp.where(causal, gap, 0.0)), 0.0)
        weights = (decay * scores).astype(BF)
        grad_h, step_h = r.grad[:, cols], r.stepped[:, cols]
        term = decay * mm(grad_h, step_h, 1, 1)
        r.score_grad[...] = term if h == 0 else r.score_grad[...] + term
        r.z[:, cols] = mm(weights, grad_h, 0, 0)
        r.y[:, cols] = mm(weights, step_h, 1, 0)

    def strip(j):
        return slice(j * LANES, (j + 1) * LANES)

    def halo(j):
        return rcopy(r.hal_o.at[j], r.hal_i.at[j], r.hal_s.at[0], r.hal_r.at[j], seq=below)

    def strip_sum(j):
        cols = strip(j)

        @pl.when(spots[1] == S - 1)
        def _():
            for piece in range(j * per, (j + 1) * per):
                carry(1, piece).wait_recv()

        ending = r.fading[:, cols] * mm(into, r.end[cols, :], 1, 1)
        r.ending[:, cols] = ending
        direct = r.skips[0:1, cols] * r.grad[:, cols].astype(F32)
        total = (r.step_wide[:, cols] * (r.z[:, cols] + ending) + direct) * r.slope_in[:, cols]
        r.pad_in[0:length, cols] = total
        r.hal_o[j] = total[0:8, :]

        @pl.when(me > 0)
        def _():
            halo(j).start()

    def part(p, e, k):
        return r.gin.at[k, e, :, pl.ds(p * LANES, LANES)]

    def zcopy(p, way, k):
        send = (r.u_s if way == "up" else r.d_s).at[k]
        here = part(p, mine, k)
        return rcopy(here, here, send, r.z_r.at[p, k], seq=above if way == "up" else below)

    def ccopy(p, k, e, to):
        return rcopy(part(p, e, k), part(p, e, k), r.x_s.at[to, k], r.c_r.at[e, k], dp=to)

    def strip_out(j):
        cols = strip(j)

        @pl.when(me < S - 1)
        def _():
            halo(j).wait_recv()
            r.pad_in[length:, cols] = r.hal_i[j]

        r.gin[me, mine, :, cols] = spread_back(r.pad_in, r.conv_in, 0, length, cols)
        for e in others:
            ccopy(j, me, mine, e).start()

    def strip_up(j):
        zcopy(j, "up", me).start()

    def strip_early(j):
        strip_out(j)
        strip_up(j)

    def strip_along(j, sent):
        @pl.when((me < S - 1) & (spots[1] != 2) if sent else me < S - 1)
        def _():
            strip_up(j)

        @pl.when(me > 0)
        def _():
            zcopy(j, "down", me).start()

    beats = pieces + lags[0] * max(S - 3, 0)
    early = heads // 2
    for h in range(early):
        head(h)
    near = spots[1] <= 1
    crossed()
    each(C, lambda d: gather(lax.rem(ch + d, C), ch, ch).start())
    r.xc[:, :, ch] = r.xs[...]
    if beats <= 24:
        sums = {per * j + per - 1: j for j in range(strips)}
        late = {lag + t: j for t, j in sums.items()}
        for t in range(max(beats, heads - early)):
            beat(t)
            if early + t < heads:
                head(early + t)
            if t in sums:
                pl.when(near)(functools.partial(strip_sum, sums[t]))
            if t in late:
                pl.when(near)(functools.partial(strip_out, late[t]))
                pl.when(spots[1] == 2)(functools.partial(strip_sum, late[t]))
            if t - 2 in late:
                pl.when(spots[1] == 2)(functools.partial(strip_early, late[t - 2]))
        done = {j: t + 2 < max(beats, heads - early) for t, j in late.items()}
        for j in range(strips):
            pl.when(spots[1] > 2)(functools.partial(strip_sum, j))
            pl.when(spots[1] > (2 if done[j] else 1))(functools.partial(strip_out, j))
            strip_along(j, done[j])
    else:
        for h in range(early, heads):
            head(h)
        lax.fori_loop(0, beats, lambda t, c: (beat(t), c)[1], 0)
        for j in range(strips):
            strip_sum(j)
        for j in range(strips):
            strip_out(j)
            strip_along(j, False)

    @pl.when(spots[0] == S - 1)
    def _():
        for piece in range(pieces):
            carry(0, piece).wait_recv()

    start, end = r.start[...], r.end[...]
    score_grad = r.score_grad[...]
    mixer = r.sum_mix[...]
    gate = jax.nn.sigmoid(mixer)
    mixer_slope = gate * (1.0 + mixer * (1.0 - gate))
    faded = (r.fading[...] * r.stepped[...].astype(F32)).astype(BF)
    into_grad = mm(score_grad, out_of, 0, 0) + mm(faded, end, 1, 0)
    out_grad = mm(score_grad, into, 1, 0) + mm(r.pulled[...], start, 1, 0)
    r.pad_mix[0:length, :half] = into_grad * mixer_slope[:, :half]
    r.pad_mix[0:length, half:] = out_grad * mixer_slope[:, half:]
    r.am[0:length, :] = r.pad_mix[0:length, :].astype(BF)
    r.am[length:, :] = jnp.zeros((PAD, mixed), BF)
    r.halm_o[...] = r.pad_mix[0:8, :]

    def share_mix(q, landing, slot):
        some = r.am.at[pl.ds(pl.multiple_of(q * rows, rows), rows + PAD)]
        return rcopy(some, r.gm_in.at[landing], r.gm_s.at[q], r.gm_r.at[slot], chan=q)

    def mix_tail(slot):
        return rcopy(
            r.am.at[pl.ds(0, PAD)], r.mt_in.at[slot], r.mt_s.at[0], r.mt_r.at[slot],
            seq=below, chan=jnp.int32(C - 1),
        )

    def mix_halo():
        return rcopy(r.halm_o, r.halm_i, r.halm_s.at[0], r.halm_s.at[1], seq=below)

    each(C, lambda d: share_mix(lax.rem(ch + d, C), ch, ch).start())

    @pl.when(me > 0)
    def _():
        mix_tail(ch).start()
        mix_halo().start()

    r.gm_in[ch] = r.am[pl.ds(pl.multiple_of(ch * rows, rows), rows + PAD), :]
    r.gmp[...] = spread_back(r.pad_mix, r.conv_mix, 0, length)

    def forward(p, way, d):
        k = me - d if way == "up" else me + d
        there = (k >= 0) if way == "up" else (k < S)
        more = (me < S - 1) if way == "up" else (me > 0)

        @pl.when(there)
        def _():
            zcopy(p, way, k).wait_recv()

        @pl.when(there & more)
        def _():
            zcopy(p, way, k).start()

        @pl.when(there)
        def _():
            for e in others:
                ccopy(p, k, mine, e).start()

    def both(p, d):
        forward(p, "up", d)
        forward(p, "down", d)

    def hop(d):
        for p in range(strips):
            both(p, d)

    upstream = r.grad[...].astype(F32)
    stepped = r.stepped[...].astype(F32)
    ending = r.ending[...]
    carried = r.grown[...] * mm(out_of, start, 1, 1)
    to_heads = functools.partial(exact, b=spread, da=1, db=1)
    z = r.z[...]
    step_grad = to_heads(r.act[...] * (z + ending))
    tail_term = to_heads(stepped * ending)
    sum_grad = to_heads(upstream * (r.y[...] + carried) - stepped * z) - tail_term
    held = jnp.sum(start.astype(F32) * end.astype(F32), axis=1, keepdims=True)
    last = cumulative[length - 1 : length, :]
    overall = jnp.sum(tail_term, axis=0, keepdims=True) + jnp.exp(last) * jnp.sum(
        head_mask(width, False) * held, axis=0, keepdims=True
    )
    decay_grad = exact_left(lower, sum_grad, 0, 0) + overall
    rate = jnp.exp(r.vec[1:2, :])
    step_grad = (step_grad - rate * decay_grad) * jax.nn.sigmoid(r.raw[...] + r.vec[0:1, :])
    steps = step_grad.astype(BF)
    r.gsm[me, mine, rows:, 0:LANES] = step_grad.T[0:PAD, :].astype(BF)
    steps = steps[:, 0:PAD]

    both(0, 1)

    each(C, lambda d: share_mix(lax.rem(ch + d, C), ch, lax.rem(ch + d, C)).wait_recv())
    mix = r.gm_in[0].astype(F32)
    for q in range(1, C):
        mix = mix + r.gm_in[q].astype(F32)
    r.gmt[...] = mix

    @pl.when((me < S - 1) & (ch == C - 1))
    def _():
        for q in range(C):
            mix_tail(q).wait_recv()
        tail = r.mt_in[0].astype(F32)
        for q in range(1, C):
            tail = tail + r.mt_in[q].astype(F32)
        r.gmt[rows:, :] = tail

    r.gsm[me, mine, 0:rows, :] = spread_back(r.gmt, r.conv_mix, 0, rows)

    def small_along(e, k, q):
        here = r.gsm.at[k, e]
        return rcopy(here, here, r.z2_s.at[e, q], r.z2_r.at[e, k], seq=q)

    def cross_small(to):
        here = r.gsm.at[me, mine]
        return rcopy(here, here, r.z2_s.at[to, me], r.z2_r.at[mine, me], dp=to)

    def crossed_small(e):
        here = r.gsm.at[me, e]
        return rcopy(here, here, r.z2_s.at[e, me], r.z2_r.at[e, me], dp=e)

    def send_small(e):
        each(S, lambda d: small_along(e, me, lax.rem(me + d, S)).start())

    def small_all(do):
        for e in [mine] + others:
            each(S, lambda d, e=e: do(e, lax.rem(me + d, S)))

    both(1, 1)
    both(2, 1)

    def share_p(j, q, landing, slot):
        piece = pl.ds(j * cut, cut)
        return rcopy(
            r.p_o.at[q, :, piece], r.p_i.at[landing, :, piece], r.p_s.at[q], r.p_r.at[slot], chan=q
        )

    def whole_p(q):
        return rcopy(r.p_o.at[q], r.p_i.at[q], r.p_s.at[q], r.p_r.at[q], chan=q)

    grads = r.gin[me, mine]
    mixes = r.gmp[...]

    def send_p(j, final):
        def one(d):
            q = lax.rem(ch + d, C)

            @pl.when((q == C - 1) if final else (q < C - 1))
            def _():
                share_p(j, q, ch, ch).start()

        each(C, one)

    for j in range(parts):
        piece = slice(j * cut, (j + 1) * cut)
        out = mm(grads, r.w_in[piece, :], 1, 1) + mm(mixes, r.w_mix[piece, :], 1, 1)
        out = out + mm(steps, r.wst[0:PAD, piece], 1, 0)
        r.p_o[:, :, piece] = out.astype(BF).reshape(C, rows, cut)
        r.p_last[:, piece] = out[length - PAD :, :]
        send_p(j, False)
        if j + 3 < strips:
            both(j + 3, 1)
        if j == 0:
            send_small(mine)
            for e in others:
                cross_small(e).start()
    for p in range(parts + 3, strips):
        both(p, 1)

    @pl.when(me < S - 1)
    def _():
        mix_halo().wait_recv()
        r.pad_mix[length:, :] = r.halm_i[...]
        final = spread_back(r.pad_mix, r.conv_mix, length - PAD, PAD)
        change = final.astype(F32) - r.gmp[length - PAD :, :].astype(F32)
        fixed = r.p_last[...] + mm(change, r.w_mix[...], 1, 1)
        r.p_o[C - 1, rows - PAD :, :] = fixed.astype(BF)

    for j in range(parts):
        send_p(j, True)
    for p in range(strips):
        both(p, 2)
        if p == strips // 2:
            for e in others:
                crossed_small(e).wait_recv()
                send_small(e)
    if S <= 12:
        for d in range(3, S):
            hop(d)
    else:
        lax.fori_loop(3, S, lambda d, c: (hop(d), c)[1], 0)
    small_all(lambda e, q: small_along(e, q, q).wait_recv())
    norm = 1.0 / math.sqrt(D * S * length)
    columns = r.xc.shape[-1]

    def settle_gather(d):
        q = lax.rem(ch + d, C)
        gather(q, q, q).wait()

    each(C, settle_gather)
    mixer_columns = r.xc[:, :, ch].reshape(S * D * rows, columns)
    mixer_grads = r.gsm[:, :, 0:rows, :].reshape(S * D * rows, mixed)
    mixer_term = norm * mm(mixer_columns, mixer_grads, 0, 0)
    band = columns // C
    for q in range(C):
        r.m_o[q] = mixer_term[q * band : (q + 1) * band, :].astype(BF)

    def share_m(q, landing, slot):
        return rcopy(r.m_o.at[q], r.m_i.at[landing], r.m_s.at[q], r.m_r.at[slot], chan=q)

    each(C, lambda d: share_m(lax.rem(ch + d, C), ch, ch).start())
    def step_term(k, total):
        for e in range(D):
            x = r.xc[k, e].reshape(length, columns)
            total = total + mm(r.gsm[k, e, rows:, 0:LANES], x, 1, 0)
        return total

    step_total = jnp.zeros((PAD, columns), F32)
    if S <= 12:
        for k in range(S):
            step_total = step_term(k, step_total)
    else:
        step_total = lax.fori_loop(0, S, step_term, step_total)
    r.o_dws[...] = (norm * step_total)[:heads, :]

    def whole(k, e, send, recv):
        return rcopy(r.gin.at[k, e], r.gin.at[k, e], send, recv, seq=above)

    def weight_term(k, first=False):
        for e in others:
            whole(k, e, r.x_s.at[e, k], r.c_r.at[e, k]).wait_recv()
        x = r.xc[k].reshape(D * length, columns)
        term = norm * mm(x, r.gin[k].reshape(D * length, width), 0, 0)
        r.o_dw[...] = term if first else r.o_dw[...] + term

    def weight_terms(d):
        for k, there in ((me + d, me + d < S), (me - d, me >= d)):
            pl.when(there)(functools.partial(weight_term, k))

    weight_term(me, True)
    each(S, weight_terms)
    r.p_i[ch] = r.p_o[ch]
    r.m_i[ch] = r.m_o[ch]
    each(C, lambda d: whole_p(lax.rem(ch + d, C)).wait_recv())
    each(C, lambda d: share_m(lax.rem(ch + d, C), ch, lax.rem(ch + d, C)).wait_recv())

    for way in (0, 1):

        @pl.when(spots[way] < S - 1)
        def _(way=way):
            rcopy(terms[way], outs[way], r.chain_s.at[way], r.chain_r.at[way, 0], seq=above).wait_send()

    @pl.when(me > 0)
    def _():
        rcopy(r.hal_o, r.hal_i, r.hal_s.at[0], r.hal_r.at[0], seq=below).wait_send()
        mix_halo().wait_send()
        mix_tail(ch).wait_send()

    def settle_chan(d):
        q = lax.rem(ch + d, C)
        share_mix(q, ch, ch).wait_send()
        share_m(q, ch, ch).wait_send()
        whole_p(q).wait_send()

    each(C, settle_chan)

    def settle_line(k):
        for e in others:
            whole(k, mine, r.x_s.at[e, k], r.c_r.at[mine, k]).wait_send()
        for way, sent in (("up", (k <= me) & (me < S - 1)), ("down", (k >= me) & (me > 0))):

            @pl.when(sent)
            def _(way=way):
                whole(k, mine, (r.u_s if way == "up" else r.d_s).at[k], r.z_r.at[0, k]).wait_send()

    settle_line(0)
    each(S, settle_line)
    small_all(lambda e, q: small_along(e, me, q).wait_send())
    for e in others:
        cross_small(e).wait_send()


def finish_kernel(parts, dw, mixes, dws, o_ig, o_dw, o_dwm, o_dws, ig, dwm, sems):
    copies = [
        pltpu.make_async_copy(a, b, sems.at[i])
        for i, (a, b) in enumerate(((dw, o_dw), (dws, o_dws), (ig, o_ig), (dwm, o_dwm)))
    ]
    copies[0].start()
    copies[1].start()
    total = parts[0].astype(F32)
    for q in range(1, parts.shape[0]):
        total = total + parts[q].astype(F32)
    ig[...] = total.astype(BF)
    copies[2].start()
    total = mixes[0].astype(F32)
    for q in range(1, mixes.shape[0]):
        total = total + mixes[q].astype(F32)
    dwm[...] = total
    copies[3].start()
    for copy in copies:
        copy.wait()


def body(
    sizes,
    layer_input,
    inner_weight,
    mixer_weight,
    step_weight,
    conv_inner,
    conv_mixer,
    step_bias,
    decay_log,
    skip_gain,
    output_grad,
):
    own = layer_input[0]
    rows, model = own.shape
    chans, seqs, dps = sizes["chan"], sizes["seq"], sizes["dp"]
    groups = dps * seqs
    length = rows * chans
    width = inner_weight.shape[1]
    mixed = mixer_weight.shape[1]
    heads = step_bias.shape[0]
    cols = model // groups
    state_size = mixed // 2
    assert width % PIECES == 0 and chans % 2 == 0 and seqs > 2
    assert rows == 2 * PAD and width % LANES == 0 and PIECES % (width // LANES) == 0
    assert length == LANES and heads + conv_inner.shape[0] - 1 <= PAD
    upstream = output_grad[0]
    step_rows = step_weight.T
    bias, rates, skips = (v.reshape(1, heads) for v in (step_bias, decay_log, skip_gain))
    dma = pltpu.SemaphoreType.DMA
    vmem = pl.BlockSpec(memory_space=pltpu.VMEM)
    hbm = pl.BlockSpec(memory_space=pltpu.HBM)
    small = rows + PAD
    strips = width // LANES
    band = cols // chans

    def low(*shape):
        return pltpu.VMEM(shape, BF)

    def full(*shape):
        return pltpu.VMEM(shape, F32)

    inputs = dict(
        own=own, w_in=inner_weight, w_mix=mixer_weight, w_step=step_rows, conv_in=conv_inner,
        conv_mix=conv_mixer, bias=bias, log=rates, skip=skips, grad=upstream,
    )
    outputs = dict(
        p_i=jax.ShapeDtypeStruct((chans, rows, model), BF),
        o_dw=jax.ShapeDtypeStruct((cols, width), F32),
        m_i=jax.ShapeDtypeStruct((chans, band, mixed), BF),
        o_dws=jax.ShapeDtypeStruct((heads, cols), F32),
    )
    scratch = {key: pltpu.VMEM(v.shape, v.dtype) for key, v in inputs.items()}
    scratch |= dict(
        wst=low(LANES, model), xg=low(length, model),
        blocks=low(dps, seqs, rows, cols),
        xs=low(seqs, dps, rows, cols), xc=low(seqs, dps, chans, rows, cols),
        wide_in=full(PAD + length, width), wide_mix=full(PAD + length, mixed),
        fh_o=low(PAD, width + mixed), fh_i=low(PAD, width + mixed), vec=full(8, LANES),
        sum_in=full(length, width), sum_mix=full(length, mixed), raw=full(length, LANES),
        cum=full(length, LANES), step_wide=full(length, width), fading=full(length, width),
        grown=full(length, width), pulled=low(length, width), decay=full(width, state_size),
        mix=low(length, mixed), act=full(length, width), stepped=low(length, width),
        state_term=low(width, state_size), back_term=low(width, state_size),
        start=low(width, state_size), end=low(width, state_size),
        scr0=low(width, state_size), scr1=low(width, state_size),
        z=full(length, width), y=full(length, width), score_grad=full(length, length),
        slope_in=full(length, width),
        pad_in=full(length + 8, width), pad_mix=full(length + 8, mixed),
        gin=low(seqs, dps, length, width), gsm=low(seqs, dps, small, mixed),
        hal_o=full(strips, 8, LANES), hal_i=full(strips, 8, LANES),
        halm_o=full(8, mixed), halm_i=full(8, mixed), p_last=full(PAD, model),
        skips=full(8, width), ending=full(length, width),
        gmp=low(length, mixed), gm_in=low(chans, small, mixed), gmt=full(small, mixed),
        am=low(length + PAD, mixed), mt_in=low(chans, PAD, mixed),
        p_o=low(chans, rows, model), m_o=low(chans, band, mixed),
        load_sem=dma((len(LOADED),)), fh_sem=dma((2,)), halm_s=dma((2,)),
        hal_s=dma((1,)), hal_r=dma((strips,)),
        near_s=dma((1,)), near_r=dma((chans,)),
        far_s=dma((chans // 2,)), far_r=dma((chans // 2, chans)),
        relay_s=dma((chans // 2,)), relay_r=dma((chans // 2, chans)),
        cross_s=dma((dps, seqs)), cross_r=dma((dps, seqs)),
        gat_s=dma((chans,)), gat_r=dma((chans,)),
        chain_s=dma((2,)), chain_r=dma((2, PIECES)),
        z_r=dma((strips, seqs)), c_r=dma((dps, seqs)),
        u_s=dma((seqs,)), d_s=dma((seqs,)), x_s=dma((dps, seqs)),
        z2_r=dma((dps, seqs)),
        z2_s=dma((dps, seqs)), mt_s=dma((1,)), mt_r=dma((chans,)),
        gm_s=dma((chans,)), gm_r=dma((chans,)),
        p_s=dma((chans,)), p_r=dma((chans,)), m_s=dma((chans,)), m_r=dma((chans,)),
    )
    names = [key + "_h" for key in inputs] + list(outputs) + list(scratch)
    parts, inner_grad, mix_parts, step_grad = pl.pallas_call(
        functools.partial(layer_kernel, names, sizes, heads),
        out_shape=tuple(outputs.values()),
        in_specs=[hbm] * len(inputs),
        out_specs=(vmem,) * len(outputs),
        scratch_shapes=list(scratch.values()),
        compiler_params=pltpu.CompilerParams(
            collective_id=0, has_side_effects=True, vmem_limit_bytes=LIMIT
        ),
        name="layer",
    )(*(pltpu.with_memory_space_constraint(v, pltpu.HBM) for v in inputs.values()))
    input_grad, inner_grad, mixer_grad, step_grad = pl.pallas_call(
        finish_kernel,
        out_shape=(
            jax.ShapeDtypeStruct((rows, model), BF),
            jax.ShapeDtypeStruct((cols, width), F32),
            jax.ShapeDtypeStruct((band, mixed), F32),
            jax.ShapeDtypeStruct((heads, cols), F32),
        ),
        in_specs=[vmem] * 4,
        out_specs=(pl.BlockSpec(memory_space=pl.ANY),) * 4,
        scratch_shapes=[
            pltpu.VMEM((rows, model), BF),
            pltpu.VMEM((band, mixed), F32),
            dma((4,)),
        ],
        compiler_params=pltpu.CompilerParams(vmem_limit_bytes=LIMIT),
        name="finish",
    )(parts, inner_grad, mix_parts, step_grad)
    return input_grad[None], inner_grad, mixer_grad, step_grad.T


def solution(mesh):
    sizes = dict(mesh.shape)
    in_specs = (
        P("dp", ("seq", "chan"), None),
        P(None, "chan"),
        P(),
        P(None, "chan"),
        P(None, "chan"),
        P(),
        P("chan"),
        P("chan"),
        P("chan"),
        P("dp", "seq", "chan"),
    )
    out_specs = (
        P("dp", ("seq", "chan"), None),
        P(("dp", "seq"), "chan"),
        P(("dp", "seq", "chan"), None),
        P(("dp", "seq"), "chan"),
    )
    return jax.shard_map(
        functools.partial(body, sizes),
        mesh=mesh,
        in_specs=in_specs,
        out_specs=out_specs,
        check_vma=False,
    )
```
